32 devices in a mesh: section: 4 (over y, x), slab: 2 (over core), img: 4 (over z).
Axes of the slice: x: 2, y: 2, z: 4, core: 2. Of those that a mesh axis runs over, the one named last changes fastest.
Arguments:
- strips: bfloat16 [4, 4, 8, 16, 320], P('img', None, None, 'slab'), may hold values from -6 to 6
- kernels: bfloat16 [4, 2, 9, 320, 320], P('section'), may hold values from -0.109375 to 0.109375
- cotangent: bfloat16 [4, 4, 8, 16, 320], P('img', None, None, 'slab'), may hold values from -18 to 18
Outputs:
- grad_kernels: float32 [4, 2, 9, 320, 320], P('section', None, None, 'slab', 'img')
- grad_inputs: bfloat16 [4, 4, 4, 8, 16, 320], P('section', 'img', None, None, 'slab')
The draws below stay inside these ranges and needn't reach their ends.
All inputs are finite; a program needn't handle non-finite values.
Results may differ from the reference program's by a relative error of at most 0.023.
Values may be sent and summed in bfloat16 or wider, within the bound.
No kernel may reach another device: no remote copies, remote signals or barrier semaphores. Data moves between devices by JAX's collectives and lax.ppermute only.
A program may use at most 128 MiB of HBM per device.

```python
import math
import jax
import jax.numpy as jnp
from jax import lax

C = 320
ROWS = 8
STRIPS = 4
SECTIONS = 4
IMAGES = 4
WIDTH = 16


def draw_cotangent(key, part):
    full_shape = (IMAGES, STRIPS, ROWS, WIDTH, C)
    column = jnp.arange(WIDTH).astype(jnp.float32) / max(WIDTH - 1, 1)
    image_pos = jnp.arange(IMAGES).astype(jnp.float32) / max(IMAGES - 1, 1)
    scales = 0.5 * jnp.power(3.0, column)[None, None, None, :, None] * jnp.power(3.0, image_pos)[:, None, None, None, None]
    own_key = jax.random.fold_in(jax.random.fold_in(key, 7), 0)
    values = jnp.clip(jax.random.normal(own_key, full_shape, jnp.float32), -4.0, 4.0)
    return (values * scales).astype(jnp.bfloat16)


def levels(rng, shape, cuts, low, high):
    factor_of = 1.0
    for axis_at, blocks in cuts:
        heights = jax.random.uniform(jax.random.fold_in(jax.random.fold_in(rng, 6), axis_at), (blocks,), jnp.float32, low / len(cuts), high / len(cuts))
        factor_of = factor_of * jnp.repeat(jnp.exp(heights), shape[axis_at] // blocks).reshape((-1,) + (1,) * (len(shape) - 1 - axis_at))
    return factor_of


def centred(rng, extent, deviation, most, shards=(), kind=jnp.bfloat16):
    factor_of = levels(rng, extent, shards, -0.22, 0.18) if shards else 1.0
    array = jax.random.normal(rng, extent, jnp.float32) * deviation * factor_of
    return jnp.minimum(jnp.maximum(array, -most), most).astype(kind)


def setup_inputs(seed: int = 0) -> dict:
    key_of = jax.random.split(jax.random.key(seed), 4)
    strips = centred(key_of[0], (IMAGES, STRIPS, ROWS, WIDTH, C), 1.0, 6.0, ((0, 4), (3, 2)))
    kernels = centred(key_of[1], (SECTIONS, 2, 9, C, C), (9 * C) ** -0.5, 0.109375, ((0, 4),))
    cotangent = draw_cotangent(jax.random.fold_in(key_of[3], 71), 0)
    return dict(strips=strips, kernels=kernels, cotangent=cotangent)


def unfold(padded, row_count, col_count):
    tap_list = [padded[:, down_at:down_at + row_count, right_at:right_at + col_count, :] for down_at in range(3) for right_at in range(3)]
    stacked = jnp.concatenate(tap_list, axis=3)
    return stacked.reshape(-1, stacked.shape[3])

def columns_of(wide_field):
    row_count = wide_field.shape[1]
    col_count = wide_field.shape[2] - 2
    padded = jnp.pad(wide_field, ((0, 0), (1, 1), (0, 0), (0, 0)))
    return unfold(padded, row_count, col_count)

def convolve(matrix, wide_field):
    count, row_count = (wide_field.shape[0], wide_field.shape[1])
    col_count = wide_field.shape[2] - 2
    flat_out = jnp.dot(columns_of(wide_field), matrix, preferred_element_type=jnp.float32)
    return flat_out.reshape(count, row_count, col_count, matrix.shape[1])

def contract(wide_field, grad_out):
    flat_grad = grad_out.reshape(-1, grad_out.shape[3])
    return lax.dot_general(columns_of(wide_field), flat_grad, (((0,), (0,)), ((), ())), preferred_element_type=jnp.float32)

def silu_slope(hidden):
    sigmoid_at = jax.nn.sigmoid(hidden)
    return sigmoid_at * (1.0 + hidden * (1.0 - sigmoid_at))

def pad_cols(field_in):
    return jnp.pad(field_in, ((0, 0), (0, 0), (1, 1), (0, 0)))

def forward_matrix(kernel):
    return kernel.reshape(9 * kernel.shape[1], kernel.shape[2])

def backward_matrix(kernel):
    return jnp.transpose(kernel[::-1], (0, 2, 1)).reshape(9 * kernel.shape[1], kernel.shape[2])

def reference(strips, kernels, cotangent):
    channels = kernels.shape[3]
    batch_size = IMAGES * STRIPS
    scaling = 1.0 / math.sqrt(IMAGES * STRIPS * ROWS * WIDTH)
    field_in = strips.reshape(batch_size, ROWS, WIDTH, channels)
    saved_list = []
    for section_no in range(SECTIONS):
        wide_field = pad_cols(field_in)
        hidden = convolve(forward_matrix(kernels[section_no, 0]), wide_field)
        active = jax.nn.silu(hidden).astype(jnp.bfloat16)
        wide_active = pad_cols(active)
        result_out = field_in.astype(jnp.float32) + convolve(forward_matrix(kernels[section_no, 1]), wide_active)
        saved_list.append((wide_field, hidden, wide_active))
        field_in = result_out.astype(jnp.bfloat16)
    grad_out = cotangent.reshape(batch_size, ROWS, WIDTH, channels)
    kernel_list = [None for section_no in range(SECTIONS)]
    grad_list = [None for section_no in range(SECTIONS)]
    for section_no in reversed(range(SECTIONS)):
        wide_field, hidden, wide_active = saved_list[section_no]
        upper_term = contract(wide_active, grad_out)
        grad_active = convolve(backward_matrix(kernels[section_no, 1]), pad_cols(grad_out))
        grad_hidden = (grad_active * silu_slope(hidden)).astype(jnp.bfloat16)
        lower_term = contract(wide_field, grad_hidden)
        grad_sum = grad_out.astype(jnp.float32) + convolve(backward_matrix(kernels[section_no, 0]), pad_cols(grad_hidden))
        grad_out = grad_sum.astype(jnp.bfloat16)
        kernel_list[section_no] = jnp.stack([lower_term, upper_term]).reshape(2, 9, channels, channels)
        grad_list[section_no] = grad_out.reshape(IMAGES, STRIPS, ROWS, WIDTH, channels)
    grad_kernels = jnp.stack(kernel_list, axis=0) * scaling
    grad_inputs = jnp.stack(grad_list, axis=0)
    return (grad_kernels, grad_inputs)
```

```python
import math

import jax
import jax.numpy as jnp
from jax import lax
from jax.experimental import pallas as pl
from jax.experimental.pallas import tpu as pltpu
from jax.sharding import PartitionSpec as P


def passed_along(value, axis, steps):
    count = lax.axis_size(axis)
    initial, last = (max(0, -steps), min(count, count - steps))
    return lax.ppermute(value, axis, [(source, source + steps) for source in range(initial, last)])


def padded_2(cells, sides, width):
    for axis, dim in sides:
        count = lax.axis_size(axis)
        ends = count - 1
        head = lax.slice_in_dim(cells, 0, width, axis=dim)
        tail = lax.slice_in_dim(cells, cells.shape[dim] - width, cells.shape[dim], axis=dim)
        cells = jnp.concatenate(
            [
                lax.ppermute(tail, axis, [(i, (i + 1) % count) for i in range(ends)]),
                cells,
                lax.ppermute(head, axis, [((i + 1) % count, i) for i in range(ends)]),
            ],
            axis=dim,
        )
    return cells


def unfold(padded, row_count, col_count):
    tap_list = [
        padded[:, down_at : down_at + row_count, right_at : right_at + col_count, :]
        for down_at in range(3)
        for right_at in range(3)
    ]
    stacked = jnp.concatenate(tap_list, axis=3)
    return stacked.reshape(-1, stacked.shape[3])


def columns_of(wide_field):
    row_count = wide_field.shape[1]
    col_count = wide_field.shape[2] - 2
    padded = jnp.pad(wide_field, ((0, 0), (1, 1), (0, 0), (0, 0)))
    return unfold(padded, row_count, col_count)


def convolve(matrix, wide_field):
    count, row_count = (wide_field.shape[0], wide_field.shape[1])
    col_count = wide_field.shape[2] - 2
    flat_out = jnp.dot(columns_of(wide_field), matrix, preferred_element_type=jnp.float32)
    return flat_out.reshape(count, row_count, col_count, matrix.shape[1])


def contract(wide_field, grad_out):
    flat_grad = grad_out.reshape(-1, grad_out.shape[3])
    return lax.dot_general(
        columns_of(wide_field),
        flat_grad,
        (((0,), (0,)), ((), ())),
        preferred_element_type=jnp.float32,
    )


def silu_slope(hidden):
    sigmoid_at = jax.nn.sigmoid(hidden)
    return sigmoid_at * (1.0 + hidden * (1.0 - sigmoid_at))


def store(buffer, value, slot_index, is_valid, axis_at):
    current = lax.dynamic_index_in_dim(buffer, slot_index, axis_at, keepdims=False)
    return lax.dynamic_update_index_in_dim(
        buffer, jnp.where(is_valid, value, current), slot_index, axis_at
    )


def column_shards(strips, kernels, cotangent):
    section_count = lax.axis_size("section")
    section_index = lax.axis_index("section")
    slab_count = lax.axis_size("slab")
    slab_index = lax.axis_index("slab")
    images, strip_count, row_count, col_count, channels = strips.shape
    weights = kernels[0]
    first_forward = weights[0].reshape(9 * channels, channels)
    second_forward = weights[1].reshape(9 * channels, channels)
    first_backward = jnp.transpose(weights[0][::-1], (0, 2, 1)).reshape(9 * channels, channels)
    second_backward = jnp.transpose(weights[1][::-1], (0, 2, 1)).reshape(9 * channels, channels)
    scaling = 1.0 / math.sqrt(
        images * lax.axis_size("img") * strip_count * row_count * col_count * slab_count
    )
    position = slab_index * col_count - 1 + jnp.arange(col_count + 2, dtype=jnp.int32)
    inside = ((position >= 0) & (position < slab_count * col_count))[None, None, :, None]
    tick_count = strip_count + section_count - 1
    hidden_cols = col_count + 2
    empty_field = jnp.zeros((images, row_count, col_count, channels), jnp.bfloat16)
    saved_field = jnp.zeros((strip_count, images, row_count, col_count + 2, channels), jnp.bfloat16)
    saved_hidden = jnp.zeros((strip_count, images, row_count, hidden_cols, channels), jnp.float32)
    saved_active = jnp.zeros(
        (strip_count, images, row_count, col_count + 2, channels), jnp.bfloat16
    )
    outgoing = empty_field
    for step_no in range(tick_count):
        micro_index = step_no - section_index
        is_valid = (micro_index >= 0) & (micro_index < strip_count)
        slot_index = jnp.clip(micro_index, 0, strip_count - 1)
        if step_no == 0:
            incoming = empty_field
        else:
            incoming = passed_along(outgoing, "section", 1)
        first_strip = lax.dynamic_index_in_dim(strips, slot_index, 1, keepdims=False)
        field_in = jnp.where(section_index == 0, first_strip, incoming)
        wide_deep = padded_2(field_in, (("slab", 2),), 2)
        hidden = convolve(first_forward, wide_deep)
        wide_active = jnp.where(inside, jax.nn.silu(hidden), 0.0).astype(jnp.bfloat16)
        wide_field = wide_deep[:, :, 1:-1, :]
        outgoing = (field_in.astype(jnp.float32) + convolve(second_forward, wide_active)).astype(
            jnp.bfloat16
        )
        saved_field = store(saved_field, wide_field, slot_index, is_valid, 0)
        saved_hidden = store(saved_hidden, hidden, slot_index, is_valid, 0)
        saved_active = store(saved_active, wide_active, slot_index, is_valid, 0)
    grad_slots = jnp.zeros((images, strip_count, row_count, col_count, channels), jnp.bfloat16)
    saved_grad_out = jnp.zeros((strip_count, images, row_count, col_count, channels), jnp.bfloat16)
    saved_grad_hidden = jnp.zeros(
        (strip_count, images, row_count, col_count, channels), jnp.bfloat16
    )
    sending = empty_field
    for step_no in range(tick_count):
        micro_index = step_no - (section_count - 1 - section_index)
        is_valid = (micro_index >= 0) & (micro_index < strip_count)
        slot_index = jnp.clip(micro_index, 0, strip_count - 1)
        if step_no == 0:
            arriving = empty_field
        else:
            arriving = passed_along(sending, "section", -1)
        top_grad = lax.dynamic_index_in_dim(cotangent, slot_index, 1, keepdims=False)
        grad_out = jnp.where(section_index == section_count - 1, top_grad, arriving)
        grad_out = jnp.where(is_valid, grad_out, jnp.zeros_like(grad_out))
        hidden = lax.dynamic_index_in_dim(saved_hidden, slot_index, 0, keepdims=False)
        wide_grad = padded_2(grad_out, (("slab", 2),), 2)
        grad_active = convolve(second_backward, wide_grad)
        wide_hidden_grad = jnp.where(inside, grad_active * silu_slope(hidden), 0.0).astype(
            jnp.bfloat16
        )
        grad_hidden = wide_hidden_grad[:, :, 1:-1, :]
        sending = (
            grad_out.astype(jnp.float32) + convolve(first_backward, wide_hidden_grad)
        ).astype(jnp.bfloat16)
        saved_grad_out = store(saved_grad_out, grad_out, slot_index, is_valid, 0)
        saved_grad_hidden = store(saved_grad_hidden, grad_hidden, slot_index, is_valid, 0)
        grad_slots = store(grad_slots, sending, slot_index, is_valid, 1)
    flat_count = strip_count * images
    lower_part = contract(
        saved_field.reshape(flat_count, row_count, col_count + 2, channels),
        saved_grad_hidden.reshape(flat_count, row_count, col_count, channels),
    )
    upper_part = contract(
        saved_active.reshape(flat_count, row_count, col_count + 2, channels),
        saved_grad_out.reshape(flat_count, row_count, col_count, channels),
    )
    grad_terms = jnp.stack([lower_part, upper_part]).reshape(2, 9, channels, channels)
    row_share = lax.psum_scatter(
        grad_terms.astype(jnp.bfloat16), "slab", scatter_dimension=2, tiled=True
    )
    own_share = lax.psum_scatter(row_share, "img", scatter_dimension=3, tiled=True).astype(
        jnp.float32
    )
    grad_kernels = (own_share * scaling)[None]
    return (grad_kernels, grad_slots[None])


def call(kernel, outs, operands, scratch, aliases, name):
    return pl.pallas_call(
        kernel,
        out_shape=outs,
        in_specs=[pl.BlockSpec(memory_space=pltpu.VMEM)] * len(operands),
        out_specs=[pl.BlockSpec(memory_space=pltpu.VMEM)] * len(outs),
        scratch_shapes=scratch,
        input_output_aliases=aliases,
        compiler_params=pltpu.CompilerParams(vmem_limit_bytes=24 << 20),
        name=name,
    )(*operands)


def neighbours(value, shifted, width):
    count, channels = value.shape
    shifted[8 : 8 + count, :] = value
    column = lax.rem(lax.broadcasted_iota(jnp.int32, (count, channels), 0), width)
    before = jnp.where(column == 0, 0.0, shifted[7 : 7 + count, :])
    after = jnp.where(column == width - 1, 0.0, shifted[9 : 9 + count, :])
    return before, after


def convolved(value, matrix, taps, shifted, width):
    count, channels = value.shape
    before, after = neighbours(value, shifted, width)
    for place, part in enumerate((before, value, after)):
        taps[width : width + count, place * channels : (place + 1) * channels] = part.astype(
            jnp.bfloat16
        )
    edge = jnp.zeros((width, 3 * channels), jnp.bfloat16)
    taps[0:width, :] = edge
    taps[width + count : 2 * width + count, :] = edge
    total = jnp.dot(taps[0:count, :], matrix[0], preferred_element_type=jnp.float32)
    for down in (1, 2):
        total = total + jnp.dot(
            taps[down * width : down * width + count, :],
            matrix[down],
            preferred_element_type=jnp.float32,
        )
    return total


def forward_call(field, weights, state, section, crop, crops, width):
    count, channels = field.shape

    def kernel(field_ref, weights_ref, *refs):
        out_ref, saved_ref, hidden_ref, taps, shifted = refs[-5:]

        @pl.when(lax.axis_index("section") == section)
        def _():
            field_in = field_ref[...]
            wide = field_in.astype(jnp.float32)
            saved_ref[0, crop] = field_in
            hidden = convolved(wide, weights_ref.at[0], taps, shifted, width)
            hidden_ref[crop] = hidden
            active = (hidden * jax.nn.sigmoid(hidden)).astype(jnp.bfloat16)
            saved_ref[1, crop] = active
            added = convolved(active.astype(jnp.float32), weights_ref.at[1], taps, shifted, width)
            out_ref[...] = (wide + added).astype(jnp.bfloat16)

    outs = [
        jax.ShapeDtypeStruct((count, channels), jnp.bfloat16),
        jax.ShapeDtypeStruct((2, crops, count, channels), jnp.bfloat16),
        jax.ShapeDtypeStruct((crops, count, channels), jnp.float32),
    ]
    scratch = [
        pltpu.VMEM((count + 2 * width, 3 * channels), jnp.bfloat16),
        pltpu.VMEM((count + 16, channels), jnp.float32),
    ]
    aliases = {2 + k: 1 + k for k in range(len(state))}
    out, *state = call(
        kernel, outs, [field, weights, *state], scratch, aliases, f"fwd_{section}_{crop}"
    )
    return out, state


def backward_call(grad, turned, hidden, state, section, crop, crops, width, parts):
    count, channels = grad.shape
    share = channels // parts

    def kernel(grad_ref, turned_ref, hidden_ref, *refs):
        out_ref, sent_ref, inputs_ref, taps, shifted = refs[-5:]

        @pl.when(lax.axis_index("section") == section)
        def _():
            own = lax.axis_index("img")

            def keep(kind, value):
                flipped = value.T.astype(jnp.bfloat16)
                for part in range(parts):
                    slot = lax.rem(part + parts - own, parts)
                    sent_ref[slot, kind, :, crop * count : (crop + 1) * count] = flipped[
                        part * share : (part + 1) * share, :
                    ]

            wide = grad_ref[...].astype(jnp.float32)
            keep(0, wide)
            grad_active = convolved(wide, turned_ref.at[1], taps, shifted, width)
            hidden = hidden_ref[crop]
            gate = jax.nn.sigmoid(hidden)
            grad_hidden = (grad_active * (gate * (1.0 + hidden * (1.0 - gate)))).astype(
                jnp.bfloat16
            ).astype(jnp.float32)
            keep(1, grad_hidden)
            added = convolved(grad_hidden, turned_ref.at[0], taps, shifted, width)
            result = (wide + added).astype(jnp.bfloat16)
            out_ref[...] = result
            inputs_ref[crop] = result

    outs = [
        jax.ShapeDtypeStruct((count, channels), jnp.bfloat16),
        jax.ShapeDtypeStruct((parts, 2, share, crops * count), jnp.bfloat16),
        jax.ShapeDtypeStruct((crops, count, channels), jnp.bfloat16),
    ]
    scratch = [
        pltpu.VMEM((count + 2 * width, 3 * channels), jnp.bfloat16),
        pltpu.VMEM((count + 16, channels), jnp.float32),
    ]
    aliases = {3 + k: 1 + k for k in range(len(state))}
    out, *state = call(
        kernel, outs, [grad, turned, hidden, *state], scratch, aliases, f"bwd_{section}_{crop}"
    )
    return out, state


def turn_call(weights, after):
    two, three, rows, channels = weights.shape

    def kernel(weights_ref, after_ref, turned_ref):
        for which in range(two):
            for tap in range(9):
                down, right = divmod(tap, 3)
                flipped = weights_ref[which, down, right * channels : (right + 1) * channels, :].T
                down, right = divmod(8 - tap, 3)
                turned_ref[which, down, right * channels : (right + 1) * channels, :] = flipped

    return pl.pallas_call(
        kernel,
        out_shape=jax.ShapeDtypeStruct(weights.shape, weights.dtype),
        in_specs=[pl.BlockSpec(memory_space=pltpu.VMEM), pl.BlockSpec(memory_space=pl.ANY)],
        out_specs=pl.BlockSpec(memory_space=pltpu.VMEM),
        compiler_params=pltpu.CompilerParams(vmem_limit_bytes=24 << 20),
        name="turn",
    )(weights, after)


def flip_call(saved, parts, after):
    two, crops, count, channels = saved.shape
    share = channels // parts

    def kernel(saved_ref, after_ref, flipped_ref):
        own = lax.axis_index("slab")
        for kind in range(two):
            for crop in range(crops):
                flipped = saved_ref[kind, crop].T
                for part in range(parts):
                    slot = lax.rem(part + parts - own, parts)
                    flipped_ref[slot, kind, :, crop * count : (crop + 1) * count] = flipped[
                        part * share : (part + 1) * share, :
                    ]

    return pl.pallas_call(
        kernel,
        out_shape=jax.ShapeDtypeStruct((parts, two, share, crops * count), saved.dtype),
        in_specs=[pl.BlockSpec(memory_space=pltpu.VMEM), pl.BlockSpec(memory_space=pl.ANY)],
        out_specs=pl.BlockSpec(memory_space=pltpu.VMEM),
        compiler_params=pltpu.CompilerParams(vmem_limit_bytes=24 << 20),
        name="flip",
    )(saved, after)


def terms_call(fields, grads, count, width, scaling):
    blocks = len(fields)
    rows, cells = fields[0].shape[1:]
    columns = grads[0].shape[1]
    crops = cells // count

    def kernel(*refs):
        field_refs, grad_refs = refs[:blocks], refs[blocks : 2 * blocks]
        out_ref, right, shifted = refs[2 * blocks :]
        for which, kind in ((0, 1), (1, 0)):
            for block in range(blocks):
                for crop in range(crops):
                    grad = grad_refs[block][kind, :, crop * count : (crop + 1) * count]
                    grad = grad.T.astype(jnp.float32)
                    before, after = neighbours(grad, shifted, width)
                    at = (block * crops + crop) * count
                    edge = jnp.zeros((width, 3 * columns), jnp.bfloat16)
                    right[0, at + count - width : at + count, :] = edge
                    right[2, at : at + width, :] = edge
                    for place, part in enumerate((after, grad, before)):
                        lanes = slice(place * columns, (place + 1) * columns)
                        part = part.astype(jnp.bfloat16)
                        right[0, at : at + count - width, lanes] = part[width:, :]
                        right[1, at : at + count, lanes] = part
                        right[2, at + width : at + count, lanes] = part[: count - width, :]
            left = jnp.concatenate([ref[which] for ref in field_refs], axis=1)
            for down in range(3):
                total = jnp.dot(left, right[down], preferred_element_type=jnp.float32) * scaling
                for place in range(3):
                    out_ref[which, 3 * down + place] = total[
                        :, place * columns : (place + 1) * columns
                    ]

    return pl.pallas_call(
        kernel,
        out_shape=jax.ShapeDtypeStruct((2, 9, rows, columns), jnp.float32),
        in_specs=[pl.BlockSpec(memory_space=pltpu.VMEM)] * (2 * blocks),
        out_specs=pl.BlockSpec(memory_space=pltpu.VMEM),
        scratch_shapes=[
            pltpu.VMEM((3, blocks * cells, 3 * columns), jnp.bfloat16),
            pltpu.VMEM((count + 16, columns), jnp.float32),
        ],
        compiler_params=pltpu.CompilerParams(vmem_limit_bytes=32 << 20),
        name="terms",
    )(*fields, *grads)


def rotated(value, axis, steps):
    count = lax.axis_size(axis)
    return lax.ppermute(value, axis, [(source, (source + steps) % count) for source in range(count)])


def to_crops(local):
    count, own = lax.axis_size("slab"), lax.axis_index("slab")
    images, strips, rows, cols, channels = local.shape
    share = strips // count
    whole = jnp.zeros((images, share, rows, cols * count, channels), local.dtype)
    for step in range(count):
        part = lax.dynamic_slice_in_dim(local, lax.rem(own + step, count) * share, share, axis=1)
        if step:
            part = rotated(part, "slab", step)
        source = lax.rem(own + count - step, count)
        whole = lax.dynamic_update_slice_in_dim(whole, part, source * cols, axis=3)
    return whole.reshape(images * share, rows * cols * count, channels)


def to_columns(crops, shape):
    count, own = lax.axis_size("slab"), lax.axis_index("slab")
    images, strips, rows, cols, channels = shape
    share = strips // count
    whole = crops.reshape(images, share, rows, cols * count, channels)
    local = jnp.zeros(shape, crops.dtype)
    for step in range(count):
        part = lax.dynamic_slice_in_dim(whole, lax.rem(own + step, count) * cols, cols, axis=3)
        if step:
            part = rotated(part, "slab", step)
        source = lax.rem(own + count - step, count)
        local = lax.dynamic_update_slice_in_dim(local, part, source * share, axis=1)
    return local


def crop_shards(strips, kernels, cotangent):
    sections = lax.axis_size("section")
    section = lax.axis_index("section")
    slabs, groups = lax.axis_size("slab"), lax.axis_size("img")
    images, strip_count, row_count, col_count, channels = strips.shape
    width = col_count * slabs
    count = row_count * width
    crops = images * strip_count // slabs
    scaling = 1.0 / math.sqrt(images * groups * strip_count * count)
    weights = kernels[0].reshape(2, 3, 3 * channels, channels)
    if sections == 1:
        fields, tops = to_crops(strips), to_crops(cotangent)
    else:
        fields = to_crops(jnp.where(section == sections - 1, cotangent, strips))
        tops = fields
    incoming = [fields[crop] for crop in range(crops)]
    state = []
    turned = None
    for place in range(sections):
        outgoing = []
        for crop in range(crops):
            out, state = forward_call(
                incoming[crop], weights, state, place, crop, crops, width
            )
            outgoing.append(out)
        if place == 0:
            turned = turn_call(weights, state[0])
        if place + 1 < sections:
            incoming = [lax.ppermute(out, "section", [(place, place + 1)]) for out in outgoing]
    saved, hidden = state
    incoming = [tops[crop] for crop in range(crops)]
    grads = []
    for place in reversed(range(sections)):
        outgoing = []
        for crop in range(crops):
            out, grads = backward_call(
                incoming[crop], turned, hidden, grads, place, crop, crops, width, groups
            )
            outgoing.append(out)
        if place == sections - 1:
            flipped = flip_call(saved, slabs, grads[0])
            halves = [flipped[0]]
            for step in range(1, slabs):
                halves.append(rotated(flipped[step], "slab", step))
            both = jnp.stack(halves)
            left = [both]
            for step in range(1, groups):
                left.append(rotated(both, "img", step))
        if place:
            incoming = [lax.ppermute(out, "section", [(place, place - 1)]) for out in outgoing]
    sent, inputs = grads
    right = [sent[0]]
    for step in range(1, groups):
        right.append(rotated(sent[step], "img", step))
    left_blocks, right_blocks = [], []
    for step in range(slabs):
        for block in range(groups):
            left_blocks.append(left[block][step])
            right_blocks.append(right[block] if step == 0 else rotated(right[block], "slab", step))
    grad_kernels = terms_call(left_blocks, right_blocks, count, width, scaling)
    grad_inputs = to_columns(inputs, strips.shape)
    return (grad_kernels[None], grad_inputs[None])


def shards(strips, kernels, cotangent):
    slabs, groups = lax.axis_size("slab"), lax.axis_size("img")
    strip_count, row_count, col_count, channels = strips.shape[1:]
    width = col_count * slabs
    whole_crops = strip_count % slabs == 0 and width % 16 == 0 and (row_count * width) % 128 == 0
    if whole_crops and channels % (16 * slabs) == 0 and channels % (16 * groups) == 0:
        return crop_shards(strips, kernels, cotangent)
    return column_shards(strips, kernels, cotangent)


def solution(mesh):
    in_specs = (
        P("img", None, None, "slab", None),
        P("section", None, None, None, None),
        P("img", None, None, "slab", None),
    )
    out_specs = (
        P("section", None, None, "slab", "img"),
        P("section", "img", None, None, "slab", None),
    )
    return jax.shard_map(shards, mesh=mesh, in_specs=in_specs, out_specs=out_specs, check_vma=False)
```

```python
import math

import jax
import jax.numpy as jnp
from jax import lax
from jax.experimental import pallas as pl
from jax.experimental.pallas import tpu as pltpu
from jax.sharding import PartitionSpec as P


def passed_along(value, axis, steps):
    count = lax.axis_size(axis)
    initial, last = (max(0, -steps), min(count, count - steps))
    return lax.ppermute(value, axis, [(source, source + steps) for source in range(initial, last)])


def padded_2(cells, sides, width):
    for axis, dim in sides:
        count = lax.axis_size(axis)
        ends = count - 1
        head = lax.slice_in_dim(cells, 0, width, axis=dim)
        tail = lax.slice_in_dim(cells, cells.shape[dim] - width, cells.shape[dim], axis=dim)
        cells = jnp.concatenate(
            [
                lax.ppermute(tail, axis, [(i, (i + 1) % count) for i in range(ends)]),
                cells,
                lax.ppermute(head, axis, [((i + 1) % count, i) for i in range(ends)]),
            ],
            axis=dim,
        )
    return cells


def unfold(padded, row_count, col_count):
    tap_list = [
        padded[:, down_at : down_at + row_count, right_at : right_at + col_count, :]
        for down_at in range(3)
        for right_at in range(3)
    ]
    stacked = jnp.concatenate(tap_list, axis=3)
    return stacked.reshape(-1, stacked.shape[3])


def columns_of(wide_field):
    row_count = wide_field.shape[1]
    col_count = wide_field.shape[2] - 2
    padded = jnp.pad(wide_field, ((0, 0), (1, 1), (0, 0), (0, 0)))
    return unfold(padded, row_count, col_count)


def convolve(matrix, wide_field):
    count, row_count = (wide_field.shape[0], wide_field.shape[1])
    col_count = wide_field.shape[2] - 2
    flat_out = jnp.dot(columns_of(wide_field), matrix, preferred_element_type=jnp.float32)
    return flat_out.reshape(count, row_count, col_count, matrix.shape[1])


def contract(wide_field, grad_out):
    flat_grad = grad_out.reshape(-1, grad_out.shape[3])
    return lax.dot_general(
        columns_of(wide_field),
        flat_grad,
        (((0,), (0,)), ((), ())),
        preferred_element_type=jnp.float32,
    )


def silu_slope(hidden):
    sigmoid_at = jax.nn.sigmoid(hidden)
    return sigmoid_at * (1.0 + hidden * (1.0 - sigmoid_at))


def store(buffer, value, slot_index, is_valid, axis_at):
    current = lax.dynamic_index_in_dim(buffer, slot_index, axis_at, keepdims=False)
    return lax.dynamic_update_index_in_dim(
        buffer, jnp.where(is_valid, value, current), slot_index, axis_at
    )


def column_shards(strips, kernels, cotangent):
    section_count = lax.axis_size("section")
    section_index = lax.axis_index("section")
    slab_count = lax.axis_size("slab")
    slab_index = lax.axis_index("slab")
    images, strip_count, row_count, col_count, channels = strips.shape
    weights = kernels[0]
    first_forward = weights[0].reshape(9 * channels, channels)
    second_forward = weights[1].reshape(9 * channels, channels)
    first_backward = jnp.transpose(weights[0][::-1], (0, 2, 1)).reshape(9 * channels, channels)
    second_backward = jnp.transpose(weights[1][::-1], (0, 2, 1)).reshape(9 * channels, channels)
    scaling = 1.0 / math.sqrt(
        images * lax.axis_size("img") * strip_count * row_count * col_count * slab_count
    )
    position = slab_index * col_count - 1 + jnp.arange(col_count + 2, dtype=jnp.int32)
    inside = ((position >= 0) & (position < slab_count * col_count))[None, None, :, None]
    tick_count = strip_count + section_count - 1
    hidden_cols = col_count + 2
    empty_field = jnp.zeros((images, row_count, col_count, channels), jnp.bfloat16)
    saved_field = jnp.zeros((strip_count, images, row_count, col_count + 2, channels), jnp.bfloat16)
    saved_hidden = jnp.zeros((strip_count, images, row_count, hidden_cols, channels), jnp.float32)
    saved_active = jnp.zeros(
        (strip_count, images, row_count, col_count + 2, channels), jnp.bfloat16
    )
    outgoing = empty_field
    for step_no in range(tick_count):
        micro_index = step_no - section_index
        is_valid = (micro_index >= 0) & (micro_index < strip_count)
        slot_index = jnp.clip(micro_index, 0, strip_count - 1)
        if step_no == 0:
            incoming = empty_field
        else:
            incoming = passed_along(outgoing, "section", 1)
        first_strip = lax.dynamic_index_in_dim(strips, slot_index, 1, keepdims=False)
        field_in = jnp.where(section_index == 0, first_strip, incoming)
        wide_deep = padded_2(field_in, (("slab", 2),), 2)
        hidden = convolve(first_forward, wide_deep)
        wide_active = jnp.where(inside, jax.nn.silu(hidden), 0.0).astype(jnp.bfloat16)
        wide_field = wide_deep[:, :, 1:-1, :]
        outgoing = (field_in.astype(jnp.float32) + convolve(second_forward, wide_active)).astype(
            jnp.bfloat16
        )
        saved_field = store(saved_field, wide_field, slot_index, is_valid, 0)
        saved_hidden = store(saved_hidden, hidden, slot_index, is_valid, 0)
        saved_active = store(saved_active, wide_active, slot_index, is_valid, 0)
    grad_slots = jnp.zeros((images, strip_count, row_count, col_count, channels), jnp.bfloat16)
    saved_grad_out = jnp.zeros((strip_count, images, row_count, col_count, channels), jnp.bfloat16)
    saved_grad_hidden = jnp.zeros(
        (strip_count, images, row_count, col_count, channels), jnp.bfloat16
    )
    sending = empty_field
    for step_no in range(tick_count):
        micro_index = step_no - (section_count - 1 - section_index)
        is_valid = (micro_index >= 0) & (micro_index < strip_count)
        slot_index = jnp.clip(micro_index, 0, strip_count - 1)
        if step_no == 0:
            arriving = empty_field
        else:
            arriving = passed_along(sending, "section", -1)
        top_grad = lax.dynamic_index_in_dim(cotangent, slot_index, 1, keepdims=False)
        grad_out = jnp.where(section_index == section_count - 1, top_grad, arriving)
        grad_out = jnp.where(is_valid, grad_out, jnp.zeros_like(grad_out))
        hidden = lax.dynamic_index_in_dim(saved_hidden, slot_index, 0, keepdims=False)
        wide_grad = padded_2(grad_out, (("slab", 2),), 2)
        grad_active = convolve(second_backward, wide_grad)
        wide_hidden_grad = jnp.where(inside, grad_active * silu_slope(hidden), 0.0).astype(
            jnp.bfloat16
        )
        grad_hidden = wide_hidden_grad[:, :, 1:-1, :]
        sending = (
            grad_out.astype(jnp.float32) + convolve(first_backward, wide_hidden_grad)
        ).astype(jnp.bfloat16)
        saved_grad_out = store(saved_grad_out, grad_out, slot_index, is_valid, 0)
        saved_grad_hidden = store(saved_grad_hidden, grad_hidden, slot_index, is_valid, 0)
        grad_slots = store(grad_slots, sending, slot_index, is_valid, 1)
    flat_count = strip_count * images
    lower_part = contract(
        saved_field.reshape(flat_count, row_count, col_count + 2, channels),
        saved_grad_hidden.reshape(flat_count, row_count, col_count, channels),
    )
    upper_part = contract(
        saved_active.reshape(flat_count, row_count, col_count + 2, channels),
        saved_grad_out.reshape(flat_count, row_count, col_count, channels),
    )
    grad_terms = jnp.stack([lower_part, upper_part]).reshape(2, 9, channels, channels)
    row_share = lax.psum_scatter(
        grad_terms.astype(jnp.bfloat16), "slab", scatter_dimension=2, tiled=True
    )
    own_share = lax.psum_scatter(row_share, "img", scatter_dimension=3, tiled=True).astype(
        jnp.float32
    )
    grad_kernels = (own_share * scaling)[None]
    return (grad_kernels, grad_slots[None])


def call(kernel, outs, operands, unread, scratch, aliases):
    return pl.pallas_call(
        kernel,
        out_shape=outs,
        in_specs=[
            pl.BlockSpec(memory_space=pl.ANY if place in unread else pltpu.VMEM)
            for place in range(len(operands))
        ],
        out_specs=[pl.BlockSpec(memory_space=pltpu.VMEM)] * len(outs),
        scratch_shapes=scratch,
        input_output_aliases=aliases,
        compiler_params=pltpu.CompilerParams(vmem_limit_bytes=8 << 20),
    )(*operands)


def neighbours(value, shifted, width):
    count, channels = value.shape
    shifted[8 : 8 + count, :] = value
    column = lax.rem(lax.broadcasted_iota(jnp.int32, (count, channels), 0), width)
    before = jnp.where(column == 0, 0.0, shifted[7 : 7 + count, :])
    after = jnp.where(column == width - 1, 0.0, shifted[9 : 9 + count, :])
    return before, after


def convolved(value, matrix, taps, shifted, width):
    count, channels = value.shape
    before, after = neighbours(value, shifted, width)
    for place, part in enumerate((before, value, after)):
        taps[width : width + count, place * channels : (place + 1) * channels] = part.astype(
            jnp.bfloat16
        )
    edge = jnp.zeros((width, 3 * channels), jnp.bfloat16)
    taps[0:width, :] = edge
    taps[width + count : 2 * width + count, :] = edge
    total = jnp.dot(taps[0:count, :], matrix[0], preferred_element_type=jnp.float32)
    for down in (1, 2):
        total = total + jnp.dot(
            taps[down * width : down * width + count, :],
            matrix[down],
            preferred_element_type=jnp.float32,
        )
    return total


def forward_call(field, weights, state, section, crop, crops, width, last, after):
    count, channels = field.shape

    def kernel(field_ref, weights_ref, after_ref, *refs):
        *_, saved_ref, hidden_ref, taps, shifted = refs

        @pl.when(lax.axis_index("section") == section)
        def _():
            field_in = field_ref[...]
            wide = field_in.astype(jnp.float32)
            saved_ref[0, crop] = field_in
            hidden = convolved(wide, weights_ref.at[0], taps, shifted, width)
            hidden_ref[crop] = hidden
            active = (hidden * jax.nn.sigmoid(hidden)).astype(jnp.bfloat16)
            saved_ref[1, crop] = active
            if not last:
                added = convolved(
                    active.astype(jnp.float32), weights_ref.at[1], taps, shifted, width
                )
                refs[-5][...] = (wide + added).astype(jnp.bfloat16)

    outs = [
        jax.ShapeDtypeStruct((count, channels), jnp.bfloat16),
        jax.ShapeDtypeStruct((2, crops, count, channels), jnp.bfloat16),
        jax.ShapeDtypeStruct((crops, count, channels), jnp.float32),
    ][1 if last else 0 :]
    scratch = [
        pltpu.VMEM((count + 2 * width, 3 * channels), jnp.bfloat16),
        pltpu.VMEM((count + 16, channels), jnp.float32),
    ]
    aliases = {3 + k: k + (0 if last else 1) for k in range(len(state))}
    outputs = call(kernel, outs, [field, weights, after, *state], (2,), scratch, aliases)
    return (None if last else outputs[0]), outputs[-2:]


def backward_call(
    grad, turned, hidden, state, section, crop, crops, width, parts, after
):
    count, channels = grad.shape
    share = channels // parts
    first = section == 0

    def kernel(grad_ref, turned_ref, hidden_ref, after_ref, *refs):
        *_, kept_ref, sent_ref, taps, shifted = refs

        @pl.when(lax.axis_index("section") == section)
        def _():
            wide = grad_ref[...].astype(jnp.float32)
            kept_ref[0, crop] = grad_ref[...]
            grad_active = convolved(wide, turned_ref.at[1], taps, shifted, width)
            hidden = hidden_ref[crop]
            gate = jax.nn.sigmoid(hidden)
            grad_hidden = (grad_active * (gate * (1.0 + hidden * (1.0 - gate)))).astype(
                jnp.bfloat16
            )
            place_parts(sent_ref, (), grad_hidden, crop, parts, lax.axis_index("img"))
            added = convolved(
                grad_hidden.astype(jnp.float32), turned_ref.at[0], taps, shifted, width
            )
            result = (wide + added).astype(jnp.bfloat16)
            kept_ref[1, crop] = result
            if not first:
                refs[-5][...] = result

    outs = [
        jax.ShapeDtypeStruct((count, channels), jnp.bfloat16),
        jax.ShapeDtypeStruct((2, crops, count, channels), jnp.bfloat16),
        jax.ShapeDtypeStruct((parts, share, crops * count), jnp.bfloat16),
    ][1 if first else 0 :]
    scratch = [
        pltpu.VMEM((count + 2 * width, 3 * channels), jnp.bfloat16),
        pltpu.VMEM((count + 16, channels), jnp.float32),
    ]
    aliases = {4 + k: k + (0 if first else 1) for k in range(len(state))}
    operands = [grad, turned, hidden, after, *state]
    outputs = call(kernel, outs, operands, (3,), scratch, aliases)
    return (None if first else outputs[0]), outputs[-2:]


def place_parts(target, lead, value, crop, parts, own):
    count, channels = value.shape
    share = channels // parts
    flipped = value.T
    for part in range(parts):
        slot = lax.rem(part + parts - own, parts)
        target[(slot, *lead, slice(None), slice(crop * count, (crop + 1) * count))] = flipped[
            part * share : (part + 1) * share, :
        ]


def flip_call(kept, kinds, parts, axis, after):
    _, crops, count, channels = kept.shape

    def kernel(kept_ref, after_ref, flipped_ref):
        for place, kind in enumerate(kinds):
            for crop in range(crops):
                place_parts(
                    flipped_ref, (place,), kept_ref[kind, crop], crop, parts, lax.axis_index(axis)
                )

    shape = (parts, len(kinds), channels // parts, crops * count)
    (flipped,) = call(kernel, [jax.ShapeDtypeStruct(shape, kept.dtype)], [kept, after], (1,), [], {})
    return flipped


def turn_call(weights, after):
    two, _, _, channels = weights.shape

    def kernel(weights_ref, after_ref, turned_ref):
        for which in range(two):
            for tap in range(9):
                down, right = divmod(tap, 3)
                flipped = weights_ref[which, down, right * channels : (right + 1) * channels, :].T
                down, right = divmod(8 - tap, 3)
                turned_ref[which, down, right * channels : (right + 1) * channels, :] = flipped

    out = jax.ShapeDtypeStruct(weights.shape, weights.dtype)
    (turned,) = call(kernel, [out], [weights, after], (1,), [], {})
    return turned


def split_call(strips, cotangent, last):
    images, strip_count, rows, cols, channels = strips.shape
    share = strip_count // 2

    def kernel(strips_ref, cotangent_ref, own_ref, other_ref):
        own = lax.axis_index("slab")
        is_last = lax.axis_index("section") == last
        for image in range(images):
            for crop in range(share):
                at = image * share + crop
                for ref, half in ((own_ref, own), (other_ref, 1 - own)):
                    top = cotangent_ref[image, half * share + crop]
                    ref[at] = jnp.where(is_last, top, strips_ref[image, half * share + crop])

    out = jax.ShapeDtypeStruct((images * share, rows, cols, channels), strips.dtype)
    return call(kernel, [out, out], [strips, cotangent], (), [], {})


def join_call(own, other):
    crops, rows, cols, channels = own.shape

    def kernel(own_ref, other_ref, *out_refs):
        is_left = lax.axis_index("slab") == 0
        for crop, out_ref in enumerate(out_refs):
            mine = own_ref[crop].astype(jnp.float32)
            theirs = other_ref[crop].astype(jnp.float32)
            left = jnp.where(is_left, mine, theirs)
            right = jnp.where(is_left, theirs, mine)
            whole = jnp.concatenate([left, right], axis=1)
            out_ref[...] = whole.reshape(rows * 2 * cols, channels).astype(jnp.bfloat16)

    out = jax.ShapeDtypeStruct((rows * 2 * cols, channels), own.dtype)
    return call(kernel, [out] * crops, [own, other], (), [], {})


def part_call(kept, rows, after):
    _, crops, count, channels = kept.shape
    cols = count // rows // 2

    def kernel(kept_ref, after_ref, own_ref, other_ref):
        is_left = lax.axis_index("slab") == 0
        for crop in range(crops):
            whole = kept_ref[1, crop].astype(jnp.float32).reshape(rows, 2 * cols, channels)
            left, right = whole[:, :cols], whole[:, cols:]
            own_ref[crop] = jnp.where(is_left, left, right).astype(jnp.bfloat16)
            other_ref[crop] = jnp.where(is_left, right, left).astype(jnp.bfloat16)

    out = jax.ShapeDtypeStruct((crops, rows, cols, channels), kept.dtype)
    return call(kernel, [out, out], [kept, after], (1,), [], {})


def merge_call(own, other, images):
    crops, rows, cols, channels = own.shape
    share = crops // images

    def kernel(own_ref, other_ref, out_ref):
        place = lax.axis_index("slab")
        for image in range(images):
            for crop in range(share):
                out_ref[image, place * share + crop] = own_ref[image * share + crop]
                out_ref[image, (1 - place) * share + crop] = other_ref[image * share + crop]

    out = jax.ShapeDtypeStruct((images, 2 * share, rows, cols, channels), own.dtype)
    (merged,) = call(kernel, [out], [own, other], (), [], {})
    return merged


def choose_call(home, early, late, slot, last):
    blocks = 1 + len(early)

    def kernel(*refs):
        home_ref, out_ref = refs[0], refs[-1]
        early_refs, late_refs = refs[1:blocks], refs[blocks:-1]
        is_last = lax.axis_index("section") == last
        out_ref[0] = home_ref[slot]
        for block in range(1, blocks):
            out_ref[block] = jnp.where(
                is_last, late_refs[block - 1][slot], early_refs[block - 1][slot]
            )

    out = jax.ShapeDtypeStruct((blocks, *home.shape[1:]), home.dtype)
    (chosen,) = call(kernel, [out], [home, *early, *late], (), [], {})
    return chosen


def stack_call(inner, outer):
    blocks = len(outer)

    def kernel(*refs):
        out_ref = refs[-1]
        for block in range(blocks):
            value = refs[block][...]
            if inner:
                is_first = lax.axis_index("section") == 0
                value = jnp.where(is_first, refs[blocks + block][...], value)
            out_ref[block] = value

    out = jax.ShapeDtypeStruct((blocks, *outer[0].shape), outer[0].dtype)
    (stacked,) = call(kernel, [out], [*outer, *inner], (), [], {})
    return stacked


def spread_call(own, other, count, width):
    blocks, two, share, cells = own.shape
    crops = cells // count
    stride = count + width
    total = 2 * blocks * crops * stride + width

    def kernel(own_ref, other_ref, out_ref, done_ref, shifted):
        done_ref[...] = jnp.zeros_like(done_ref)
        edge = jnp.zeros((width, 3 * share), jnp.bfloat16)
        for kind in range(two):
            out_ref[kind, total - width : total, :] = edge
            for block in range(2 * blocks):
                ref = own_ref if block < blocks else other_ref
                for crop in range(crops):
                    value = ref[block % blocks, kind, :, crop * count : (crop + 1) * count]
                    value = value.T.astype(jnp.float32)
                    before, after = neighbours(value, shifted, width)
                    at = (block * crops + crop) * stride
                    out_ref[kind, at : at + width, :] = edge
                    for place, part in enumerate((before, value, after)):
                        lanes = slice(place * share, (place + 1) * share)
                        out_ref[kind, at + width : at + stride, lanes] = part.astype(jnp.bfloat16)

    outs = [
        jax.ShapeDtypeStruct((two, total, 3 * share), jnp.bfloat16),
        jax.ShapeDtypeStruct((8, 128), jnp.float32),
    ]
    scratch = [pltpu.VMEM((count + 16, share), jnp.float32)]
    return call(kernel, outs, [own, other], (), scratch, {})


def terms_call(around, kind, own, other, others, count, width, scaling):
    blocks, columns, cells = own.shape
    rows = around.shape[2] // 3
    stride = count + width
    crops = cells // count

    def kernel(around_ref, own_ref, other_ref, *refs):
        out_ref = refs[-1]
        if others:
            refs[-1][1] = refs[0][...]
            out_ref = refs[-1].at[0]
        for down in range(3):
            total = None
            for block in range(2 * blocks):
                left = own_ref[block] if block < blocks else other_ref[block - blocks]
                at = [(block * crops + k) * stride + down * width for k in range(crops)]
                right = jnp.concatenate(
                    [around_ref[kind, start : start + count, :] for start in at], axis=0
                )
                term = jnp.dot(left, right, preferred_element_type=jnp.float32)
                total = term if total is None else total + term
            total = (total * scaling).T.reshape(3, rows, columns)
            for place in range(3):
                out_ref[3 * down + place] = total[place]

    shape = (9, rows, columns)
    out = jax.ShapeDtypeStruct((2, *shape) if others else shape, jnp.float32)
    (terms,) = call(kernel, [out], [around, own, other, *others], (), [], {})
    return terms


def rotated(value, axis, steps):
    count = lax.axis_size(axis)
    return lax.ppermute(value, axis, [(source, (source + steps) % count) for source in range(count)])


def crop_shards(strips, kernels, cotangent):
    sections = lax.axis_size("section")
    slabs, groups = lax.axis_size("slab"), lax.axis_size("img")
    images, strip_count, row_count, col_count, channels = strips.shape
    width = col_count * slabs
    count = row_count * width
    crops = images * strip_count // slabs
    last = sections - 1
    scaling = 1.0 / math.sqrt(images * groups * strip_count * count)
    weights = kernels[0].reshape(2, 3, 3 * channels, channels)

    def hop(value, source, target):
        return lax.ppermute(value, "section", [(source, target)])

    def shared(values, step, routes):
        pairs = [
            (source * groups + i, target * groups + (i + step) % groups)
            for source, target in routes
            for i in range(groups)
        ]
        return lax.ppermute(values, ("section", "img"), pairs)

    own, other = split_call(strips, cotangent, last)
    fields = join_call(own, rotated(other, "slab", 1))
    incoming = fields
    state, saved_sets = [], []
    turned, after = None, weights
    for place in range(sections):
        outgoing = []
        for crop in range(crops):
            out, state = forward_call(
                incoming[crop], weights, state, place, crop, crops, width, place == last, after
            )
            outgoing.append(out)
        if place == 0:
            turned = turn_call(weights, state[0])
        if place < last:
            incoming = [hop(out, place, place + 1) for out in outgoing]
        if place == last - 1:
            flipped = flip_call(state[0], (0, 1), slabs, "slab", state[1])
            after = flipped
            routes = [(source, source) for source in range(last)]
            saved_sets.append([shared(flipped, step, routes) for step in range(1, groups)])
    saved, hidden = state
    incoming = fields
    grads = []
    around, after = None, hidden
    for place in reversed(range(sections)):
        outgoing = []
        for crop in range(crops):
            out, grads = backward_call(
                incoming[crop], turned, hidden, grads, place, crop, crops, width, groups, after
            )
            outgoing.append(out)
        if place:
            incoming = [hop(out, place, place - 1) for out in outgoing]
        if place == last:
            flipped = flip_call(saved, (0, 1), slabs, "slab", grads[0])
            saved_sets.append([shared(flipped, step, [(last, last)]) for step in range(1, groups)])
        if place == 1:
            handed = flip_call(grads[0], (0, 1), groups, "img", grads[1])
            routes = [(source, source) for source in range(1, sections)]
            later = [handed[0, 0]]
            for step in range(1, groups):
                later.append(shared(handed[step, 0], step, routes))
            first = [shared(handed[step, 1], step, [(1, 0)]) for step in range(groups)]
            own = choose_call(flipped, *saved_sets, 0, last)
            other = choose_call(flipped, *saved_sets, 1, last)
            other = rotated(other, "slab", 1)
            around, after = spread_call(own, other, count, width)
    kept, sent = grads
    hidden_grads = [sent[0]]
    for step in range(1, groups):
        hidden_grads.append(shared(sent[step], step, [(place, place) for place in range(sections)]))
    out_grads = stack_call(first, later)
    other = rotated(out_grads, "slab", 1)
    upper = terms_call(around, 1, out_grads, other, [], count, width, scaling)
    hidden_grads = stack_call([], hidden_grads)
    other = rotated(hidden_grads, "slab", 1)
    terms = terms_call(around, 0, hidden_grads, other, [upper], count, width, scaling)
    own, other = part_call(kept, row_count, hidden_grads)
    grad_inputs = merge_call(own, rotated(other, "slab", 1), images)
    return (terms[None], grad_inputs[None])


def shards(strips, kernels, cotangent):
    slabs, groups = lax.axis_size("slab"), lax.axis_size("img")
    strip_count, row_count, col_count, channels = strips.shape[1:]
    width = col_count * slabs
    whole_crops = strip_count % slabs == 0 and width % 16 == 0 and (row_count * width) % 128 == 0
    whole_crops = whole_crops and slabs == 2 and lax.axis_size("section") > 1
    if whole_crops and channels % (16 * slabs) == 0 and channels % (16 * groups) == 0:
        return crop_shards(strips, kernels, cotangent)
    return column_shards(strips, kernels, cotangent)


def solution(mesh):
    in_specs = (
        P("img", None, None, "slab", None),
        P("section", None, None, None, None),
        P("img", None, None, "slab", None),
    )
    out_specs = (
        P("section", None, None, "slab", "img"),
        P("section", "img", None, None, "slab", None),
    )
    return jax.shard_map(shards, mesh=mesh, in_specs=in_specs, out_specs=out_specs, check_vma=False)
```

```python
import math

import jax
import jax.numpy as jnp
from jax import lax
from jax.experimental import pallas as pl
from jax.experimental.pallas import tpu as pltpu
from jax.sharding import PartitionSpec as P


def passed_along(value, axis, steps):
    count = lax.axis_size(axis)
    initial, last = (max(0, -steps), min(count, count - steps))
    return lax.ppermute(value, axis, [(source, source + steps) for source in range(initial, last)])


def padded_2(cells, sides, width):
    for axis, dim in sides:
        count = lax.axis_size(axis)
        ends = count - 1
        head = lax.slice_in_dim(cells, 0, width, axis=dim)
        tail = lax.slice_in_dim(cells, cells.shape[dim] - width, cells.shape[dim], axis=dim)
        cells = jnp.concatenate(
            [
                lax.ppermute(tail, axis, [(i, (i + 1) % count) for i in range(ends)]),
                cells,
                lax.ppermute(head, axis, [((i + 1) % count, i) for i in range(ends)]),
            ],
            axis=dim,
        )
    return cells


def unfold(padded, row_count, col_count):
    tap_list = [
        padded[:, down_at : down_at + row_count, right_at : right_at + col_count, :]
        for down_at in range(3)
        for right_at in range(3)
    ]
    stacked = jnp.concatenate(tap_list, axis=3)
    return stacked.reshape(-1, stacked.shape[3])


def columns_of(wide_field):
    row_count = wide_field.shape[1]
    col_count = wide_field.shape[2] - 2
    padded = jnp.pad(wide_field, ((0, 0), (1, 1), (0, 0), (0, 0)))
    return unfold(padded, row_count, col_count)


def convolve(matrix, wide_field):
    count, row_count = (wide_field.shape[0], wide_field.shape[1])
    col_count = wide_field.shape[2] - 2
    flat_out = jnp.dot(columns_of(wide_field), matrix, preferred_element_type=jnp.float32)
    return flat_out.reshape(count, row_count, col_count, matrix.shape[1])


def contract(wide_field, grad_out):
    flat_grad = grad_out.reshape(-1, grad_out.shape[3])
    return lax.dot_general(
        columns_of(wide_field),
        flat_grad,
        (((0,), (0,)), ((), ())),
        preferred_element_type=jnp.float32,
    )


def silu_slope(hidden):
    sigmoid_at = jax.nn.sigmoid(hidden)
    return sigmoid_at * (1.0 + hidden * (1.0 - sigmoid_at))


def store(buffer, value, slot_index, is_valid, axis_at):
    current = lax.dynamic_index_in_dim(buffer, slot_index, axis_at, keepdims=False)
    return lax.dynamic_update_index_in_dim(
        buffer, jnp.where(is_valid, value, current), slot_index, axis_at
    )


def column_shards(strips, kernels, cotangent):
    section_count = lax.axis_size("section")
    section_index = lax.axis_index("section")
    slab_count = lax.axis_size("slab")
    slab_index = lax.axis_index("slab")
    images, strip_count, row_count, col_count, channels = strips.shape
    weights = kernels[0]
    first_forward = weights[0].reshape(9 * channels, channels)
    second_forward = weights[1].reshape(9 * channels, channels)
    first_backward = jnp.transpose(weights[0][::-1], (0, 2, 1)).reshape(9 * channels, channels)
    second_backward = jnp.transpose(weights[1][::-1], (0, 2, 1)).reshape(9 * channels, channels)
    scaling = 1.0 / math.sqrt(
        images * lax.axis_size("img") * strip_count * row_count * col_count * slab_count
    )
    position = slab_index * col_count - 1 + jnp.arange(col_count + 2, dtype=jnp.int32)
    inside = ((position >= 0) & (position < slab_count * col_count))[None, None, :, None]
    tick_count = strip_count + section_count - 1
    hidden_cols = col_count + 2
    empty_field = jnp.zeros((images, row_count, col_count, channels), jnp.bfloat16)
    saved_field = jnp.zeros((strip_count, images, row_count, col_count + 2, channels), jnp.bfloat16)
    saved_hidden = jnp.zeros((strip_count, images, row_count, hidden_cols, channels), jnp.float32)
    saved_active = jnp.zeros(
        (strip_count, images, row_count, col_count + 2, channels), jnp.bfloat16
    )
    outgoing = empty_field
    for step_no in range(tick_count):
        micro_index = step_no - section_index
        is_valid = (micro_index >= 0) & (micro_index < strip_count)
        slot_index = jnp.clip(micro_index, 0, strip_count - 1)
        if step_no == 0:
            incoming = empty_field
        else:
            incoming = passed_along(outgoing, "section", 1)
        first_strip = lax.dynamic_index_in_dim(strips, slot_index, 1, keepdims=False)
        field_in = jnp.where(section_index == 0, first_strip, incoming)
        wide_deep = padded_2(field_in, (("slab", 2),), 2)
        hidden = convolve(first_forward, wide_deep)
        wide_active = jnp.where(inside, jax.nn.silu(hidden), 0.0).astype(jnp.bfloat16)
        wide_field = wide_deep[:, :, 1:-1, :]
        outgoing = (field_in.astype(jnp.float32) + convolve(second_forward, wide_active)).astype(
            jnp.bfloat16
        )
        saved_field = store(saved_field, wide_field, slot_index, is_valid, 0)
        saved_hidden = store(saved_hidden, hidden, slot_index, is_valid, 0)
        saved_active = store(saved_active, wide_active, slot_index, is_valid, 0)
    grad_slots = jnp.zeros((images, strip_count, row_count, col_count, channels), jnp.bfloat16)
    saved_grad_out = jnp.zeros((strip_count, images, row_count, col_count, channels), jnp.bfloat16)
    saved_grad_hidden = jnp.zeros(
        (strip_count, images, row_count, col_count, channels), jnp.bfloat16
    )
    sending = empty_field
    for step_no in range(tick_count):
        micro_index = step_no - (section_count - 1 - section_index)
        is_valid = (micro_index >= 0) & (micro_index < strip_count)
        slot_index = jnp.clip(micro_index, 0, strip_count - 1)
        if step_no == 0:
            arriving = empty_field
        else:
            arriving = passed_along(sending, "section", -1)
        top_grad = lax.dynamic_index_in_dim(cotangent, slot_index, 1, keepdims=False)
        grad_out = jnp.where(section_index == section_count - 1, top_grad, arriving)
        grad_out = jnp.where(is_valid, grad_out, jnp.zeros_like(grad_out))
        hidden = lax.dynamic_index_in_dim(saved_hidden, slot_index, 0, keepdims=False)
        wide_grad = padded_2(grad_out, (("slab", 2),), 2)
        grad_active = convolve(second_backward, wide_grad)
        wide_hidden_grad = jnp.where(inside, grad_active * silu_slope(hidden), 0.0).astype(
            jnp.bfloat16
        )
        grad_hidden = wide_hidden_grad[:, :, 1:-1, :]
        sending = (
            grad_out.astype(jnp.float32) + convolve(first_backward, wide_hidden_grad)
        ).astype(jnp.bfloat16)
        saved_grad_out = store(saved_grad_out, grad_out, slot_index, is_valid, 0)
        saved_grad_hidden = store(saved_grad_hidden, grad_hidden, slot_index, is_valid, 0)
        grad_slots = store(grad_slots, sending, slot_index, is_valid, 1)
    flat_count = strip_count * images
    lower_part = contract(
        saved_field.reshape(flat_count, row_count, col_count + 2, channels),
        saved_grad_hidden.reshape(flat_count, row_count, col_count, channels),
    )
    upper_part = contract(
        saved_active.reshape(flat_count, row_count, col_count + 2, channels),
        saved_grad_out.reshape(flat_count, row_count, col_count, channels),
    )
    grad_terms = jnp.stack([lower_part, upper_part]).reshape(2, 9, channels, channels)
    row_share = lax.psum_scatter(
        grad_terms.astype(jnp.bfloat16), "slab", scatter_dimension=2, tiled=True
    )
    own_share = lax.psum_scatter(row_share, "img", scatter_dimension=3, tiled=True).astype(
        jnp.float32
    )
    grad_kernels = (own_share * scaling)[None]
    return (grad_kernels, grad_slots[None])


def call(kernel, outs, operands, unread, scratch, aliases, apart=()):
    spaces = {**dict.fromkeys(unread, pl.ANY), **dict.fromkeys(apart, pltpu.HBM)}
    return pl.pallas_call(
        kernel,
        out_shape=outs,
        in_specs=[
            pl.BlockSpec(memory_space=spaces.get(place, pltpu.VMEM))
            for place in range(len(operands))
        ],
        out_specs=[pl.BlockSpec(memory_space=pltpu.VMEM)] * len(outs),
        scratch_shapes=scratch,
        input_output_aliases=aliases,
        compiler_params=pltpu.CompilerParams(vmem_limit_bytes=8 << 20),
    )(*operands)


def neighbours(value, shifted, width):
    count, channels = value.shape
    shifted[8 : 8 + count, :] = value
    column = lax.rem(lax.broadcasted_iota(jnp.int32, (count, channels), 0), width)
    before = jnp.where(column == 0, 0.0, shifted[7 : 7 + count, :])
    after = jnp.where(column == width - 1, 0.0, shifted[9 : 9 + count, :])
    return before, after


def convolved(value, matrix, taps, shifted, width):
    count, channels = value.shape
    before, after = neighbours(value, shifted, width)
    for place, part in enumerate((before, value, after)):
        taps[width : width + count, place * channels : (place + 1) * channels] = part.astype(
            jnp.bfloat16
        )
    edge = jnp.zeros((width, 3 * channels), jnp.bfloat16)
    taps[0:width, :] = edge
    taps[width + count : 2 * width + count, :] = edge
    total = jnp.dot(taps[0:count, :], matrix[0], preferred_element_type=jnp.float32)
    for down in (1, 2):
        total = total + jnp.dot(
            taps[down * width : down * width + count, :],
            matrix[down],
            preferred_element_type=jnp.float32,
        )
    return total


def forward_call(field, weights, state, section, crop, crops, width, last, after):
    count, channels = field.shape

    def kernel(field_ref, weights_ref, after_ref, *refs):
        *_, saved_ref, hidden_ref, taps, shifted = refs

        @pl.when(lax.axis_index("section") == section)
        def _():
            field_in = field_ref[...]
            wide = field_in.astype(jnp.float32)
            saved_ref[0, crop] = field_in
            hidden = convolved(wide, weights_ref.at[0], taps, shifted, width)
            hidden_ref[crop] = hidden
            active = (hidden * jax.nn.sigmoid(hidden)).astype(jnp.bfloat16)
            saved_ref[1, crop] = active
            if not last:
                added = convolved(
                    active.astype(jnp.float32), weights_ref.at[1], taps, shifted, width
                )
                refs[-5][...] = (wide + added).astype(jnp.bfloat16)

    outs = [
        jax.ShapeDtypeStruct((count, channels), jnp.bfloat16),
        jax.ShapeDtypeStruct((2, crops, count, channels), jnp.bfloat16),
        jax.ShapeDtypeStruct((crops, count, channels), jnp.float32),
    ][1 if last else 0 :]
    scratch = [
        pltpu.VMEM((count + 2 * width, 3 * channels), jnp.bfloat16),
        pltpu.VMEM((count + 16, channels), jnp.float32),
    ]
    aliases = {3 + k: k + (0 if last else 1) for k in range(len(state))}
    outputs = call(kernel, outs, [field, weights, after, *state], (2,), scratch, aliases)
    return (None if last else outputs[0]), outputs[-2:]


def backward_call(
    grad, turned, hidden, state, section, crop, crops, width, parts, after
):
    count, channels = grad.shape
    share = channels // parts
    first = section == 0

    def kernel(grad_ref, turned_ref, hidden_ref, after_ref, *refs):
        *_, kept_ref, sent_ref, taps, shifted = refs

        @pl.when(lax.axis_index("section") == section)
        def _():
            wide = grad_ref[...].astype(jnp.float32)
            own = lax.axis_index("img")
            place_parts(sent_ref, (0,), grad_ref[...], crop, parts, own)
            grad_active = convolved(wide, turned_ref.at[1], taps, shifted, width)
            hidden = hidden_ref[crop]
            gate = jax.nn.sigmoid(hidden)
            grad_hidden = (grad_active * (gate * (1.0 + hidden * (1.0 - gate)))).astype(
                jnp.bfloat16
            )
            place_parts(sent_ref, (1,), grad_hidden, crop, parts, own)
            added = convolved(
                grad_hidden.astype(jnp.float32), turned_ref.at[0], taps, shifted, width
            )
            result = (wide + added).astype(jnp.bfloat16)
            kept_ref[crop] = result
            if not first:
                refs[-5][...] = result

    outs = [
        jax.ShapeDtypeStruct((count, channels), jnp.bfloat16),
        jax.ShapeDtypeStruct((crops, count, channels), jnp.bfloat16),
        jax.ShapeDtypeStruct((parts, 2, share, crops * count), jnp.bfloat16),
    ][1 if first else 0 :]
    scratch = [
        pltpu.VMEM((count + 2 * width, 3 * channels), jnp.bfloat16),
        pltpu.VMEM((count + 16, channels), jnp.float32),
    ]
    aliases = {4 + k: k + (0 if first else 1) for k in range(len(state))}
    operands = [grad, turned, hidden, after, *state]
    outputs = call(kernel, outs, operands, (3,), scratch, aliases)
    return (None if first else outputs[0]), outputs[-2:]


def place_parts(target, lead, value, crop, parts, own):
    count, channels = value.shape
    share = channels // parts
    flipped = value.T
    for part in range(parts):
        slot = lax.rem(part + parts - own, parts)
        target[(slot, *lead, slice(None), slice(crop * count, (crop + 1) * count))] = flipped[
            part * share : (part + 1) * share, :
        ]


def flip_call(kept, kinds, parts, axis, after):
    _, crops, count, channels = kept.shape

    def kernel(kept_ref, after_ref, flipped_ref):
        for place, kind in enumerate(kinds):
            for crop in range(crops):
                place_parts(
                    flipped_ref, (place,), kept_ref[kind, crop], crop, parts, lax.axis_index(axis)
                )

    shape = (parts, len(kinds), channels // parts, crops * count)
    (flipped,) = call(kernel, [jax.ShapeDtypeStruct(shape, kept.dtype)], [kept, after], (1,), [], {})
    return flipped


def turn_call(weights, after):
    two, _, _, channels = weights.shape

    def kernel(weights_ref, after_ref, turned_ref):
        for which in range(two):
            for tap in range(9):
                down, right = divmod(tap, 3)
                flipped = weights_ref[which, down, right * channels : (right + 1) * channels, :].T
                down, right = divmod(8 - tap, 3)
                turned_ref[which, down, right * channels : (right + 1) * channels, :] = flipped

    out = jax.ShapeDtypeStruct(weights.shape, weights.dtype)
    (turned,) = call(kernel, [out], [weights, after], (1,), [], {})
    return turned


def split_call(strips, cotangent, last):
    images, strip_count, rows, cols, channels = strips.shape
    share = strip_count // 2

    def kernel(strips_ref, cotangent_ref, own_ref, other_ref, sems):
        own = lax.axis_index("slab")
        is_last = lax.axis_index("section") == last

        def fetch(source_ref):
            copies = []
            for image in range(images):
                at = pl.ds(image * share, share)
                for side, (ref, half) in enumerate(((own_ref, own), (other_ref, 1 - own))):
                    source = source_ref.at[image, pl.ds(half * share, share)]
                    copies.append(pltpu.make_async_copy(source, ref.at[at], sems.at[2 * image + side]))
            for copy in copies:
                copy.start()
            for copy in copies:
                copy.wait()

        @pl.when(is_last)
        def _():
            fetch(cotangent_ref)

        @pl.when(jnp.logical_not(is_last))
        def _():
            fetch(strips_ref)

    out = jax.ShapeDtypeStruct((images * share, rows, cols, channels), strips.dtype)
    sems = [pltpu.SemaphoreType.DMA((2 * images,))]
    return call(kernel, [out, out], [strips, cotangent], (), sems, {}, (0, 1))


def load_call(weights):
    def kernel(weights_ref, out_ref, sems):
        copies = [
            pltpu.make_async_copy(weights_ref.at[which], out_ref.at[which], sems.at[which])
            for which in range(2)
        ]
        for copy in copies:
            copy.start()
        for copy in copies:
            copy.wait()

    out = jax.ShapeDtypeStruct(weights.shape, weights.dtype)
    sems = [pltpu.SemaphoreType.DMA((2,))]
    (loaded,) = call(kernel, [out], [weights], (), sems, {}, (0,))
    return loaded


def join_call(own, other):
    crops, rows, cols, channels = own.shape

    def kernel(own_ref, other_ref, *out_refs):
        is_left = lax.axis_index("slab") == 0
        for crop, out_ref in enumerate(out_refs):
            mine = own_ref[crop].astype(jnp.float32)
            theirs = other_ref[crop].astype(jnp.float32)
            left = jnp.where(is_left, mine, theirs)
            right = jnp.where(is_left, theirs, mine)
            whole = jnp.concatenate([left, right], axis=1)
            out_ref[...] = whole.reshape(rows * 2 * cols, channels).astype(jnp.bfloat16)

    out = jax.ShapeDtypeStruct((rows * 2 * cols, channels), own.dtype)
    return call(kernel, [out] * crops, [own, other], (), [], {})


def part_call(kept, rows, after):
    crops, count, channels = kept.shape
    cols = count // rows // 2

    def kernel(kept_ref, after_ref, own_ref, other_ref):
        is_left = lax.axis_index("slab") == 0
        for crop in range(crops):
            whole = kept_ref[crop].astype(jnp.float32).reshape(rows, 2 * cols, channels)
            left, right = whole[:, :cols], whole[:, cols:]
            own_ref[crop] = jnp.where(is_left, left, right).astype(jnp.bfloat16)
            other_ref[crop] = jnp.where(is_left, right, left).astype(jnp.bfloat16)

    out = jax.ShapeDtypeStruct((crops, rows, cols, channels), kept.dtype)
    return call(kernel, [out, out], [kept, after], (1,), [], {})


def merge_call(own, other, images):
    crops, rows, cols, channels = own.shape
    share = crops // images

    def kernel(own_ref, other_ref, out_ref):
        place = lax.axis_index("slab")
        for image in range(images):
            for crop in range(share):
                out_ref[image, place * share + crop] = own_ref[image * share + crop]
                out_ref[image, (1 - place) * share + crop] = other_ref[image * share + crop]

    out = jax.ShapeDtypeStruct((images, 2 * share, rows, cols, channels), own.dtype)
    (merged,) = call(kernel, [out], [own, other], (), [], {})
    return merged


def stack_call(blocks, slot, after):
    def kernel(*refs):
        for place in range(len(blocks)):
            refs[-1][place] = refs[place][...] if slot is None else refs[place][slot]

    shape = blocks[0].shape if slot is None else blocks[0].shape[1:]
    out = jax.ShapeDtypeStruct((len(blocks), *shape), blocks[0].dtype)
    (stacked,) = call(kernel, [out], [*blocks, after], (len(blocks),), [], {})
    return stacked


def spread_call(sources, slots, blocks, around, is_last, last, count, width):
    two, share, cells = sources[0].shape[-3:]
    crops = cells // count
    stride = count + width
    fresh = isinstance(around, jax.ShapeDtypeStruct)
    total = around.shape[1]

    def kernel(*refs):
        out_ref, shifted = refs[-2:]
        mine = (lax.axis_index("section") == last) == is_last

        @pl.when(mine)
        def _():
            edge = jnp.zeros((width, 3 * share), jnp.bfloat16)
            for kind in range(two):
                out_ref[kind, total - width : total, :] = edge
                for ref, slot, block in zip(refs, slots, blocks):
                    for crop in range(crops):
                        cell = slice(crop * count, (crop + 1) * count)
                        value = ref[(*slot, kind, slice(None), cell)].T.astype(jnp.float32)
                        before, after = neighbours(value, shifted, width)
                        at = (block * crops + crop) * stride
                        out_ref[kind, at : at + width, :] = edge
                        for place, part in enumerate((before, value, after)):
                            lanes = slice(place * share, (place + 1) * share)
                            out_ref[kind, at + width : at + stride, lanes] = part.astype(
                                jnp.bfloat16
                            )

    operands = [*sources] if fresh else [*sources, around]
    aliases = {} if fresh else {len(sources): 0}
    out = jax.ShapeDtypeStruct(around.shape, around.dtype)
    scratch = [pltpu.VMEM((count + 16, share), jnp.float32)]
    (spread,) = call(kernel, [out], operands, (), scratch, aliases)
    return spread


def terms_call(around, own, other, count, width, scaling):
    blocks, _, columns, cells = own.shape
    rows = around.shape[2] // 3
    stride = count + width
    crops = cells // count

    def kernel(around_ref, own_ref, other_ref, out_ref):
        for kind in range(2):
            for down in range(3):
                total = None
                for block in range(2 * blocks):
                    left = own_ref if block < blocks else other_ref
                    left = left[block % blocks, 1 - kind]
                    at = [(block * crops + k) * stride + down * width for k in range(crops)]
                    right = jnp.concatenate(
                        [around_ref[kind, start : start + count, :] for start in at], axis=0
                    )
                    term = jnp.dot(left, right, preferred_element_type=jnp.float32)
                    total = term if total is None else total + term
                total = (total * scaling).T.reshape(3, rows, columns)
                for place in range(3):
                    out_ref[kind, 3 * down + place] = total[place]

    out = jax.ShapeDtypeStruct((2, 9, rows, columns), jnp.float32)
    (terms,) = call(kernel, [out], [around, own, other], (), [], {})
    return terms


def rotated(value, axis, steps):
    count = lax.axis_size(axis)
    return lax.ppermute(value, axis, [(source, (source + steps) % count) for source in range(count)])


def crop_shards(strips, kernels, cotangent):
    sections = lax.axis_size("section")
    slabs, groups = lax.axis_size("slab"), lax.axis_size("img")
    images, strip_count, row_count, col_count, channels = strips.shape
    width = col_count * slabs
    count = row_count * width
    crops = images * strip_count // slabs
    last = sections - 1
    scaling = 1.0 / math.sqrt(images * groups * strip_count * count)

    def hop(value, source, target):
        return lax.ppermute(value, "section", [(source, target)])

    def shared(values, step, routes):
        pairs = [
            (source * groups + i, source * groups + (i + step) % groups)
            for source in routes
            for i in range(groups)
        ]
        return lax.ppermute(values, ("section", "img"), pairs)

    everywhere = range(sections)
    own, other = split_call(strips, cotangent, last)
    other = rotated(other, "slab", 1)
    weights = load_call(kernels[0].reshape(2, 3, 3 * channels, channels))
    fields = join_call(own, other)
    incoming = fields
    state, early = [], []
    turned, after = None, weights
    for place in range(sections):
        outgoing = []
        for crop in range(crops):
            out, state = forward_call(
                incoming[crop], weights, state, place, crop, crops, width, place == last, after
            )
            outgoing.append(out)
        if place == 0:
            turned = turn_call(weights, state[0])
        if place < last:
            incoming = [hop(out, place, place + 1) for out in outgoing]
        if place == last - 1:
            flipped = flip_call(state[0], (0, 1), slabs, "slab", state[1])
            after = flipped
            early = [flipped]
            for step in range(1, groups):
                early.append(shared(flipped, step, everywhere))
    saved, hidden = state
    incoming = fields
    grads = []
    around, after = None, hidden
    late = []
    for place in reversed(range(sections)):
        outgoing = []
        for crop in range(crops):
            out, grads = backward_call(
                incoming[crop], turned, hidden, grads, place, crop, crops, width, groups, after
            )
            outgoing.append(out)
        if place:
            incoming = [hop(out, place, place - 1) for out in outgoing]
        if place == last:
            flipped = flip_call(saved, (0, 1), slabs, "slab", grads[0])
            pairs = [(last * slabs + i, last * slabs + (i + 1) % slabs) for i in range(slabs)]
            other = lax.ppermute(flipped[1], ("section", "slab"), pairs)
            both = stack_call([flipped[0], other], None, grads[0])
            late = [both]
            for step in range(1, groups):
                late.append(shared(both, step, [last]))
        if place == 1:
            other = stack_call(early, 1, outgoing[-1])
            other = rotated(other, "slab", 1)
            stride = count + width
            shape = (2, slabs * groups * crops * stride + width, 3 * (channels // slabs))
            around = spread_call(
                [*early, *([other] * groups)],
                [(0,)] * groups + [(block,) for block in range(groups)],
                list(range(slabs * groups)),
                jax.ShapeDtypeStruct(shape, jnp.bfloat16),
                False,
                last,
                count,
                width,
            )
            after = around
    kept, sent = grads
    own = [sent[0]]
    for step in range(1, groups):
        own.append(shared(sent[step], step, everywhere))
    around, sent = lax.optimization_barrier((around, sent))
    for block in range(groups):
        around = spread_call(
            [late[block]] * slabs,
            [(slab,) for slab in range(slabs)],
            [slab * groups + block for slab in range(slabs)],
            around,
            True,
            last,
            count,
            width,
        )
    own = stack_call(own, None, around)
    other = rotated(own, "slab", 1)
    terms = terms_call(around, own, other, count, width, scaling)
    own, other = part_call(kept, row_count, sent)
    other = rotated(other, "slab", 1)
    grad_inputs = merge_call(own, other, images)
    return (terms[None], grad_inputs[None])


def shards(strips, kernels, cotangent):
    slabs, groups = lax.axis_size("slab"), lax.axis_size("img")
    strip_count, row_count, col_count, channels = strips.shape[1:]
    width = col_count * slabs
    whole_crops = strip_count % slabs == 0 and width % 16 == 0 and (row_count * width) % 128 == 0
    whole_crops = whole_crops and slabs == 2 and lax.axis_size("section") > 1
    if whole_crops and channels % (16 * slabs) == 0 and channels % (16 * groups) == 0:
        return crop_shards(strips, kernels, cotangent)
    return column_shards(strips, kernels, cotangent)


def solution(mesh):
    in_specs = (
        P("img", None, None, "slab", None),
        P("section", None, None, None, None),
        P("img", None, None, "slab", None),
    )
    out_specs = (
        P("section", None, None, "slab", "img"),
        P("section", "img", None, None, "slab", None),
    )
    return jax.shard_map(shards, mesh=mesh, in_specs=in_specs, out_specs=out_specs, check_vma=False)
```

```python
import math

import jax
import jax.numpy as jnp
from jax import lax
from jax.experimental import pallas as pl
from jax.experimental.pallas import tpu as pltpu
from jax.sharding import PartitionSpec as P


def passed_along(value, axis, steps):
    count = lax.axis_size(axis)
    initial, last = (max(0, -steps), min(count, count - steps))
    return lax.ppermute(value, axis, [(source, source + steps) for source in range(initial, last)])


def padded_2(cells, sides, width):
    for axis, dim in sides:
        count = lax.axis_size(axis)
        ends = count - 1
        head = lax.slice_in_dim(cells, 0, width, axis=dim)
        tail = lax.slice_in_dim(cells, cells.shape[dim] - width, cells.shape[dim], axis=dim)
        cells = jnp.concatenate(
            [
                lax.ppermute(tail, axis, [(i, (i + 1) % count) for i in range(ends)]),
                cells,
                lax.ppermute(head, axis, [((i + 1) % count, i) for i in range(ends)]),
            ],
            axis=dim,
        )
    return cells


def unfold(padded, row_count, col_count):
    tap_list = [
        padded[:, down_at : down_at + row_count, right_at : right_at + col_count, :]
        for down_at in range(3)
        for right_at in range(3)
    ]
    stacked = jnp.concatenate(tap_list, axis=3)
    return stacked.reshape(-1, stacked.shape[3])


def columns_of(wide_field):
    row_count = wide_field.shape[1]
    col_count = wide_field.shape[2] - 2
    padded = jnp.pad(wide_field, ((0, 0), (1, 1), (0, 0), (0, 0)))
    return unfold(padded, row_count, col_count)


def convolve(matrix, wide_field):
    count, row_count = (wide_field.shape[0], wide_field.shape[1])
    col_count = wide_field.shape[2] - 2
    flat_out = jnp.dot(columns_of(wide_field), matrix, preferred_element_type=jnp.float32)
    return flat_out.reshape(count, row_count, col_count, matrix.shape[1])


def contract(wide_field, grad_out):
    flat_grad = grad_out.reshape(-1, grad_out.shape[3])
    return lax.dot_general(
        columns_of(wide_field),
        flat_grad,
        (((0,), (0,)), ((), ())),
        preferred_element_type=jnp.float32,
    )


def silu_slope(hidden):
    sigmoid_at = jax.nn.sigmoid(hidden)
    return sigmoid_at * (1.0 + hidden * (1.0 - sigmoid_at))


def store(buffer, value, slot_index, is_valid, axis_at):
    current = lax.dynamic_index_in_dim(buffer, slot_index, axis_at, keepdims=False)
    return lax.dynamic_update_index_in_dim(
        buffer, jnp.where(is_valid, value, current), slot_index, axis_at
    )


def column_shards(strips, kernels, cotangent):
    section_count = lax.axis_size("section")
    section_index = lax.axis_index("section")
    slab_count = lax.axis_size("slab")
    slab_index = lax.axis_index("slab")
    images, strip_count, row_count, col_count, channels = strips.shape
    weights = kernels[0]
    first_forward = weights[0].reshape(9 * channels, channels)
    second_forward = weights[1].reshape(9 * channels, channels)
    first_backward = jnp.transpose(weights[0][::-1], (0, 2, 1)).reshape(9 * channels, channels)
    second_backward = jnp.transpose(weights[1][::-1], (0, 2, 1)).reshape(9 * channels, channels)
    scaling = 1.0 / math.sqrt(
        images * lax.axis_size("img") * strip_count * row_count * col_count * slab_count
    )
    position = slab_index * col_count - 1 + jnp.arange(col_count + 2, dtype=jnp.int32)
    inside = ((position >= 0) & (position < slab_count * col_count))[None, None, :, None]
    tick_count = strip_count + section_count - 1
    hidden_cols = col_count + 2
    empty_field = jnp.zeros((images, row_count, col_count, channels), jnp.bfloat16)
    saved_field = jnp.zeros((strip_count, images, row_count, col_count + 2, channels), jnp.bfloat16)
    saved_hidden = jnp.zeros((strip_count, images, row_count, hidden_cols, channels), jnp.float32)
    saved_active = jnp.zeros(
        (strip_count, images, row_count, col_count + 2, channels), jnp.bfloat16
    )
    outgoing = empty_field
    for step_no in range(tick_count):
        micro_index = step_no - section_index
        is_valid = (micro_index >= 0) & (micro_index < strip_count)
        slot_index = jnp.clip(micro_index, 0, strip_count - 1)
        if step_no == 0:
            incoming = empty_field
        else:
            incoming = passed_along(outgoing, "section", 1)
        first_strip = lax.dynamic_index_in_dim(strips, slot_index, 1, keepdims=False)
        field_in = jnp.where(section_index == 0, first_strip, incoming)
        wide_deep = padded_2(field_in, (("slab", 2),), 2)
        hidden = convolve(first_forward, wide_deep)
        wide_active = jnp.where(inside, jax.nn.silu(hidden), 0.0).astype(jnp.bfloat16)
        wide_field = wide_deep[:, :, 1:-1, :]
        outgoing = (field_in.astype(jnp.float32) + convolve(second_forward, wide_active)).astype(
            jnp.bfloat16
        )
        saved_field = store(saved_field, wide_field, slot_index, is_valid, 0)
        saved_hidden = store(saved_hidden, hidden, slot_index, is_valid, 0)
        saved_active = store(saved_active, wide_active, slot_index, is_valid, 0)
    grad_slots = jnp.zeros((images, strip_count, row_count, col_count, channels), jnp.bfloat16)
    saved_grad_out = jnp.zeros((strip_count, images, row_count, col_count, channels), jnp.bfloat16)
    saved_grad_hidden = jnp.zeros(
        (strip_count, images, row_count, col_count, channels), jnp.bfloat16
    )
    sending = empty_field
    for step_no in range(tick_count):
        micro_index = step_no - (section_count - 1 - section_index)
        is_valid = (micro_index >= 0) & (micro_index < strip_count)
        slot_index = jnp.clip(micro_index, 0, strip_count - 1)
        if step_no == 0:
            arriving = empty_field
        else:
            arriving = passed_along(sending, "section", -1)
        top_grad = lax.dynamic_index_in_dim(cotangent, slot_index, 1, keepdims=False)
        grad_out = jnp.where(section_index == section_count - 1, top_grad, arriving)
        grad_out = jnp.where(is_valid, grad_out, jnp.zeros_like(grad_out))
        hidden = lax.dynamic_index_in_dim(saved_hidden, slot_index, 0, keepdims=False)
        wide_grad = padded_2(grad_out, (("slab", 2),), 2)
        grad_active = convolve(second_backward, wide_grad)
        wide_hidden_grad = jnp.where(inside, grad_active * silu_slope(hidden), 0.0).astype(
            jnp.bfloat16
        )
        grad_hidden = wide_hidden_grad[:, :, 1:-1, :]
        sending = (
            grad_out.astype(jnp.float32) + convolve(first_backward, wide_hidden_grad)
        ).astype(jnp.bfloat16)
        saved_grad_out = store(saved_grad_out, grad_out, slot_index, is_valid, 0)
        saved_grad_hidden = store(saved_grad_hidden, grad_hidden, slot_index, is_valid, 0)
        grad_slots = store(grad_slots, sending, slot_index, is_valid, 1)
    flat_count = strip_count * images
    lower_part = contract(
        saved_field.reshape(flat_count, row_count, col_count + 2, channels),
        saved_grad_hidden.reshape(flat_count, row_count, col_count, channels),
    )
    upper_part = contract(
        saved_active.reshape(flat_count, row_count, col_count + 2, channels),
        saved_grad_out.reshape(flat_count, row_count, col_count, channels),
    )
    grad_terms = jnp.stack([lower_part, upper_part]).reshape(2, 9, channels, channels)
    row_share = lax.psum_scatter(
        grad_terms.astype(jnp.bfloat16), "slab", scatter_dimension=2, tiled=True
    )
    own_share = lax.psum_scatter(row_share, "img", scatter_dimension=3, tiled=True).astype(
        jnp.float32
    )
    grad_kernels = (own_share * scaling)[None]
    return (grad_kernels, grad_slots[None])


def call(kernel, outs, operands, unread, scratch, aliases, apart=()):
    spaces = {**dict.fromkeys(unread, pl.ANY), **dict.fromkeys(apart, pltpu.HBM)}
    return pl.pallas_call(
        kernel,
        out_shape=outs,
        in_specs=[
            pl.BlockSpec(memory_space=spaces.get(place, pltpu.VMEM))
            for place in range(len(operands))
        ],
        out_specs=[pl.BlockSpec(memory_space=pltpu.VMEM)] * len(outs),
        scratch_shapes=scratch,
        input_output_aliases=aliases,
        compiler_params=pltpu.CompilerParams(vmem_limit_bytes=8 << 20),
    )(*operands)


def neighbours(value, shifted, width):
    count, channels = value.shape
    shifted[8 : 8 + count, :] = value
    column = lax.rem(lax.broadcasted_iota(jnp.int32, (count, channels), 0), width)
    before = jnp.where(column == 0, 0.0, shifted[7 : 7 + count, :])
    after = jnp.where(column == width - 1, 0.0, shifted[9 : 9 + count, :])
    return before, after


def convolved(value, matrix, taps, shifted, width):
    count, channels = value.shape
    before, after = neighbours(value, shifted, width)
    for place, part in enumerate((before, value, after)):
        taps[width : width + count, place * channels : (place + 1) * channels] = part.astype(
            jnp.bfloat16
        )
    edge = jnp.zeros((width, 3 * channels), jnp.bfloat16)
    taps[0:width, :] = edge
    taps[width + count : 2 * width + count, :] = edge
    total = jnp.dot(taps[0:count, :], matrix[0], preferred_element_type=jnp.float32)
    for down in (1, 2):
        total = total + jnp.dot(
            taps[down * width : down * width + count, :],
            matrix[down],
            preferred_element_type=jnp.float32,
        )
    return total


def forward_call(field, weights, state, section, crop, crops, width, last, after):
    count, channels = field.shape

    def kernel(field_ref, weights_ref, after_ref, *refs):
        *_, saved_ref, hidden_ref, taps, shifted = refs

        @pl.when(lax.axis_index("section") == section)
        def _():
            field_in = field_ref[...]
            wide = field_in.astype(jnp.float32)
            saved_ref[0, crop] = field_in
            hidden = convolved(wide, weights_ref.at[0], taps, shifted, width)
            hidden_ref[crop] = hidden
            active = (hidden * jax.nn.sigmoid(hidden)).astype(jnp.bfloat16)
            saved_ref[1, crop] = active
            if not last:
                added = convolved(
                    active.astype(jnp.float32), weights_ref.at[1], taps, shifted, width
                )
                refs[-5][...] = (wide + added).astype(jnp.bfloat16)

    outs = [
        jax.ShapeDtypeStruct((count, channels), jnp.bfloat16),
        jax.ShapeDtypeStruct((2, crops, count, channels), jnp.bfloat16),
        jax.ShapeDtypeStruct((crops, count, channels), jnp.float32),
    ][1 if last else 0 :]
    scratch = [
        pltpu.VMEM((count + 2 * width, 3 * channels), jnp.bfloat16),
        pltpu.VMEM((count + 16, channels), jnp.float32),
    ]
    aliases = {3 + k: k + (0 if last else 1) for k in range(len(state))}
    outputs = call(kernel, outs, [field, weights, after, *state], (2,), scratch, aliases)
    return (None if last else outputs[0]), outputs[-2:]


def backward_call(
    grad, turned, hidden, state, section, crop, crops, width, parts, after
):
    count, channels = grad.shape
    share = channels // parts
    first = section == 0

    def kernel(grad_ref, turned_ref, hidden_ref, after_ref, *refs):
        *_, kept_ref, sent_ref, taps, shifted = refs

        @pl.when(lax.axis_index("section") == section)
        def _():
            wide = grad_ref[...].astype(jnp.float32)
            own = lax.axis_index("img")
            place_parts(sent_ref, (0,), grad_ref[...], crop, parts, own)
            grad_active = convolved(wide, turned_ref.at[1], taps, shifted, width)
            hidden = hidden_ref[crop]
            gate = jax.nn.sigmoid(hidden)
            grad_hidden = (grad_active * (gate * (1.0 + hidden * (1.0 - gate)))).astype(
                jnp.bfloat16
            )
            place_parts(sent_ref, (1,), grad_hidden, crop, parts, own)
            added = convolved(
                grad_hidden.astype(jnp.float32), turned_ref.at[0], taps, shifted, width
            )
            result = (wide + added).astype(jnp.bfloat16)
            kept_ref[crop] = result
            if not first:
                refs[-5][...] = result

    outs = [
        jax.ShapeDtypeStruct((count, channels), jnp.bfloat16),
        jax.ShapeDtypeStruct((crops, count, channels), jnp.bfloat16),
        jax.ShapeDtypeStruct((parts, 2, share, crops * count), jnp.bfloat16),
    ][1 if first else 0 :]
    scratch = [
        pltpu.VMEM((count + 2 * width, 3 * channels), jnp.bfloat16),
        pltpu.VMEM((count + 16, channels), jnp.float32),
    ]
    aliases = {4 + k: k + (0 if first else 1) for k in range(len(state))}
    operands = [grad, turned, hidden, after, *state]
    outputs = call(kernel, outs, operands, (3,), scratch, aliases)
    return (None if first else outputs[0]), outputs[-2:]


def place_parts(target, lead, value, crop, parts, own):
    count, channels = value.shape
    share = channels // parts
    flipped = value.T
    for part in range(parts):
        slot = lax.rem(part + parts - own, parts)
        target[(slot, *lead, slice(None), slice(crop * count, (crop + 1) * count))] = flipped[
            part * share : (part + 1) * share, :
        ]


def flip_call(kept, parts, axis, after):
    def kernel(*refs):
        flipped_ref = refs[-1]
        for crop, (place, index) in enumerate(kept):
            value = refs[place][index]
            place_parts(flipped_ref, (), value, crop, parts, lax.axis_index(axis))

    operands = []
    for array, index in kept:
        if all(array is not other for other in operands):
            operands.append(array)
    kept = [
        ([array is other for other in operands].index(True), index) for array, index in kept
    ]
    count, channels = operands[0].shape[-2:]
    out = jax.ShapeDtypeStruct((parts, channels // parts, len(kept) * count), operands[0].dtype)
    (flipped,) = call(kernel, [out], [*operands, after], (len(operands),), [], {})
    return flipped


def turn_call(weights, after):
    two, _, _, channels = weights.shape

    def kernel(weights_ref, after_ref, turned_ref):
        for which in range(two):
            for tap in range(9):
                down, right = divmod(tap, 3)
                flipped = weights_ref[which, down, right * channels : (right + 1) * channels, :].T
                down, right = divmod(8 - tap, 3)
                turned_ref[which, down, right * channels : (right + 1) * channels, :] = flipped

    out = jax.ShapeDtypeStruct(weights.shape, weights.dtype)
    (turned,) = call(kernel, [out], [weights, after], (1,), [], {})
    return turned


def split_call(strips, cotangent, last):
    images, strip_count, rows, cols, channels = strips.shape
    share = strip_count // 2

    def kernel(strips_ref, cotangent_ref, own_ref, other_ref, sems):
        own = lax.axis_index("slab")
        is_last = lax.axis_index("section") == last

        def fetch(source_ref):
            copies = []
            for image in range(images):
                at = pl.ds(image * share, share)
                for side, (ref, half) in enumerate(((own_ref, own), (other_ref, 1 - own))):
                    source = source_ref.at[image, pl.ds(half * share, share)]
                    copies.append(pltpu.make_async_copy(source, ref.at[at], sems.at[2 * image + side]))
            for copy in copies:
                copy.start()
            for copy in copies:
                copy.wait()

        @pl.when(is_last)
        def _():
            fetch(cotangent_ref)

        @pl.when(jnp.logical_not(is_last))
        def _():
            fetch(strips_ref)

    out = jax.ShapeDtypeStruct((images * share, rows, cols, channels), strips.dtype)
    sems = [pltpu.SemaphoreType.DMA((2 * images,))]
    return call(kernel, [out, out], [strips, cotangent], (), sems, {}, (0, 1))


def load_call(weights):
    def kernel(weights_ref, out_ref, sems):
        copies = [
            pltpu.make_async_copy(weights_ref.at[which], out_ref.at[which], sems.at[which])
            for which in range(2)
        ]
        for copy in copies:
            copy.start()
        for copy in copies:
            copy.wait()

    out = jax.ShapeDtypeStruct(weights.shape, weights.dtype)
    sems = [pltpu.SemaphoreType.DMA((2,))]
    (loaded,) = call(kernel, [out], [weights], (), sems, {}, (0,))
    return loaded


def join_call(own, other):
    crops, rows, cols, channels = own.shape

    def kernel(own_ref, other_ref, *out_refs):
        is_left = lax.axis_index("slab") == 0
        for crop, out_ref in enumerate(out_refs):
            mine = own_ref[crop].astype(jnp.float32)
            theirs = other_ref[crop].astype(jnp.float32)
            left = jnp.where(is_left, mine, theirs)
            right = jnp.where(is_left, theirs, mine)
            whole = jnp.concatenate([left, right], axis=1)
            out_ref[...] = whole.reshape(rows * 2 * cols, channels).astype(jnp.bfloat16)

    out = jax.ShapeDtypeStruct((rows * 2 * cols, channels), own.dtype)
    return call(kernel, [out] * crops, [own, other], (), [], {})


def part_call(kept, rows, after):
    crops, count, channels = kept.shape
    cols = count // rows // 2

    def kernel(kept_ref, after_ref, own_ref, other_ref):
        is_left = lax.axis_index("slab") == 0
        for crop in range(crops):
            whole = kept_ref[crop].astype(jnp.float32).reshape(rows, 2 * cols, channels)
            left, right = whole[:, :cols], whole[:, cols:]
            own_ref[crop] = jnp.where(is_left, left, right).astype(jnp.bfloat16)
            other_ref[crop] = jnp.where(is_left, right, left).astype(jnp.bfloat16)

    out = jax.ShapeDtypeStruct((crops, rows, cols, channels), kept.dtype)
    return call(kernel, [out, out], [kept, after], (1,), [], {})


def merge_call(own, other, images):
    crops, rows, cols, channels = own.shape
    share = crops // images

    def kernel(own_ref, other_ref, out_ref):
        place = lax.axis_index("slab")
        for image in range(images):
            for crop in range(share):
                out_ref[image, place * share + crop] = own_ref[image * share + crop]
                out_ref[image, (1 - place) * share + crop] = other_ref[image * share + crop]

    out = jax.ShapeDtypeStruct((images, 2 * share, rows, cols, channels), own.dtype)
    (merged,) = call(kernel, [out], [own, other], (), [], {})
    return merged


def stack_call(blocks, slot, after):
    def kernel(*refs):
        for place in range(len(blocks)):
            refs[-1][place] = refs[place][...] if slot is None else refs[place][slot]

    shape = blocks[0].shape if slot is None else blocks[0].shape[1:]
    out = jax.ShapeDtypeStruct((len(blocks), *shape), blocks[0].dtype)
    (stacked,) = call(kernel, [out], [*blocks, after], (len(blocks),), [], {})
    return stacked


def pick_call(home, received, sections, after):
    slots = home.shape[0]
    arrays = [array for section in range(sections) for array in received[section]]
    each = len(arrays) // sections

    def kernel(home_ref, *refs):
        for slot in range(slots):
            refs[-slots + slot][0] = home_ref[slot]
        for section in range(sections):

            @pl.when(lax.axis_index("section") == section)
            def _():
                for block in range(each):
                    for slot in range(slots):
                        refs[-slots + slot][1 + block] = refs[section * each + block][slot]

    out = jax.ShapeDtypeStruct((1 + each, *home.shape[1:]), home.dtype)
    operands = [home, *arrays, after]
    return call(kernel, [out] * slots, operands, (len(operands) - 1,), [], {})


def spread_call(sources, slots, blocks, kind, around, sections, count, width):
    share, cells = sources[0].shape[-2:]
    crops = cells // count
    stride = count + width
    fresh = isinstance(around, jax.ShapeDtypeStruct)
    total = around.shape[1]

    def kernel(*refs):
        out_ref, shifted = refs[-2:]
        section = lax.axis_index("section")

        @pl.when((section >= sections[0]) & (section <= sections[1]))
        def _():
            edge = jnp.zeros((width, 3 * share), jnp.bfloat16)
            out_ref[kind, total - width : total, :] = edge
            for ref, slot, block in zip(refs, slots, blocks):
                for crop in range(crops):
                    cell = slice(crop * count, (crop + 1) * count)
                    value = ref[(*slot, slice(None), cell)].T.astype(jnp.float32)
                    before, after = neighbours(value, shifted, width)
                    at = (block * crops + crop) * stride
                    out_ref[kind, at : at + width, :] = edge
                    for place, part in enumerate((before, value, after)):
                        lanes = slice(place * share, (place + 1) * share)
                        out_ref[kind, at + width : at + stride, lanes] = part.astype(jnp.bfloat16)

    operands = [*sources] if fresh else [*sources, around]
    aliases = {} if fresh else {len(sources): 0}
    out = jax.ShapeDtypeStruct(around.shape, around.dtype)
    scratch = [pltpu.VMEM((count + 16, share), jnp.float32)]
    (spread,) = call(kernel, [out], operands, (), scratch, aliases)
    return spread


def terms_call(around, own, other, count, width, scaling):
    blocks, _, columns, cells = own.shape
    rows = around.shape[2] // 3
    stride = count + width
    crops = cells // count

    def kernel(around_ref, own_ref, other_ref, out_ref):
        for kind in range(2):
            for down in range(3):
                total = None
                for block in range(2 * blocks):
                    left = own_ref if block < blocks else other_ref
                    left = left[block % blocks, 1 - kind]
                    at = [(block * crops + k) * stride + down * width for k in range(crops)]
                    right = jnp.concatenate(
                        [around_ref[kind, start : start + count, :] for start in at], axis=0
                    )
                    term = jnp.dot(left, right, preferred_element_type=jnp.float32)
                    total = term if total is None else total + term
                total = (total * scaling).T.reshape(3, rows, columns)
                for place in range(3):
                    out_ref[kind, 3 * down + place] = total[place]

    out = jax.ShapeDtypeStruct((2, 9, rows, columns), jnp.float32)
    (terms,) = call(kernel, [out], [around, own, other], (), [], {})
    return terms


def rotated(value, axis, steps):
    count = lax.axis_size(axis)
    return lax.ppermute(value, axis, [(source, (source + steps) % count) for source in range(count)])


def crop_shards(strips, kernels, cotangent):
    sections = lax.axis_size("section")
    slabs, groups = lax.axis_size("slab"), lax.axis_size("img")
    images, strip_count, row_count, col_count, channels = strips.shape
    width = col_count * slabs
    count = row_count * width
    crops = images * strip_count // slabs
    last = sections - 1
    scaling = 1.0 / math.sqrt(images * groups * strip_count * count)

    def hop(value, source, target):
        return lax.ppermute(value, "section", [(source, target)])

    def shared(values, step, routes):
        pairs = [
            (source * groups + i, target * groups + (i + step) % groups)
            for source, target in routes
            for i in range(groups)
        ]
        return lax.ppermute(values, ("section", "img"), pairs)

    steps = range(1, groups)
    everywhere = [(place, place) for place in range(sections)]
    soon, late_from = everywhere[: max(1, sections - 2)], max(1, sections - 2)
    own, other = split_call(
        pltpu.with_memory_space_constraint(strips, pltpu.HBM),
        pltpu.with_memory_space_constraint(cotangent, pltpu.HBM),
        last,
    )
    other = rotated(other, "slab", 1)
    weights = kernels[0].reshape(2, 3, 3 * channels, channels)
    weights = load_call(pltpu.with_memory_space_constraint(weights, pltpu.HBM))
    fields = join_call(own, other)
    incoming = fields
    state, handed = [], {}
    turned, after = None, weights
    for place in range(sections):
        outgoing = []
        for crop in range(crops):
            out, state = forward_call(
                incoming[crop], weights, state, place, crop, crops, width, place == last, after
            )
            outgoing.append(out)
        if place == 0:
            turned = turn_call(weights, state[0])
        if place < last:
            incoming = [hop(out, place, place + 1) for out in outgoing]
        if 0 < place < last:
            flipped = flip_call([(out, Ellipsis) for out in outgoing], slabs, "slab", state[1])
            handed[place + 1] = [shared(flipped, step, [(place, place + 1)]) for step in steps]
            after = flipped
        if place == 0:
            flipped_outgoing = outgoing
        if place == min(1, last - 1):
            flipped = flip_call([(field, Ellipsis) for field in fields], slabs, "slab", state[1])
            handed[0] = [shared(flipped, step, [(0, 0)]) for step in steps]
    saved, hidden = state
    incoming = fields
    grads = []
    around, after = None, hidden
    late = []
    for place in reversed(range(sections)):
        outgoing = []
        for crop in range(crops):
            out, grads = backward_call(
                incoming[crop], turned, hidden, grads, place, crop, crops, width, groups, after
            )
            outgoing.append(out)
        if place:
            incoming = [hop(out, place, place - 1) for out in outgoing]
        if place == min(last, 2):
            active = flip_call([(saved, (1, crop)) for crop in range(crops)], slabs, "slab", grads[0])
            pairs = [
                (source * slabs + i, source * slabs + (i + 1) % slabs)
                for source in range(late_from, sections)
                for i in range(slabs)
            ]
            other = lax.ppermute(active[1], ("section", "slab"), pairs)
            both = stack_call([active[0], other], None, grads[0])
            late = [both]
            for step in steps:
                late.append(shared(both, step, everywhere[late_from:]))
            flipped = flip_call([(out, Ellipsis) for out in flipped_outgoing], slabs, "slab", both)
            handed[1] = [shared(flipped, step, [(0, 1)]) for step in steps]
            early = [shared(active, step, soon) for step in steps]
        if place == 1:
            mine = flip_call([(saved, (0, crop)) for crop in range(crops)], slabs, "slab", outgoing[-1])
            inputs = pick_call(mine, handed, sections, outgoing[-1])
            active = [active, *early]
            other = stack_call(active, 1, outgoing[-1])
            other = rotated(other, "slab", 1)
            outer = rotated(inputs[1], "slab", 1)
            stride = count + width
            shape = (2, slabs * groups * crops * stride + width, 3 * (channels // slabs))
            slots = [(block,) for block in range(groups)]
            around = spread_call(
                [inputs[0]] * groups + [outer] * groups,
                slots + slots,
                list(range(slabs * groups)),
                0,
                jax.ShapeDtypeStruct(shape, jnp.bfloat16),
                (0, last),
                count,
                width,
            )
            around = spread_call(
                active + [other] * groups,
                [(0,)] * groups + slots,
                list(range(slabs * groups)),
                1,
                around,
                (0, late_from - 1),
                count,
                width,
            )
            after = around
    kept, sent = grads
    own = [sent[0]]
    for step in steps:
        own.append(shared(sent[step], step, everywhere))
    around, sent = lax.optimization_barrier((around, sent))
    for block in range(groups):
        around = spread_call(
            [late[block]] * slabs,
            [(slab,) for slab in range(slabs)],
            [slab * groups + block for slab in range(slabs)],
            1,
            around,
            (late_from, last),
            count,
            width,
        )
    own = stack_call(own, None, around)
    other = rotated(own, "slab", 1)
    terms = terms_call(around, own, other, count, width, scaling)
    own, other = part_call(kept, row_count, sent)
    other = rotated(other, "slab", 1)
    grad_inputs = merge_call(own, other, images)
    return (terms[None], grad_inputs[None])


def shards(strips, kernels, cotangent):
    slabs, groups = lax.axis_size("slab"), lax.axis_size("img")
    strip_count, row_count, col_count, channels = strips.shape[1:]
    width = col_count * slabs
    whole_crops = strip_count % slabs == 0 and width % 16 == 0 and (row_count * width) % 128 == 0
    whole_crops = whole_crops and slabs == 2 and lax.axis_size("section") > 1
    if whole_crops and channels % (16 * slabs) == 0 and channels % (16 * groups) == 0:
        return crop_shards(strips, kernels, cotangent)
    return column_shards(strips, kernels, cotangent)


def solution(mesh):
    in_specs = (
        P("img", None, None, "slab", None),
        P("section", None, None, None, None),
        P("img", None, None, "slab", None),
    )
    out_specs = (
        P("section", None, None, "slab", "img"),
        P("section", "img", None, None, "slab", None),
    )
    return jax.shard_map(shards, mesh=mesh, in_specs=in_specs, out_specs=out_specs, check_vma=False)
```

```python
import math

import jax
import jax.numpy as jnp
from jax import lax
from jax.experimental import pallas as pl
from jax.experimental.pallas import tpu as pltpu
from jax.sharding import PartitionSpec as P


def passed_along(value, axis, steps):
    count = lax.axis_size(axis)
    initial, last = (max(0, -steps), min(count, count - steps))
    return lax.ppermute(value, axis, [(source, source + steps) for source in range(initial, last)])


def padded_2(cells, sides, width):
    for axis, dim in sides:
        count = lax.axis_size(axis)
        ends = count - 1
        head = lax.slice_in_dim(cells, 0, width, axis=dim)
        tail = lax.slice_in_dim(cells, cells.shape[dim] - width, cells.shape[dim], axis=dim)
        cells = jnp.concatenate(
            [
                lax.ppermute(tail, axis, [(i, (i + 1) % count) for i in range(ends)]),
                cells,
                lax.ppermute(head, axis, [((i + 1) % count, i) for i in range(ends)]),
            ],
            axis=dim,
        )
    return cells


def unfold(padded, row_count, col_count):
    tap_list = [
        padded[:, down_at : down_at + row_count, right_at : right_at + col_count, :]
        for down_at in range(3)
        for right_at in range(3)
    ]
    stacked = jnp.concatenate(tap_list, axis=3)
    return stacked.reshape(-1, stacked.shape[3])


def columns_of(wide_field):
    row_count = wide_field.shape[1]
    col_count = wide_field.shape[2] - 2
    padded = jnp.pad(wide_field, ((0, 0), (1, 1), (0, 0), (0, 0)))
    return unfold(padded, row_count, col_count)


def convolve(matrix, wide_field):
    count, row_count = (wide_field.shape[0], wide_field.shape[1])
    col_count = wide_field.shape[2] - 2
    flat_out = jnp.dot(columns_of(wide_field), matrix, preferred_element_type=jnp.float32)
    return flat_out.reshape(count, row_count, col_count, matrix.shape[1])


def contract(wide_field, grad_out):
    flat_grad = grad_out.reshape(-1, grad_out.shape[3])
    return lax.dot_general(
        columns_of(wide_field),
        flat_grad,
        (((0,), (0,)), ((), ())),
        preferred_element_type=jnp.float32,
    )


def silu_slope(hidden):
    sigmoid_at = jax.nn.sigmoid(hidden)
    return sigmoid_at * (1.0 + hidden * (1.0 - sigmoid_at))


def store(buffer, value, slot_index, is_valid, axis_at):
    current = lax.dynamic_index_in_dim(buffer, slot_index, axis_at, keepdims=False)
    return lax.dynamic_update_index_in_dim(
        buffer, jnp.where(is_valid, value, current), slot_index, axis_at
    )


def column_shards(strips, kernels, cotangent):
    section_count = lax.axis_size("section")
    section_index = lax.axis_index("section")
    slab_count = lax.axis_size("slab")
    slab_index = lax.axis_index("slab")
    images, strip_count, row_count, col_count, channels = strips.shape
    weights = kernels[0]
    first_forward = weights[0].reshape(9 * channels, channels)
    second_forward = weights[1].reshape(9 * channels, channels)
    first_backward = jnp.transpose(weights[0][::-1], (0, 2, 1)).reshape(9 * channels, channels)
    second_backward = jnp.transpose(weights[1][::-1], (0, 2, 1)).reshape(9 * channels, channels)
    scaling = 1.0 / math.sqrt(
        images * lax.axis_size("img") * strip_count * row_count * col_count * slab_count
    )
    position = slab_index * col_count - 1 + jnp.arange(col_count + 2, dtype=jnp.int32)
    inside = ((position >= 0) & (position < slab_count * col_count))[None, None, :, None]
    tick_count = strip_count + section_count - 1
    hidden_cols = col_count + 2
    empty_field = jnp.zeros((images, row_count, col_count, channels), jnp.bfloat16)
    saved_field = jnp.zeros((strip_count, images, row_count, col_count + 2, channels), jnp.bfloat16)
    saved_hidden = jnp.zeros((strip_count, images, row_count, hidden_cols, channels), jnp.float32)
    saved_active = jnp.zeros(
        (strip_count, images, row_count, col_count + 2, channels), jnp.bfloat16
    )
    outgoing = empty_field
    for step_no in range(tick_count):
        micro_index = step_no - section_index
        is_valid = (micro_index >= 0) & (micro_index < strip_count)
        slot_index = jnp.clip(micro_index, 0, strip_count - 1)
        if step_no == 0:
            incoming = empty_field
        else:
            incoming = passed_along(outgoing, "section", 1)
        first_strip = lax.dynamic_index_in_dim(strips, slot_index, 1, keepdims=False)
        field_in = jnp.where(section_index == 0, first_strip, incoming)
        wide_deep = padded_2(field_in, (("slab", 2),), 2)
        hidden = convolve(first_forward, wide_deep)
        wide_active = jnp.where(inside, jax.nn.silu(hidden), 0.0).astype(jnp.bfloat16)
        wide_field = wide_deep[:, :, 1:-1, :]
        outgoing = (field_in.astype(jnp.float32) + convolve(second_forward, wide_active)).astype(
            jnp.bfloat16
        )
        saved_field = store(saved_field, wide_field, slot_index, is_valid, 0)
        saved_hidden = store(saved_hidden, hidden, slot_index, is_valid, 0)
        saved_active = store(saved_active, wide_active, slot_index, is_valid, 0)
    grad_slots = jnp.zeros((images, strip_count, row_count, col_count, channels), jnp.bfloat16)
    saved_grad_out = jnp.zeros((strip_count, images, row_count, col_count, channels), jnp.bfloat16)
    saved_grad_hidden = jnp.zeros(
        (strip_count, images, row_count, col_count, channels), jnp.bfloat16
    )
    sending = empty_field
    for step_no in range(tick_count):
        micro_index = step_no - (section_count - 1 - section_index)
        is_valid = (micro_index >= 0) & (micro_index < strip_count)
        slot_index = jnp.clip(micro_index, 0, strip_count - 1)
        if step_no == 0:
            arriving = empty_field
        else:
            arriving = passed_along(sending, "section", -1)
        top_grad = lax.dynamic_index_in_dim(cotangent, slot_index, 1, keepdims=False)
        grad_out = jnp.where(section_index == section_count - 1, top_grad, arriving)
        grad_out = jnp.where(is_valid, grad_out, jnp.zeros_like(grad_out))
        hidden = lax.dynamic_index_in_dim(saved_hidden, slot_index, 0, keepdims=False)
        wide_grad = padded_2(grad_out, (("slab", 2),), 2)
        grad_active = convolve(second_backward, wide_grad)
        wide_hidden_grad = jnp.where(inside, grad_active * silu_slope(hidden), 0.0).astype(
            jnp.bfloat16
        )
        grad_hidden = wide_hidden_grad[:, :, 1:-1, :]
        sending = (
            grad_out.astype(jnp.float32) + convolve(first_backward, wide_hidden_grad)
        ).astype(jnp.bfloat16)
        saved_grad_out = store(saved_grad_out, grad_out, slot_index, is_valid, 0)
        saved_grad_hidden = store(saved_grad_hidden, grad_hidden, slot_index, is_valid, 0)
        grad_slots = store(grad_slots, sending, slot_index, is_valid, 1)
    flat_count = strip_count * images
    lower_part = contract(
        saved_field.reshape(flat_count, row_count, col_count + 2, channels),
        saved_grad_hidden.reshape(flat_count, row_count, col_count, channels),
    )
    upper_part = contract(
        saved_active.reshape(flat_count, row_count, col_count + 2, channels),
        saved_grad_out.reshape(flat_count, row_count, col_count, channels),
    )
    grad_terms = jnp.stack([lower_part, upper_part]).reshape(2, 9, channels, channels)
    row_share = lax.psum_scatter(
        grad_terms.astype(jnp.bfloat16), "slab", scatter_dimension=2, tiled=True
    )
    own_share = lax.psum_scatter(row_share, "img", scatter_dimension=3, tiled=True).astype(
        jnp.float32
    )
    grad_kernels = (own_share * scaling)[None]
    return (grad_kernels, grad_slots[None])


def call(kernel, outs, operands, unread, scratch, aliases, apart=()):
    spaces = {**dict.fromkeys(unread, pl.ANY), **dict.fromkeys(apart, pltpu.HBM)}
    return pl.pallas_call(
        kernel,
        out_shape=outs,
        in_specs=[
            pl.BlockSpec(memory_space=spaces.get(place, pltpu.VMEM))
            for place in range(len(operands))
        ],
        out_specs=[pl.BlockSpec(memory_space=pltpu.VMEM)] * len(outs),
        scratch_shapes=scratch,
        input_output_aliases=aliases,
        compiler_params=pltpu.CompilerParams(vmem_limit_bytes=8 << 20),
    )(*operands)


def neighbours(value, shifted, width):
    count, channels = value.shape
    shifted[8 : 8 + count, :] = value
    column = lax.rem(lax.broadcasted_iota(jnp.int32, (count, channels), 0), width)
    before = jnp.where(column == 0, 0.0, shifted[7 : 7 + count, :])
    after = jnp.where(column == width - 1, 0.0, shifted[9 : 9 + count, :])
    return before, after


def convolved(value, matrix, taps, shifted, width):
    count, channels = value.shape
    before, after = neighbours(value, shifted, width)
    for place, part in enumerate((before, value, after)):
        taps[width : width + count, place * channels : (place + 1) * channels] = part.astype(
            jnp.bfloat16
        )
    edge = jnp.zeros((width, 3 * channels), jnp.bfloat16)
    taps[0:width, :] = edge
    taps[width + count : 2 * width + count, :] = edge
    total = jnp.dot(taps[0:count, :], matrix[0], preferred_element_type=jnp.float32)
    for down in (1, 2):
        total = total + jnp.dot(
            taps[down * width : down * width + count, :],
            matrix[down],
            preferred_element_type=jnp.float32,
        )
    return total


def forward_call(field, weights, state, section, crop, crops, width, last, after):
    count, channels = field.shape

    def kernel(field_ref, weights_ref, after_ref, *refs):
        *_, saved_ref, hidden_ref, taps, shifted = refs

        @pl.when(lax.axis_index("section") == section)
        def _():
            field_in = field_ref[...]
            wide = field_in.astype(jnp.float32)
            saved_ref[0, crop] = field_in
            hidden = convolved(wide, weights_ref.at[0], taps, shifted, width)
            hidden_ref[crop] = hidden
            active = (hidden * jax.nn.sigmoid(hidden)).astype(jnp.bfloat16)
            saved_ref[1, crop] = active
            if not last:
                added = convolved(
                    active.astype(jnp.float32), weights_ref.at[1], taps, shifted, width
                )
                refs[-5][...] = (wide + added).astype(jnp.bfloat16)

    outs = [
        jax.ShapeDtypeStruct((count, channels), jnp.bfloat16),
        jax.ShapeDtypeStruct((2, crops, count, channels), jnp.bfloat16),
        jax.ShapeDtypeStruct((crops, count, channels), jnp.float32),
    ][1 if last else 0 :]
    scratch = [
        pltpu.VMEM((count + 2 * width, 3 * channels), jnp.bfloat16),
        pltpu.VMEM((count + 16, channels), jnp.float32),
    ]
    aliases = {3 + k: k + (0 if last else 1) for k in range(len(state))}
    outputs = call(kernel, outs, [field, weights, after, *state], (2,), scratch, aliases)
    return (None if last else outputs[0]), outputs[-2:]


def backward_call(
    grad, turned, hidden, state, section, crop, crops, width, parts, after
):
    count, channels = grad.shape
    share = channels // parts
    first = section == 0

    def kernel(grad_ref, turned_ref, hidden_ref, after_ref, *refs):
        *_, kept_ref, sent_ref, taps, shifted = refs

        @pl.when(lax.axis_index("section") == section)
        def _():
            wide = grad_ref[...].astype(jnp.float32)
            own = lax.axis_index("img")
            place_parts(sent_ref, (0,), grad_ref[...], crop, parts, own)
            grad_active = convolved(wide, turned_ref.at[1], taps, shifted, width)
            hidden = hidden_ref[crop]
            gate = jax.nn.sigmoid(hidden)
            grad_hidden = (grad_active * (gate * (1.0 + hidden * (1.0 - gate)))).astype(
                jnp.bfloat16
            )
            place_parts(sent_ref, (1,), grad_hidden, crop, parts, own)
            added = convolved(
                grad_hidden.astype(jnp.float32), turned_ref.at[0], taps, shifted, width
            )
            result = (wide + added).astype(jnp.bfloat16)
            kept_ref[crop] = result
            if not first:
                refs[-5][...] = result

    outs = [
        jax.ShapeDtypeStruct((count, channels), jnp.bfloat16),
        jax.ShapeDtypeStruct((crops, count, channels), jnp.bfloat16),
        jax.ShapeDtypeStruct((parts, 2, share, crops * count), jnp.bfloat16),
    ][1 if first else 0 :]
    scratch = [
        pltpu.VMEM((count + 2 * width, 3 * channels), jnp.bfloat16),
        pltpu.VMEM((count + 16, channels), jnp.float32),
    ]
    aliases = {4 + k: k + (0 if first else 1) for k in range(len(state))}
    operands = [grad, turned, hidden, after, *state]
    outputs = call(kernel, outs, operands, (3,), scratch, aliases)
    return (None if first else outputs[0]), outputs[-2:]


def place_parts(target, lead, value, crop, parts, own):
    count, channels = value.shape
    share = channels // parts
    flipped = value.T
    for part in range(parts):
        slot = lax.rem(part + parts - own, parts)
        target[(slot, *lead, slice(None), slice(crop * count, (crop + 1) * count))] = flipped[
            part * share : (part + 1) * share, :
        ]


def flip_call(kept, parts, axis, after):
    def kernel(*refs):
        flipped_ref = refs[-1]
        for crop, (place, index) in enumerate(kept):
            value = refs[place][index]
            place_parts(flipped_ref, (), value, crop, parts, lax.axis_index(axis))

    operands = []
    for array, index in kept:
        if all(array is not other for other in operands):
            operands.append(array)
    kept = [
        ([array is other for other in operands].index(True), index) for array, index in kept
    ]
    count, channels = operands[0].shape[-2:]
    out = jax.ShapeDtypeStruct((parts, channels // parts, len(kept) * count), operands[0].dtype)
    (flipped,) = call(kernel, [out], [*operands, after], (len(operands),), [], {})
    return flipped


def turn_call(weights, after):
    two, _, _, channels = weights.shape

    def kernel(weights_ref, after_ref, turned_ref):
        for which in range(two):
            for tap in range(9):
                down, right = divmod(tap, 3)
                flipped = weights_ref[which, down, right * channels : (right + 1) * channels, :].T
                down, right = divmod(8 - tap, 3)
                turned_ref[which, down, right * channels : (right + 1) * channels, :] = flipped

    out = jax.ShapeDtypeStruct(weights.shape, weights.dtype)
    (turned,) = call(kernel, [out], [weights, after], (1,), [], {})
    return turned


def split_call(strips, cotangent, last):
    images, strip_count, rows, cols, channels = strips.shape
    share = strip_count // 2

    def kernel(strips_ref, cotangent_ref, own_ref, other_ref, sems):
        own = lax.axis_index("slab")
        is_last = lax.axis_index("section") == last

        def fetch(source_ref):
            copies = []
            for image in range(images):
                at = pl.ds(image * share, share)
                for side, (ref, half) in enumerate(((own_ref, own), (other_ref, 1 - own))):
                    source = source_ref.at[image, pl.ds(half * share, share)]
                    copies.append(pltpu.make_async_copy(source, ref.at[at], sems.at[2 * image + side]))
            for copy in copies:
                copy.start()
            for copy in copies:
                copy.wait()

        @pl.when(is_last)
        def _():
            fetch(cotangent_ref)

        @pl.when(jnp.logical_not(is_last))
        def _():
            fetch(strips_ref)

    out = jax.ShapeDtypeStruct((images * share, rows, cols, channels), strips.dtype)
    sems = [pltpu.SemaphoreType.DMA((2 * images,))]
    return call(kernel, [out, out], [strips, cotangent], (), sems, {}, (0, 1))


def load_call(weights):
    def kernel(weights_ref, out_ref, sems):
        copies = [
            pltpu.make_async_copy(weights_ref.at[which], out_ref.at[which], sems.at[which])
            for which in range(2)
        ]
        for copy in copies:
            copy.start()
        for copy in copies:
            copy.wait()

    out = jax.ShapeDtypeStruct(weights.shape, weights.dtype)
    sems = [pltpu.SemaphoreType.DMA((2,))]
    (loaded,) = call(kernel, [out], [weights], (), sems, {}, (0,))
    return loaded


def join_call(own, other):
    crops, rows, cols, channels = own.shape

    def kernel(own_ref, other_ref, *out_refs):
        is_left = lax.axis_index("slab") == 0
        for crop, out_ref in enumerate(out_refs):
            mine = own_ref[crop].astype(jnp.float32)
            theirs = other_ref[crop].astype(jnp.float32)
            left = jnp.where(is_left, mine, theirs)
            right = jnp.where(is_left, theirs, mine)
            whole = jnp.concatenate([left, right], axis=1)
            out_ref[...] = whole.reshape(rows * 2 * cols, channels).astype(jnp.bfloat16)

    out = jax.ShapeDtypeStruct((rows * 2 * cols, channels), own.dtype)
    return call(kernel, [out] * crops, [own, other], (), [], {})


def part_call(kept, rows, after):
    crops, count, channels = kept.shape
    cols = count // rows // 2

    def kernel(kept_ref, after_ref, own_ref, other_ref):
        is_left = lax.axis_index("slab") == 0
        for crop in range(crops):
            whole = kept_ref[crop].astype(jnp.float32).reshape(rows, 2 * cols, channels)
            left, right = whole[:, :cols], whole[:, cols:]
            own_ref[crop] = jnp.where(is_left, left, right).astype(jnp.bfloat16)
            other_ref[crop] = jnp.where(is_left, right, left).astype(jnp.bfloat16)

    out = jax.ShapeDtypeStruct((crops, rows, cols, channels), kept.dtype)
    return call(kernel, [out, out], [kept, after], (1,), [], {})


def merge_call(own, other, images):
    crops, rows, cols, channels = own.shape
    share = crops // images

    def kernel(own_ref, other_ref, out_ref):
        place = lax.axis_index("slab")
        for image in range(images):
            for crop in range(share):
                out_ref[image, place * share + crop] = own_ref[image * share + crop]
                out_ref[image, (1 - place) * share + crop] = other_ref[image * share + crop]

    out = jax.ShapeDtypeStruct((images, 2 * share, rows, cols, channels), own.dtype)
    (merged,) = call(kernel, [out], [own, other], (), [], {})
    return merged


def stack_call(blocks):
    def kernel(*refs):
        for place in range(len(blocks)):
            refs[-1][place] = refs[place][...]

    out = jax.ShapeDtypeStruct((len(blocks), *blocks[0].shape), blocks[0].dtype)
    (stacked,) = call(kernel, [out], [*blocks], (), [], {})
    return stacked


def remake_call(saved, weights, received, width):
    _, crops, count, channels = saved.shape
    share = channels // 2
    sections, each = len(received), len(received[0])

    def kernel(saved_ref, weights_ref, *refs):
        home_ref, outer_ref, taps, shifted = refs[-4:]
        is_left = lax.axis_index("slab") == 0

        def put(kind, block, crop, value):
            cells = slice(crop * count, (crop + 1) * count)
            flipped = value.T
            low, high = flipped[:share], flipped[share:]
            home_ref[kind, block, :, cells] = jnp.where(is_left, low, high)
            outer_ref[kind, block, :, cells] = jnp.where(is_left, high, low)

        for crop in range(crops):
            for kind in range(2):
                put(kind, 0, crop, saved_ref[kind, crop])
        for section in range(sections):

            @pl.when(lax.axis_index("section") == section)
            def _():
                for block in range(each):
                    home_ref[0, 1 + block] = refs[section * each + block][0]
                    outer_ref[0, 1 + block] = refs[section * each + block][1]

        for block in range(1, 1 + each):
            for crop in range(crops):
                cells = slice(crop * count, (crop + 1) * count)
                mine, theirs = home_ref[0, block, :, cells], outer_ref[0, block, :, cells]
                low, high = jnp.where(is_left, mine, theirs), jnp.where(is_left, theirs, mine)
                field = jnp.concatenate([low, high], axis=0).T.astype(jnp.float32)
                hidden = convolved(field, weights_ref.at[0], taps, shifted, width)
                put(1, block, crop, (hidden * jax.nn.sigmoid(hidden)).astype(jnp.bfloat16))

    out = jax.ShapeDtypeStruct((2, 1 + each, share, crops * count), saved.dtype)
    scratch = [
        pltpu.VMEM((count + 2 * width, 3 * channels), jnp.bfloat16),
        pltpu.VMEM((count + 16, channels), jnp.float32),
    ]
    operands = [saved, weights, *[array for arrays in received for array in arrays]]
    return call(kernel, [out, out], operands, (), scratch, {})


def spread_call(own, other, count, width, after):
    two, blocks, share, cells = own.shape
    crops = cells // count
    stride = count + width
    total = 2 * blocks * crops * stride + width

    def kernel(own_ref, other_ref, after_ref, out_ref, shifted):
        edge = jnp.zeros((width, 3 * share), jnp.bfloat16)
        for kind in range(two):
            out_ref[kind, total - width : total, :] = edge
            for block in range(2 * blocks):
                ref = own_ref if block < blocks else other_ref
                for crop in range(crops):
                    cell = slice(crop * count, (crop + 1) * count)
                    value = ref[kind, block % blocks, :, cell].T.astype(jnp.float32)
                    before, after = neighbours(value, shifted, width)
                    at = (block * crops + crop) * stride
                    out_ref[kind, at : at + width, :] = edge
                    for place, part in enumerate((before, value, after)):
                        lanes = slice(place * share, (place + 1) * share)
                        out_ref[kind, at + width : at + stride, lanes] = part.astype(jnp.bfloat16)

    out = jax.ShapeDtypeStruct((two, total, 3 * share), jnp.bfloat16)
    scratch = [pltpu.VMEM((count + 16, share), jnp.float32)]
    (spread,) = call(kernel, [out], [own, other, after], (2,), scratch, {})
    return spread


def terms_call(around, own, other, count, width, scaling):
    blocks, _, columns, cells = own.shape
    rows = around.shape[2] // 3
    stride = count + width
    crops = cells // count

    def kernel(around_ref, own_ref, other_ref, out_ref):
        for kind in range(2):
            for down in range(3):
                total = None
                for block in range(2 * blocks):
                    left = own_ref if block < blocks else other_ref
                    left = left[block % blocks, 1 - kind]
                    at = [(block * crops + k) * stride + down * width for k in range(crops)]
                    right = jnp.concatenate(
                        [around_ref[kind, start : start + count, :] for start in at], axis=0
                    )
                    term = jnp.dot(left, right, preferred_element_type=jnp.float32)
                    total = term if total is None else total + term
                total = (total * scaling).T.reshape(3, rows, columns)
                for place in range(3):
                    out_ref[kind, 3 * down + place] = total[place]

    out = jax.ShapeDtypeStruct((2, 9, rows, columns), jnp.float32)
    (terms,) = call(kernel, [out], [around, own, other], (), [], {})
    return terms


def rotated(value, axis, steps):
    count = lax.axis_size(axis)
    return lax.ppermute(value, axis, [(source, (source + steps) % count) for source in range(count)])


def crop_shards(strips, kernels, cotangent):
    sections = lax.axis_size("section")
    slabs, groups = lax.axis_size("slab"), lax.axis_size("img")
    images, strip_count, row_count, col_count, channels = strips.shape
    width = col_count * slabs
    count = row_count * width
    crops = images * strip_count // slabs
    last = sections - 1
    early, middle = min(1, last - 1), min(2, last)
    steps = range(1, groups)
    scaling = 1.0 / math.sqrt(images * groups * strip_count * count)

    def hop(values, source, target):
        arrived = []
        for value in values:
            arrived.append(lax.ppermute(value, "section", [(source, target)]))
        return arrived

    def shared(values, step, routes):
        pairs = [
            (source * groups + i, target * groups + (i + step) % groups)
            for source, target in routes
            for i in range(groups)
        ]
        return lax.ppermute(values, ("section", "img"), pairs)

    def swapped(value):
        return rotated(value, "slab", 1)

    def flipped(values):
        return flip_call([(value, Ellipsis) for value in values], slabs, "slab", values[-1])

    own, other = split_call(
        pltpu.with_memory_space_constraint(strips, pltpu.HBM),
        pltpu.with_memory_space_constraint(cotangent, pltpu.HBM),
        last,
    )
    other = swapped(other)
    weights = kernels[0].reshape(2, 3, 3 * channels, channels)
    weights = load_call(pltpu.with_memory_space_constraint(weights, pltpu.HBM))
    fields = join_call(own, other)
    incoming = fields
    state, received = [], [None] * sections
    turned, after = None, weights
    for place in range(sections):
        outgoing = []
        for crop in range(crops):
            out, state = forward_call(
                incoming[crop], weights, state, place, crop, crops, width, place == last, after
            )
            outgoing.append(out)
        if place < last:
            incoming = hop(outgoing, place, place + 1)
            handed = flipped(outgoing)
            routes = [(place, place + 1)]
            received[place + 1] = [shared(handed, step, routes) for step in steps]
        if place == early:
            handed = flipped(fields)
            received[0] = [shared(handed, step, [(0, 0)]) for step in steps]
            turned = turn_call(weights, state[0])
            after = turned
    saved, hidden = state
    incoming = fields
    grads = []
    around, after = None, hidden
    for place in reversed(range(sections)):
        outgoing = []
        for crop in range(crops):
            out, grads = backward_call(
                incoming[crop], turned, hidden, grads, place, crop, crops, width, groups, after
            )
            outgoing.append(out)
        if place:
            incoming = hop(outgoing, place, place - 1)
        if place == middle:
            home, outer = remake_call(saved, weights, received, width)
            after = home
            outer = swapped(outer)
        if place == 1:
            around = spread_call(home, outer, count, width, outgoing[-1])
            after = around
    kept, sent = grads
    own = [sent[0]]
    everywhere = [(place, place) for place in range(sections)]
    for step in steps:
        own.append(shared(sent[step], step, everywhere))
    own = stack_call(own)
    other = swapped(own)
    terms = terms_call(around, own, other, count, width, scaling)
    own, other = part_call(kept, row_count, sent)
    other = swapped(other)
    grad_inputs = merge_call(own, other, images)
    return (terms[None], grad_inputs[None])


def shards(strips, kernels, cotangent):
    slabs, groups = lax.axis_size("slab"), lax.axis_size("img")
    strip_count, row_count, col_count, channels = strips.shape[1:]
    width = col_count * slabs
    whole_crops = strip_count % slabs == 0 and width % 16 == 0 and (row_count * width) % 128 == 0
    whole_crops = whole_crops and slabs == 2 and lax.axis_size("section") > 1
    if whole_crops and channels % (16 * slabs) == 0 and channels % (16 * groups) == 0:
        return crop_shards(strips, kernels, cotangent)
    return column_shards(strips, kernels, cotangent)


def solution(mesh):
    in_specs = (
        P("img", None, None, "slab", None),
        P("section", None, None, None, None),
        P("img", None, None, "slab", None),
    )
    out_specs = (
        P("section", None, None, "slab", "img"),
        P("section", "img", None, None, "slab", None),
    )
    return jax.shard_map(shards, mesh=mesh, in_specs=in_specs, out_specs=out_specs, check_vma=False)
```

```python
import math

import jax
import jax.numpy as jnp
from jax import lax
from jax.experimental import pallas as pl
from jax.experimental.pallas import tpu as pltpu
from jax.sharding import PartitionSpec as P


def passed_along(value, axis, steps):
    count = lax.axis_size(axis)
    initial, last = (max(0, -steps), min(count, count - steps))
    return lax.ppermute(value, axis, [(source, source + steps) for source in range(initial, last)])


def padded_2(cells, sides, width):
    for axis, dim in sides:
        count = lax.axis_size(axis)
        ends = count - 1
        head = lax.slice_in_dim(cells, 0, width, axis=dim)
        tail = lax.slice_in_dim(cells, cells.shape[dim] - width, cells.shape[dim], axis=dim)
        cells = jnp.concatenate(
            [
                lax.ppermute(tail, axis, [(i, (i + 1) % count) for i in range(ends)]),
                cells,
                lax.ppermute(head, axis, [((i + 1) % count, i) for i in range(ends)]),
            ],
            axis=dim,
        )
    return cells


def unfold(padded, row_count, col_count):
    tap_list = [
        padded[:, down_at : down_at + row_count, right_at : right_at + col_count, :]
        for down_at in range(3)
        for right_at in range(3)
    ]
    stacked = jnp.concatenate(tap_list, axis=3)
    return stacked.reshape(-1, stacked.shape[3])


def columns_of(wide_field):
    row_count = wide_field.shape[1]
    col_count = wide_field.shape[2] - 2
    padded = jnp.pad(wide_field, ((0, 0), (1, 1), (0, 0), (0, 0)))
    return unfold(padded, row_count, col_count)


def convolve(matrix, wide_field):
    count, row_count = (wide_field.shape[0], wide_field.shape[1])
    col_count = wide_field.shape[2] - 2
    flat_out = jnp.dot(columns_of(wide_field), matrix, preferred_element_type=jnp.float32)
    return flat_out.reshape(count, row_count, col_count, matrix.shape[1])


def contract(wide_field, grad_out):
    flat_grad = grad_out.reshape(-1, grad_out.shape[3])
    return lax.dot_general(
        columns_of(wide_field),
        flat_grad,
        (((0,), (0,)), ((), ())),
        preferred_element_type=jnp.float32,
    )


def silu_slope(hidden):
    sigmoid_at = jax.nn.sigmoid(hidden)
    return sigmoid_at * (1.0 + hidden * (1.0 - sigmoid_at))


def store(buffer, value, slot_index, is_valid, axis_at):
    current = lax.dynamic_index_in_dim(buffer, slot_index, axis_at, keepdims=False)
    return lax.dynamic_update_index_in_dim(
        buffer, jnp.where(is_valid, value, current), slot_index, axis_at
    )


def column_shards(strips, kernels, cotangent):
    section_count = lax.axis_size("section")
    section_index = lax.axis_index("section")
    slab_count = lax.axis_size("slab")
    slab_index = lax.axis_index("slab")
    images, strip_count, row_count, col_count, channels = strips.shape
    weights = kernels[0]
    first_forward = weights[0].reshape(9 * channels, channels)
    second_forward = weights[1].reshape(9 * channels, channels)
    first_backward = jnp.transpose(weights[0][::-1], (0, 2, 1)).reshape(9 * channels, channels)
    second_backward = jnp.transpose(weights[1][::-1], (0, 2, 1)).reshape(9 * channels, channels)
    scaling = 1.0 / math.sqrt(
        images * lax.axis_size("img") * strip_count * row_count * col_count * slab_count
    )
    position = slab_index * col_count - 1 + jnp.arange(col_count + 2, dtype=jnp.int32)
    inside = ((position >= 0) & (position < slab_count * col_count))[None, None, :, None]
    tick_count = strip_count + section_count - 1
    hidden_cols = col_count + 2
    empty_field = jnp.zeros((images, row_count, col_count, channels), jnp.bfloat16)
    saved_field = jnp.zeros((strip_count, images, row_count, col_count + 2, channels), jnp.bfloat16)
    saved_hidden = jnp.zeros((strip_count, images, row_count, hidden_cols, channels), jnp.float32)
    saved_active = jnp.zeros(
        (strip_count, images, row_count, col_count + 2, channels), jnp.bfloat16
    )
    outgoing = empty_field
    for step_no in range(tick_count):
        micro_index = step_no - section_index
        is_valid = (micro_index >= 0) & (micro_index < strip_count)
        slot_index = jnp.clip(micro_index, 0, strip_count - 1)
        if step_no == 0:
            incoming = empty_field
        else:
            incoming = passed_along(outgoing, "section", 1)
        first_strip = lax.dynamic_index_in_dim(strips, slot_index, 1, keepdims=False)
        field_in = jnp.where(section_index == 0, first_strip, incoming)
        wide_deep = padded_2(field_in, (("slab", 2),), 2)
        hidden = convolve(first_forward, wide_deep)
        wide_active = jnp.where(inside, jax.nn.silu(hidden), 0.0).astype(jnp.bfloat16)
        wide_field = wide_deep[:, :, 1:-1, :]
        outgoing = (field_in.astype(jnp.float32) + convolve(second_forward, wide_active)).astype(
            jnp.bfloat16
        )
        saved_field = store(saved_field, wide_field, slot_index, is_valid, 0)
        saved_hidden = store(saved_hidden, hidden, slot_index, is_valid, 0)
        saved_active = store(saved_active, wide_active, slot_index, is_valid, 0)
    grad_slots = jnp.zeros((images, strip_count, row_count, col_count, channels), jnp.bfloat16)
    saved_grad_out = jnp.zeros((strip_count, images, row_count, col_count, channels), jnp.bfloat16)
    saved_grad_hidden = jnp.zeros(
        (strip_count, images, row_count, col_count, channels), jnp.bfloat16
    )
    sending = empty_field
    for step_no in range(tick_count):
        micro_index = step_no - (section_count - 1 - section_index)
        is_valid = (micro_index >= 0) & (micro_index < strip_count)
        slot_index = jnp.clip(micro_index, 0, strip_count - 1)
        if step_no == 0:
            arriving = empty_field
        else:
            arriving = passed_along(sending, "section", -1)
        top_grad = lax.dynamic_index_in_dim(cotangent, slot_index, 1, keepdims=False)
        grad_out = jnp.where(section_index == section_count - 1, top_grad, arriving)
        grad_out = jnp.where(is_valid, grad_out, jnp.zeros_like(grad_out))
        hidden = lax.dynamic_index_in_dim(saved_hidden, slot_index, 0, keepdims=False)
        wide_grad = padded_2(grad_out, (("slab", 2),), 2)
        grad_active = convolve(second_backward, wide_grad)
        wide_hidden_grad = jnp.where(inside, grad_active * silu_slope(hidden), 0.0).astype(
            jnp.bfloat16
        )
        grad_hidden = wide_hidden_grad[:, :, 1:-1, :]
        sending = (
            grad_out.astype(jnp.float32) + convolve(first_backward, wide_hidden_grad)
        ).astype(jnp.bfloat16)
        saved_grad_out = store(saved_grad_out, grad_out, slot_index, is_valid, 0)
        saved_grad_hidden = store(saved_grad_hidden, grad_hidden, slot_index, is_valid, 0)
        grad_slots = store(grad_slots, sending, slot_index, is_valid, 1)
    flat_count = strip_count * images
    lower_part = contract(
        saved_field.reshape(flat_count, row_count, col_count + 2, channels),
        saved_grad_hidden.reshape(flat_count, row_count, col_count, channels),
    )
    upper_part = contract(
        saved_active.reshape(flat_count, row_count, col_count + 2, channels),
        saved_grad_out.reshape(flat_count, row_count, col_count, channels),
    )
    grad_terms = jnp.stack([lower_part, upper_part]).reshape(2, 9, channels, channels)
    row_share = lax.psum_scatter(
        grad_terms.astype(jnp.bfloat16), "slab", scatter_dimension=2, tiled=True
    )
    own_share = lax.psum_scatter(row_share, "img", scatter_dimension=3, tiled=True).astype(
        jnp.float32
    )
    grad_kernels = (own_share * scaling)[None]
    return (grad_kernels, grad_slots[None])


def call(kernel, outs, operands, unread, scratch, aliases, apart=()):
    spaces = {**dict.fromkeys(unread, pl.ANY), **dict.fromkeys(apart, pltpu.HBM)}
    return pl.pallas_call(
        kernel,
        out_shape=outs,
        in_specs=[
            pl.BlockSpec(memory_space=spaces.get(place, pltpu.VMEM))
            for place in range(len(operands))
        ],
        out_specs=[pl.BlockSpec(memory_space=pltpu.VMEM)] * len(outs),
        scratch_shapes=scratch,
        input_output_aliases=aliases,
        compiler_params=pltpu.CompilerParams(vmem_limit_bytes=8 << 20),
    )(*operands)


def neighbours(value, shifted, width):
    count, channels = value.shape
    shifted[8 : 8 + count, :] = value
    column = lax.rem(lax.broadcasted_iota(jnp.int32, (count, channels), 0), width)
    before = jnp.where(column == 0, 0.0, shifted[7 : 7 + count, :])
    after = jnp.where(column == width - 1, 0.0, shifted[9 : 9 + count, :])
    return before, after


def convolved(value, matrix, taps, shifted, width):
    count, channels = value.shape
    before, after = neighbours(value, shifted, width)
    for place, part in enumerate((before, value, after)):
        taps[width : width + count, place * channels : (place + 1) * channels] = part.astype(
            jnp.bfloat16
        )
    edge = jnp.zeros((width, 3 * channels), jnp.bfloat16)
    taps[0:width, :] = edge
    taps[width + count : 2 * width + count, :] = edge
    total = jnp.dot(taps[0:count, :], matrix[0], preferred_element_type=jnp.float32)
    for down in (1, 2):
        total = total + jnp.dot(
            taps[down * width : down * width + count, :],
            matrix[down],
            preferred_element_type=jnp.float32,
        )
    return total


def forward_call(field, weights, state, section, crop, crops, width, last, after):
    count, channels = field.shape

    def kernel(field_ref, weights_ref, after_ref, *refs):
        *_, saved_ref, hidden_ref, taps, shifted = refs

        @pl.when(lax.axis_index("section") == section)
        def _():
            field_in = field_ref[...]
            wide = field_in.astype(jnp.float32)
            saved_ref[0, crop] = field_in
            hidden = convolved(wide, weights_ref.at[0], taps, shifted, width)
            hidden_ref[crop] = hidden
            active = (hidden * jax.nn.sigmoid(hidden)).astype(jnp.bfloat16)
            saved_ref[1, crop] = active
            if not last:
                added = convolved(
                    active.astype(jnp.float32), weights_ref.at[1], taps, shifted, width
                )
                refs[-5][...] = (wide + added).astype(jnp.bfloat16)

    outs = [
        jax.ShapeDtypeStruct((count, channels), jnp.bfloat16),
        jax.ShapeDtypeStruct((2, crops, count, channels), jnp.bfloat16),
        jax.ShapeDtypeStruct((crops, count, channels), jnp.float32),
    ][1 if last else 0 :]
    scratch = [
        pltpu.VMEM((count + 2 * width, 3 * channels), jnp.bfloat16),
        pltpu.VMEM((count + 16, channels), jnp.float32),
    ]
    aliases = {3 + k: k + (0 if last else 1) for k in range(len(state))}
    outputs = call(kernel, outs, [field, weights, after, *state], (2,), scratch, aliases)
    return (None if last else outputs[0]), outputs[-2:]


def backward_call(
    grad, turned, hidden, state, section, crop, crops, width, parts, after
):
    count, channels = grad.shape
    share = channels // parts
    first = section == 0

    def kernel(grad_ref, turned_ref, hidden_ref, after_ref, *refs):
        *_, kept_ref, sent_ref, taps, shifted = refs

        @pl.when(lax.axis_index("section") == section)
        def _():
            wide = grad_ref[...].astype(jnp.float32)
            own = lax.axis_index("img")
            place_parts(sent_ref, (0,), grad_ref[...], crop, parts, own)
            grad_active = convolved(wide, turned_ref.at[1], taps, shifted, width)
            hidden = hidden_ref[crop]
            gate = jax.nn.sigmoid(hidden)
            grad_hidden = (grad_active * (gate * (1.0 + hidden * (1.0 - gate)))).astype(
                jnp.bfloat16
            )
            place_parts(sent_ref, (1,), grad_hidden, crop, parts, own)
            added = convolved(
                grad_hidden.astype(jnp.float32), turned_ref.at[0], taps, shifted, width
            )
            result = (wide + added).astype(jnp.bfloat16)
            kept_ref[crop] = result
            if not first:
                refs[-5][...] = result

    outs = [
        jax.ShapeDtypeStruct((count, channels), jnp.bfloat16),
        jax.ShapeDtypeStruct((crops, count, channels), jnp.bfloat16),
        jax.ShapeDtypeStruct((parts, 2, share, crops * count), jnp.bfloat16),
    ][1 if first else 0 :]
    scratch = [
        pltpu.VMEM((count + 2 * width, 3 * channels), jnp.bfloat16),
        pltpu.VMEM((count + 16, channels), jnp.float32),
    ]
    aliases = {4 + k: k + (0 if first else 1) for k in range(len(state))}
    operands = [grad, turned, hidden, after, *state]
    outputs = call(kernel, outs, operands, (3,), scratch, aliases)
    return (None if first else outputs[0]), outputs[-2:]


def place_parts(target, lead, value, crop, parts, own):
    count, channels = value.shape
    share = channels // parts
    flipped = value.T
    for part in range(parts):
        slot = lax.rem(part + parts - own, parts)
        target[(slot, *lead, slice(None), slice(crop * count, (crop + 1) * count))] = flipped[
            part * share : (part + 1) * share, :
        ]


def flip_call(kept, parts, axis, after):
    def kernel(*refs):
        flipped_ref = refs[-1]
        for crop, (place, index) in enumerate(kept):
            value = refs[place][index]
            place_parts(flipped_ref, (), value, crop, parts, lax.axis_index(axis))

    operands = []
    for array, index in kept:
        if all(array is not other for other in operands):
            operands.append(array)
    kept = [
        ([array is other for other in operands].index(True), index) for array, index in kept
    ]
    count, channels = operands[0].shape[-2:]
    out = jax.ShapeDtypeStruct((parts, channels // parts, len(kept) * count), operands[0].dtype)
    (flipped,) = call(kernel, [out], [*operands, after], (len(operands),), [], {})
    return flipped


def turn_call(weights, after):
    two, _, _, channels = weights.shape

    def kernel(weights_ref, after_ref, turned_ref):
        for which in range(two):
            for tap in range(9):
                down, right = divmod(tap, 3)
                flipped = weights_ref[which, down, right * channels : (right + 1) * channels, :].T
                down, right = divmod(8 - tap, 3)
                turned_ref[which, down, right * channels : (right + 1) * channels, :] = flipped

    out = jax.ShapeDtypeStruct(weights.shape, weights.dtype)
    (turned,) = call(kernel, [out], [weights, after], (1,), [], {})
    return turned


def split_call(strips, cotangent, last):
    images, strip_count, rows, cols, channels = strips.shape
    share = strip_count // 2

    def kernel(strips_ref, cotangent_ref, own_ref, other_ref, sems):
        own = lax.axis_index("slab")
        is_last = lax.axis_index("section") == last

        def fetch(source_ref):
            copies = []
            for image in range(images):
                at = pl.ds(image * share, share)
                for side, (ref, half) in enumerate(((own_ref, own), (other_ref, 1 - own))):
                    source = source_ref.at[image, pl.ds(half * share, share)]
                    copies.append(pltpu.make_async_copy(source, ref.at[at], sems.at[2 * image + side]))
            for copy in copies:
                copy.start()
            for copy in copies:
                copy.wait()

        @pl.when(is_last)
        def _():
            fetch(cotangent_ref)

        @pl.when(jnp.logical_not(is_last))
        def _():
            fetch(strips_ref)

    out = jax.ShapeDtypeStruct((images * share, rows, cols, channels), strips.dtype)
    sems = [pltpu.SemaphoreType.DMA((2 * images,))]
    return call(kernel, [out, out], [strips, cotangent], (), sems, {}, (0, 1))


def load_call(weights):
    def kernel(weights_ref, out_ref, sems):
        copies = [
            pltpu.make_async_copy(weights_ref.at[which], out_ref.at[which], sems.at[which])
            for which in range(2)
        ]
        for copy in copies:
            copy.start()
        for copy in copies:
            copy.wait()

    out = jax.ShapeDtypeStruct(weights.shape, weights.dtype)
    sems = [pltpu.SemaphoreType.DMA((2,))]
    (loaded,) = call(kernel, [out], [weights], (), sems, {}, (0,))
    return loaded


def join_call(own, other):
    crops, rows, cols, channels = own.shape

    def kernel(own_ref, other_ref, *out_refs):
        is_left = lax.axis_index("slab") == 0
        for crop, out_ref in enumerate(out_refs):
            mine = own_ref[crop].astype(jnp.float32)
            theirs = other_ref[crop].astype(jnp.float32)
            left = jnp.where(is_left, mine, theirs)
            right = jnp.where(is_left, theirs, mine)
            whole = jnp.concatenate([left, right], axis=1)
            out_ref[...] = whole.reshape(rows * 2 * cols, channels).astype(jnp.bfloat16)

    out = jax.ShapeDtypeStruct((rows * 2 * cols, channels), own.dtype)
    return call(kernel, [out] * crops, [own, other], (), [], {})


def part_call(kept, rows, after):
    crops, count, channels = kept.shape
    cols = count // rows // 2

    def kernel(kept_ref, after_ref, own_ref, other_ref):
        is_left = lax.axis_index("slab") == 0
        for crop in range(crops):
            whole = kept_ref[crop].astype(jnp.float32).reshape(rows, 2 * cols, channels)
            left, right = whole[:, :cols], whole[:, cols:]
            own_ref[crop] = jnp.where(is_left, left, right).astype(jnp.bfloat16)
            other_ref[crop] = jnp.where(is_left, right, left).astype(jnp.bfloat16)

    out = jax.ShapeDtypeStruct((crops, rows, cols, channels), kept.dtype)
    return call(kernel, [out, out], [kept, after], (1,), [], {})


def merge_call(own, other, images):
    crops, rows, cols, channels = own.shape
    share = crops // images

    def kernel(own_ref, other_ref, out_ref):
        place = lax.axis_index("slab")
        for image in range(images):
            for crop in range(share):
                out_ref[image, place * share + crop] = own_ref[image * share + crop]
                out_ref[image, (1 - place) * share + crop] = other_ref[image * share + crop]

    out = jax.ShapeDtypeStruct((images, 2 * share, rows, cols, channels), own.dtype)
    (merged,) = call(kernel, [out], [own, other], (), [], {})
    return merged


def stack_call(blocks):
    def kernel(*refs):
        for place in range(len(blocks)):
            refs[-1][place] = refs[place][...]

    out = jax.ShapeDtypeStruct((len(blocks), *blocks[0].shape), blocks[0].dtype)
    (stacked,) = call(kernel, [out], [*blocks], (), [], {})
    return stacked


def remake_call(saved, weights, received, width):
    _, crops, count, channels = saved.shape
    share = channels // 2
    sections, each = len(received), len(received[0])

    def kernel(saved_ref, weights_ref, *refs):
        home_ref, outer_ref, taps, shifted = refs[-4:]
        is_left = lax.axis_index("slab") == 0

        def put(kind, block, crop, value):
            cells = slice(crop * count, (crop + 1) * count)
            flipped = value.T
            low, high = flipped[:share], flipped[share:]
            home_ref[kind, block, :, cells] = jnp.where(is_left, low, high)
            outer_ref[kind, block, :, cells] = jnp.where(is_left, high, low)

        for crop in range(crops):
            for kind in range(2):
                put(kind, 0, crop, saved_ref[kind, crop])
        for section in range(sections):

            @pl.when(lax.axis_index("section") == section)
            def _():
                for block in range(each):
                    home_ref[0, 1 + block] = refs[section * each + block][0]
                    outer_ref[0, 1 + block] = refs[section * each + block][1]

        for block in range(1, 1 + each):
            for crop in range(crops):
                cells = slice(crop * count, (crop + 1) * count)
                mine, theirs = home_ref[0, block, :, cells], outer_ref[0, block, :, cells]
                low, high = jnp.where(is_left, mine, theirs), jnp.where(is_left, theirs, mine)
                field = jnp.concatenate([low, high], axis=0).T.astype(jnp.float32)
                hidden = convolved(field, weights_ref.at[0], taps, shifted, width)
                put(1, block, crop, (hidden * jax.nn.sigmoid(hidden)).astype(jnp.bfloat16))

    out = jax.ShapeDtypeStruct((2, 1 + each, share, crops * count), saved.dtype)
    scratch = [
        pltpu.VMEM((count + 2 * width, 3 * channels), jnp.bfloat16),
        pltpu.VMEM((count + 16, channels), jnp.float32),
    ]
    operands = [saved, weights, *[array for arrays in received for array in arrays]]
    return call(kernel, [out, out], operands, (), scratch, {})


def spread_call(cells_of, around, place, count, width):
    two, blocks, share, cells = cells_of.shape
    crops = cells // count
    stride = count + width
    total = 2 * blocks * crops * stride + width

    def kernel(cells_ref, *refs):
        out_ref, shifted = refs[-2:]
        edge = jnp.zeros((width, 3 * share), jnp.bfloat16)
        for kind in range(two):
            out_ref[kind, total - width : total, :] = edge
            for block in range(blocks):
                for crop in range(crops):
                    cell = slice(crop * count, (crop + 1) * count)
                    value = cells_ref[kind, block, :, cell].T.astype(jnp.float32)
                    before, after = neighbours(value, shifted, width)
                    at = ((place * blocks + block) * crops + crop) * stride
                    out_ref[kind, at : at + width, :] = edge
                    for side, part in enumerate((before, value, after)):
                        lanes = slice(side * share, (side + 1) * share)
                        out_ref[kind, at + width : at + stride, lanes] = part.astype(jnp.bfloat16)

    out = jax.ShapeDtypeStruct((two, total, 3 * share), jnp.bfloat16)
    scratch = [pltpu.VMEM((count + 16, share), jnp.float32)]
    operands = [cells_of] if around is None else [cells_of, around]
    aliases = {} if around is None else {1: 0}
    (spread,) = call(kernel, [out], operands, (), scratch, aliases)
    return spread


def terms_call(around, own, other, count, width, scaling):
    blocks, _, columns, cells = own.shape
    rows = around.shape[2] // 3
    stride = count + width
    crops = cells // count

    def kernel(around_ref, own_ref, other_ref, out_ref):
        for kind in range(2):
            for down in range(3):
                total = None
                for block in range(2 * blocks):
                    left = own_ref if block < blocks else other_ref
                    left = left[block % blocks, 1 - kind]
                    at = [(block * crops + k) * stride + down * width for k in range(crops)]
                    right = jnp.concatenate(
                        [around_ref[kind, start : start + count, :] for start in at], axis=0
                    )
                    term = jnp.dot(left, right, preferred_element_type=jnp.float32)
                    total = term if total is None else total + term
                total = (total * scaling).T.reshape(3, rows, columns)
                for place in range(3):
                    out_ref[kind, 3 * down + place] = total[place]

    out = jax.ShapeDtypeStruct((2, 9, rows, columns), jnp.float32)
    (terms,) = call(kernel, [out], [around, own, other], (), [], {})
    return terms


def rotated(value, axis, steps):
    count = lax.axis_size(axis)
    return lax.ppermute(value, axis, [(source, (source + steps) % count) for source in range(count)])


def crop_shards(strips, kernels, cotangent):
    sections = lax.axis_size("section")
    slabs, groups = lax.axis_size("slab"), lax.axis_size("img")
    images, strip_count, row_count, col_count, channels = strips.shape
    width = col_count * slabs
    count = row_count * width
    crops = images * strip_count // slabs
    last = sections - 1
    early = min(1, last - 1)
    steps = range(1, groups)
    scaling = 1.0 / math.sqrt(images * groups * strip_count * count)

    def hop(values, source, target):
        arrived = []
        for value in values:
            arrived.append(lax.ppermute(value, "section", [(source, target)]))
        return arrived

    def shared(values, step, routes):
        pairs = [
            (source * groups + i, target * groups + (i + step) % groups)
            for source, target in routes
            for i in range(groups)
        ]
        return lax.ppermute(values, ("section", "img"), pairs)

    def swapped(value):
        return rotated(value, "slab", 1)

    def flipped(values):
        return flip_call([(value, Ellipsis) for value in values], slabs, "slab", values[-1])

    own, other = split_call(
        pltpu.with_memory_space_constraint(strips, pltpu.HBM),
        pltpu.with_memory_space_constraint(cotangent, pltpu.HBM),
        last,
    )
    other = swapped(other)
    weights = kernels[0].reshape(2, 3, 3 * channels, channels)
    weights = load_call(pltpu.with_memory_space_constraint(weights, pltpu.HBM))
    fields = join_call(own, other)
    incoming = fields
    state, received = [], [None] * sections
    turned, after = None, weights
    for place in range(sections):
        outgoing = []
        for crop in range(crops):
            out, state = forward_call(
                incoming[crop], weights, state, place, crop, crops, width, place == last, after
            )
            outgoing.append(out)
        if place < last:
            incoming = hop(outgoing, place, place + 1)
            handed = flipped(outgoing)
            routes = [(place, place + 1)]
            received[place + 1] = [shared(handed, step, routes) for step in steps]
        if place == early:
            handed = flipped(fields)
            received[0] = [shared(handed, step, [(0, 0)]) for step in steps]
            turned = turn_call(weights, state[0])
            after = turned
    saved, hidden = state
    incoming = fields
    grads = []
    after = hidden
    for place in reversed(range(sections)):
        outgoing = []
        for crop in range(crops):
            out, grads = backward_call(
                incoming[crop], turned, hidden, grads, place, crop, crops, width, groups, after
            )
            outgoing.append(out)
        if place:
            incoming = hop(outgoing, place, place - 1)
    kept, sent = grads
    own = [sent[0]]
    everywhere = [(place, place) for place in range(sections)]
    for step in steps:
        own.append(shared(sent[step], step, everywhere))
    home, outer = remake_call(saved, weights, received, width)
    outer = swapped(outer)
    around = spread_call(home, None, 0, count, width)
    around = spread_call(outer, around, 1, count, width)
    own = stack_call(own)
    other = swapped(own)
    terms = terms_call(around, own, other, count, width, scaling)
    own, other = part_call(kept, row_count, sent)
    other = swapped(other)
    grad_inputs = merge_call(own, other, images)
    return (terms[None], grad_inputs[None])


def shards(strips, kernels, cotangent):
    slabs, groups = lax.axis_size("slab"), lax.axis_size("img")
    strip_count, row_count, col_count, channels = strips.shape[1:]
    width = col_count * slabs
    whole_crops = strip_count % slabs == 0 and width % 16 == 0 and (row_count * width) % 128 == 0
    whole_crops = whole_crops and slabs == 2 and lax.axis_size("section") > 1
    if whole_crops and channels % (16 * slabs) == 0 and channels % (16 * groups) == 0:
        return crop_shards(strips, kernels, cotangent)
    return column_shards(strips, kernels, cotangent)


def solution(mesh):
    in_specs = (
        P("img", None, None, "slab", None),
        P("section", None, None, None, None),
        P("img", None, None, "slab", None),
    )
    out_specs = (
        P("section", None, None, "slab", "img"),
        P("section", "img", None, None, "slab", None),
    )
    return jax.shard_map(shards, mesh=mesh, in_specs=in_specs, out_specs=out_specs, check_vma=False)
```

```python
import math

import jax
import jax.numpy as jnp
from jax import lax
from jax.experimental import pallas as pl
from jax.experimental.pallas import tpu as pltpu
from jax.sharding import PartitionSpec as P


def passed_along(value, axis, steps):
    count = lax.axis_size(axis)
    initial, last = (max(0, -steps), min(count, count - steps))
    return lax.ppermute(value, axis, [(source, source + steps) for source in range(initial, last)])


def padded_2(cells, sides, width):
    for axis, dim in sides:
        count = lax.axis_size(axis)
        ends = count - 1
        head = lax.slice_in_dim(cells, 0, width, axis=dim)
        tail = lax.slice_in_dim(cells, cells.shape[dim] - width, cells.shape[dim], axis=dim)
        cells = jnp.concatenate(
            [
                lax.ppermute(tail, axis, [(i, (i + 1) % count) for i in range(ends)]),
                cells,
                lax.ppermute(head, axis, [((i + 1) % count, i) for i in range(ends)]),
            ],
            axis=dim,
        )
    return cells


def unfold(padded, row_count, col_count):
    tap_list = [
        padded[:, down_at : down_at + row_count, right_at : right_at + col_count, :]
        for down_at in range(3)
        for right_at in range(3)
    ]
    stacked = jnp.concatenate(tap_list, axis=3)
    return stacked.reshape(-1, stacked.shape[3])


def columns_of(wide_field):
    row_count = wide_field.shape[1]
    col_count = wide_field.shape[2] - 2
    padded = jnp.pad(wide_field, ((0, 0), (1, 1), (0, 0), (0, 0)))
    return unfold(padded, row_count, col_count)


def convolve(matrix, wide_field):
    count, row_count = (wide_field.shape[0], wide_field.shape[1])
    col_count = wide_field.shape[2] - 2
    flat_out = jnp.dot(columns_of(wide_field), matrix, preferred_element_type=jnp.float32)
    return flat_out.reshape(count, row_count, col_count, matrix.shape[1])


def contract(wide_field, grad_out):
    flat_grad = grad_out.reshape(-1, grad_out.shape[3])
    return lax.dot_general(
        columns_of(wide_field),
        flat_grad,
        (((0,), (0,)), ((), ())),
        preferred_element_type=jnp.float32,
    )


def silu_slope(hidden):
    sigmoid_at = jax.nn.sigmoid(hidden)
    return sigmoid_at * (1.0 + hidden * (1.0 - sigmoid_at))


def store(buffer, value, slot_index, is_valid, axis_at):
    current = lax.dynamic_index_in_dim(buffer, slot_index, axis_at, keepdims=False)
    return lax.dynamic_update_index_in_dim(
        buffer, jnp.where(is_valid, value, current), slot_index, axis_at
    )


def column_shards(strips, kernels, cotangent):
    section_count = lax.axis_size("section")
    section_index = lax.axis_index("section")
    slab_count = lax.axis_size("slab")
    slab_index = lax.axis_index("slab")
    images, strip_count, row_count, col_count, channels = strips.shape
    weights = kernels[0]
    first_forward = weights[0].reshape(9 * channels, channels)
    second_forward = weights[1].reshape(9 * channels, channels)
    first_backward = jnp.transpose(weights[0][::-1], (0, 2, 1)).reshape(9 * channels, channels)
    second_backward = jnp.transpose(weights[1][::-1], (0, 2, 1)).reshape(9 * channels, channels)
    scaling = 1.0 / math.sqrt(
        images * lax.axis_size("img") * strip_count * row_count * col_count * slab_count
    )
    position = slab_index * col_count - 1 + jnp.arange(col_count + 2, dtype=jnp.int32)
    inside = ((position >= 0) & (position < slab_count * col_count))[None, None, :, None]
    tick_count = strip_count + section_count - 1
    hidden_cols = col_count + 2
    empty_field = jnp.zeros((images, row_count, col_count, channels), jnp.bfloat16)
    saved_field = jnp.zeros((strip_count, images, row_count, col_count + 2, channels), jnp.bfloat16)
    saved_hidden = jnp.zeros((strip_count, images, row_count, hidden_cols, channels), jnp.float32)
    saved_active = jnp.zeros(
        (strip_count, images, row_count, col_count + 2, channels), jnp.bfloat16
    )
    outgoing = empty_field
    for step_no in range(tick_count):
        micro_index = step_no - section_index
        is_valid = (micro_index >= 0) & (micro_index < strip_count)
        slot_index = jnp.clip(micro_index, 0, strip_count - 1)
        if step_no == 0:
            incoming = empty_field
        else:
            incoming = passed_along(outgoing, "section", 1)
        first_strip = lax.dynamic_index_in_dim(strips, slot_index, 1, keepdims=False)
        field_in = jnp.where(section_index == 0, first_strip, incoming)
        wide_deep = padded_2(field_in, (("slab", 2),), 2)
        hidden = convolve(first_forward, wide_deep)
        wide_active = jnp.where(inside, jax.nn.silu(hidden), 0.0).astype(jnp.bfloat16)
        wide_field = wide_deep[:, :, 1:-1, :]
        outgoing = (field_in.astype(jnp.float32) + convolve(second_forward, wide_active)).astype(
            jnp.bfloat16
        )
        saved_field = store(saved_field, wide_field, slot_index, is_valid, 0)
        saved_hidden = store(saved_hidden, hidden, slot_index, is_valid, 0)
        saved_active = store(saved_active, wide_active, slot_index, is_valid, 0)
    grad_slots = jnp.zeros((images, strip_count, row_count, col_count, channels), jnp.bfloat16)
    saved_grad_out = jnp.zeros((strip_count, images, row_count, col_count, channels), jnp.bfloat16)
    saved_grad_hidden = jnp.zeros(
        (strip_count, images, row_count, col_count, channels), jnp.bfloat16
    )
    sending = empty_field
    for step_no in range(tick_count):
        micro_index = step_no - (section_count - 1 - section_index)
        is_valid = (micro_index >= 0) & (micro_index < strip_count)
        slot_index = jnp.clip(micro_index, 0, strip_count - 1)
        if step_no == 0:
            arriving = empty_field
        else:
            arriving = passed_along(sending, "section", -1)
        top_grad = lax.dynamic_index_in_dim(cotangent, slot_index, 1, keepdims=False)
        grad_out = jnp.where(section_index == section_count - 1, top_grad, arriving)
        grad_out = jnp.where(is_valid, grad_out, jnp.zeros_like(grad_out))
        hidden = lax.dynamic_index_in_dim(saved_hidden, slot_index, 0, keepdims=False)
        wide_grad = padded_2(grad_out, (("slab", 2),), 2)
        grad_active = convolve(second_backward, wide_grad)
        wide_hidden_grad = jnp.where(inside, grad_active * silu_slope(hidden), 0.0).astype(
            jnp.bfloat16
        )
        grad_hidden = wide_hidden_grad[:, :, 1:-1, :]
        sending = (
            grad_out.astype(jnp.float32) + convolve(first_backward, wide_hidden_grad)
        ).astype(jnp.bfloat16)
        saved_grad_out = store(saved_grad_out, grad_out, slot_index, is_valid, 0)
        saved_grad_hidden = store(saved_grad_hidden, grad_hidden, slot_index, is_valid, 0)
        grad_slots = store(grad_slots, sending, slot_index, is_valid, 1)
    flat_count = strip_count * images
    lower_part = contract(
        saved_field.reshape(flat_count, row_count, col_count + 2, channels),
        saved_grad_hidden.reshape(flat_count, row_count, col_count, channels),
    )
    upper_part = contract(
        saved_active.reshape(flat_count, row_count, col_count + 2, channels),
        saved_grad_out.reshape(flat_count, row_count, col_count, channels),
    )
    grad_terms = jnp.stack([lower_part, upper_part]).reshape(2, 9, channels, channels)
    row_share = lax.psum_scatter(
        grad_terms.astype(jnp.bfloat16), "slab", scatter_dimension=2, tiled=True
    )
    own_share = lax.psum_scatter(row_share, "img", scatter_dimension=3, tiled=True).astype(
        jnp.float32
    )
    grad_kernels = (own_share * scaling)[None]
    return (grad_kernels, grad_slots[None])


def call(kernel, outs, operands, unread, scratch, aliases, apart=()):
    spaces = {**dict.fromkeys(unread, pl.ANY), **dict.fromkeys(apart, pltpu.HBM)}
    return pl.pallas_call(
        kernel,
        out_shape=outs,
        in_specs=[
            pl.BlockSpec(memory_space=spaces.get(place, pltpu.VMEM))
            for place in range(len(operands))
        ],
        out_specs=[pl.BlockSpec(memory_space=pltpu.VMEM)] * len(outs),
        scratch_shapes=scratch,
        input_output_aliases=aliases,
        compiler_params=pltpu.CompilerParams(vmem_limit_bytes=8 << 20),
    )(*operands)


def neighbours(value, shifted, width):
    count, channels = value.shape
    shifted[8 : 8 + count, :] = value
    column = lax.rem(lax.broadcasted_iota(jnp.int32, (count, channels), 0), width)
    before = jnp.where(column == 0, 0.0, shifted[7 : 7 + count, :])
    after = jnp.where(column == width - 1, 0.0, shifted[9 : 9 + count, :])
    return before, after


def convolved(value, matrix, taps, shifted, width):
    count, channels = value.shape
    before, after = neighbours(value, shifted, width)
    for place, part in enumerate((before, value, after)):
        taps[width : width + count, place * channels : (place + 1) * channels] = part.astype(
            jnp.bfloat16
        )
    edge = jnp.zeros((width, 3 * channels), jnp.bfloat16)
    taps[0:width, :] = edge
    taps[width + count : 2 * width + count, :] = edge
    total = jnp.dot(taps[0:count, :], matrix[0], preferred_element_type=jnp.float32)
    for down in (1, 2):
        total = total + jnp.dot(
            taps[down * width : down * width + count, :],
            matrix[down],
            preferred_element_type=jnp.float32,
        )
    return total


def forward_call(field, weights, state, section, crop, crops, width, last, after):
    count, channels = field.shape

    def kernel(field_ref, weights_ref, after_ref, *refs):
        *_, saved_ref, hidden_ref, taps, shifted = refs

        @pl.when(lax.axis_index("section") == section)
        def _():
            field_in = field_ref[...]
            wide = field_in.astype(jnp.float32)
            saved_ref[0, crop] = field_in
            hidden = convolved(wide, weights_ref.at[0], taps, shifted, width)
            hidden_ref[crop] = hidden
            active = (hidden * jax.nn.sigmoid(hidden)).astype(jnp.bfloat16)
            saved_ref[1, crop] = active
            if not last:
                added = convolved(
                    active.astype(jnp.float32), weights_ref.at[1], taps, shifted, width
                )
                refs[-5][...] = (wide + added).astype(jnp.bfloat16)

    outs = [
        jax.ShapeDtypeStruct((count, channels), jnp.bfloat16),
        jax.ShapeDtypeStruct((2, crops, count, channels), jnp.bfloat16),
        jax.ShapeDtypeStruct((crops, count, channels), jnp.float32),
    ][1 if last else 0 :]
    scratch = [
        pltpu.VMEM((count + 2 * width, 3 * channels), jnp.bfloat16),
        pltpu.VMEM((count + 16, channels), jnp.float32),
    ]
    aliases = {3 + k: k + (0 if last else 1) for k in range(len(state))}
    outputs = call(kernel, outs, [field, weights, after, *state], (2,), scratch, aliases)
    return (None if last else outputs[0]), outputs[-2:]


def backward_call(
    grad, turned, hidden, state, section, crop, crops, width, parts, after
):
    count, channels = grad.shape
    share = channels // parts
    first = section == 0

    def kernel(grad_ref, turned_ref, hidden_ref, after_ref, *refs):
        *_, kept_ref, sent_ref, taps, shifted = refs

        @pl.when(lax.axis_index("section") == section)
        def _():
            wide = grad_ref[...].astype(jnp.float32)
            own = lax.axis_index("img")
            place_parts(sent_ref, (0,), grad_ref[...], crop, parts, own)
            grad_active = convolved(wide, turned_ref.at[1], taps, shifted, width)
            hidden = hidden_ref[crop]
            gate = jax.nn.sigmoid(hidden)
            grad_hidden = (grad_active * (gate * (1.0 + hidden * (1.0 - gate)))).astype(
                jnp.bfloat16
            )
            place_parts(sent_ref, (1,), grad_hidden, crop, parts, own)
            added = convolved(
                grad_hidden.astype(jnp.float32), turned_ref.at[0], taps, shifted, width
            )
            result = (wide + added).astype(jnp.bfloat16)
            kept_ref[crop] = result
            if not first:
                refs[-5][...] = result

    outs = [
        jax.ShapeDtypeStruct((count, channels), jnp.bfloat16),
        jax.ShapeDtypeStruct((crops, count, channels), jnp.bfloat16),
        jax.ShapeDtypeStruct((parts, 2, share, crops * count), jnp.bfloat16),
    ][1 if first else 0 :]
    scratch = [
        pltpu.VMEM((count + 2 * width, 3 * channels), jnp.bfloat16),
        pltpu.VMEM((count + 16, channels), jnp.float32),
    ]
    aliases = {4 + k: k + (0 if first else 1) for k in range(len(state))}
    operands = [grad, turned, hidden, after, *state]
    outputs = call(kernel, outs, operands, (3,), scratch, aliases)
    return (None if first else outputs[0]), outputs[-2:]


def place_parts(target, lead, value, crop, parts, own):
    count, channels = value.shape
    share = channels // parts
    flipped = value.T
    for part in range(parts):
        slot = lax.rem(part + parts - own, parts)
        target[(slot, *lead, slice(None), slice(crop * count, (crop + 1) * count))] = flipped[
            part * share : (part + 1) * share, :
        ]


def flip_call(kept, parts, axis, after):
    def kernel(*refs):
        flipped_ref = refs[-1]
        for crop, (place, index) in enumerate(kept):
            value = refs[place][index]
            place_parts(flipped_ref, (), value, crop, parts, lax.axis_index(axis))

    operands = []
    for array, index in kept:
        if all(array is not other for other in operands):
            operands.append(array)
    kept = [
        ([array is other for other in operands].index(True), index) for array, index in kept
    ]
    count, channels = operands[0].shape[-2:]
    out = jax.ShapeDtypeStruct((parts, channels // parts, len(kept) * count), operands[0].dtype)
    (flipped,) = call(kernel, [out], [*operands, after], (len(operands),), [], {})
    return flipped


def turn_call(weights, after):
    two, _, _, channels = weights.shape

    def kernel(weights_ref, after_ref, turned_ref):
        for which in range(two):
            for tap in range(9):
                down, right = divmod(tap, 3)
                flipped = weights_ref[which, down, right * channels : (right + 1) * channels, :].T
                down, right = divmod(8 - tap, 3)
                turned_ref[which, down, right * channels : (right + 1) * channels, :] = flipped

    out = jax.ShapeDtypeStruct(weights.shape, weights.dtype)
    (turned,) = call(kernel, [out], [weights, after], (1,), [], {})
    return turned


def split_call(strips, cotangent, last):
    images, strip_count, rows, cols, channels = strips.shape
    share = strip_count // 2

    def kernel(strips_ref, cotangent_ref, own_ref, other_ref, sems):
        own = lax.axis_index("slab")
        is_last = lax.axis_index("section") == last

        def fetch(source_ref):
            copies = []
            for image in range(images):
                at = pl.ds(image * share, share)
                for side, (ref, half) in enumerate(((own_ref, own), (other_ref, 1 - own))):
                    source = source_ref.at[image, pl.ds(half * share, share)]
                    copies.append(pltpu.make_async_copy(source, ref.at[at], sems.at[2 * image + side]))
            for copy in copies:
                copy.start()
            for copy in copies:
                copy.wait()

        @pl.when(is_last)
        def _():
            fetch(cotangent_ref)

        @pl.when(jnp.logical_not(is_last))
        def _():
            fetch(strips_ref)

    out = jax.ShapeDtypeStruct((images * share, rows, cols, channels), strips.dtype)
    sems = [pltpu.SemaphoreType.DMA((2 * images,))]
    return call(kernel, [out, out], [strips, cotangent], (), sems, {}, (0, 1))


def load_call(weights):
    def kernel(weights_ref, out_ref, sems):
        copies = [
            pltpu.make_async_copy(weights_ref.at[which], out_ref.at[which], sems.at[which])
            for which in range(2)
        ]
        for copy in copies:
            copy.start()
        for copy in copies:
            copy.wait()

    out = jax.ShapeDtypeStruct(weights.shape, weights.dtype)
    sems = [pltpu.SemaphoreType.DMA((2,))]
    (loaded,) = call(kernel, [out], [weights], (), sems, {}, (0,))
    return loaded


def join_call(own, other):
    crops, rows, cols, channels = own.shape

    def kernel(own_ref, other_ref, *out_refs):
        is_left = lax.axis_index("slab") == 0
        for crop, out_ref in enumerate(out_refs):
            mine = own_ref[crop].astype(jnp.float32)
            theirs = other_ref[crop].astype(jnp.float32)
            left = jnp.where(is_left, mine, theirs)
            right = jnp.where(is_left, theirs, mine)
            whole = jnp.concatenate([left, right], axis=1)
            out_ref[...] = whole.reshape(rows * 2 * cols, channels).astype(jnp.bfloat16)

    out = jax.ShapeDtypeStruct((rows * 2 * cols, channels), own.dtype)
    return call(kernel, [out] * crops, [own, other], (), [], {})


def part_call(kept, rows, after):
    crops, count, channels = kept.shape
    cols = count // rows // 2

    def kernel(kept_ref, after_ref, own_ref, other_ref):
        is_left = lax.axis_index("slab") == 0
        for crop in range(crops):
            whole = kept_ref[crop].astype(jnp.float32).reshape(rows, 2 * cols, channels)
            left, right = whole[:, :cols], whole[:, cols:]
            own_ref[crop] = jnp.where(is_left, left, right).astype(jnp.bfloat16)
            other_ref[crop] = jnp.where(is_left, right, left).astype(jnp.bfloat16)

    out = jax.ShapeDtypeStruct((crops, rows, cols, channels), kept.dtype)
    return call(kernel, [out, out], [kept, after], (1,), [], {})


def merge_call(own, other, images):
    crops, rows, cols, channels = own.shape
    share = crops // images

    def kernel(own_ref, other_ref, out_ref):
        place = lax.axis_index("slab")
        for image in range(images):
            for crop in range(share):
                out_ref[image, place * share + crop] = own_ref[image * share + crop]
                out_ref[image, (1 - place) * share + crop] = other_ref[image * share + crop]

    out = jax.ShapeDtypeStruct((images, 2 * share, rows, cols, channels), own.dtype)
    (merged,) = call(kernel, [out], [own, other], (), [], {})
    return merged


def stack_call(blocks):
    def kernel(*refs):
        for place in range(len(blocks)):
            refs[-1][place] = refs[place][...]

    out = jax.ShapeDtypeStruct((len(blocks), *blocks[0].shape), blocks[0].dtype)
    (stacked,) = call(kernel, [out], [*blocks], (), [], {})
    return stacked


def remake_call(saved, weights, soon, late, late_from, width):
    _, crops, count, channels = saved.shape
    share = channels // 2
    each = len(soon)

    def kernel(saved_ref, weights_ref, *refs):
        home_ref, outer_ref, taps, shifted = refs[-4:]
        is_left = lax.axis_index("slab") == 0

        def put(kind, block, crop, value):
            cells = slice(crop * count, (crop + 1) * count)
            flipped = value.T
            low, high = flipped[:share], flipped[share:]
            home_ref[kind, block, :, cells] = jnp.where(is_left, low, high)
            outer_ref[kind, block, :, cells] = jnp.where(is_left, high, low)

        for crop in range(crops):
            for kind in range(2):
                put(kind, 0, crop, saved_ref[kind, crop])
        is_late = lax.axis_index("section") >= late_from
        for block in range(each):
            for slot, ref in enumerate((home_ref, outer_ref)):
                ref[0, 1 + block] = jnp.where(
                    is_late, refs[each + block][slot], refs[block][slot]
                )
        for block in range(1, 1 + each):
            for crop in range(crops):
                cells = slice(crop * count, (crop + 1) * count)
                mine, theirs = home_ref[0, block, :, cells], outer_ref[0, block, :, cells]
                low, high = jnp.where(is_left, mine, theirs), jnp.where(is_left, theirs, mine)
                field = jnp.concatenate([low, high], axis=0).T.astype(jnp.float32)
                hidden = convolved(field, weights_ref.at[0], taps, shifted, width)
                put(1, block, crop, (hidden * jax.nn.sigmoid(hidden)).astype(jnp.bfloat16))

    out = jax.ShapeDtypeStruct((2, 1 + each, share, crops * count), saved.dtype)
    scratch = [
        pltpu.VMEM((count + 2 * width, 3 * channels), jnp.bfloat16),
        pltpu.VMEM((count + 16, channels), jnp.float32),
    ]
    operands = [saved, weights, *soon, *late]
    return call(kernel, [out, out], operands, (), scratch, {})


def spread_call(cells_of, around, place, count, width):
    two, blocks, share, cells = cells_of.shape
    crops = cells // count
    stride = count + width
    total = 2 * blocks * crops * stride + width

    def kernel(cells_ref, *refs):
        out_ref, shifted = refs[-2:]
        edge = jnp.zeros((width, 3 * share), jnp.bfloat16)
        for kind in range(two):
            out_ref[kind, total - width : total, :] = edge
            for block in range(blocks):
                for crop in range(crops):
                    cell = slice(crop * count, (crop + 1) * count)
                    value = cells_ref[kind, block, :, cell].T.astype(jnp.float32)
                    before, after = neighbours(value, shifted, width)
                    at = ((place * blocks + block) * crops + crop) * stride
                    out_ref[kind, at : at + width, :] = edge
                    for side, part in enumerate((before, value, after)):
                        lanes = slice(side * share, (side + 1) * share)
                        out_ref[kind, at + width : at + stride, lanes] = part.astype(jnp.bfloat16)

    out = jax.ShapeDtypeStruct((two, total, 3 * share), jnp.bfloat16)
    scratch = [pltpu.VMEM((count + 16, share), jnp.float32)]
    operands = [cells_of] if around is None else [cells_of, around]
    aliases = {} if around is None else {1: 0}
    (spread,) = call(kernel, [out], operands, (), scratch, aliases)
    return spread


def terms_call(around, own, other, count, width, scaling):
    blocks, _, columns, cells = own.shape
    rows = around.shape[2] // 3
    stride = count + width
    crops = cells // count

    def kernel(around_ref, own_ref, other_ref, out_ref):
        for kind in range(2):
            for down in range(3):
                total = None
                for block in range(2 * blocks):
                    left = own_ref if block < blocks else other_ref
                    left = left[block % blocks, 1 - kind]
                    at = [(block * crops + k) * stride + down * width for k in range(crops)]
                    right = jnp.concatenate(
                        [around_ref[kind, start : start + count, :] for start in at], axis=0
                    )
                    term = jnp.dot(left, right, preferred_element_type=jnp.float32)
                    total = term if total is None else total + term
                total = (total * scaling).T.reshape(3, rows, columns)
                for place in range(3):
                    out_ref[kind, 3 * down + place] = total[place]

    out = jax.ShapeDtypeStruct((2, 9, rows, columns), jnp.float32)
    (terms,) = call(kernel, [out], [around, own, other], (), [], {})
    return terms


def rotated(value, axis, steps):
    count = lax.axis_size(axis)
    return lax.ppermute(value, axis, [(source, (source + steps) % count) for source in range(count)])


def crop_shards(strips, kernels, cotangent):
    sections = lax.axis_size("section")
    slabs, groups = lax.axis_size("slab"), lax.axis_size("img")
    images, strip_count, row_count, col_count, channels = strips.shape
    width = col_count * slabs
    count = row_count * width
    crops = images * strip_count // slabs
    last = sections - 1
    early, middle, late_from = min(1, last - 1), min(2, last), max(1, sections - 2)
    steps = range(1, groups)
    scaling = 1.0 / math.sqrt(images * groups * strip_count * count)

    def hop(values, source, target):
        arrived = []
        for value in values:
            arrived.append(lax.ppermute(value, "section", [(source, target)]))
        return arrived

    def shared(values, step, routes):
        pairs = [
            (place * groups + i, place * groups + (i + step) % groups)
            for place in routes
            for i in range(groups)
        ]
        return lax.ppermute(values, ("section", "img"), pairs)

    def swapped(value):
        return rotated(value, "slab", 1)

    def flipped(saved, after):
        return flip_call([(saved, (0, crop)) for crop in range(crops)], slabs, "slab", after)

    own, other = split_call(
        pltpu.with_memory_space_constraint(strips, pltpu.HBM),
        pltpu.with_memory_space_constraint(cotangent, pltpu.HBM),
        last,
    )
    other = swapped(other)
    weights = kernels[0].reshape(2, 3, 3 * channels, channels)
    weights = load_call(pltpu.with_memory_space_constraint(weights, pltpu.HBM))
    fields = join_call(own, other)
    incoming = fields
    state = []
    turned, after = None, weights
    for place in range(sections):
        outgoing = []
        for crop in range(crops):
            out, state = forward_call(
                incoming[crop], weights, state, place, crop, crops, width, place == last, after
            )
            outgoing.append(out)
        if place < last:
            incoming = hop(outgoing, place, place + 1)
        if place == early:
            inputs = flipped(state[0], state[1])
            soon = [shared(inputs, step, range(late_from)) for step in steps]
            turned = turn_call(weights, state[0])
            after = turned
    saved, hidden = state
    incoming = fields
    grads = []
    after = hidden
    for place in reversed(range(sections)):
        outgoing = []
        for crop in range(crops):
            out, grads = backward_call(
                incoming[crop], turned, hidden, grads, place, crop, crops, width, groups, after
            )
            outgoing.append(out)
        if place:
            incoming = hop(outgoing, place, place - 1)
        if place == middle:
            inputs = flipped(saved, outgoing[-1])
            late = [shared(inputs, step, range(late_from, sections)) for step in steps]
    kept, sent = grads
    own = [sent[0]]
    for step in steps:
        own.append(shared(sent[step], step, range(sections)))
    home, outer = remake_call(saved, weights, soon, late, late_from, width)
    outer = swapped(outer)
    around = spread_call(home, None, 0, count, width)
    around = spread_call(outer, around, 1, count, width)
    own = stack_call(own)
    other = swapped(own)
    terms = terms_call(around, own, other, count, width, scaling)
    own, other = part_call(kept, row_count, sent)
    other = swapped(other)
    grad_inputs = merge_call(own, other, images)
    return (terms[None], grad_inputs[None])


def shards(strips, kernels, cotangent):
    slabs, groups = lax.axis_size("slab"), lax.axis_size("img")
    strip_count, row_count, col_count, channels = strips.shape[1:]
    width = col_count * slabs
    whole_crops = strip_count % slabs == 0 and width % 16 == 0 and (row_count * width) % 128 == 0
    whole_crops = whole_crops and slabs == 2 and lax.axis_size("section") > 1
    if whole_crops and channels % (16 * slabs) == 0 and channels % (16 * groups) == 0:
        return crop_shards(strips, kernels, cotangent)
    return column_shards(strips, kernels, cotangent)


def solution(mesh):
    in_specs = (
        P("img", None, None, "slab", None),
        P("section", None, None, None, None),
        P("img", None, None, "slab", None),
    )
    out_specs = (
        P("section", None, None, "slab", "img"),
        P("section", "img", None, None, "slab", None),
    )
    return jax.shard_map(shards, mesh=mesh, in_specs=in_specs, out_specs=out_specs, check_vma=False)
```

```python
import math

import jax
import jax.numpy as jnp
from jax import lax
from jax.experimental import pallas as pl
from jax.experimental.pallas import tpu as pltpu
from jax.sharding import PartitionSpec as P


def passed_along(value, axis, steps):
    count = lax.axis_size(axis)
    initial, last = (max(0, -steps), min(count, count - steps))
    return lax.ppermute(value, axis, [(source, source + steps) for source in range(initial, last)])


def padded_2(cells, sides, width):
    for axis, dim in sides:
        count = lax.axis_size(axis)
        ends = count - 1
        head = lax.slice_in_dim(cells, 0, width, axis=dim)
        tail = lax.slice_in_dim(cells, cells.shape[dim] - width, cells.shape[dim], axis=dim)
        cells = jnp.concatenate(
            [
                lax.ppermute(tail, axis, [(i, (i + 1) % count) for i in range(ends)]),
                cells,
                lax.ppermute(head, axis, [((i + 1) % count, i) for i in range(ends)]),
            ],
            axis=dim,
        )
    return cells


def unfold(padded, row_count, col_count):
    tap_list = [
        padded[:, down_at : down_at + row_count, right_at : right_at + col_count, :]
        for down_at in range(3)
        for right_at in range(3)
    ]
    stacked = jnp.concatenate(tap_list, axis=3)
    return stacked.reshape(-1, stacked.shape[3])


def columns_of(wide_field):
    row_count = wide_field.shape[1]
    col_count = wide_field.shape[2] - 2
    padded = jnp.pad(wide_field, ((0, 0), (1, 1), (0, 0), (0, 0)))
    return unfold(padded, row_count, col_count)


def convolve(matrix, wide_field):
    count, row_count = (wide_field.shape[0], wide_field.shape[1])
    col_count = wide_field.shape[2] - 2
    flat_out = jnp.dot(columns_of(wide_field), matrix, preferred_element_type=jnp.float32)
    return flat_out.reshape(count, row_count, col_count, matrix.shape[1])


def contract(wide_field, grad_out):
    flat_grad = grad_out.reshape(-1, grad_out.shape[3])
    return lax.dot_general(
        columns_of(wide_field),
        flat_grad,
        (((0,), (0,)), ((), ())),
        preferred_element_type=jnp.float32,
    )


def silu_slope(hidden):
    sigmoid_at = jax.nn.sigmoid(hidden)
    return sigmoid_at * (1.0 + hidden * (1.0 - sigmoid_at))


def store(buffer, value, slot_index, is_valid, axis_at):
    current = lax.dynamic_index_in_dim(buffer, slot_index, axis_at, keepdims=False)
    return lax.dynamic_update_index_in_dim(
        buffer, jnp.where(is_valid, value, current), slot_index, axis_at
    )


def column_shards(strips, kernels, cotangent):
    section_count = lax.axis_size("section")
    section_index = lax.axis_index("section")
    slab_count = lax.axis_size("slab")
    slab_index = lax.axis_index("slab")
    images, strip_count, row_count, col_count, channels = strips.shape
    weights = kernels[0]
    first_forward = weights[0].reshape(9 * channels, channels)
    second_forward = weights[1].reshape(9 * channels, channels)
    first_backward = jnp.transpose(weights[0][::-1], (0, 2, 1)).reshape(9 * channels, channels)
    second_backward = jnp.transpose(weights[1][::-1], (0, 2, 1)).reshape(9 * channels, channels)
    scaling = 1.0 / math.sqrt(
        images * lax.axis_size("img") * strip_count * row_count * col_count * slab_count
    )
    position = slab_index * col_count - 1 + jnp.arange(col_count + 2, dtype=jnp.int32)
    inside = ((position >= 0) & (position < slab_count * col_count))[None, None, :, None]
    tick_count = strip_count + section_count - 1
    hidden_cols = col_count + 2
    empty_field = jnp.zeros((images, row_count, col_count, channels), jnp.bfloat16)
    saved_field = jnp.zeros((strip_count, images, row_count, col_count + 2, channels), jnp.bfloat16)
    saved_hidden = jnp.zeros((strip_count, images, row_count, hidden_cols, channels), jnp.float32)
    saved_active = jnp.zeros(
        (strip_count, images, row_count, col_count + 2, channels), jnp.bfloat16
    )
    outgoing = empty_field
    for step_no in range(tick_count):
        micro_index = step_no - section_index
        is_valid = (micro_index >= 0) & (micro_index < strip_count)
        slot_index = jnp.clip(micro_index, 0, strip_count - 1)
        if step_no == 0:
            incoming = empty_field
        else:
            incoming = passed_along(outgoing, "section", 1)
        first_strip = lax.dynamic_index_in_dim(strips, slot_index, 1, keepdims=False)
        field_in = jnp.where(section_index == 0, first_strip, incoming)
        wide_deep = padded_2(field_in, (("slab", 2),), 2)
        hidden = convolve(first_forward, wide_deep)
        wide_active = jnp.where(inside, jax.nn.silu(hidden), 0.0).astype(jnp.bfloat16)
        wide_field = wide_deep[:, :, 1:-1, :]
        outgoing = (field_in.astype(jnp.float32) + convolve(second_forward, wide_active)).astype(
            jnp.bfloat16
        )
        saved_field = store(saved_field, wide_field, slot_index, is_valid, 0)
        saved_hidden = store(saved_hidden, hidden, slot_index, is_valid, 0)
        saved_active = store(saved_active, wide_active, slot_index, is_valid, 0)
    grad_slots = jnp.zeros((images, strip_count, row_count, col_count, channels), jnp.bfloat16)
    saved_grad_out = jnp.zeros((strip_count, images, row_count, col_count, channels), jnp.bfloat16)
    saved_grad_hidden = jnp.zeros(
        (strip_count, images, row_count, col_count, channels), jnp.bfloat16
    )
    sending = empty_field
    for step_no in range(tick_count):
        micro_index = step_no - (section_count - 1 - section_index)
        is_valid = (micro_index >= 0) & (micro_index < strip_count)
        slot_index = jnp.clip(micro_index, 0, strip_count - 1)
        if step_no == 0:
            arriving = empty_field
        else:
            arriving = passed_along(sending, "section", -1)
        top_grad = lax.dynamic_index_in_dim(cotangent, slot_index, 1, keepdims=False)
        grad_out = jnp.where(section_index == section_count - 1, top_grad, arriving)
        grad_out = jnp.where(is_valid, grad_out, jnp.zeros_like(grad_out))
        hidden = lax.dynamic_index_in_dim(saved_hidden, slot_index, 0, keepdims=False)
        wide_grad = padded_2(grad_out, (("slab", 2),), 2)
        grad_active = convolve(second_backward, wide_grad)
        wide_hidden_grad = jnp.where(inside, grad_active * silu_slope(hidden), 0.0).astype(
            jnp.bfloat16
        )
        grad_hidden = wide_hidden_grad[:, :, 1:-1, :]
        sending = (
            grad_out.astype(jnp.float32) + convolve(first_backward, wide_hidden_grad)
        ).astype(jnp.bfloat16)
        saved_grad_out = store(saved_grad_out, grad_out, slot_index, is_valid, 0)
        saved_grad_hidden = store(saved_grad_hidden, grad_hidden, slot_index, is_valid, 0)
        grad_slots = store(grad_slots, sending, slot_index, is_valid, 1)
    flat_count = strip_count * images
    lower_part = contract(
        saved_field.reshape(flat_count, row_count, col_count + 2, channels),
        saved_grad_hidden.reshape(flat_count, row_count, col_count, channels),
    )
    upper_part = contract(
        saved_active.reshape(flat_count, row_count, col_count + 2, channels),
        saved_grad_out.reshape(flat_count, row_count, col_count, channels),
    )
    grad_terms = jnp.stack([lower_part, upper_part]).reshape(2, 9, channels, channels)
    row_share = lax.psum_scatter(
        grad_terms.astype(jnp.bfloat16), "slab", scatter_dimension=2, tiled=True
    )
    own_share = lax.psum_scatter(row_share, "img", scatter_dimension=3, tiled=True).astype(
        jnp.float32
    )
    grad_kernels = (own_share * scaling)[None]
    return (grad_kernels, grad_slots[None])


def call(kernel, outs, operands, unread, scratch, aliases, apart=()):
    spaces = {**dict.fromkeys(unread, pl.ANY), **dict.fromkeys(apart, pltpu.HBM)}
    return pl.pallas_call(
        kernel,
        out_shape=outs,
        in_specs=[
            pl.BlockSpec(memory_space=spaces.get(place, pltpu.VMEM))
            for place in range(len(operands))
        ],
        out_specs=[pl.BlockSpec(memory_space=pltpu.VMEM)] * len(outs),
        scratch_shapes=scratch,
        input_output_aliases=aliases,
        compiler_params=pltpu.CompilerParams(vmem_limit_bytes=8 << 20),
    )(*operands)


def neighbours(value, shifted, width):
    count, channels = value.shape
    shifted[8 : 8 + count, :] = value
    column = lax.rem(lax.broadcasted_iota(jnp.int32, (count, channels), 0), width)
    before = jnp.where(column == 0, 0.0, shifted[7 : 7 + count, :])
    after = jnp.where(column == width - 1, 0.0, shifted[9 : 9 + count, :])
    return before, after


def convolved(value, matrix, taps, shifted, width):
    count, channels = value.shape
    before, after = neighbours(value, shifted, width)
    for place, part in enumerate((before, value, after)):
        taps[width : width + count, place * channels : (place + 1) * channels] = part.astype(
            jnp.bfloat16
        )
    edge = jnp.zeros((width, 3 * channels), jnp.bfloat16)
    taps[0:width, :] = edge
    taps[width + count : 2 * width + count, :] = edge
    total = jnp.dot(taps[0:count, :], matrix[0], preferred_element_type=jnp.float32)
    for down in (1, 2):
        total = total + jnp.dot(
            taps[down * width : down * width + count, :],
            matrix[down],
            preferred_element_type=jnp.float32,
        )
    return total


def forward_call(field, weights, state, section, crop, crops, width, last, after):
    count, channels = field.shape

    def kernel(field_ref, weights_ref, after_ref, *refs):
        *_, saved_ref, hidden_ref, taps, shifted = refs

        @pl.when(lax.axis_index("section") == section)
        def _():
            field_in = field_ref[...]
            wide = field_in.astype(jnp.float32)
            saved_ref[0, crop] = field_in
            hidden = convolved(wide, weights_ref.at[0], taps, shifted, width)
            hidden_ref[crop] = hidden
            active = (hidden * jax.nn.sigmoid(hidden)).astype(jnp.bfloat16)
            saved_ref[1, crop] = active
            if not last:
                added = convolved(
                    active.astype(jnp.float32), weights_ref.at[1], taps, shifted, width
                )
                refs[-5][...] = (wide + added).astype(jnp.bfloat16)

    outs = [
        jax.ShapeDtypeStruct((count, channels), jnp.bfloat16),
        jax.ShapeDtypeStruct((2, crops, count, channels), jnp.bfloat16),
        jax.ShapeDtypeStruct((crops, count, channels), jnp.float32),
    ][1 if last else 0 :]
    scratch = [
        pltpu.VMEM((count + 2 * width, 3 * channels), jnp.bfloat16),
        pltpu.VMEM((count + 16, channels), jnp.float32),
    ]
    aliases = {3 + k: k + (0 if last else 1) for k in range(len(state))}
    outputs = call(kernel, outs, [field, weights, after, *state], (2,), scratch, aliases)
    return (None if last else outputs[0]), outputs[-2:]


def backward_call(
    grad, turned, hidden, state, section, crop, crops, width, parts, after
):
    count, channels = grad.shape
    share = channels // parts
    first = section == 0

    def kernel(grad_ref, turned_ref, hidden_ref, after_ref, *refs):
        *_, kept_ref, sent_ref, taps, shifted = refs

        @pl.when(lax.axis_index("section") == section)
        def _():
            wide = grad_ref[...].astype(jnp.float32)
            own = lax.axis_index("img")
            place_parts(sent_ref, (0,), grad_ref[...], crop, parts, own)
            grad_active = convolved(wide, turned_ref.at[1], taps, shifted, width)
            hidden = hidden_ref[crop]
            gate = jax.nn.sigmoid(hidden)
            grad_hidden = (grad_active * (gate * (1.0 + hidden * (1.0 - gate)))).astype(
                jnp.bfloat16
            )
            place_parts(sent_ref, (1,), grad_hidden, crop, parts, own)
            added = convolved(
                grad_hidden.astype(jnp.float32), turned_ref.at[0], taps, shifted, width
            )
            result = (wide + added).astype(jnp.bfloat16)
            kept_ref[crop] = result
            if not first:
                refs[-5][...] = result

    outs = [
        jax.ShapeDtypeStruct((count, channels), jnp.bfloat16),
        jax.ShapeDtypeStruct((crops, count, channels), jnp.bfloat16),
        jax.ShapeDtypeStruct((parts, 2, share, crops * count), jnp.bfloat16),
    ][1 if first else 0 :]
    scratch = [
        pltpu.VMEM((count + 2 * width, 3 * channels), jnp.bfloat16),
        pltpu.VMEM((count + 16, channels), jnp.float32),
    ]
    aliases = {4 + k: k + (0 if first else 1) for k in range(len(state))}
    operands = [grad, turned, hidden, after, *state]
    outputs = call(kernel, outs, operands, (3,), scratch, aliases)
    return (None if first else outputs[0]), outputs[-2:]


def place_parts(target, lead, value, crop, parts, own):
    count, channels = value.shape
    share = channels // parts
    flipped = value.T
    for part in range(parts):
        slot = lax.rem(part + parts - own, parts)
        target[(slot, *lead, slice(None), slice(crop * count, (crop + 1) * count))] = flipped[
            part * share : (part + 1) * share, :
        ]


def flip_call(kept, parts, axis, after):
    def kernel(*refs):
        flipped_ref = refs[-1]
        for crop, (place, index) in enumerate(kept):
            value = refs[place][index]
            place_parts(flipped_ref, (), value, crop, parts, lax.axis_index(axis))

    operands = []
    for array, index in kept:
        if all(array is not other for other in operands):
            operands.append(array)
    kept = [
        ([array is other for other in operands].index(True), index) for array, index in kept
    ]
    count, channels = operands[0].shape[-2:]
    out = jax.ShapeDtypeStruct((parts, channels // parts, len(kept) * count), operands[0].dtype)
    (flipped,) = call(kernel, [out], [*operands, after], (len(operands),), [], {})
    return flipped


def turn_call(weights, after):
    two, _, _, channels = weights.shape

    def kernel(weights_ref, after_ref, turned_ref):
        for which in range(two):
            for tap in range(9):
                down, right = divmod(tap, 3)
                flipped = weights_ref[which, down, right * channels : (right + 1) * channels, :].T
                down, right = divmod(8 - tap, 3)
                turned_ref[which, down, right * channels : (right + 1) * channels, :] = flipped

    out = jax.ShapeDtypeStruct(weights.shape, weights.dtype)
    (turned,) = call(kernel, [out], [weights, after], (1,), [], {})
    return turned


def split_call(strips, cotangent, last):
    images, strip_count, rows, cols, channels = strips.shape
    share = strip_count // 2

    def kernel(strips_ref, cotangent_ref, own_ref, other_ref, sems):
        own = lax.axis_index("slab")
        is_last = lax.axis_index("section") == last

        def fetch(source_ref):
            copies = []
            for image in range(images):
                at = pl.ds(image * share, share)
                for side, (ref, half) in enumerate(((own_ref, own), (other_ref, 1 - own))):
                    source = source_ref.at[image, pl.ds(half * share, share)]
                    copies.append(pltpu.make_async_copy(source, ref.at[at], sems.at[2 * image + side]))
            for copy in copies:
                copy.start()
            for copy in copies:
                copy.wait()

        @pl.when(is_last)
        def _():
            fetch(cotangent_ref)

        @pl.when(jnp.logical_not(is_last))
        def _():
            fetch(strips_ref)

    out = jax.ShapeDtypeStruct((images * share, rows, cols, channels), strips.dtype)
    sems = [pltpu.SemaphoreType.DMA((2 * images,))]
    return call(kernel, [out, out], [strips, cotangent], (), sems, {}, (0, 1))


def load_call(weights):
    def kernel(weights_ref, out_ref, sems):
        copies = [
            pltpu.make_async_copy(weights_ref.at[which], out_ref.at[which], sems.at[which])
            for which in range(2)
        ]
        for copy in copies:
            copy.start()
        for copy in copies:
            copy.wait()

    out = jax.ShapeDtypeStruct(weights.shape, weights.dtype)
    sems = [pltpu.SemaphoreType.DMA((2,))]
    (loaded,) = call(kernel, [out], [weights], (), sems, {}, (0,))
    return loaded


def join_call(own, other):
    crops, rows, cols, channels = own.shape

    def kernel(own_ref, other_ref, *out_refs):
        is_left = lax.axis_index("slab") == 0
        for crop, out_ref in enumerate(out_refs):
            mine = own_ref[crop].astype(jnp.float32)
            theirs = other_ref[crop].astype(jnp.float32)
            left = jnp.where(is_left, mine, theirs)
            right = jnp.where(is_left, theirs, mine)
            whole = jnp.concatenate([left, right], axis=1)
            out_ref[...] = whole.reshape(rows * 2 * cols, channels).astype(jnp.bfloat16)

    out = jax.ShapeDtypeStruct((rows * 2 * cols, channels), own.dtype)
    return call(kernel, [out] * crops, [own, other], (), [], {})


def part_call(kept, rows, after):
    crops, count, channels = kept.shape
    cols = count // rows // 2

    def kernel(kept_ref, after_ref, own_ref, other_ref):
        is_left = lax.axis_index("slab") == 0
        for crop in range(crops):
            whole = kept_ref[crop].astype(jnp.float32).reshape(rows, 2 * cols, channels)
            left, right = whole[:, :cols], whole[:, cols:]
            own_ref[crop] = jnp.where(is_left, left, right).astype(jnp.bfloat16)
            other_ref[crop] = jnp.where(is_left, right, left).astype(jnp.bfloat16)

    out = jax.ShapeDtypeStruct((crops, rows, cols, channels), kept.dtype)
    return call(kernel, [out, out], [kept, after], (1,), [], {})


def merge_call(own, other, images):
    crops, rows, cols, channels = own.shape
    share = crops // images

    def kernel(own_ref, other_ref, out_ref):
        place = lax.axis_index("slab")
        for image in range(images):
            for crop in range(share):
                out_ref[image, place * share + crop] = own_ref[image * share + crop]
                out_ref[image, (1 - place) * share + crop] = other_ref[image * share + crop]

    out = jax.ShapeDtypeStruct((images, 2 * share, rows, cols, channels), own.dtype)
    (merged,) = call(kernel, [out], [own, other], (), [], {})
    return merged


def stack_call(blocks):
    def kernel(*refs):
        for place in range(len(blocks)):
            refs[-1][place] = refs[place][...]

    out = jax.ShapeDtypeStruct((len(blocks), *blocks[0].shape), blocks[0].dtype)
    (stacked,) = call(kernel, [out], [*blocks], (), [], {})
    return stacked


def remake_call(saved, weights, blocks, width, sections):
    _, crops, count, channels = saved.shape
    share = channels // 2
    each = len(blocks)

    def kernel(saved_ref, weights_ref, *refs):
        home_ref, outer_ref, taps, shifted = refs[-4:]
        is_left = lax.axis_index("slab") == 0
        section = lax.axis_index("section")

        def put(kind, block, crop, value):
            cells = slice(crop * count, (crop + 1) * count)
            flipped = value.T
            low, high = flipped[:share], flipped[share:]
            home_ref[kind, block, :, cells] = jnp.where(is_left, low, high)
            outer_ref[kind, block, :, cells] = jnp.where(is_left, high, low)

        @pl.when((section >= sections[0]) & (section <= sections[1]))
        def _():
            for crop in range(crops):
                for kind in range(2):
                    put(kind, 0, crop, saved_ref[kind, crop])
            for block in range(each):
                home_ref[0, 1 + block] = refs[block][0]
                outer_ref[0, 1 + block] = refs[block][1]
                for crop in range(crops):
                    cells = slice(crop * count, (crop + 1) * count)
                    mine, theirs = refs[block][0, :, cells], refs[block][1, :, cells]
                    low, high = jnp.where(is_left, mine, theirs), jnp.where(is_left, theirs, mine)
                    field = jnp.concatenate([low, high], axis=0).T.astype(jnp.float32)
                    hidden = convolved(field, weights_ref.at[0], taps, shifted, width)
                    active = (hidden * jax.nn.sigmoid(hidden)).astype(jnp.bfloat16)
                    put(1, 1 + block, crop, active)

    out = jax.ShapeDtypeStruct((2, 1 + each, share, crops * count), saved.dtype)
    scratch = [
        pltpu.VMEM((count + 2 * width, 3 * channels), jnp.bfloat16),
        pltpu.VMEM((count + 16, channels), jnp.float32),
    ]
    return call(kernel, [out, out], [saved, weights, *blocks], (), scratch, {})


def spread_call(cells_of, around, place, count, width, sections):
    two, blocks, share, cells = cells_of.shape
    crops = cells // count
    stride = count + width
    total = 2 * blocks * crops * stride + width

    def kernel(cells_ref, *refs):
        out_ref, done_ref, shifted = refs[-3:]
        section = lax.axis_index("section")
        done_ref[...] = jnp.zeros_like(done_ref)

        @pl.when((section >= sections[0]) & (section <= sections[1]))
        def _():
            edge = jnp.zeros((width, 3 * share), jnp.bfloat16)
            for kind in range(two):
                out_ref[kind, total - width : total, :] = edge
                for block in range(blocks):
                    for crop in range(crops):
                        cell = slice(crop * count, (crop + 1) * count)
                        value = cells_ref[kind, block, :, cell].T.astype(jnp.float32)
                        before, after = neighbours(value, shifted, width)
                        at = ((place * blocks + block) * crops + crop) * stride
                        out_ref[kind, at : at + width, :] = edge
                        for side, part in enumerate((before, value, after)):
                            lanes = slice(side * share, (side + 1) * share)
                            out_ref[kind, at + width : at + stride, lanes] = part.astype(
                                jnp.bfloat16
                            )

    out = jax.ShapeDtypeStruct((two, total, 3 * share), jnp.bfloat16)
    scratch = [pltpu.VMEM((count + 16, share), jnp.float32)]
    operands = [cells_of] if around is None else [cells_of, around]
    aliases = {} if around is None else {1: 0}
    token = jax.ShapeDtypeStruct((8, 128), jnp.float32)
    return call(kernel, [out, token], operands, (), scratch, aliases)


def terms_call(around, own, other, count, width, scaling):
    blocks, _, columns, cells = own.shape
    rows = around.shape[2] // 3
    stride = count + width
    crops = cells // count

    def kernel(around_ref, own_ref, other_ref, out_ref):
        for kind in range(2):
            for down in range(3):
                total = None
                for block in range(2 * blocks):
                    left = own_ref if block < blocks else other_ref
                    left = left[block % blocks, 1 - kind]
                    at = [(block * crops + k) * stride + down * width for k in range(crops)]
                    right = jnp.concatenate(
                        [around_ref[kind, start : start + count, :] for start in at], axis=0
                    )
                    term = jnp.dot(left, right, preferred_element_type=jnp.float32)
                    total = term if total is None else total + term
                total = (total * scaling).T.reshape(3, rows, columns)
                for place in range(3):
                    out_ref[kind, 3 * down + place] = total[place]

    out = jax.ShapeDtypeStruct((2, 9, rows, columns), jnp.float32)
    (terms,) = call(kernel, [out], [around, own, other], (), [], {})
    return terms


def rotated(value, axis, steps):
    count = lax.axis_size(axis)
    return lax.ppermute(value, axis, [(source, (source + steps) % count) for source in range(count)])


def crop_shards(strips, kernels, cotangent):
    sections = lax.axis_size("section")
    slabs, groups = lax.axis_size("slab"), lax.axis_size("img")
    images, strip_count, row_count, col_count, channels = strips.shape
    width = col_count * slabs
    count = row_count * width
    crops = images * strip_count // slabs
    last = sections - 1
    early = min(1, last - 1)
    steps = range(1, groups)
    scaling = 1.0 / math.sqrt(images * groups * strip_count * count)

    def hop(values, source, target):
        arrived = []
        for value in values:
            arrived.append(lax.ppermute(value, "section", [(source, target)]))
        return arrived

    def shared(values, step, routes):
        pairs = [
            (place * groups + i, place * groups + (i + step) % groups)
            for place in routes
            for i in range(groups)
        ]
        return lax.ppermute(values, ("section", "img"), pairs)

    def swapped(value):
        return rotated(value, "slab", 1)

    def flipped(saved, after):
        return flip_call([(saved, (0, crop)) for crop in range(crops)], slabs, "slab", after)

    own, other = split_call(
        pltpu.with_memory_space_constraint(strips, pltpu.HBM),
        pltpu.with_memory_space_constraint(cotangent, pltpu.HBM),
        last,
    )
    other = swapped(other)
    weights = kernels[0].reshape(2, 3, 3 * channels, channels)
    weights = load_call(pltpu.with_memory_space_constraint(weights, pltpu.HBM))
    fields = join_call(own, other)
    incoming = fields
    state = []
    turned, after = None, weights
    for place in range(sections):
        outgoing = []
        for crop in range(crops):
            out, state = forward_call(
                incoming[crop], weights, state, place, crop, crops, width, place == last, after
            )
            outgoing.append(out)
        if place < last:
            incoming = hop(outgoing, place, place + 1)
        if place == early:
            inputs = flipped(state[0], state[1])
            soon = [shared(inputs, step, [0]) for step in steps]
            turned = turn_call(weights, state[0])
            after = turned
    saved, hidden = state
    incoming = fields
    grads = []
    after = hidden
    for place in reversed(range(sections)):
        outgoing = []
        for crop in range(crops):
            out, grads = backward_call(
                incoming[crop], turned, hidden, grads, place, crop, crops, width, groups, after
            )
            outgoing.append(out)
        if place:
            incoming = hop(outgoing, place, place - 1)
        if place == last:
            inputs = flipped(saved, outgoing[-1])
            late = [shared(inputs, step, range(sections)) for step in steps]
        if place == 1:
            home, outer = remake_call(saved, weights, soon, width, (0, 0))
            outer = swapped(outer)
            around, after = spread_call(home, None, 0, count, width, (0, 0))
            around, after = spread_call(outer, around, 1, count, width, (0, 0))
    kept, sent = grads
    own = [sent[0]]
    for step in steps:
        own.append(shared(sent[step], step, range(sections)))
    home, outer = remake_call(saved, weights, late, width, (1, last))
    outer = swapped(outer)
    around, _ = spread_call(home, around, 0, count, width, (1, last))
    around, _ = spread_call(outer, around, 1, count, width, (1, last))
    own = stack_call(own)
    other = swapped(own)
    terms = terms_call(around, own, other, count, width, scaling)
    own, other = part_call(kept, row_count, sent)
    other = swapped(other)
    grad_inputs = merge_call(own, other, images)
    return (terms[None], grad_inputs[None])


def shards(strips, kernels, cotangent):
    slabs, groups = lax.axis_size("slab"), lax.axis_size("img")
    strip_count, row_count, col_count, channels = strips.shape[1:]
    width = col_count * slabs
    whole_crops = strip_count % slabs == 0 and width % 16 == 0 and (row_count * width) % 128 == 0
    whole_crops = whole_crops and slabs == 2 and lax.axis_size("section") > 1
    if whole_crops and channels % (16 * slabs) == 0 and channels % (16 * groups) == 0:
        return crop_shards(strips, kernels, cotangent)
    return column_shards(strips, kernels, cotangent)


def solution(mesh):
    in_specs = (
        P("img", None, None, "slab", None),
        P("section", None, None, None, None),
        P("img", None, None, "slab", None),
    )
    out_specs = (
        P("section", None, None, "slab", "img"),
        P("section", "img", None, None, "slab", None),
    )
    return jax.shard_map(shards, mesh=mesh, in_specs=in_specs, out_specs=out_specs, check_vma=False)
```

```python
import math

import jax
import jax.numpy as jnp
from jax import lax
from jax.experimental import pallas as pl
from jax.experimental.pallas import tpu as pltpu
from jax.sharding import PartitionSpec as P


def passed_along(value, axis, steps):
    count = lax.axis_size(axis)
    initial, last = (max(0, -steps), min(count, count - steps))
    return lax.ppermute(value, axis, [(source, source + steps) for source in range(initial, last)])


def padded_2(cells, sides, width):
    for axis, dim in sides:
        count = lax.axis_size(axis)
        ends = count - 1
        head = lax.slice_in_dim(cells, 0, width, axis=dim)
        tail = lax.slice_in_dim(cells, cells.shape[dim] - width, cells.shape[dim], axis=dim)
        cells = jnp.concatenate(
            [
                lax.ppermute(tail, axis, [(i, (i + 1) % count) for i in range(ends)]),
                cells,
                lax.ppermute(head, axis, [((i + 1) % count, i) for i in range(ends)]),
            ],
            axis=dim,
        )
    return cells


def unfold(padded, row_count, col_count):
    tap_list = [
        padded[:, down_at : down_at + row_count, right_at : right_at + col_count, :]
        for down_at in range(3)
        for right_at in range(3)
    ]
    stacked = jnp.concatenate(tap_list, axis=3)
    return stacked.reshape(-1, stacked.shape[3])


def columns_of(wide_field):
    row_count = wide_field.shape[1]
    col_count = wide_field.shape[2] - 2
    padded = jnp.pad(wide_field, ((0, 0), (1, 1), (0, 0), (0, 0)))
    return unfold(padded, row_count, col_count)


def convolve(matrix, wide_field):
    count, row_count = (wide_field.shape[0], wide_field.shape[1])
    col_count = wide_field.shape[2] - 2
    flat_out = jnp.dot(columns_of(wide_field), matrix, preferred_element_type=jnp.float32)
    return flat_out.reshape(count, row_count, col_count, matrix.shape[1])


def contract(wide_field, grad_out):
    flat_grad = grad_out.reshape(-1, grad_out.shape[3])
    return lax.dot_general(
        columns_of(wide_field),
        flat_grad,
        (((0,), (0,)), ((), ())),
        preferred_element_type=jnp.float32,
    )


def silu_slope(hidden):
    sigmoid_at = jax.nn.sigmoid(hidden)
    return sigmoid_at * (1.0 + hidden * (1.0 - sigmoid_at))


def store(buffer, value, slot_index, is_valid, axis_at):
    current = lax.dynamic_index_in_dim(buffer, slot_index, axis_at, keepdims=False)
    return lax.dynamic_update_index_in_dim(
        buffer, jnp.where(is_valid, value, current), slot_index, axis_at
    )


def column_shards(strips, kernels, cotangent):
    section_count = lax.axis_size("section")
    section_index = lax.axis_index("section")
    slab_count = lax.axis_size("slab")
    slab_index = lax.axis_index("slab")
    images, strip_count, row_count, col_count, channels = strips.shape
    weights = kernels[0]
    first_forward = weights[0].reshape(9 * channels, channels)
    second_forward = weights[1].reshape(9 * channels, channels)
    first_backward = jnp.transpose(weights[0][::-1], (0, 2, 1)).reshape(9 * channels, channels)
    second_backward = jnp.transpose(weights[1][::-1], (0, 2, 1)).reshape(9 * channels, channels)
    scaling = 1.0 / math.sqrt(
        images * lax.axis_size("img") * strip_count * row_count * col_count * slab_count
    )
    position = slab_index * col_count - 1 + jnp.arange(col_count + 2, dtype=jnp.int32)
    inside = ((position >= 0) & (position < slab_count * col_count))[None, None, :, None]
    tick_count = strip_count + section_count - 1
    hidden_cols = col_count + 2
    empty_field = jnp.zeros((images, row_count, col_count, channels), jnp.bfloat16)
    saved_field = jnp.zeros((strip_count, images, row_count, col_count + 2, channels), jnp.bfloat16)
    saved_hidden = jnp.zeros((strip_count, images, row_count, hidden_cols, channels), jnp.float32)
    saved_active = jnp.zeros(
        (strip_count, images, row_count, col_count + 2, channels), jnp.bfloat16
    )
    outgoing = empty_field
    for step_no in range(tick_count):
        micro_index = step_no - section_index
        is_valid = (micro_index >= 0) & (micro_index < strip_count)
        slot_index = jnp.clip(micro_index, 0, strip_count - 1)
        if step_no == 0:
            incoming = empty_field
        else:
            incoming = passed_along(outgoing, "section", 1)
        first_strip = lax.dynamic_index_in_dim(strips, slot_index, 1, keepdims=False)
        field_in = jnp.where(section_index == 0, first_strip, incoming)
        wide_deep = padded_2(field_in, (("slab", 2),), 2)
        hidden = convolve(first_forward, wide_deep)
        wide_active = jnp.where(inside, jax.nn.silu(hidden), 0.0).astype(jnp.bfloat16)
        wide_field = wide_deep[:, :, 1:-1, :]
        outgoing = (field_in.astype(jnp.float32) + convolve(second_forward, wide_active)).astype(
            jnp.bfloat16
        )
        saved_field = store(saved_field, wide_field, slot_index, is_valid, 0)
        saved_hidden = store(saved_hidden, hidden, slot_index, is_valid, 0)
        saved_active = store(saved_active, wide_active, slot_index, is_valid, 0)
    grad_slots = jnp.zeros((images, strip_count, row_count, col_count, channels), jnp.bfloat16)
    saved_grad_out = jnp.zeros((strip_count, images, row_count, col_count, channels), jnp.bfloat16)
    saved_grad_hidden = jnp.zeros(
        (strip_count, images, row_count, col_count, channels), jnp.bfloat16
    )
    sending = empty_field
    for step_no in range(tick_count):
        micro_index = step_no - (section_count - 1 - section_index)
        is_valid = (micro_index >= 0) & (micro_index < strip_count)
        slot_index = jnp.clip(micro_index, 0, strip_count - 1)
        if step_no == 0:
            arriving = empty_field
        else:
            arriving = passed_along(sending, "section", -1)
        top_grad = lax.dynamic_index_in_dim(cotangent, slot_index, 1, keepdims=False)
        grad_out = jnp.where(section_index == section_count - 1, top_grad, arriving)
        grad_out = jnp.where(is_valid, grad_out, jnp.zeros_like(grad_out))
        hidden = lax.dynamic_index_in_dim(saved_hidden, slot_index, 0, keepdims=False)
        wide_grad = padded_2(grad_out, (("slab", 2),), 2)
        grad_active = convolve(second_backward, wide_grad)
        wide_hidden_grad = jnp.where(inside, grad_active * silu_slope(hidden), 0.0).astype(
            jnp.bfloat16
        )
        grad_hidden = wide_hidden_grad[:, :, 1:-1, :]
        sending = (
            grad_out.astype(jnp.float32) + convolve(first_backward, wide_hidden_grad)
        ).astype(jnp.bfloat16)
        saved_grad_out = store(saved_grad_out, grad_out, slot_index, is_valid, 0)
        saved_grad_hidden = store(saved_grad_hidden, grad_hidden, slot_index, is_valid, 0)
        grad_slots = store(grad_slots, sending, slot_index, is_valid, 1)
    flat_count = strip_count * images
    lower_part = contract(
        saved_field.reshape(flat_count, row_count, col_count + 2, channels),
        saved_grad_hidden.reshape(flat_count, row_count, col_count, channels),
    )
    upper_part = contract(
        saved_active.reshape(flat_count, row_count, col_count + 2, channels),
        saved_grad_out.reshape(flat_count, row_count, col_count, channels),
    )
    grad_terms = jnp.stack([lower_part, upper_part]).reshape(2, 9, channels, channels)
    row_share = lax.psum_scatter(
        grad_terms.astype(jnp.bfloat16), "slab", scatter_dimension=2, tiled=True
    )
    own_share = lax.psum_scatter(row_share, "img", scatter_dimension=3, tiled=True).astype(
        jnp.float32
    )
    grad_kernels = (own_share * scaling)[None]
    return (grad_kernels, grad_slots[None])


def call(kernel, outs, operands, unread, scratch, aliases, apart=()):
    spaces = {**dict.fromkeys(unread, pl.ANY), **dict.fromkeys(apart, pltpu.HBM)}
    return pl.pallas_call(
        kernel,
        out_shape=outs,
        in_specs=[
            pl.BlockSpec(memory_space=spaces.get(place, pltpu.VMEM))
            for place in range(len(operands))
        ],
        out_specs=[pl.BlockSpec(memory_space=pltpu.VMEM)] * len(outs),
        scratch_shapes=scratch,
        input_output_aliases=aliases,
        compiler_params=pltpu.CompilerParams(vmem_limit_bytes=8 << 20),
    )(*operands)


def half_lanes(count, channels):
    return channels % 128 == 64 and count % 32 == 0


def packed_shape(count, channels):
    return (count * channels // 128, 128) if half_lanes(count, channels) else (count, channels)


def pack(value):
    count, channels = value.shape
    if not half_lanes(count, channels):
        return value
    parts = [value[:, at : at + 128] for at in range(0, channels - 64, 128)]
    rest = value[:, channels - 64 :]
    parts.append(jnp.concatenate([rest[: count // 2], rest[count // 2 :]], axis=1))
    return jnp.concatenate(parts, axis=0)


def unpack(value, count, channels):
    if not half_lanes(count, channels):
        return value
    whole = channels // 128
    parts = [value[k * count : (k + 1) * count] for k in range(whole)]
    rest = value[whole * count :]
    parts.append(jnp.concatenate([rest[:, :64], rest[:, 64:]], axis=0))
    return jnp.concatenate(parts, axis=1)


def neighbours(value, shifted, width):
    count, channels = value.shape
    shifted[8 : 8 + count, :] = value
    column = lax.rem(lax.broadcasted_iota(jnp.int32, (count, channels), 0), width)
    before = jnp.where(column == 0, 0.0, shifted[7 : 7 + count, :])
    after = jnp.where(column == width - 1, 0.0, shifted[9 : 9 + count, :])
    return before, after


def convolved(value, matrix, taps, shifted, width):
    count, channels = value.shape
    before, after = neighbours(value, shifted, width)
    for place, part in enumerate((before, value, after)):
        taps[width : width + count, place * channels : (place + 1) * channels] = part.astype(
            jnp.bfloat16
        )
    edge = jnp.zeros((width, 3 * channels), jnp.bfloat16)
    taps[0:width, :] = edge
    taps[width + count : 2 * width + count, :] = edge
    total = jnp.dot(taps[0:count, :], matrix[0], preferred_element_type=jnp.float32)
    for down in (1, 2):
        total = total + jnp.dot(
            taps[down * width : down * width + count, :],
            matrix[down],
            preferred_element_type=jnp.float32,
        )
    return total


def forward_call(field, weights, state, section, crop, crops, shape, width, last, after):
    count, channels = shape

    def kernel(field_ref, weights_ref, after_ref, *refs):
        *_, saved_ref, hidden_ref, taps, shifted = refs

        @pl.when(lax.axis_index("section") == section)
        def _():
            field_in = field_ref[...]
            if section:
                field_in = unpack(field_in, count, channels)
            wide = field_in.astype(jnp.float32)
            saved_ref[0, crop] = field_in
            hidden = convolved(wide, weights_ref.at[0], taps, shifted, width)
            hidden_ref[crop] = hidden
            active = (hidden * jax.nn.sigmoid(hidden)).astype(jnp.bfloat16)
            saved_ref[1, crop] = active
            if not last:
                added = convolved(
                    active.astype(jnp.float32), weights_ref.at[1], taps, shifted, width
                )
                refs[-5][...] = pack((wide + added).astype(jnp.bfloat16))

    outs = [
        jax.ShapeDtypeStruct(packed_shape(count, channels), jnp.bfloat16),
        jax.ShapeDtypeStruct((2, crops, count, channels), jnp.bfloat16),
        jax.ShapeDtypeStruct((crops, count, channels), jnp.float32),
    ][1 if last else 0 :]
    scratch = [
        pltpu.VMEM((count + 2 * width, 3 * channels), jnp.bfloat16),
        pltpu.VMEM((count + 16, channels), jnp.float32),
    ]
    aliases = {3 + k: k + (0 if last else 1) for k in range(len(state))}
    outputs = call(kernel, outs, [field, weights, after, *state], (2,), scratch, aliases)
    return (None if last else outputs[0]), outputs[-2:]


def backward_call(
    grad, turned, hidden, state, section, crop, crops, shape, width, last, parts, after
):
    count, channels = shape
    share = channels // parts
    first = section == 0

    def kernel(grad_ref, turned_ref, hidden_ref, after_ref, *refs):
        *_, kept_ref, sent_ref, taps, shifted = refs

        @pl.when(lax.axis_index("section") == section)
        def _():
            grad = grad_ref[...]
            if not last:
                grad = unpack(grad, count, channels)
            wide = grad.astype(jnp.float32)
            own = lax.axis_index("img")
            place_parts(sent_ref, (0,), grad, crop, parts, own)
            grad_active = convolved(wide, turned_ref.at[1], taps, shifted, width)
            hidden = hidden_ref[crop]
            gate = jax.nn.sigmoid(hidden)
            grad_hidden = (grad_active * (gate * (1.0 + hidden * (1.0 - gate)))).astype(
                jnp.bfloat16
            )
            place_parts(sent_ref, (1,), grad_hidden, crop, parts, own)
            added = convolved(
                grad_hidden.astype(jnp.float32), turned_ref.at[0], taps, shifted, width
            )
            result = (wide + added).astype(jnp.bfloat16)
            kept_ref[crop] = result
            if not first:
                refs[-5][...] = pack(result)

    outs = [
        jax.ShapeDtypeStruct(packed_shape(count, channels), jnp.bfloat16),
        jax.ShapeDtypeStruct((crops, count, channels), jnp.bfloat16),
        jax.ShapeDtypeStruct((parts, 2, share, crops * count), jnp.bfloat16),
    ][1 if first else 0 :]
    scratch = [
        pltpu.VMEM((count + 2 * width, 3 * channels), jnp.bfloat16),
        pltpu.VMEM((count + 16, channels), jnp.float32),
    ]
    aliases = {4 + k: k + (0 if first else 1) for k in range(len(state))}
    operands = [grad, turned, hidden, after, *state]
    outputs = call(kernel, outs, operands, (3,), scratch, aliases)
    return (None if first else outputs[0]), outputs[-2:]


def place_parts(target, lead, value, crop, parts, own):
    count, channels = value.shape
    share = channels // parts
    flipped = value.T
    for part in range(parts):
        slot = lax.rem(part + parts - own, parts)
        target[(slot, *lead, slice(None), slice(crop * count, (crop + 1) * count))] = flipped[
            part * share : (part + 1) * share, :
        ]


def flip_call(kept, parts, axis, after):
    def kernel(*refs):
        flipped_ref = refs[-1]
        for crop, (place, index) in enumerate(kept):
            value = refs[place][index]
            place_parts(flipped_ref, (), value, crop, parts, lax.axis_index(axis))

    operands = []
    for array, index in kept:
        if all(array is not other for other in operands):
            operands.append(array)
    kept = [
        ([array is other for other in operands].index(True), index) for array, index in kept
    ]
    count, channels = operands[0].shape[-2:]
    out = jax.ShapeDtypeStruct((parts, channels // parts, len(kept) * count), operands[0].dtype)
    (flipped,) = call(kernel, [out], [*operands, after], (len(operands),), [], {})
    return flipped


def turn_call(weights, after):
    two, _, _, channels = weights.shape

    def kernel(weights_ref, after_ref, turned_ref):
        for which in range(two):
            for tap in range(9):
                down, right = divmod(tap, 3)
                flipped = weights_ref[which, down, right * channels : (right + 1) * channels, :].T
                down, right = divmod(8 - tap, 3)
                turned_ref[which, down, right * channels : (right + 1) * channels, :] = flipped

    out = jax.ShapeDtypeStruct(weights.shape, weights.dtype)
    (turned,) = call(kernel, [out], [weights, after], (1,), [], {})
    return turned


def split_call(strips, cotangent, last):
    images, strip_count, rows, cols, channels = strips.shape
    share = strip_count // 2

    def kernel(strips_ref, cotangent_ref, own_ref, other_ref, sems):
        own = lax.axis_index("slab")
        is_last = lax.axis_index("section") == last

        def fetch(source_ref):
            copies = []
            for image in range(images):
                at = pl.ds(image * share, share)
                for side, (ref, half) in enumerate(((own_ref, own), (other_ref, 1 - own))):
                    source = source_ref.at[image, pl.ds(half * share, share)]
                    copies.append(pltpu.make_async_copy(source, ref.at[at], sems.at[2 * image + side]))
            for copy in copies:
                copy.start()
            for copy in copies:
                copy.wait()

        @pl.when(is_last)
        def _():
            fetch(cotangent_ref)

        @pl.when(jnp.logical_not(is_last))
        def _():
            fetch(strips_ref)

    out = jax.ShapeDtypeStruct((images * share, rows, cols, channels), strips.dtype)
    sems = [pltpu.SemaphoreType.DMA((2 * images,))]
    return call(kernel, [out, out], [strips, cotangent], (), sems, {}, (0, 1))


def load_call(weights, first, after):
    def kernel(weights_ref, after_ref, *refs):
        out_ref, sems = refs[-2:]

        @pl.when((lax.axis_index("section") == 0) | (not first))
        def _():
            copies = [
                pltpu.make_async_copy(weights_ref.at[which], out_ref.at[which], sems.at[which])
                for which in range(2)
            ]
            for copy in copies:
                copy.start()
            for copy in copies:
                copy.wait()

    out = jax.ShapeDtypeStruct(weights.shape, weights.dtype)
    sems = [pltpu.SemaphoreType.DMA((2,))]
    (loaded,) = call(kernel, [out], [weights, after], (1,), sems, {}, (0,))
    return loaded


def join_call(own, other):
    crops, rows, cols, channels = own.shape

    def kernel(own_ref, other_ref, *out_refs):
        is_left = lax.axis_index("slab") == 0
        for crop, out_ref in enumerate(out_refs):
            mine = own_ref[crop].astype(jnp.float32)
            theirs = other_ref[crop].astype(jnp.float32)
            left = jnp.where(is_left, mine, theirs)
            right = jnp.where(is_left, theirs, mine)
            whole = jnp.concatenate([left, right], axis=1)
            out_ref[...] = whole.reshape(rows * 2 * cols, channels).astype(jnp.bfloat16)

    out = jax.ShapeDtypeStruct((rows * 2 * cols, channels), own.dtype)
    return call(kernel, [out] * crops, [own, other], (), [], {})


def part_call(kept, rows, after):
    crops, count, channels = kept.shape
    cols = count // rows // 2

    def kernel(kept_ref, after_ref, own_ref, other_ref):
        is_left = lax.axis_index("slab") == 0
        for crop in range(crops):
            whole = kept_ref[crop].astype(jnp.float32).reshape(rows, 2 * cols, channels)
            left, right = whole[:, :cols], whole[:, cols:]
            own_ref[crop] = jnp.where(is_left, left, right).astype(jnp.bfloat16)
            other_ref[crop] = jnp.where(is_left, right, left).astype(jnp.bfloat16)

    out = jax.ShapeDtypeStruct((crops, rows, cols, channels), kept.dtype)
    return call(kernel, [out, out], [kept, after], (1,), [], {})


def merge_call(own, other, images):
    crops, rows, cols, channels = own.shape
    share = crops // images

    def kernel(own_ref, other_ref, out_ref):
        place = lax.axis_index("slab")
        for image in range(images):
            for crop in range(share):
                out_ref[image, place * share + crop] = own_ref[image * share + crop]
                out_ref[image, (1 - place) * share + crop] = other_ref[image * share + crop]

    out = jax.ShapeDtypeStruct((images, 2 * share, rows, cols, channels), own.dtype)
    (merged,) = call(kernel, [out], [own, other], (), [], {})
    return merged


def stack_call(blocks):
    def kernel(*refs):
        for place in range(len(blocks)):
            refs[-1][place] = refs[place][...]

    out = jax.ShapeDtypeStruct((len(blocks), *blocks[0].shape), blocks[0].dtype)
    (stacked,) = call(kernel, [out], [*blocks], (), [], {})
    return stacked


def remake_call(saved, weights, blocks, width, sections):
    _, crops, count, channels = saved.shape
    share = channels // 2
    each = len(blocks)

    def kernel(saved_ref, weights_ref, *refs):
        home_ref, outer_ref, taps, shifted = refs[-4:]
        is_left = lax.axis_index("slab") == 0
        section = lax.axis_index("section")

        def put(kind, block, crop, value):
            cells = slice(crop * count, (crop + 1) * count)
            flipped = value.T
            low, high = flipped[:share], flipped[share:]
            home_ref[kind, block, :, cells] = jnp.where(is_left, low, high)
            outer_ref[kind, block, :, cells] = jnp.where(is_left, high, low)

        @pl.when((section >= sections[0]) & (section <= sections[1]))
        def _():
            for crop in range(crops):
                for kind in range(2):
                    put(kind, 0, crop, saved_ref[kind, crop])
            for block in range(each):
                home_ref[0, 1 + block] = refs[block][0]
                outer_ref[0, 1 + block] = refs[block][1]
                for crop in range(crops):
                    cells = slice(crop * count, (crop + 1) * count)
                    mine, theirs = refs[block][0, :, cells], refs[block][1, :, cells]
                    low, high = jnp.where(is_left, mine, theirs), jnp.where(is_left, theirs, mine)
                    field = jnp.concatenate([low, high], axis=0).T.astype(jnp.float32)
                    hidden = convolved(field, weights_ref.at[0], taps, shifted, width)
                    active = (hidden * jax.nn.sigmoid(hidden)).astype(jnp.bfloat16)
                    put(1, 1 + block, crop, active)

    out = jax.ShapeDtypeStruct((2, 1 + each, share, crops * count), saved.dtype)
    scratch = [
        pltpu.VMEM((count + 2 * width, 3 * channels), jnp.bfloat16),
        pltpu.VMEM((count + 16, channels), jnp.float32),
    ]
    return call(kernel, [out, out], [saved, weights, *blocks], (), scratch, {})


def spread_call(cells_of, around, place, count, width, sections, marked=False):
    two, blocks, share, cells = cells_of.shape
    crops = cells // count
    stride = count + width
    total = 2 * blocks * crops * stride + width

    def kernel(cells_ref, *refs):
        out_ref, shifted = refs[-3 if marked else -2], refs[-1]
        section = lax.axis_index("section")
        if marked:
            refs[-2][...] = jnp.zeros_like(refs[-2])

        @pl.when((section >= sections[0]) & (section <= sections[1]))
        def _():
            edge = jnp.zeros((width, 3 * share), jnp.bfloat16)
            for kind in range(two):
                out_ref[kind, total - width : total, :] = edge
                for block in range(blocks):
                    for crop in range(crops):
                        cell = slice(crop * count, (crop + 1) * count)
                        value = cells_ref[kind, block, :, cell].T.astype(jnp.float32)
                        before, after = neighbours(value, shifted, width)
                        at = ((place * blocks + block) * crops + crop) * stride
                        out_ref[kind, at : at + width, :] = edge
                        for side, part in enumerate((before, value, after)):
                            lanes = slice(side * share, (side + 1) * share)
                            out_ref[kind, at + width : at + stride, lanes] = part.astype(
                                jnp.bfloat16
                            )

    out = jax.ShapeDtypeStruct((two, total, 3 * share), jnp.bfloat16)
    scratch = [pltpu.VMEM((count + 16, share), jnp.float32)]
    operands = [cells_of] if around is None else [cells_of, around]
    aliases = {} if around is None else {1: 0}
    token = jax.ShapeDtypeStruct((8, 128), jnp.float32)
    outs = [out, token] if marked else [out]
    return call(kernel, outs, operands, (), scratch, aliases)


def terms_call(around, own, other, count, width, scaling):
    blocks, _, columns, cells = own.shape
    rows = around.shape[2] // 3
    stride = count + width
    crops = cells // count

    def kernel(around_ref, own_ref, other_ref, out_ref, held, sems):
        copies = []
        for kind in (1, 0):
            for down in range(3):
                total = None
                for block in range(2 * blocks):
                    left = own_ref if block < blocks else other_ref
                    left = left[block % blocks, 1 - kind]
                    at = [(block * crops + k) * stride + down * width for k in range(crops)]
                    right = jnp.concatenate(
                        [around_ref[kind, start : start + count, :] for start in at], axis=0
                    )
                    term = jnp.dot(left, right, preferred_element_type=jnp.float32)
                    total = term if total is None else total + term
                total = (total * scaling).T.reshape(3, rows, columns)
                third = pl.ds(3 * down, 3)
                for place in range(3):
                    held[kind, 3 * down + place] = total[place]
                copy = pltpu.make_async_copy(
                    held.at[kind, third], out_ref.at[kind, third], sems.at[3 * kind + down]
                )
                copy.start()
                copies.append(copy)
        for copy in copies:
            copy.wait()

    shape = (2, 9, rows, columns)
    return pl.pallas_call(
        kernel,
        out_shape=jax.ShapeDtypeStruct(shape, jnp.float32),
        in_specs=[pl.BlockSpec(memory_space=pltpu.VMEM)] * 3,
        out_specs=pl.BlockSpec(memory_space=pltpu.HBM),
        scratch_shapes=[pltpu.VMEM(shape, jnp.float32), pltpu.SemaphoreType.DMA((6,))],
        compiler_params=pltpu.CompilerParams(vmem_limit_bytes=8 << 20),
        name="terms",
    )(around, own, other)


def rotated(value, axis, steps):
    count = lax.axis_size(axis)
    return lax.ppermute(value, axis, [(source, (source + steps) % count) for source in range(count)])


def crop_shards(strips, kernels, cotangent):
    sections = lax.axis_size("section")
    slabs, groups = lax.axis_size("slab"), lax.axis_size("img")
    images, strip_count, row_count, col_count, channels = strips.shape
    width = col_count * slabs
    count = row_count * width
    crops = images * strip_count // slabs
    shape = (count, channels)
    last = sections - 1
    early = min(1, last - 1)
    steps = range(1, groups)
    scaling = 1.0 / math.sqrt(images * groups * strip_count * count)

    def hop(values, source, target):
        arrived = []
        for value in values:
            arrived.append(lax.ppermute(value, "section", [(source, target)]))
        return arrived

    def shared(values, step, routes):
        pairs = [
            (place * groups + i, place * groups + (i + step) % groups)
            for place in routes
            for i in range(groups)
        ]
        return lax.ppermute(values, ("section", "img"), pairs)

    def swapped(value):
        return rotated(value, "slab", 1)

    def flipped(saved, after):
        return flip_call([(saved, (0, crop)) for crop in range(crops)], slabs, "slab", after)

    own, other = split_call(
        pltpu.with_memory_space_constraint(strips, pltpu.HBM),
        pltpu.with_memory_space_constraint(cotangent, pltpu.HBM),
        last,
    )
    other = swapped(other)
    weights = kernels[0].reshape(2, 3, 3 * channels, channels)
    stored = pltpu.with_memory_space_constraint(weights, pltpu.HBM)
    weights = load_call(stored, True, own)
    fields = join_call(own, other)
    incoming = fields
    state = []
    turned, after = None, weights
    for place in range(sections):
        outgoing = []
        for crop in range(crops):
            out, state = forward_call(
                incoming[crop], weights, state, place, crop, crops, shape, width, place == last, after
            )
            outgoing.append(out)
        if place == 0:
            weights = load_call(stored, False, state[0])
        if place < last:
            incoming = hop(outgoing, place, place + 1)
        if place == early:
            inputs = flipped(state[0], state[1])
            soon = [shared(inputs, step, [0]) for step in steps]
            turned = turn_call(weights, state[0])
            after = turned
    saved, hidden = state
    incoming = fields
    grads = []
    after = hidden
    for place in reversed(range(sections)):
        outgoing = []
        for crop in range(crops):
            out, grads = backward_call(
                incoming[crop],
                turned,
                hidden,
                grads,
                place,
                crop,
                crops,
                shape,
                width,
                place == last,
                groups,
                after,
            )
            outgoing.append(out)
        if place:
            incoming = hop(outgoing, place, place - 1)
        if place == last:
            inputs = flipped(saved, outgoing[-1])
            late = [shared(inputs, step, range(sections)) for step in steps]
        if place == 1:
            home, outer = remake_call(saved, weights, soon, width, (0, 0))
            outer = lax.ppermute(
                outer, ("section", "slab"), [(i, (i + 1) % slabs) for i in range(slabs)]
            )
            (around,) = spread_call(home, None, 0, count, width, (0, 0))
            around, after = spread_call(outer, around, 1, count, width, (0, 0), True)
    kept, sent = grads
    own = [sent[0]]
    for step in steps:
        own.append(shared(sent[step], step, range(sections)))
    home, outer = remake_call(saved, weights, late, width, (1, last))
    outer = swapped(outer)
    (around,) = spread_call(home, around, 0, count, width, (1, last))
    (around,) = spread_call(outer, around, 1, count, width, (1, last))
    own = stack_call(own)
    other = swapped(own)
    terms = terms_call(around, own, other, count, width, scaling)
    own, other = part_call(kept, row_count, sent)
    other = swapped(other)
    grad_inputs = merge_call(own, other, images)
    return (terms[None], grad_inputs[None])


def shards(strips, kernels, cotangent):
    slabs, groups = lax.axis_size("slab"), lax.axis_size("img")
    strip_count, row_count, col_count, channels = strips.shape[1:]
    width = col_count * slabs
    whole_crops = strip_count % slabs == 0 and width % 16 == 0 and (row_count * width) % 128 == 0
    whole_crops = whole_crops and slabs == 2 and lax.axis_size("section") > 1
    if whole_crops and channels % (16 * slabs) == 0 and channels % (16 * groups) == 0:
        return crop_shards(strips, kernels, cotangent)
    return column_shards(strips, kernels, cotangent)


def solution(mesh):
    in_specs = (
        P("img", None, None, "slab", None),
        P("section", None, None, None, None),
        P("img", None, None, "slab", None),
    )
    out_specs = (
        P("section", None, None, "slab", "img"),
        P("section", "img", None, None, "slab", None),
    )
    return jax.shard_map(shards, mesh=mesh, in_specs=in_specs, out_specs=out_specs, check_vma=False)
```

```python
import math

import jax
import jax.numpy as jnp
from jax import lax
from jax.experimental import pallas as pl
from jax.experimental.pallas import tpu as pltpu
from jax.sharding import PartitionSpec as P


def passed_along(value, axis, steps):
    count = lax.axis_size(axis)
    initial, last = (max(0, -steps), min(count, count - steps))
    return lax.ppermute(value, axis, [(source, source + steps) for source in range(initial, last)])


def padded_2(cells, sides, width):
    for axis, dim in sides:
        count = lax.axis_size(axis)
        ends = count - 1
        head = lax.slice_in_dim(cells, 0, width, axis=dim)
        tail = lax.slice_in_dim(cells, cells.shape[dim] - width, cells.shape[dim], axis=dim)
        cells = jnp.concatenate(
            [
                lax.ppermute(tail, axis, [(i, (i + 1) % count) for i in range(ends)]),
                cells,
                lax.ppermute(head, axis, [((i + 1) % count, i) for i in range(ends)]),
            ],
            axis=dim,
        )
    return cells


def unfold(padded, row_count, col_count):
    tap_list = [
        padded[:, down_at : down_at + row_count, right_at : right_at + col_count, :]
        for down_at in range(3)
        for right_at in range(3)
    ]
    stacked = jnp.concatenate(tap_list, axis=3)
    return stacked.reshape(-1, stacked.shape[3])


def columns_of(wide_field):
    row_count = wide_field.shape[1]
    col_count = wide_field.shape[2] - 2
    padded = jnp.pad(wide_field, ((0, 0), (1, 1), (0, 0), (0, 0)))
    return unfold(padded, row_count, col_count)


def convolve(matrix, wide_field):
    count, row_count = (wide_field.shape[0], wide_field.shape[1])
    col_count = wide_field.shape[2] - 2
    flat_out = jnp.dot(columns_of(wide_field), matrix, preferred_element_type=jnp.float32)
    return flat_out.reshape(count, row_count, col_count, matrix.shape[1])


def contract(wide_field, grad_out):
    flat_grad = grad_out.reshape(-1, grad_out.shape[3])
    return lax.dot_general(
        columns_of(wide_field),
        flat_grad,
        (((0,), (0,)), ((), ())),
        preferred_element_type=jnp.float32,
    )


def silu_slope(hidden):
    sigmoid_at = jax.nn.sigmoid(hidden)
    return sigmoid_at * (1.0 + hidden * (1.0 - sigmoid_at))


def store(buffer, value, slot_index, is_valid, axis_at):
    current = lax.dynamic_index_in_dim(buffer, slot_index, axis_at, keepdims=False)
    return lax.dynamic_update_index_in_dim(
        buffer, jnp.where(is_valid, value, current), slot_index, axis_at
    )


def column_shards(strips, kernels, cotangent):
    section_count = lax.axis_size("section")
    section_index = lax.axis_index("section")
    slab_count = lax.axis_size("slab")
    slab_index = lax.axis_index("slab")
    images, strip_count, row_count, col_count, channels = strips.shape
    weights = kernels[0]
    first_forward = weights[0].reshape(9 * channels, channels)
    second_forward = weights[1].reshape(9 * channels, channels)
    first_backward = jnp.transpose(weights[0][::-1], (0, 2, 1)).reshape(9 * channels, channels)
    second_backward = jnp.transpose(weights[1][::-1], (0, 2, 1)).reshape(9 * channels, channels)
    scaling = 1.0 / math.sqrt(
        images * lax.axis_size("img") * strip_count * row_count * col_count * slab_count
    )
    position = slab_index * col_count - 1 + jnp.arange(col_count + 2, dtype=jnp.int32)
    inside = ((position >= 0) & (position < slab_count * col_count))[None, None, :, None]
    tick_count = strip_count + section_count - 1
    hidden_cols = col_count + 2
    empty_field = jnp.zeros((images, row_count, col_count, channels), jnp.bfloat16)
    saved_field = jnp.zeros((strip_count, images, row_count, col_count + 2, channels), jnp.bfloat16)
    saved_hidden = jnp.zeros((strip_count, images, row_count, hidden_cols, channels), jnp.float32)
    saved_active = jnp.zeros(
        (strip_count, images, row_count, col_count + 2, channels), jnp.bfloat16
    )
    outgoing = empty_field
    for step_no in range(tick_count):
        micro_index = step_no - section_index
        is_valid = (micro_index >= 0) & (micro_index < strip_count)
        slot_index = jnp.clip(micro_index, 0, strip_count - 1)
        if step_no == 0:
            incoming = empty_field
        else:
            incoming = passed_along(outgoing, "section", 1)
        first_strip = lax.dynamic_index_in_dim(strips, slot_index, 1, keepdims=False)
        field_in = jnp.where(section_index == 0, first_strip, incoming)
        wide_deep = padded_2(field_in, (("slab", 2),), 2)
        hidden = convolve(first_forward, wide_deep)
        wide_active = jnp.where(inside, jax.nn.silu(hidden), 0.0).astype(jnp.bfloat16)
        wide_field = wide_deep[:, :, 1:-1, :]
        outgoing = (field_in.astype(jnp.float32) + convolve(second_forward, wide_active)).astype(
            jnp.bfloat16
        )
        saved_field = store(saved_field, wide_field, slot_index, is_valid, 0)
        saved_hidden = store(saved_hidden, hidden, slot_index, is_valid, 0)
        saved_active = store(saved_active, wide_active, slot_index, is_valid, 0)
    grad_slots = jnp.zeros((images, strip_count, row_count, col_count, channels), jnp.bfloat16)
    saved_grad_out = jnp.zeros((strip_count, images, row_count, col_count, channels), jnp.bfloat16)
    saved_grad_hidden = jnp.zeros(
        (strip_count, images, row_count, col_count, channels), jnp.bfloat16
    )
    sending = empty_field
    for step_no in range(tick_count):
        micro_index = step_no - (section_count - 1 - section_index)
        is_valid = (micro_index >= 0) & (micro_index < strip_count)
        slot_index = jnp.clip(micro_index, 0, strip_count - 1)
        if step_no == 0:
            arriving = empty_field
        else:
            arriving = passed_along(sending, "section", -1)
        top_grad = lax.dynamic_index_in_dim(cotangent, slot_index, 1, keepdims=False)
        grad_out = jnp.where(section_index == section_count - 1, top_grad, arriving)
        grad_out = jnp.where(is_valid, grad_out, jnp.zeros_like(grad_out))
        hidden = lax.dynamic_index_in_dim(saved_hidden, slot_index, 0, keepdims=False)
        wide_grad = padded_2(grad_out, (("slab", 2),), 2)
        grad_active = convolve(second_backward, wide_grad)
        wide_hidden_grad = jnp.where(inside, grad_active * silu_slope(hidden), 0.0).astype(
            jnp.bfloat16
        )
        grad_hidden = wide_hidden_grad[:, :, 1:-1, :]
        sending = (
            grad_out.astype(jnp.float32) + convolve(first_backward, wide_hidden_grad)
        ).astype(jnp.bfloat16)
        saved_grad_out = store(saved_grad_out, grad_out, slot_index, is_valid, 0)
        saved_grad_hidden = store(saved_grad_hidden, grad_hidden, slot_index, is_valid, 0)
        grad_slots = store(grad_slots, sending, slot_index, is_valid, 1)
    flat_count = strip_count * images
    lower_part = contract(
        saved_field.reshape(flat_count, row_count, col_count + 2, channels),
        saved_grad_hidden.reshape(flat_count, row_count, col_count, channels),
    )
    upper_part = contract(
        saved_active.reshape(flat_count, row_count, col_count + 2, channels),
        saved_grad_out.reshape(flat_count, row_count, col_count, channels),
    )
    grad_terms = jnp.stack([lower_part, upper_part]).reshape(2, 9, channels, channels)
    row_share = lax.psum_scatter(
        grad_terms.astype(jnp.bfloat16), "slab", scatter_dimension=2, tiled=True
    )
    own_share = lax.psum_scatter(row_share, "img", scatter_dimension=3, tiled=True).astype(
        jnp.float32
    )
    grad_kernels = (own_share * scaling)[None]
    return (grad_kernels, grad_slots[None])


def call(kernel, outs, operands, unread, scratch, aliases, apart=()):
    spaces = {**dict.fromkeys(unread, pl.ANY), **dict.fromkeys(apart, pltpu.HBM)}
    return pl.pallas_call(
        kernel,
        out_shape=outs,
        in_specs=[
            pl.BlockSpec(memory_space=spaces.get(place, pltpu.VMEM))
            for place in range(len(operands))
        ],
        out_specs=[pl.BlockSpec(memory_space=pltpu.VMEM)] * len(outs),
        scratch_shapes=scratch,
        input_output_aliases=aliases,
        compiler_params=pltpu.CompilerParams(vmem_limit_bytes=8 << 20),
    )(*operands)


def half_lanes(count, channels):
    return channels % 128 == 64 and count % 32 == 0


def packed_shape(count, channels):
    return (count * channels // 128, 128) if half_lanes(count, channels) else (count, channels)


def pack(value):
    count, channels = value.shape
    if not half_lanes(count, channels):
        return value
    parts = [value[:, at : at + 128] for at in range(0, channels - 64, 128)]
    rest = value[:, channels - 64 :]
    parts.append(jnp.concatenate([rest[: count // 2], rest[count // 2 :]], axis=1))
    return jnp.concatenate(parts, axis=0)


def unpack(value, count, channels):
    if not half_lanes(count, channels):
        return value
    whole = channels // 128
    parts = [value[k * count : (k + 1) * count] for k in range(whole)]
    rest = value[whole * count :]
    parts.append(jnp.concatenate([rest[:, :64], rest[:, 64:]], axis=0))
    return jnp.concatenate(parts, axis=1)


def neighbours(value, shifted, width):
    count, channels = value.shape
    shifted[8 : 8 + count, :] = value
    column = lax.rem(lax.broadcasted_iota(jnp.int32, (count, channels), 0), width)
    before = jnp.where(column == 0, 0.0, shifted[7 : 7 + count, :])
    after = jnp.where(column == width - 1, 0.0, shifted[9 : 9 + count, :])
    return before, after


def convolved(value, matrix, taps, shifted, width):
    count, channels = value.shape
    before, after = neighbours(value, shifted, width)
    for place, part in enumerate((before, value, after)):
        taps[width : width + count, place * channels : (place + 1) * channels] = part.astype(
            jnp.bfloat16
        )
    edge = jnp.zeros((width, 3 * channels), jnp.bfloat16)
    taps[0:width, :] = edge
    taps[width + count : 2 * width + count, :] = edge
    total = jnp.dot(taps[0:count, :], matrix[0], preferred_element_type=jnp.float32)
    for down in (1, 2):
        total = total + jnp.dot(
            taps[down * width : down * width + count, :],
            matrix[down],
            preferred_element_type=jnp.float32,
        )
    return total


def forward_call(field, weights, state, section, crop, crops, shape, width, last, after):
    count, channels = shape

    def kernel(field_ref, weights_ref, after_ref, *refs):
        *_, saved_ref, hidden_ref, taps, shifted = refs

        @pl.when(lax.axis_index("section") == section)
        def _():
            field_in = field_ref[...]
            if section:
                field_in = unpack(field_in, count, channels)
            wide = field_in.astype(jnp.float32)
            saved_ref[0, crop] = field_in
            hidden = convolved(wide, weights_ref.at[0], taps, shifted, width)
            hidden_ref[crop] = hidden
            active = (hidden * jax.nn.sigmoid(hidden)).astype(jnp.bfloat16)
            saved_ref[1, crop] = active
            if not last:
                added = convolved(
                    active.astype(jnp.float32), weights_ref.at[1], taps, shifted, width
                )
                refs[-5][...] = pack((wide + added).astype(jnp.bfloat16))

    outs = [
        jax.ShapeDtypeStruct(packed_shape(count, channels), jnp.bfloat16),
        jax.ShapeDtypeStruct((2, crops, count, channels), jnp.bfloat16),
        jax.ShapeDtypeStruct((crops, count, channels), jnp.float32),
    ][1 if last else 0 :]
    scratch = [
        pltpu.VMEM((count + 2 * width, 3 * channels), jnp.bfloat16),
        pltpu.VMEM((count + 16, channels), jnp.float32),
    ]
    aliases = {3 + k: k + (0 if last else 1) for k in range(len(state))}
    outputs = call(kernel, outs, [field, weights, after, *state], (2,), scratch, aliases)
    return (None if last else outputs[0]), outputs[-2:]


def backward_call(
    grad, turned, hidden, state, section, crop, crops, shape, width, last, parts, after
):
    count, channels = shape
    share = channels // parts
    first = section == 0

    def kernel(grad_ref, turned_ref, hidden_ref, after_ref, *refs):
        *_, kept_ref, sent_ref, taps, shifted = refs

        @pl.when(lax.axis_index("section") == section)
        def _():
            grad = grad_ref[...]
            if not last:
                grad = unpack(grad, count, channels)
            wide = grad.astype(jnp.float32)
            own = lax.axis_index("img")
            place_parts(sent_ref, (0,), grad, crop, parts, own)
            grad_active = convolved(wide, turned_ref.at[1], taps, shifted, width)
            hidden = hidden_ref[crop]
            gate = jax.nn.sigmoid(hidden)
            grad_hidden = (grad_active * (gate * (1.0 + hidden * (1.0 - gate)))).astype(
                jnp.bfloat16
            )
            place_parts(sent_ref, (1,), grad_hidden, crop, parts, own)
            added = convolved(
                grad_hidden.astype(jnp.float32), turned_ref.at[0], taps, shifted, width
            )
            result = (wide + added).astype(jnp.bfloat16)
            kept_ref[crop] = result
            if not first:
                refs[-5][...] = pack(result)

    outs = [
        jax.ShapeDtypeStruct(packed_shape(count, channels), jnp.bfloat16),
        jax.ShapeDtypeStruct((crops, count, channels), jnp.bfloat16),
        jax.ShapeDtypeStruct((parts, 2, share, crops * count), jnp.bfloat16),
    ][1 if first else 0 :]
    scratch = [
        pltpu.VMEM((count + 2 * width, 3 * channels), jnp.bfloat16),
        pltpu.VMEM((count + 16, channels), jnp.float32),
    ]
    aliases = {4 + k: k + (0 if first else 1) for k in range(len(state))}
    operands = [grad, turned, hidden, after, *state]
    outputs = call(kernel, outs, operands, (3,), scratch, aliases)
    return (None if first else outputs[0]), outputs[-2:]


def place_parts(target, lead, value, crop, parts, own):
    count, channels = value.shape
    share = channels // parts
    flipped = value.T
    for part in range(parts):
        slot = lax.rem(part + parts - own, parts)
        target[(slot, *lead, slice(None), slice(crop * count, (crop + 1) * count))] = flipped[
            part * share : (part + 1) * share, :
        ]


def flip_call(kept, parts, axis, after):
    def kernel(*refs):
        flipped_ref = refs[-1]
        for crop, (place, index) in enumerate(kept):
            value = refs[place][index]
            place_parts(flipped_ref, (), value, crop, parts, lax.axis_index(axis))

    operands = []
    for array, index in kept:
        if all(array is not other for other in operands):
            operands.append(array)
    kept = [
        ([array is other for other in operands].index(True), index) for array, index in kept
    ]
    count, channels = operands[0].shape[-2:]
    out = jax.ShapeDtypeStruct((parts, channels // parts, len(kept) * count), operands[0].dtype)
    (flipped,) = call(kernel, [out], [*operands, after], (len(operands),), [], {})
    return flipped


def turn_call(weights, after):
    two, _, _, channels = weights.shape

    def kernel(weights_ref, after_ref, turned_ref):
        for which in range(two):
            for tap in range(9):
                down, right = divmod(tap, 3)
                flipped = weights_ref[which, down, right * channels : (right + 1) * channels, :].T
                down, right = divmod(8 - tap, 3)
                turned_ref[which, down, right * channels : (right + 1) * channels, :] = flipped

    out = jax.ShapeDtypeStruct(weights.shape, weights.dtype)
    (turned,) = call(kernel, [out], [weights, after], (1,), [], {})
    return turned


def split_call(strips, cotangent, last):
    images, strip_count, rows, cols, channels = strips.shape
    share = strip_count // 2

    def kernel(strips_ref, cotangent_ref, own_ref, other_ref, sems):
        own = lax.axis_index("slab")
        is_last = lax.axis_index("section") == last

        def fetch(source_ref):
            copies = []
            for image in range(images):
                at = pl.ds(image * share, share)
                for side, (ref, half) in enumerate(((own_ref, own), (other_ref, 1 - own))):
                    source = source_ref.at[image, pl.ds(half * share, share)]
                    copies.append(pltpu.make_async_copy(source, ref.at[at], sems.at[2 * image + side]))
            for copy in copies:
                copy.start()
            for copy in copies:
                copy.wait()

        @pl.when(is_last)
        def _():
            fetch(cotangent_ref)

        @pl.when(jnp.logical_not(is_last))
        def _():
            fetch(strips_ref)

    out = jax.ShapeDtypeStruct((images * share, rows, cols, channels), strips.dtype)
    sems = [pltpu.SemaphoreType.DMA((2 * images,))]
    return call(kernel, [out, out], [strips, cotangent], (), sems, {}, (0, 1))


def load_call(weights, first, after):
    def kernel(weights_ref, after_ref, *refs):
        out_ref, sems = refs[-2:]

        @pl.when((lax.axis_index("section") == 0) | (not first))
        def _():
            copies = [
                pltpu.make_async_copy(weights_ref.at[which], out_ref.at[which], sems.at[which])
                for which in range(2)
            ]
            for copy in copies:
                copy.start()
            for copy in copies:
                copy.wait()

    out = jax.ShapeDtypeStruct(weights.shape, weights.dtype)
    sems = [pltpu.SemaphoreType.DMA((2,))]
    (loaded,) = call(kernel, [out], [weights, after], (1,), sems, {}, (0,))
    return loaded


def join_call(own, other):
    crops, rows, cols, channels = own.shape

    def kernel(own_ref, other_ref, *out_refs):
        is_left = lax.axis_index("slab") == 0
        for crop, out_ref in enumerate(out_refs):
            mine = own_ref[crop].astype(jnp.float32)
            theirs = other_ref[crop].astype(jnp.float32)
            left = jnp.where(is_left, mine, theirs)
            right = jnp.where(is_left, theirs, mine)
            whole = jnp.concatenate([left, right], axis=1)
            out_ref[...] = whole.reshape(rows * 2 * cols, channels).astype(jnp.bfloat16)

    out = jax.ShapeDtypeStruct((rows * 2 * cols, channels), own.dtype)
    return call(kernel, [out] * crops, [own, other], (), [], {})


def part_call(kept, rows, after):
    crops, count, channels = kept.shape
    cols = count // rows // 2

    def kernel(kept_ref, after_ref, own_ref, other_ref):
        is_left = lax.axis_index("slab") == 0
        for crop in range(crops):
            whole = kept_ref[crop].astype(jnp.float32).reshape(rows, 2 * cols, channels)
            left, right = whole[:, :cols], whole[:, cols:]
            own_ref[crop] = jnp.where(is_left, left, right).astype(jnp.bfloat16)
            other_ref[crop] = jnp.where(is_left, right, left).astype(jnp.bfloat16)

    out = jax.ShapeDtypeStruct((crops, rows, cols, channels), kept.dtype)
    return call(kernel, [out, out], [kept, after], (1,), [], {})


def merge_call(own, other, images):
    crops, rows, cols, channels = own.shape
    share = crops // images

    def kernel(own_ref, other_ref, out_ref):
        place = lax.axis_index("slab")
        for image in range(images):
            for crop in range(share):
                out_ref[image, place * share + crop] = own_ref[image * share + crop]
                out_ref[image, (1 - place) * share + crop] = other_ref[image * share + crop]

    out = jax.ShapeDtypeStruct((images, 2 * share, rows, cols, channels), own.dtype)
    (merged,) = call(kernel, [out], [own, other], (), [], {})
    return merged


def stack_call(blocks):
    def kernel(*refs):
        for place in range(len(blocks)):
            refs[-1][place] = refs[place][...]

    out = jax.ShapeDtypeStruct((len(blocks), *blocks[0].shape), blocks[0].dtype)
    (stacked,) = call(kernel, [out], [*blocks], (), [], {})
    return stacked


def remake_call(saved, weights, blocks, width, sections):
    _, crops, count, channels = saved.shape
    share = channels // 2
    each = len(blocks)

    def kernel(saved_ref, weights_ref, *refs):
        home_ref, outer_ref, taps, shifted = refs[-4:]
        is_left = lax.axis_index("slab") == 0
        section = lax.axis_index("section")

        def put(kind, block, crop, value):
            cells = slice(crop * count, (crop + 1) * count)
            flipped = value.T
            low, high = flipped[:share], flipped[share:]
            home_ref[kind, block, :, cells] = jnp.where(is_left, low, high)
            outer_ref[kind, block, :, cells] = jnp.where(is_left, high, low)

        @pl.when((section >= sections[0]) & (section <= sections[1]))
        def _():
            for crop in range(crops):
                for kind in range(2):
                    put(kind, 0, crop, saved_ref[kind, crop])
            for block in range(each):
                home_ref[0, 1 + block] = refs[block][0]
                outer_ref[0, 1 + block] = refs[block][1]
                for crop in range(crops):
                    cells = slice(crop * count, (crop + 1) * count)
                    mine, theirs = refs[block][0, :, cells], refs[block][1, :, cells]
                    low, high = jnp.where(is_left, mine, theirs), jnp.where(is_left, theirs, mine)
                    field = jnp.concatenate([low, high], axis=0).T.astype(jnp.float32)
                    hidden = convolved(field, weights_ref.at[0], taps, shifted, width)
                    active = (hidden * jax.nn.sigmoid(hidden)).astype(jnp.bfloat16)
                    put(1, 1 + block, crop, active)

    out = jax.ShapeDtypeStruct((2, 1 + each, share, crops * count), saved.dtype)
    scratch = [
        pltpu.VMEM((count + 2 * width, 3 * channels), jnp.bfloat16),
        pltpu.VMEM((count + 16, channels), jnp.float32),
    ]
    return call(kernel, [out, out], [saved, weights, *blocks], (), scratch, {})


def spread_call(first, cells_of, around, place, count, width):
    two, blocks, share, cells = cells_of.shape
    crops = cells // count
    total = 2 * blocks * cells

    def kernel(first_ref, cells_ref, *refs):
        out_ref, shifted = refs[-2:]
        is_first = lax.axis_index("section") == 0
        for kind in range(two):
            for block in range(blocks):
                for crop in range(crops):
                    cell = slice(crop * count, (crop + 1) * count)
                    value = jnp.where(
                        is_first, first_ref[kind, block, :, cell], cells_ref[kind, block, :, cell]
                    )
                    value = value.T.astype(jnp.float32)
                    before, after = neighbours(value, shifted, width)
                    at = (place * blocks + block) * cells + crop * count
                    for side, part in enumerate((before, value, after)):
                        lanes = slice(side * share, (side + 1) * share)
                        out_ref[kind, at : at + count, lanes] = part.astype(jnp.bfloat16)

    out = jax.ShapeDtypeStruct((two, total, 3 * share), jnp.bfloat16)
    scratch = [pltpu.VMEM((count + 16, share), jnp.float32)]
    operands = [first, cells_of] if around is None else [first, cells_of, around]
    aliases = {} if around is None else {2: 0}
    (spread,) = call(kernel, [out], operands, (), scratch, aliases)
    return spread


def terms_call(around, own, other, count, width, scaling):
    blocks, _, columns, cells = own.shape
    rows = around.shape[2] // 3
    crops = cells // count

    def moved(value, down):
        parts = []
        edge = jnp.zeros((columns, width), value.dtype)
        for crop in range(crops):
            part = value[:, crop * count : (crop + 1) * count]
            if down == 0:
                part = jnp.concatenate([part[:, width:], edge], axis=1)
            elif down == 2:
                part = jnp.concatenate([edge, part[:, : count - width]], axis=1)
            parts.append(part)
        return jnp.concatenate(parts, axis=1)

    def kernel(around_ref, own_ref, other_ref, out_ref, held, sems):
        copies = []
        for kind in (1, 0):
            total = None
            for block in range(2 * blocks):
                left = own_ref if block < blocks else other_ref
                left = left[block % blocks, 1 - kind]
                left = jnp.concatenate([moved(left, down) for down in range(3)], axis=0)
                right = around_ref[kind, block * cells : (block + 1) * cells, :]
                term = jnp.dot(left, right, preferred_element_type=jnp.float32)
                total = term if total is None else total + term
            for down in range(3):
                part = total[down * columns : (down + 1) * columns] * scaling
                part = part.T.reshape(3, rows, columns)
                for place in range(3):
                    held[kind, 3 * down + place] = part[place]
            copy = pltpu.make_async_copy(held.at[kind], out_ref.at[kind], sems.at[kind])
            copy.start()
            copies.append(copy)
        for copy in copies:
            copy.wait()

    shape = (2, 9, rows, columns)
    return pl.pallas_call(
        kernel,
        out_shape=jax.ShapeDtypeStruct(shape, jnp.float32),
        in_specs=[pl.BlockSpec(memory_space=pltpu.VMEM)] * 3,
        out_specs=pl.BlockSpec(memory_space=pltpu.HBM),
        scratch_shapes=[pltpu.VMEM(shape, jnp.float32), pltpu.SemaphoreType.DMA((2,))],
        compiler_params=pltpu.CompilerParams(vmem_limit_bytes=8 << 20),
        name="terms",
    )(around, own, other)


def rotated(value, axis, steps):
    count = lax.axis_size(axis)
    return lax.ppermute(value, axis, [(source, (source + steps) % count) for source in range(count)])


def crop_shards(strips, kernels, cotangent):
    sections = lax.axis_size("section")
    slabs, groups = lax.axis_size("slab"), lax.axis_size("img")
    images, strip_count, row_count, col_count, channels = strips.shape
    width = col_count * slabs
    count = row_count * width
    crops = images * strip_count // slabs
    shape = (count, channels)
    last = sections - 1
    early = min(1, last - 1)
    steps = range(1, groups)
    scaling = 1.0 / math.sqrt(images * groups * strip_count * count)

    def hop(values, source, target):
        arrived = []
        for value in values:
            arrived.append(lax.ppermute(value, "section", [(source, target)]))
        return arrived

    def shared(values, step, routes):
        pairs = [
            (place * groups + i, place * groups + (i + step) % groups)
            for place in routes
            for i in range(groups)
        ]
        return lax.ppermute(values, ("section", "img"), pairs)

    def swapped(value):
        return rotated(value, "slab", 1)

    def flipped(saved, after):
        return flip_call([(saved, (0, crop)) for crop in range(crops)], slabs, "slab", after)

    own, other = split_call(
        pltpu.with_memory_space_constraint(strips, pltpu.HBM),
        pltpu.with_memory_space_constraint(cotangent, pltpu.HBM),
        last,
    )
    other = swapped(other)
    weights = kernels[0].reshape(2, 3, 3 * channels, channels)
    stored = pltpu.with_memory_space_constraint(weights, pltpu.HBM)
    weights = load_call(stored, True, own)
    fields = join_call(own, other)
    incoming = fields
    state = []
    turned, after = None, weights
    for place in range(sections):
        outgoing = []
        for crop in range(crops):
            out, state = forward_call(
                incoming[crop], weights, state, place, crop, crops, shape, width, place == last, after
            )
            outgoing.append(out)
        if place == 0:
            weights = load_call(stored, False, state[0])
        if place < last:
            incoming = hop(outgoing, place, place + 1)
        if place == early:
            inputs = flipped(state[0], state[1])
            soon = [shared(inputs, step, [0]) for step in steps]
            turned = turn_call(weights, state[0])
            after = turned
    saved, hidden = state
    incoming = fields
    grads = []
    after = hidden
    for place in reversed(range(sections)):
        outgoing = []
        for crop in range(crops):
            out, grads = backward_call(
                incoming[crop],
                turned,
                hidden,
                grads,
                place,
                crop,
                crops,
                shape,
                width,
                place == last,
                groups,
                after,
            )
            outgoing.append(out)
        if place:
            incoming = hop(outgoing, place, place - 1)
        if place == last:
            inputs = flipped(saved, outgoing[-1])
            late = [shared(inputs, step, range(sections)) for step in steps]
        if place == 1:
            first, early_outer = remake_call(saved, weights, soon, width, (0, 0))
            after = first
            early_outer = lax.ppermute(early_outer, ("section", "slab"), [(i, (i + 1) % slabs) for i in range(slabs)])
    kept, sent = grads
    own = [sent[0]]
    for step in steps:
        own.append(shared(sent[step], step, range(sections)))
    home, outer = remake_call(saved, weights, late, width, (1, last))
    outer = swapped(outer)
    around = spread_call(first, home, None, 0, count, width)
    around = spread_call(early_outer, outer, around, 1, count, width)
    own = stack_call(own)
    other = swapped(own)
    terms = terms_call(around, own, other, count, width, scaling)
    own, other = part_call(kept, row_count, sent)
    other = swapped(other)
    grad_inputs = merge_call(own, other, images)
    return (terms[None], grad_inputs[None])


def shards(strips, kernels, cotangent):
    slabs, groups = lax.axis_size("slab"), lax.axis_size("img")
    strip_count, row_count, col_count, channels = strips.shape[1:]
    width = col_count * slabs
    whole_crops = strip_count % slabs == 0 and width % 16 == 0 and (row_count * width) % 128 == 0
    whole_crops = whole_crops and slabs == 2 and lax.axis_size("section") > 1
    if whole_crops and channels % (16 * slabs) == 0 and channels % (16 * groups) == 0:
        return crop_shards(strips, kernels, cotangent)
    return column_shards(strips, kernels, cotangent)


def solution(mesh):
    in_specs = (
        P("img", None, None, "slab", None),
        P("section", None, None, None, None),
        P("img", None, None, "slab", None),
    )
    out_specs = (
        P("section", None, None, "slab", "img"),
        P("section", "img", None, None, "slab", None),
    )
    return jax.shard_map(shards, mesh=mesh, in_specs=in_specs, out_specs=out_specs, check_vma=False)
```

```python
import math

import jax
import jax.numpy as jnp
from jax import lax
from jax.experimental import pallas as pl
from jax.experimental.pallas import tpu as pltpu
from jax.sharding import PartitionSpec as P


def passed_along(value, axis, steps):
    count = lax.axis_size(axis)
    initial, last = (max(0, -steps), min(count, count - steps))
    return lax.ppermute(value, axis, [(source, source + steps) for source in range(initial, last)])


def padded_2(cells, sides, width):
    for axis, dim in sides:
        count = lax.axis_size(axis)
        ends = count - 1
        head = lax.slice_in_dim(cells, 0, width, axis=dim)
        tail = lax.slice_in_dim(cells, cells.shape[dim] - width, cells.shape[dim], axis=dim)
        cells = jnp.concatenate(
            [
                lax.ppermute(tail, axis, [(i, (i + 1) % count) for i in range(ends)]),
                cells,
                lax.ppermute(head, axis, [((i + 1) % count, i) for i in range(ends)]),
            ],
            axis=dim,
        )
    return cells


def unfold(padded, row_count, col_count):
    tap_list = [
        padded[:, down_at : down_at + row_count, right_at : right_at + col_count, :]
        for down_at in range(3)
        for right_at in range(3)
    ]
    stacked = jnp.concatenate(tap_list, axis=3)
    return stacked.reshape(-1, stacked.shape[3])


def columns_of(wide_field):
    row_count = wide_field.shape[1]
    col_count = wide_field.shape[2] - 2
    padded = jnp.pad(wide_field, ((0, 0), (1, 1), (0, 0), (0, 0)))
    return unfold(padded, row_count, col_count)


def convolve(matrix, wide_field):
    count, row_count = (wide_field.shape[0], wide_field.shape[1])
    col_count = wide_field.shape[2] - 2
    flat_out = jnp.dot(columns_of(wide_field), matrix, preferred_element_type=jnp.float32)
    return flat_out.reshape(count, row_count, col_count, matrix.shape[1])


def contract(wide_field, grad_out):
    flat_grad = grad_out.reshape(-1, grad_out.shape[3])
    return lax.dot_general(
        columns_of(wide_field),
        flat_grad,
        (((0,), (0,)), ((), ())),
        preferred_element_type=jnp.float32,
    )


def silu_slope(hidden):
    sigmoid_at = jax.nn.sigmoid(hidden)
    return sigmoid_at * (1.0 + hidden * (1.0 - sigmoid_at))


def store(buffer, value, slot_index, is_valid, axis_at):
    current = lax.dynamic_index_in_dim(buffer, slot_index, axis_at, keepdims=False)
    return lax.dynamic_update_index_in_dim(
        buffer, jnp.where(is_valid, value, current), slot_index, axis_at
    )


def column_shards(strips, kernels, cotangent):
    section_count = lax.axis_size("section")
    section_index = lax.axis_index("section")
    slab_count = lax.axis_size("slab")
    slab_index = lax.axis_index("slab")
    images, strip_count, row_count, col_count, channels = strips.shape
    weights = kernels[0]
    first_forward = weights[0].reshape(9 * channels, channels)
    second_forward = weights[1].reshape(9 * channels, channels)
    first_backward = jnp.transpose(weights[0][::-1], (0, 2, 1)).reshape(9 * channels, channels)
    second_backward = jnp.transpose(weights[1][::-1], (0, 2, 1)).reshape(9 * channels, channels)
    scaling = 1.0 / math.sqrt(
        images * lax.axis_size("img") * strip_count * row_count * col_count * slab_count
    )
    position = slab_index * col_count - 1 + jnp.arange(col_count + 2, dtype=jnp.int32)
    inside = ((position >= 0) & (position < slab_count * col_count))[None, None, :, None]
    tick_count = strip_count + section_count - 1
    hidden_cols = col_count + 2
    empty_field = jnp.zeros((images, row_count, col_count, channels), jnp.bfloat16)
    saved_field = jnp.zeros((strip_count, images, row_count, col_count + 2, channels), jnp.bfloat16)
    saved_hidden = jnp.zeros((strip_count, images, row_count, hidden_cols, channels), jnp.float32)
    saved_active = jnp.zeros(
        (strip_count, images, row_count, col_count + 2, channels), jnp.bfloat16
    )
    outgoing = empty_field
    for step_no in range(tick_count):
        micro_index = step_no - section_index
        is_valid = (micro_index >= 0) & (micro_index < strip_count)
        slot_index = jnp.clip(micro_index, 0, strip_count - 1)
        if step_no == 0:
            incoming = empty_field
        else:
            incoming = passed_along(outgoing, "section", 1)
        first_strip = lax.dynamic_index_in_dim(strips, slot_index, 1, keepdims=False)
        field_in = jnp.where(section_index == 0, first_strip, incoming)
        wide_deep = padded_2(field_in, (("slab", 2),), 2)
        hidden = convolve(first_forward, wide_deep)
        wide_active = jnp.where(inside, jax.nn.silu(hidden), 0.0).astype(jnp.bfloat16)
        wide_field = wide_deep[:, :, 1:-1, :]
        outgoing = (field_in.astype(jnp.float32) + convolve(second_forward, wide_active)).astype(
            jnp.bfloat16
        )
        saved_field = store(saved_field, wide_field, slot_index, is_valid, 0)
        saved_hidden = store(saved_hidden, hidden, slot_index, is_valid, 0)
        saved_active = store(saved_active, wide_active, slot_index, is_valid, 0)
    grad_slots = jnp.zeros((images, strip_count, row_count, col_count, channels), jnp.bfloat16)
    saved_grad_out = jnp.zeros((strip_count, images, row_count, col_count, channels), jnp.bfloat16)
    saved_grad_hidden = jnp.zeros(
        (strip_count, images, row_count, col_count, channels), jnp.bfloat16
    )
    sending = empty_field
    for step_no in range(tick_count):
        micro_index = step_no - (section_count - 1 - section_index)
        is_valid = (micro_index >= 0) & (micro_index < strip_count)
        slot_index = jnp.clip(micro_index, 0, strip_count - 1)
        if step_no == 0:
            arriving = empty_field
        else:
            arriving = passed_along(sending, "section", -1)
        top_grad = lax.dynamic_index_in_dim(cotangent, slot_index, 1, keepdims=False)
        grad_out = jnp.where(section_index == section_count - 1, top_grad, arriving)
        grad_out = jnp.where(is_valid, grad_out, jnp.zeros_like(grad_out))
        hidden = lax.dynamic_index_in_dim(saved_hidden, slot_index, 0, keepdims=False)
        wide_grad = padded_2(grad_out, (("slab", 2),), 2)
        grad_active = convolve(second_backward, wide_grad)
        wide_hidden_grad = jnp.where(inside, grad_active * silu_slope(hidden), 0.0).astype(
            jnp.bfloat16
        )
        grad_hidden = wide_hidden_grad[:, :, 1:-1, :]
        sending = (
            grad_out.astype(jnp.float32) + convolve(first_backward, wide_hidden_grad)
        ).astype(jnp.bfloat16)
        saved_grad_out = store(saved_grad_out, grad_out, slot_index, is_valid, 0)
        saved_grad_hidden = store(saved_grad_hidden, grad_hidden, slot_index, is_valid, 0)
        grad_slots = store(grad_slots, sending, slot_index, is_valid, 1)
    flat_count = strip_count * images
    lower_part = contract(
        saved_field.reshape(flat_count, row_count, col_count + 2, channels),
        saved_grad_hidden.reshape(flat_count, row_count, col_count, channels),
    )
    upper_part = contract(
        saved_active.reshape(flat_count, row_count, col_count + 2, channels),
        saved_grad_out.reshape(flat_count, row_count, col_count, channels),
    )
    grad_terms = jnp.stack([lower_part, upper_part]).reshape(2, 9, channels, channels)
    row_share = lax.psum_scatter(
        grad_terms.astype(jnp.bfloat16), "slab", scatter_dimension=2, tiled=True
    )
    own_share = lax.psum_scatter(row_share, "img", scatter_dimension=3, tiled=True).astype(
        jnp.float32
    )
    grad_kernels = (own_share * scaling)[None]
    return (grad_kernels, grad_slots[None])


def call(kernel, outs, operands, unread, scratch, aliases, apart=()):
    spaces = {**dict.fromkeys(unread, pl.ANY), **dict.fromkeys(apart, pltpu.HBM)}
    return pl.pallas_call(
        kernel,
        out_shape=outs,
        in_specs=[
            pl.BlockSpec(memory_space=spaces.get(place, pltpu.VMEM))
            for place in range(len(operands))
        ],
        out_specs=[pl.BlockSpec(memory_space=pltpu.VMEM)] * len(outs),
        scratch_shapes=scratch,
        input_output_aliases=aliases,
        compiler_params=pltpu.CompilerParams(vmem_limit_bytes=8 << 20),
    )(*operands)


def half_lanes(count, channels):
    return channels % 128 == 64 and count % 32 == 0


def packed_shape(count, channels):
    return (count * channels // 128, 128) if half_lanes(count, channels) else (count, channels)


def pack(value):
    count, channels = value.shape
    if not half_lanes(count, channels):
        return value
    parts = [value[:, at : at + 128] for at in range(0, channels - 64, 128)]
    rest = value[:, channels - 64 :]
    parts.append(jnp.concatenate([rest[: count // 2], rest[count // 2 :]], axis=1))
    return jnp.concatenate(parts, axis=0)


def unpack(value, count, channels):
    if not half_lanes(count, channels):
        return value
    whole = channels // 128
    parts = [value[k * count : (k + 1) * count] for k in range(whole)]
    rest = value[whole * count :]
    parts.append(jnp.concatenate([rest[:, :64], rest[:, 64:]], axis=0))
    return jnp.concatenate(parts, axis=1)


def neighbours(value, shifted, width):
    count, channels = value.shape
    shifted[8 : 8 + count, :] = value
    column = lax.rem(lax.broadcasted_iota(jnp.int32, (count, channels), 0), width)
    before = jnp.where(column == 0, 0.0, shifted[7 : 7 + count, :])
    after = jnp.where(column == width - 1, 0.0, shifted[9 : 9 + count, :])
    return before, after


def convolved(value, matrix, taps, shifted, width):
    count, channels = value.shape
    before, after = neighbours(value, shifted, width)
    for place, part in enumerate((before, value, after)):
        taps[width : width + count, place * channels : (place + 1) * channels] = part.astype(
            jnp.bfloat16
        )
    edge = jnp.zeros((width, 3 * channels), jnp.bfloat16)
    taps[0:width, :] = edge
    taps[width + count : 2 * width + count, :] = edge
    total = jnp.dot(taps[0:count, :], matrix[0], preferred_element_type=jnp.float32)
    for down in (1, 2):
        total = total + jnp.dot(
            taps[down * width : down * width + count, :],
            matrix[down],
            preferred_element_type=jnp.float32,
        )
    return total


def forward_call(field, weights, state, section, crop, crops, shape, width, last, after):
    count, channels = shape

    def kernel(field_ref, weights_ref, after_ref, *refs):
        *_, saved_ref, hidden_ref, taps, shifted = refs

        @pl.when(lax.axis_index("section") == section)
        def _():
            field_in = field_ref[...]
            if section:
                field_in = unpack(field_in, count, channels)
            wide = field_in.astype(jnp.float32)
            saved_ref[0, crop] = field_in
            hidden = convolved(wide, weights_ref.at[0], taps, shifted, width)
            hidden_ref[crop] = hidden
            active = (hidden * jax.nn.sigmoid(hidden)).astype(jnp.bfloat16)
            saved_ref[1, crop] = active
            if not last:
                added = convolved(
                    active.astype(jnp.float32), weights_ref.at[1], taps, shifted, width
                )
                refs[-5][...] = pack((wide + added).astype(jnp.bfloat16))

    outs = [
        jax.ShapeDtypeStruct(packed_shape(count, channels), jnp.bfloat16),
        jax.ShapeDtypeStruct((2, crops, count, channels), jnp.bfloat16),
        jax.ShapeDtypeStruct((crops, count, channels), jnp.float32),
    ][1 if last else 0 :]
    scratch = [
        pltpu.VMEM((count + 2 * width, 3 * channels), jnp.bfloat16),
        pltpu.VMEM((count + 16, channels), jnp.float32),
    ]
    aliases = {3 + k: k + (0 if last else 1) for k in range(len(state))}
    outputs = call(kernel, outs, [field, weights, after, *state], (2,), scratch, aliases)
    return (None if last else outputs[0]), outputs[-2:]


def backward_call(
    grad, turned, hidden, state, section, crop, crops, shape, width, last, parts, after
):
    count, channels = shape
    share = channels // parts
    first = section == 0

    def kernel(grad_ref, turned_ref, hidden_ref, after_ref, *refs):
        *_, kept_ref, sent_ref, taps, shifted = refs

        @pl.when(lax.axis_index("section") == section)
        def _():
            grad = grad_ref[...]
            if not last:
                grad = unpack(grad, count, channels)
            wide = grad.astype(jnp.float32)
            own = lax.axis_index("img")
            place_parts(sent_ref, (0,), grad, crop, parts, own)
            grad_active = convolved(wide, turned_ref.at[1], taps, shifted, width)
            hidden = hidden_ref[crop]
            gate = jax.nn.sigmoid(hidden)
            grad_hidden = (grad_active * (gate * (1.0 + hidden * (1.0 - gate)))).astype(
                jnp.bfloat16
            )
            place_parts(sent_ref, (1,), grad_hidden, crop, parts, own)
            if first:
                kept_ref[crop] = grad_hidden
            else:
                added = convolved(
                    grad_hidden.astype(jnp.float32), turned_ref.at[0], taps, shifted, width
                )
                result = (wide + added).astype(jnp.bfloat16)
                kept_ref[crop] = result
                refs[-5][...] = pack(result)

    outs = [
        jax.ShapeDtypeStruct(packed_shape(count, channels), jnp.bfloat16),
        jax.ShapeDtypeStruct((crops, count, channels), jnp.bfloat16),
        jax.ShapeDtypeStruct((parts, 2, share, crops * count), jnp.bfloat16),
    ][1 if first else 0 :]
    scratch = [
        pltpu.VMEM((count + 2 * width, 3 * channels), jnp.bfloat16),
        pltpu.VMEM((count + 16, channels), jnp.float32),
    ]
    aliases = {4 + k: k + (0 if first else 1) for k in range(len(state))}
    operands = [grad, turned, hidden, after, *state]
    outputs = call(kernel, outs, operands, (3,), scratch, aliases)
    return (None if first else outputs[0]), outputs[-2:]


def finish_call(grads, turned, kept, width):
    crops, count, channels = kept.shape

    def kernel(turned_ref, *refs):
        kept_ref, taps, shifted = refs[-3:]

        @pl.when(lax.axis_index("section") == 0)
        def _():
            for crop in range(crops):
                wide = unpack(refs[crop][...], count, channels).astype(jnp.float32)
                grad_hidden = kept_ref[crop].astype(jnp.float32)
                added = convolved(grad_hidden, turned_ref.at[0], taps, shifted, width)
                kept_ref[crop] = (wide + added).astype(jnp.bfloat16)

    out = jax.ShapeDtypeStruct(kept.shape, kept.dtype)
    scratch = [
        pltpu.VMEM((count + 2 * width, 3 * channels), jnp.bfloat16),
        pltpu.VMEM((count + 16, channels), jnp.float32),
    ]
    operands = [turned, *grads, kept]
    (kept,) = call(kernel, [out], operands, (), scratch, {len(operands) - 1: 0})
    return kept


def place_parts(target, lead, value, crop, parts, own):
    count, channels = value.shape
    share = channels // parts
    flipped = value.T
    for part in range(parts):
        slot = lax.rem(part + parts - own, parts)
        target[(slot, *lead, slice(None), slice(crop * count, (crop + 1) * count))] = flipped[
            part * share : (part + 1) * share, :
        ]


def flip_call(kept, parts, axis, after):
    def kernel(*refs):
        flipped_ref = refs[-1]
        for crop, (place, index) in enumerate(kept):
            value = refs[place][index]
            place_parts(flipped_ref, (), value, crop, parts, lax.axis_index(axis))

    operands = []
    for array, index in kept:
        if all(array is not other for other in operands):
            operands.append(array)
    kept = [
        ([array is other for other in operands].index(True), index) for array, index in kept
    ]
    count, channels = operands[0].shape[-2:]
    out = jax.ShapeDtypeStruct((parts, channels // parts, len(kept) * count), operands[0].dtype)
    (flipped,) = call(kernel, [out], [*operands, after], (len(operands),), [], {})
    return flipped


def turn_call(weights, after):
    two, _, _, channels = weights.shape

    def kernel(weights_ref, after_ref, turned_ref):
        for which in range(two):
            for tap in range(9):
                down, right = divmod(tap, 3)
                flipped = weights_ref[which, down, right * channels : (right + 1) * channels, :].T
                down, right = divmod(8 - tap, 3)
                turned_ref[which, down, right * channels : (right + 1) * channels, :] = flipped

    out = jax.ShapeDtypeStruct(weights.shape, weights.dtype)
    (turned,) = call(kernel, [out], [weights, after], (1,), [], {})
    return turned


def split_call(strips, cotangent, last):
    images, strip_count, rows, cols, channels = strips.shape
    share = strip_count // 2

    def kernel(strips_ref, cotangent_ref, own_ref, other_ref, sems):
        own = lax.axis_index("slab")
        is_last = lax.axis_index("section") == last

        def fetch(source_ref):
            copies = []
            for image in range(images):
                at = pl.ds(image * share, share)
                for side, (ref, half) in enumerate(((own_ref, own), (other_ref, 1 - own))):
                    source = source_ref.at[image, pl.ds(half * share, share)]
                    copies.append(pltpu.make_async_copy(source, ref.at[at], sems.at[2 * image + side]))
            for copy in copies:
                copy.start()
            for copy in copies:
                copy.wait()

        @pl.when(is_last)
        def _():
            fetch(cotangent_ref)

        @pl.when(jnp.logical_not(is_last))
        def _():
            fetch(strips_ref)

    out = jax.ShapeDtypeStruct((images * share, rows, cols, channels), strips.dtype)
    sems = [pltpu.SemaphoreType.DMA((2 * images,))]
    return call(kernel, [out, out], [strips, cotangent], (), sems, {}, (0, 1))


def load_call(weights, first, after):
    def kernel(weights_ref, after_ref, *refs):
        out_ref, sems = refs[-2:]

        @pl.when((lax.axis_index("section") == 0) | (not first))
        def _():
            copies = [
                pltpu.make_async_copy(weights_ref.at[which], out_ref.at[which], sems.at[which])
                for which in range(2)
            ]
            for copy in copies:
                copy.start()
            for copy in copies:
                copy.wait()

    out = jax.ShapeDtypeStruct(weights.shape, weights.dtype)
    sems = [pltpu.SemaphoreType.DMA((2,))]
    (loaded,) = call(kernel, [out], [weights, after], (1,), sems, {}, (0,))
    return loaded


def join_call(own, other):
    crops, rows, cols, channels = own.shape

    def kernel(own_ref, other_ref, *out_refs):
        is_left = lax.axis_index("slab") == 0
        for crop, out_ref in enumerate(out_refs):
            mine = own_ref[crop].astype(jnp.float32)
            theirs = other_ref[crop].astype(jnp.float32)
            left = jnp.where(is_left, mine, theirs)
            right = jnp.where(is_left, theirs, mine)
            whole = jnp.concatenate([left, right], axis=1)
            out_ref[...] = whole.reshape(rows * 2 * cols, channels).astype(jnp.bfloat16)

    out = jax.ShapeDtypeStruct((rows * 2 * cols, channels), own.dtype)
    return call(kernel, [out] * crops, [own, other], (), [], {})


def part_call(kept, rows, after):
    crops, count, channels = kept.shape
    cols = count // rows // 2

    def kernel(kept_ref, after_ref, own_ref, other_ref):
        is_left = lax.axis_index("slab") == 0
        for crop in range(crops):
            whole = kept_ref[crop].astype(jnp.float32).reshape(rows, 2 * cols, channels)
            left, right = whole[:, :cols], whole[:, cols:]
            own_ref[crop] = jnp.where(is_left, left, right).astype(jnp.bfloat16)
            other_ref[crop] = jnp.where(is_left, right, left).astype(jnp.bfloat16)

    out = jax.ShapeDtypeStruct((crops, rows, cols, channels), kept.dtype)
    return call(kernel, [out, out], [kept, after], (1,), [], {})


def merge_call(own, other, images):
    crops, rows, cols, channels = own.shape
    share = crops // images

    def kernel(own_ref, other_ref, out_ref):
        place = lax.axis_index("slab")
        for image in range(images):
            for crop in range(share):
                out_ref[image, place * share + crop] = own_ref[image * share + crop]
                out_ref[image, (1 - place) * share + crop] = other_ref[image * share + crop]

    out = jax.ShapeDtypeStruct((images, 2 * share, rows, cols, channels), own.dtype)
    (merged,) = call(kernel, [out], [own, other], (), [], {})
    return merged


def stack_call(blocks):
    def kernel(*refs):
        for place in range(len(blocks)):
            refs[-1][place] = refs[place][...]

    out = jax.ShapeDtypeStruct((len(blocks), *blocks[0].shape), blocks[0].dtype)
    (stacked,) = call(kernel, [out], [*blocks], (), [], {})
    return stacked


def remake_call(saved, weights, blocks, width, sections):
    _, crops, count, channels = saved.shape
    share = channels // 2
    each = len(blocks)

    def kernel(saved_ref, weights_ref, *refs):
        home_ref, outer_ref, taps, shifted = refs[-4:]
        is_left = lax.axis_index("slab") == 0
        section = lax.axis_index("section")

        def put(kind, block, crop, value):
            cells = slice(crop * count, (crop + 1) * count)
            flipped = value.T
            low, high = flipped[:share], flipped[share:]
            home_ref[kind, block, :, cells] = jnp.where(is_left, low, high)
            outer_ref[kind, block, :, cells] = jnp.where(is_left, high, low)

        @pl.when((section >= sections[0]) & (section <= sections[1]))
        def _():
            for crop in range(crops):
                for kind in range(2):
                    put(kind, 0, crop, saved_ref[kind, crop])
            for block in range(each):
                home_ref[0, 1 + block] = refs[block][0]
                outer_ref[0, 1 + block] = refs[block][1]
                for crop in range(crops):
                    cells = slice(crop * count, (crop + 1) * count)
                    mine, theirs = refs[block][0, :, cells], refs[block][1, :, cells]
                    low, high = jnp.where(is_left, mine, theirs), jnp.where(is_left, theirs, mine)
                    field = jnp.concatenate([low, high], axis=0).T.astype(jnp.float32)
                    hidden = convolved(field, weights_ref.at[0], taps, shifted, width)
                    active = (hidden * jax.nn.sigmoid(hidden)).astype(jnp.bfloat16)
                    put(1, 1 + block, crop, active)

    out = jax.ShapeDtypeStruct((2, 1 + each, share, crops * count), saved.dtype)
    scratch = [
        pltpu.VMEM((count + 2 * width, 3 * channels), jnp.bfloat16),
        pltpu.VMEM((count + 16, channels), jnp.float32),
    ]
    return call(kernel, [out, out], [saved, weights, *blocks], (), scratch, {})


def spread_call(first, cells_of, around, place, count, width):
    two, blocks, share, cells = cells_of.shape
    crops = cells // count
    total = 2 * blocks * cells

    def kernel(first_ref, cells_ref, *refs):
        out_ref, shifted = refs[-2:]
        is_first = lax.axis_index("section") == 0
        for kind in range(two):
            for block in range(blocks):
                for crop in range(crops):
                    cell = slice(crop * count, (crop + 1) * count)
                    value = jnp.where(
                        is_first, first_ref[kind, block, :, cell], cells_ref[kind, block, :, cell]
                    )
                    value = value.T.astype(jnp.float32)
                    before, after = neighbours(value, shifted, width)
                    at = (place * blocks + block) * cells + crop * count
                    for side, part in enumerate((before, value, after)):
                        lanes = slice(side * share, (side + 1) * share)
                        out_ref[kind, at : at + count, lanes] = part.astype(jnp.bfloat16)

    out = jax.ShapeDtypeStruct((two, total, 3 * share), jnp.bfloat16)
    scratch = [pltpu.VMEM((count + 16, share), jnp.float32)]
    operands = [first, cells_of] if around is None else [first, cells_of, around]
    aliases = {} if around is None else {2: 0}
    (spread,) = call(kernel, [out], operands, (), scratch, aliases)
    return spread


def terms_call(around, own, other, count, width, scaling):
    blocks, _, columns, cells = own.shape
    rows = around.shape[2] // 3
    crops = cells // count

    def moved(value, down):
        parts = []
        edge = jnp.zeros((columns, width), value.dtype)
        for crop in range(crops):
            part = value[:, crop * count : (crop + 1) * count]
            if down == 0:
                part = jnp.concatenate([part[:, width:], edge], axis=1)
            elif down == 2:
                part = jnp.concatenate([edge, part[:, : count - width]], axis=1)
            parts.append(part)
        return jnp.concatenate(parts, axis=1)

    def kernel(around_ref, own_ref, other_ref, out_ref, held, sems):
        copies = []
        for kind in (1, 0):
            total = None
            for block in range(2 * blocks):
                left = own_ref if block < blocks else other_ref
                left = left[block % blocks, 1 - kind]
                left = jnp.concatenate([moved(left, down) for down in range(3)], axis=0)
                right = around_ref[kind, block * cells : (block + 1) * cells, :]
                term = jnp.dot(left, right, preferred_element_type=jnp.float32)
                total = term if total is None else total + term
            for down in range(3):
                part = total[down * columns : (down + 1) * columns] * scaling
                part = part.T.reshape(3, rows, columns)
                for place in range(3):
                    held[kind, 3 * down + place] = part[place]
            copy = pltpu.make_async_copy(held.at[kind], out_ref.at[kind], sems.at[kind])
            copy.start()
            copies.append(copy)
        for copy in copies:
            copy.wait()

    shape = (2, 9, rows, columns)
    return pl.pallas_call(
        kernel,
        out_shape=jax.ShapeDtypeStruct(shape, jnp.float32),
        in_specs=[pl.BlockSpec(memory_space=pltpu.VMEM)] * 3,
        out_specs=pl.BlockSpec(memory_space=pltpu.HBM),
        scratch_shapes=[pltpu.VMEM(shape, jnp.float32), pltpu.SemaphoreType.DMA((2,))],
        compiler_params=pltpu.CompilerParams(vmem_limit_bytes=8 << 20),
        name="terms",
    )(around, own, other)


def rotated(value, axis, steps):
    count = lax.axis_size(axis)
    return lax.ppermute(value, axis, [(source, (source + steps) % count) for source in range(count)])


def crop_shards(strips, kernels, cotangent):
    sections = lax.axis_size("section")
    slabs, groups = lax.axis_size("slab"), lax.axis_size("img")
    images, strip_count, row_count, col_count, channels = strips.shape
    width = col_count * slabs
    count = row_count * width
    crops = images * strip_count // slabs
    shape = (count, channels)
    last = sections - 1
    early = min(1, last - 1)
    steps = range(1, groups)
    scaling = 1.0 / math.sqrt(images * groups * strip_count * count)

    def hop(values, source, target):
        arrived = []
        for value in values:
            arrived.append(lax.ppermute(value, "section", [(source, target)]))
        return arrived

    def shared(values, step, routes):
        pairs = [
            (place * groups + i, place * groups + (i + step) % groups)
            for place in routes
            for i in range(groups)
        ]
        return lax.ppermute(values, ("section", "img"), pairs)

    def swapped(value):
        return rotated(value, "slab", 1)

    def flipped(saved, after):
        return flip_call([(saved, (0, crop)) for crop in range(crops)], slabs, "slab", after)

    own, other = split_call(
        pltpu.with_memory_space_constraint(strips, pltpu.HBM),
        pltpu.with_memory_space_constraint(cotangent, pltpu.HBM),
        last,
    )
    other = swapped(other)
    weights = kernels[0].reshape(2, 3, 3 * channels, channels)
    stored = pltpu.with_memory_space_constraint(weights, pltpu.HBM)
    weights = load_call(stored, True, own)
    fields = join_call(own, other)
    incoming = fields
    state = []
    turned, after = None, weights
    grads = []

    def forward(place, crop):
        return forward_call(
            incoming[crop],
            weights,
            state,
            place,
            crop,
            crops,
            shape,
            width,
            place == last,
            after,
        )

    def backward(place, crop, incoming):
        return backward_call(
            incoming[crop],
            turned,
            state[1],
            grads,
            place,
            crop,
            crops,
            shape,
            width,
            place == last,
            groups,
            after,
        )

    for place in range(last):
        outgoing = []
        for crop in range(crops):
            out, state = forward(place, crop)
            outgoing.append(out)
        if place == 0:
            weights = load_call(stored, False, state[0])
        incoming = hop(outgoing, place, place + 1)
        if place == early:
            inputs = flipped(state[0], state[1])
            soon = [shared(inputs, step, [0]) for step in steps]
            turned = turn_call(weights, state[0])
            after = turned
    outgoing = []
    for crop in range(crops):
        _, state = forward(last, crop)
        out, grads = backward(last, crop, fields)
        after = out
        outgoing.append(out)
    saved, hidden = state
    incoming = hop(outgoing, last, last - 1)
    inputs = flipped(saved, outgoing[-1])
    late = [shared(inputs, step, range(sections)) for step in steps]
    after = hidden
    for place in reversed(range(last)):
        if place == 0:
            first, early_outer = remake_call(saved, weights, soon, width, (0, 0))
            after = first
            early_outer = lax.ppermute(early_outer, ("section", "slab"), [(i, (i + 1) % slabs) for i in range(slabs)])
        outgoing = []
        for crop in range(crops):
            out, grads = backward(place, crop, incoming)
            outgoing.append(out)
        if place:
            incoming = hop(outgoing, place, place - 1)
    kept, sent = grads
    kept = finish_call(incoming, turned, kept, width)
    own = [sent[0]]
    for step in steps:
        own.append(shared(sent[step], step, range(sections)))
    home, outer = remake_call(saved, weights, late, width, (1, last))
    outer = swapped(outer)
    around = spread_call(first, home, None, 0, count, width)
    around = spread_call(early_outer, outer, around, 1, count, width)
    own = stack_call(own)
    other = swapped(own)
    terms = terms_call(around, own, other, count, width, scaling)
    own, other = part_call(kept, row_count, sent)
    other = swapped(other)
    grad_inputs = merge_call(own, other, images)
    return (terms[None], grad_inputs[None])


def shards(strips, kernels, cotangent):
    slabs, groups = lax.axis_size("slab"), lax.axis_size("img")
    strip_count, row_count, col_count, channels = strips.shape[1:]
    width = col_count * slabs
    whole_crops = strip_count % slabs == 0 and width % 16 == 0 and (row_count * width) % 128 == 0
    whole_crops = whole_crops and slabs == 2 and lax.axis_size("section") > 1
    if whole_crops and channels % (16 * slabs) == 0 and channels % (16 * groups) == 0:
        return crop_shards(strips, kernels, cotangent)
    return column_shards(strips, kernels, cotangent)


def solution(mesh):
    in_specs = (
        P("img", None, None, "slab", None),
        P("section", None, None, None, None),
        P("img", None, None, "slab", None),
    )
    out_specs = (
        P("section", None, None, "slab", "img"),
        P("section", "img", None, None, "slab", None),
    )
    return jax.shard_map(shards, mesh=mesh, in_specs=in_specs, out_specs=out_specs, check_vma=False)
```

```python
import math

import jax
import jax.numpy as jnp
from jax import lax
from jax.experimental import pallas as pl
from jax.experimental.pallas import tpu as pltpu
from jax.sharding import PartitionSpec as P


def passed_along(value, axis, steps):
    count = lax.axis_size(axis)
    initial, last = (max(0, -steps), min(count, count - steps))
    return lax.ppermute(value, axis, [(source, source + steps) for source in range(initial, last)])


def padded_2(cells, sides, width):
    for axis, dim in sides:
        count = lax.axis_size(axis)
        ends = count - 1
        head = lax.slice_in_dim(cells, 0, width, axis=dim)
        tail = lax.slice_in_dim(cells, cells.shape[dim] - width, cells.shape[dim], axis=dim)
        cells = jnp.concatenate(
            [
                lax.ppermute(tail, axis, [(i, (i + 1) % count) for i in range(ends)]),
                cells,
                lax.ppermute(head, axis, [((i + 1) % count, i) for i in range(ends)]),
            ],
            axis=dim,
        )
    return cells


def unfold(padded, row_count, col_count):
    tap_list = [
        padded[:, down_at : down_at + row_count, right_at : right_at + col_count, :]
        for down_at in range(3)
        for right_at in range(3)
    ]
    stacked = jnp.concatenate(tap_list, axis=3)
    return stacked.reshape(-1, stacked.shape[3])


def columns_of(wide_field):
    row_count = wide_field.shape[1]
    col_count = wide_field.shape[2] - 2
    padded = jnp.pad(wide_field, ((0, 0), (1, 1), (0, 0), (0, 0)))
    return unfold(padded, row_count, col_count)


def convolve(matrix, wide_field):
    count, row_count = (wide_field.shape[0], wide_field.shape[1])
    col_count = wide_field.shape[2] - 2
    flat_out = jnp.dot(columns_of(wide_field), matrix, preferred_element_type=jnp.float32)
    return flat_out.reshape(count, row_count, col_count, matrix.shape[1])


def contract(wide_field, grad_out):
    flat_grad = grad_out.reshape(-1, grad_out.shape[3])
    return lax.dot_general(
        columns_of(wide_field),
        flat_grad,
        (((0,), (0,)), ((), ())),
        preferred_element_type=jnp.float32,
    )


def silu_slope(hidden):
    sigmoid_at = jax.nn.sigmoid(hidden)
    return sigmoid_at * (1.0 + hidden * (1.0 - sigmoid_at))


def store(buffer, value, slot_index, is_valid, axis_at):
    current = lax.dynamic_index_in_dim(buffer, slot_index, axis_at, keepdims=False)
    return lax.dynamic_update_index_in_dim(
        buffer, jnp.where(is_valid, value, current), slot_index, axis_at
    )


def column_shards(strips, kernels, cotangent):
    section_count = lax.axis_size("section")
    section_index = lax.axis_index("section")
    slab_count = lax.axis_size("slab")
    slab_index = lax.axis_index("slab")
    images, strip_count, row_count, col_count, channels = strips.shape
    weights = kernels[0]
    first_forward = weights[0].reshape(9 * channels, channels)
    second_forward = weights[1].reshape(9 * channels, channels)
    first_backward = jnp.transpose(weights[0][::-1], (0, 2, 1)).reshape(9 * channels, channels)
    second_backward = jnp.transpose(weights[1][::-1], (0, 2, 1)).reshape(9 * channels, channels)
    scaling = 1.0 / math.sqrt(
        images * lax.axis_size("img") * strip_count * row_count * col_count * slab_count
    )
    position = slab_index * col_count - 1 + jnp.arange(col_count + 2, dtype=jnp.int32)
    inside = ((position >= 0) & (position < slab_count * col_count))[None, None, :, None]
    tick_count = strip_count + section_count - 1
    hidden_cols = col_count + 2
    empty_field = jnp.zeros((images, row_count, col_count, channels), jnp.bfloat16)
    saved_field = jnp.zeros((strip_count, images, row_count, col_count + 2, channels), jnp.bfloat16)
    saved_hidden = jnp.zeros((strip_count, images, row_count, hidden_cols, channels), jnp.float32)
    saved_active = jnp.zeros(
        (strip_count, images, row_count, col_count + 2, channels), jnp.bfloat16
    )
    outgoing = empty_field
    for step_no in range(tick_count):
        micro_index = step_no - section_index
        is_valid = (micro_index >= 0) & (micro_index < strip_count)
        slot_index = jnp.clip(micro_index, 0, strip_count - 1)
        if step_no == 0:
            incoming = empty_field
        else:
            incoming = passed_along(outgoing, "section", 1)
        first_strip = lax.dynamic_index_in_dim(strips, slot_index, 1, keepdims=False)
        field_in = jnp.where(section_index == 0, first_strip, incoming)
        wide_deep = padded_2(field_in, (("slab", 2),), 2)
        hidden = convolve(first_forward, wide_deep)
        wide_active = jnp.where(inside, jax.nn.silu(hidden), 0.0).astype(jnp.bfloat16)
        wide_field = wide_deep[:, :, 1:-1, :]
        outgoing = (field_in.astype(jnp.float32) + convolve(second_forward, wide_active)).astype(
            jnp.bfloat16
        )
        saved_field = store(saved_field, wide_field, slot_index, is_valid, 0)
        saved_hidden = store(saved_hidden, hidden, slot_index, is_valid, 0)
        saved_active = store(saved_active, wide_active, slot_index, is_valid, 0)
    grad_slots = jnp.zeros((images, strip_count, row_count, col_count, channels), jnp.bfloat16)
    saved_grad_out = jnp.zeros((strip_count, images, row_count, col_count, channels), jnp.bfloat16)
    saved_grad_hidden = jnp.zeros(
        (strip_count, images, row_count, col_count, channels), jnp.bfloat16
    )
    sending = empty_field
    for step_no in range(tick_count):
        micro_index = step_no - (section_count - 1 - section_index)
        is_valid = (micro_index >= 0) & (micro_index < strip_count)
        slot_index = jnp.clip(micro_index, 0, strip_count - 1)
        if step_no == 0:
            arriving = empty_field
        else:
            arriving = passed_along(sending, "section", -1)
        top_grad = lax.dynamic_index_in_dim(cotangent, slot_index, 1, keepdims=False)
        grad_out = jnp.where(section_index == section_count - 1, top_grad, arriving)
        grad_out = jnp.where(is_valid, grad_out, jnp.zeros_like(grad_out))
        hidden = lax.dynamic_index_in_dim(saved_hidden, slot_index, 0, keepdims=False)
        wide_grad = padded_2(grad_out, (("slab", 2),), 2)
        grad_active = convolve(second_backward, wide_grad)
        wide_hidden_grad = jnp.where(inside, grad_active * silu_slope(hidden), 0.0).astype(
            jnp.bfloat16
        )
        grad_hidden = wide_hidden_grad[:, :, 1:-1, :]
        sending = (
            grad_out.astype(jnp.float32) + convolve(first_backward, wide_hidden_grad)
        ).astype(jnp.bfloat16)
        saved_grad_out = store(saved_grad_out, grad_out, slot_index, is_valid, 0)
        saved_grad_hidden = store(saved_grad_hidden, grad_hidden, slot_index, is_valid, 0)
        grad_slots = store(grad_slots, sending, slot_index, is_valid, 1)
    flat_count = strip_count * images
    lower_part = contract(
        saved_field.reshape(flat_count, row_count, col_count + 2, channels),
        saved_grad_hidden.reshape(flat_count, row_count, col_count, channels),
    )
    upper_part = contract(
        saved_active.reshape(flat_count, row_count, col_count + 2, channels),
        saved_grad_out.reshape(flat_count, row_count, col_count, channels),
    )
    grad_terms = jnp.stack([lower_part, upper_part]).reshape(2, 9, channels, channels)
    row_share = lax.psum_scatter(
        grad_terms.astype(jnp.bfloat16), "slab", scatter_dimension=2, tiled=True
    )
    own_share = lax.psum_scatter(row_share, "img", scatter_dimension=3, tiled=True).astype(
        jnp.float32
    )
    grad_kernels = (own_share * scaling)[None]
    return (grad_kernels, grad_slots[None])


def call(kernel, outs, operands, unread, scratch, aliases, apart=()):
    spaces = {**dict.fromkeys(unread, pl.ANY), **dict.fromkeys(apart, pltpu.HBM)}
    return pl.pallas_call(
        kernel,
        out_shape=outs,
        in_specs=[
            pl.BlockSpec(memory_space=spaces.get(place, pltpu.VMEM))
            for place in range(len(operands))
        ],
        out_specs=[pl.BlockSpec(memory_space=pltpu.VMEM)] * len(outs),
        scratch_shapes=scratch,
        input_output_aliases=aliases,
        compiler_params=pltpu.CompilerParams(vmem_limit_bytes=8 << 20),
    )(*operands)


def half_lanes(count, channels):
    return channels % 128 == 64 and count % 32 == 0


def packed_shape(count, channels):
    return (count * channels // 128, 128) if half_lanes(count, channels) else (count, channels)


def pack(value):
    count, channels = value.shape
    if not half_lanes(count, channels):
        return value
    parts = [value[:, at : at + 128] for at in range(0, channels - 64, 128)]
    rest = value[:, channels - 64 :]
    parts.append(jnp.concatenate([rest[: count // 2], rest[count // 2 :]], axis=1))
    return jnp.concatenate(parts, axis=0)


def unpack(value, count, channels):
    if not half_lanes(count, channels):
        return value
    whole = channels // 128
    parts = [value[k * count : (k + 1) * count] for k in range(whole)]
    rest = value[whole * count :]
    parts.append(jnp.concatenate([rest[:, :64], rest[:, 64:]], axis=0))
    return jnp.concatenate(parts, axis=1)


def neighbours(value, shifted, width):
    count, channels = value.shape
    shifted[8 : 8 + count, :] = value
    column = lax.rem(lax.broadcasted_iota(jnp.int32, (count, channels), 0), width)
    before = jnp.where(column == 0, 0.0, shifted[7 : 7 + count, :])
    after = jnp.where(column == width - 1, 0.0, shifted[9 : 9 + count, :])
    return before, after


def convolved(value, matrix, taps, shifted, width):
    count, channels = value.shape
    before, after = neighbours(value, shifted, width)
    for place, part in enumerate((before, value, after)):
        taps[width : width + count, place * channels : (place + 1) * channels] = part.astype(
            jnp.bfloat16
        )
    edge = jnp.zeros((width, 3 * channels), jnp.bfloat16)
    taps[0:width, :] = edge
    taps[width + count : 2 * width + count, :] = edge
    total = jnp.dot(taps[0:count, :], matrix[0], preferred_element_type=jnp.float32)
    for down in (1, 2):
        total = total + jnp.dot(
            taps[down * width : down * width + count, :],
            matrix[down],
            preferred_element_type=jnp.float32,
        )
    return total


def forward_call(field, weights, state, section, crop, crops, shape, width, last, after):
    count, channels = shape

    def kernel(field_ref, weights_ref, after_ref, *refs):
        *_, saved_ref, hidden_ref, taps, shifted = refs

        @pl.when(lax.axis_index("section") == section)
        def _():
            field_in = field_ref[...]
            if section:
                field_in = unpack(field_in, count, channels)
            wide = field_in.astype(jnp.float32)
            saved_ref[0, crop] = field_in
            hidden = convolved(wide, weights_ref.at[0], taps, shifted, width)
            hidden_ref[crop] = hidden
            active = (hidden * jax.nn.sigmoid(hidden)).astype(jnp.bfloat16)
            saved_ref[1, crop] = active
            if not last:
                added = convolved(
                    active.astype(jnp.float32), weights_ref.at[1], taps, shifted, width
                )
                refs[-5][...] = pack((wide + added).astype(jnp.bfloat16))

    outs = [
        jax.ShapeDtypeStruct(packed_shape(count, channels), jnp.bfloat16),
        jax.ShapeDtypeStruct((2, crops, count, channels), jnp.bfloat16),
        jax.ShapeDtypeStruct((crops, count, channels), jnp.float32),
    ][1 if last else 0 :]
    scratch = [
        pltpu.VMEM((count + 2 * width, 3 * channels), jnp.bfloat16),
        pltpu.VMEM((count + 16, channels), jnp.float32),
    ]
    aliases = {3 + k: k + (0 if last else 1) for k in range(len(state))}
    outputs = call(kernel, outs, [field, weights, after, *state], (2,), scratch, aliases)
    return (None if last else outputs[0]), outputs[-2:]


def backward_call(
    grad, turned, hidden, state, section, crop, crops, shape, width, last, parts, after
):
    count, channels = shape
    share = channels // parts
    first = section == 0

    def kernel(grad_ref, turned_ref, hidden_ref, after_ref, *refs):
        *_, kept_ref, sent_ref, taps, shifted = refs

        @pl.when(lax.axis_index("section") == section)
        def _():
            grad = grad_ref[...]
            if not last:
                grad = unpack(grad, count, channels)
            wide = grad.astype(jnp.float32)
            own = lax.axis_index("img")
            place_parts(sent_ref, (0,), grad, crop, parts, own)
            grad_active = convolved(wide, turned_ref.at[1], taps, shifted, width)
            hidden = hidden_ref[crop]
            gate = jax.nn.sigmoid(hidden)
            grad_hidden = (grad_active * (gate * (1.0 + hidden * (1.0 - gate)))).astype(
                jnp.bfloat16
            )
            place_parts(sent_ref, (1,), grad_hidden, crop, parts, own)
            if first:
                kept_ref[crop] = grad_hidden
            else:
                added = convolved(
                    grad_hidden.astype(jnp.float32), turned_ref.at[0], taps, shifted, width
                )
                result = (wide + added).astype(jnp.bfloat16)
                kept_ref[crop] = result
                refs[-5][...] = pack(result)

    outs = [
        jax.ShapeDtypeStruct(packed_shape(count, channels), jnp.bfloat16),
        jax.ShapeDtypeStruct((crops, count, channels), jnp.bfloat16),
        jax.ShapeDtypeStruct((parts, 2, share, crops * count), jnp.bfloat16),
    ][1 if first else 0 :]
    scratch = [
        pltpu.VMEM((count + 2 * width, 3 * channels), jnp.bfloat16),
        pltpu.VMEM((count + 16, channels), jnp.float32),
    ]
    aliases = {4 + k: k + (0 if first else 1) for k in range(len(state))}
    operands = [grad, turned, hidden, after, *state]
    outputs = call(kernel, outs, operands, (3,), scratch, aliases)
    return (None if first else outputs[0]), outputs[-2:]


def finish_call(grads, turned, kept, width):
    crops, count, channels = kept.shape

    def kernel(turned_ref, *refs):
        kept_ref, taps, shifted = refs[-3:]

        @pl.when(lax.axis_index("section") == 0)
        def _():
            for crop in range(crops):
                wide = unpack(refs[crop][...], count, channels).astype(jnp.float32)
                grad_hidden = kept_ref[crop].astype(jnp.float32)
                added = convolved(grad_hidden, turned_ref.at[0], taps, shifted, width)
                kept_ref[crop] = (wide + added).astype(jnp.bfloat16)

    out = jax.ShapeDtypeStruct(kept.shape, kept.dtype)
    scratch = [
        pltpu.VMEM((count + 2 * width, 3 * channels), jnp.bfloat16),
        pltpu.VMEM((count + 16, channels), jnp.float32),
    ]
    operands = [turned, *grads, kept]
    (kept,) = call(kernel, [out], operands, (), scratch, {len(operands) - 1: 0})
    return kept


def place_parts(target, lead, value, crop, parts, own):
    count, channels = value.shape
    share = channels // parts
    flipped = value.T
    for part in range(parts):
        slot = lax.rem(part + parts - own, parts)
        target[(slot, *lead, slice(None), slice(crop * count, (crop + 1) * count))] = flipped[
            part * share : (part + 1) * share, :
        ]


def flip_call(kept, parts, axis, after):
    def kernel(*refs):
        flipped_ref = refs[-1]
        for crop, (place, index) in enumerate(kept):
            value = refs[place][index]
            place_parts(flipped_ref, (), value, crop, parts, lax.axis_index(axis))

    operands = []
    for array, index in kept:
        if all(array is not other for other in operands):
            operands.append(array)
    kept = [
        ([array is other for other in operands].index(True), index) for array, index in kept
    ]
    count, channels = operands[0].shape[-2:]
    out = jax.ShapeDtypeStruct((parts, channels // parts, len(kept) * count), operands[0].dtype)
    (flipped,) = call(kernel, [out], [*operands, after], (len(operands),), [], {})
    return flipped


def turn_call(loaded, weights, after):
    two, _, _, channels = weights.shape

    def kernel(loaded_ref, weights_ref, after_ref, turned_ref):
        is_first = lax.axis_index("section") == 0
        for which in range(two):
            for tap in range(9):
                down, right = divmod(tap, 3)
                rows = slice(right * channels, (right + 1) * channels)
                value = jnp.where(
                    is_first, loaded_ref[which, down, rows, :], weights_ref[which, down, rows, :]
                )
                down, right = divmod(8 - tap, 3)
                turned_ref[which, down, right * channels : (right + 1) * channels, :] = value.T

    out = jax.ShapeDtypeStruct(weights.shape, weights.dtype)
    (turned,) = call(kernel, [out], [loaded, weights, after], (2,), [], {})
    return turned


def split_call(strips, cotangent, last):
    images, strip_count, rows, cols, channels = strips.shape
    share = strip_count // 2

    def kernel(strips_ref, cotangent_ref, own_ref, other_ref, sems):
        own = lax.axis_index("slab")
        is_last = lax.axis_index("section") == last

        def fetch(source_ref):
            copies = []
            for image in range(images):
                at = pl.ds(image * share, share)
                for side, (ref, half) in enumerate(((own_ref, own), (other_ref, 1 - own))):
                    source = source_ref.at[image, pl.ds(half * share, share)]
                    copies.append(pltpu.make_async_copy(source, ref.at[at], sems.at[2 * image + side]))
            for copy in copies:
                copy.start()
            for copy in copies:
                copy.wait()

        @pl.when(is_last)
        def _():
            fetch(cotangent_ref)

        @pl.when(jnp.logical_not(is_last))
        def _():
            fetch(strips_ref)

    out = jax.ShapeDtypeStruct((images * share, rows, cols, channels), strips.dtype)
    sems = [pltpu.SemaphoreType.DMA((2 * images,))]
    return call(kernel, [out, out], [strips, cotangent], (), sems, {}, (0, 1))


def load_call(weights, first, after):
    def kernel(weights_ref, after_ref, *refs):
        out_ref, sems = refs[-2:]

        @pl.when((lax.axis_index("section") == 0) == first)
        def _():
            copies = [
                pltpu.make_async_copy(weights_ref.at[which], out_ref.at[which], sems.at[which])
                for which in range(2)
            ]
            for copy in copies:
                copy.start()
            for copy in copies:
                copy.wait()

    out = jax.ShapeDtypeStruct(weights.shape, weights.dtype)
    sems = [pltpu.SemaphoreType.DMA((2,))]
    (loaded,) = call(kernel, [out], [weights, after], (1,), sems, {}, (0,))
    return loaded


def join_call(own, other):
    crops, rows, cols, channels = own.shape

    def kernel(own_ref, other_ref, *out_refs):
        is_left = lax.axis_index("slab") == 0
        for crop, out_ref in enumerate(out_refs):
            mine = own_ref[crop].astype(jnp.float32)
            theirs = other_ref[crop].astype(jnp.float32)
            left = jnp.where(is_left, mine, theirs)
            right = jnp.where(is_left, theirs, mine)
            whole = jnp.concatenate([left, right], axis=1)
            out_ref[...] = whole.reshape(rows * 2 * cols, channels).astype(jnp.bfloat16)

    out = jax.ShapeDtypeStruct((rows * 2 * cols, channels), own.dtype)
    return call(kernel, [out] * crops, [own, other], (), [], {})


def part_call(kept, rows, after):
    crops, count, channels = kept.shape
    cols = count // rows // 2

    def kernel(kept_ref, after_ref, own_ref, other_ref):
        is_left = lax.axis_index("slab") == 0
        for crop in range(crops):
            whole = kept_ref[crop].astype(jnp.float32).reshape(rows, 2 * cols, channels)
            left, right = whole[:, :cols], whole[:, cols:]
            own_ref[crop] = jnp.where(is_left, left, right).astype(jnp.bfloat16)
            other_ref[crop] = jnp.where(is_left, right, left).astype(jnp.bfloat16)

    out = jax.ShapeDtypeStruct((crops, rows, cols, channels), kept.dtype)
    return call(kernel, [out, out], [kept, after], (1,), [], {})


def merge_call(own, other, images):
    crops, rows, cols, channels = own.shape
    share = crops // images

    def kernel(own_ref, other_ref, out_ref):
        place = lax.axis_index("slab")
        for image in range(images):
            for crop in range(share):
                out_ref[image, place * share + crop] = own_ref[image * share + crop]
                out_ref[image, (1 - place) * share + crop] = other_ref[image * share + crop]

    out = jax.ShapeDtypeStruct((images, 2 * share, rows, cols, channels), own.dtype)
    (merged,) = call(kernel, [out], [own, other], (), [], {})
    return merged


def stack_call(blocks):
    def kernel(*refs):
        for place in range(len(blocks)):
            refs[-1][place] = refs[place][...]

    out = jax.ShapeDtypeStruct((len(blocks), *blocks[0].shape), blocks[0].dtype)
    (stacked,) = call(kernel, [out], [*blocks], (), [], {})
    return stacked


def remake_call(saved, weights, blocks, width, sections):
    _, crops, count, channels = saved.shape
    share = channels // 2
    each = len(blocks)

    def kernel(saved_ref, weights_ref, *refs):
        home_ref, outer_ref, taps, shifted = refs[-4:]
        is_left = lax.axis_index("slab") == 0
        section = lax.axis_index("section")

        def put(kind, block, crop, value):
            cells = slice(crop * count, (crop + 1) * count)
            flipped = value.T
            low, high = flipped[:share], flipped[share:]
            home_ref[kind, block, :, cells] = jnp.where(is_left, low, high)
            outer_ref[kind, block, :, cells] = jnp.where(is_left, high, low)

        @pl.when((section >= sections[0]) & (section <= sections[1]))
        def _():
            for crop in range(crops):
                for kind in range(2):
                    put(kind, 0, crop, saved_ref[kind, crop])
            for block in range(each):
                home_ref[0, 1 + block] = refs[block][0]
                outer_ref[0, 1 + block] = refs[block][1]
                for crop in range(crops):
                    cells = slice(crop * count, (crop + 1) * count)
                    mine, theirs = refs[block][0, :, cells], refs[block][1, :, cells]
                    low, high = jnp.where(is_left, mine, theirs), jnp.where(is_left, theirs, mine)
                    field = jnp.concatenate([low, high], axis=0).T.astype(jnp.float32)
                    hidden = convolved(field, weights_ref.at[0], taps, shifted, width)
                    active = (hidden * jax.nn.sigmoid(hidden)).astype(jnp.bfloat16)
                    put(1, 1 + block, crop, active)

    out = jax.ShapeDtypeStruct((2, 1 + each, share, crops * count), saved.dtype)
    scratch = [
        pltpu.VMEM((count + 2 * width, 3 * channels), jnp.bfloat16),
        pltpu.VMEM((count + 16, channels), jnp.float32),
    ]
    return call(kernel, [out, out], [saved, weights, *blocks], (), scratch, {})


def spread_call(first, cells_of, around, place, count, width):
    two, blocks, share, cells = cells_of.shape
    crops = cells // count
    total = 2 * blocks * cells

    def kernel(first_ref, cells_ref, *refs):
        out_ref, shifted = refs[-2:]
        is_first = lax.axis_index("section") == 0
        for kind in range(two):
            for block in range(blocks):
                for crop in range(crops):
                    cell = slice(crop * count, (crop + 1) * count)
                    value = jnp.where(
                        is_first, first_ref[kind, block, :, cell], cells_ref[kind, block, :, cell]
                    )
                    value = value.T.astype(jnp.float32)
                    before, after = neighbours(value, shifted, width)
                    at = (place * blocks + block) * cells + crop * count
                    for side, part in enumerate((before, value, after)):
                        lanes = slice(side * share, (side + 1) * share)
                        out_ref[kind, at : at + count, lanes] = part.astype(jnp.bfloat16)

    out = jax.ShapeDtypeStruct((two, total, 3 * share), jnp.bfloat16)
    scratch = [pltpu.VMEM((count + 16, share), jnp.float32)]
    operands = [first, cells_of] if around is None else [first, cells_of, around]
    aliases = {} if around is None else {2: 0}
    (spread,) = call(kernel, [out], operands, (), scratch, aliases)
    return spread


def terms_call(around, own, other, count, width, scaling):
    blocks, _, columns, cells = own.shape
    rows = around.shape[2] // 3
    crops = cells // count

    def moved(value, down):
        parts = []
        edge = jnp.zeros((columns, width), value.dtype)
        for crop in range(crops):
            part = value[:, crop * count : (crop + 1) * count]
            if down == 0:
                part = jnp.concatenate([part[:, width:], edge], axis=1)
            elif down == 2:
                part = jnp.concatenate([edge, part[:, : count - width]], axis=1)
            parts.append(part)
        return jnp.concatenate(parts, axis=1)

    def kernel(around_ref, own_ref, other_ref, out_ref, held, sems):
        copies = []
        for kind in (1, 0):
            total = None
            for block in range(2 * blocks):
                left = own_ref if block < blocks else other_ref
                left = left[block % blocks, 1 - kind]
                left = jnp.concatenate([moved(left, down) for down in range(3)], axis=0)
                right = around_ref[kind, block * cells : (block + 1) * cells, :]
                term = jnp.dot(left, right, preferred_element_type=jnp.float32)
                total = term if total is None else total + term
            for down in range(3):
                part = total[down * columns : (down + 1) * columns] * scaling
                part = part.T.reshape(3, rows, columns)
                for place in range(3):
                    held[kind, 3 * down + place] = part[place]
            copy = pltpu.make_async_copy(held.at[kind], out_ref.at[kind], sems.at[kind])
            copy.start()
            copies.append(copy)
        for copy in copies:
            copy.wait()

    shape = (2, 9, rows, columns)
    return pl.pallas_call(
        kernel,
        out_shape=jax.ShapeDtypeStruct(shape, jnp.float32),
        in_specs=[pl.BlockSpec(memory_space=pltpu.VMEM)] * 3,
        out_specs=pl.BlockSpec(memory_space=pltpu.HBM),
        scratch_shapes=[pltpu.VMEM(shape, jnp.float32), pltpu.SemaphoreType.DMA((2,))],
        compiler_params=pltpu.CompilerParams(vmem_limit_bytes=8 << 20),
        name="terms",
    )(around, own, other)


def rotated(value, axis, steps):
    count = lax.axis_size(axis)
    return lax.ppermute(value, axis, [(source, (source + steps) % count) for source in range(count)])


def crop_shards(strips, kernels, cotangent):
    sections = lax.axis_size("section")
    slabs, groups = lax.axis_size("slab"), lax.axis_size("img")
    images, strip_count, row_count, col_count, channels = strips.shape
    width = col_count * slabs
    count = row_count * width
    crops = images * strip_count // slabs
    shape = (count, channels)
    last = sections - 1
    early = min(1, last - 1)
    steps = range(1, groups)
    scaling = 1.0 / math.sqrt(images * groups * strip_count * count)

    def hop(values, source, target):
        arrived = []
        for value in values:
            arrived.append(lax.ppermute(value, "section", [(source, target)]))
        return arrived

    def shared(values, step, routes):
        pairs = [
            (place * groups + i, place * groups + (i + step) % groups)
            for place in routes
            for i in range(groups)
        ]
        return lax.ppermute(values, ("section", "img"), pairs)

    def swapped(value):
        return rotated(value, "slab", 1)

    def flipped(saved, after):
        return flip_call([(saved, (0, crop)) for crop in range(crops)], slabs, "slab", after)

    own, other = split_call(
        pltpu.with_memory_space_constraint(strips, pltpu.HBM),
        pltpu.with_memory_space_constraint(cotangent, pltpu.HBM),
        last,
    )
    other = swapped(other)
    weights = kernels[0].reshape(2, 3, 3 * channels, channels)
    stored = pltpu.with_memory_space_constraint(weights, pltpu.HBM)
    loaded = weights = load_call(stored, True, own)
    fields = join_call(own, other)
    incoming = fields
    state = []
    turned, after = None, weights
    grads = []

    def forward(place, crop):
        return forward_call(
            incoming[crop],
            weights,
            state,
            place,
            crop,
            crops,
            shape,
            width,
            place == last,
            after,
        )

    def backward(place, crop, incoming):
        return backward_call(
            incoming[crop],
            turned,
            state[1],
            grads,
            place,
            crop,
            crops,
            shape,
            width,
            place == last,
            groups,
            after,
        )

    for place in range(last):
        outgoing = []
        for crop in range(crops):
            out, state = forward(place, crop)
            outgoing.append(out)
        if place == 0:
            weights = load_call(stored, False, state[0])
        incoming = hop(outgoing, place, place + 1)
        if place == early:
            inputs = flipped(state[0], state[1])
            soon = [shared(inputs, step, [0]) for step in steps]
            turned = turn_call(loaded, weights, state[0])
            after = turned
    outgoing = []
    for crop in range(crops):
        _, state = forward(last, crop)
        out, grads = backward(last, crop, fields)
        after = out
        outgoing.append(out)
    saved, hidden = state
    incoming = hop(outgoing, last, last - 1)
    inputs = flipped(saved, outgoing[-1])
    late = [shared(inputs, step, range(sections)) for step in steps]
    after = hidden
    for place in reversed(range(last)):
        if place == 0:
            first, early_outer = remake_call(saved, loaded, soon, width, (0, 0))
            after = first
            early_outer = lax.ppermute(early_outer, ("section", "slab"), [(i, (i + 1) % slabs) for i in range(slabs)])
        outgoing = []
        for crop in range(crops):
            out, grads = backward(place, crop, incoming)
            outgoing.append(out)
        if place:
            incoming = hop(outgoing, place, place - 1)
    kept, sent = grads
    kept = finish_call(incoming, turned, kept, width)
    own = [sent[0]]
    for step in steps:
        own.append(shared(sent[step], step, range(sections)))
    home, outer = remake_call(saved, weights, late, width, (1, last))
    outer = swapped(outer)
    around = spread_call(first, home, None, 0, count, width)
    around = spread_call(early_outer, outer, around, 1, count, width)
    own = stack_call(own)
    other = swapped(own)
    terms = terms_call(around, own, other, count, width, scaling)
    own, other = part_call(kept, row_count, sent)
    other = swapped(other)
    grad_inputs = merge_call(own, other, images)
    return (terms[None], grad_inputs[None])


def shards(strips, kernels, cotangent):
    slabs, groups = lax.axis_size("slab"), lax.axis_size("img")
    strip_count, row_count, col_count, channels = strips.shape[1:]
    width = col_count * slabs
    whole_crops = strip_count % slabs == 0 and width % 16 == 0 and (row_count * width) % 128 == 0
    whole_crops = whole_crops and slabs == 2 and lax.axis_size("section") > 1
    if whole_crops and channels % (16 * slabs) == 0 and channels % (16 * groups) == 0:
        return crop_shards(strips, kernels, cotangent)
    return column_shards(strips, kernels, cotangent)


def solution(mesh):
    in_specs = (
        P("img", None, None, "slab", None),
        P("section", None, None, None, None),
        P("img", None, None, "slab", None),
    )
    out_specs = (
        P("section", None, None, "slab", "img"),
        P("section", "img", None, None, "slab", None),
    )
    return jax.shard_map(shards, mesh=mesh, in_specs=in_specs, out_specs=out_specs, check_vma=False)
```

```python
import math

import jax
import jax.numpy as jnp
from jax import lax
from jax.experimental import pallas as pl
from jax.experimental.pallas import tpu as pltpu
from jax.sharding import PartitionSpec as P


def passed_along(value, axis, steps):
    count = lax.axis_size(axis)
    initial, last = (max(0, -steps), min(count, count - steps))
    return lax.ppermute(value, axis, [(source, source + steps) for source in range(initial, last)])


def padded_2(cells, sides, width):
    for axis, dim in sides:
        count = lax.axis_size(axis)
        ends = count - 1
        head = lax.slice_in_dim(cells, 0, width, axis=dim)
        tail = lax.slice_in_dim(cells, cells.shape[dim] - width, cells.shape[dim], axis=dim)
        cells = jnp.concatenate(
            [
                lax.ppermute(tail, axis, [(i, (i + 1) % count) for i in range(ends)]),
                cells,
                lax.ppermute(head, axis, [((i + 1) % count, i) for i in range(ends)]),
            ],
            axis=dim,
        )
    return cells


def unfold(padded, row_count, col_count):
    tap_list = [
        padded[:, down_at : down_at + row_count, right_at : right_at + col_count, :]
        for down_at in range(3)
        for right_at in range(3)
    ]
    stacked = jnp.concatenate(tap_list, axis=3)
    return stacked.reshape(-1, stacked.shape[3])


def columns_of(wide_field):
    row_count = wide_field.shape[1]
    col_count = wide_field.shape[2] - 2
    padded = jnp.pad(wide_field, ((0, 0), (1, 1), (0, 0), (0, 0)))
    return unfold(padded, row_count, col_count)


def convolve(matrix, wide_field):
    count, row_count = (wide_field.shape[0], wide_field.shape[1])
    col_count = wide_field.shape[2] - 2
    flat_out = jnp.dot(columns_of(wide_field), matrix, preferred_element_type=jnp.float32)
    return flat_out.reshape(count, row_count, col_count, matrix.shape[1])


def contract(wide_field, grad_out):
    flat_grad = grad_out.reshape(-1, grad_out.shape[3])
    return lax.dot_general(
        columns_of(wide_field),
        flat_grad,
        (((0,), (0,)), ((), ())),
        preferred_element_type=jnp.float32,
    )


def silu_slope(hidden):
    sigmoid_at = jax.nn.sigmoid(hidden)
    return sigmoid_at * (1.0 + hidden * (1.0 - sigmoid_at))


def store(buffer, value, slot_index, is_valid, axis_at):
    current = lax.dynamic_index_in_dim(buffer, slot_index, axis_at, keepdims=False)
    return lax.dynamic_update_index_in_dim(
        buffer, jnp.where(is_valid, value, current), slot_index, axis_at
    )


def column_shards(strips, kernels, cotangent):
    section_count = lax.axis_size("section")
    section_index = lax.axis_index("section")
    slab_count = lax.axis_size("slab")
    slab_index = lax.axis_index("slab")
    images, strip_count, row_count, col_count, channels = strips.shape
    weights = kernels[0]
    first_forward = weights[0].reshape(9 * channels, channels)
    second_forward = weights[1].reshape(9 * channels, channels)
    first_backward = jnp.transpose(weights[0][::-1], (0, 2, 1)).reshape(9 * channels, channels)
    second_backward = jnp.transpose(weights[1][::-1], (0, 2, 1)).reshape(9 * channels, channels)
    scaling = 1.0 / math.sqrt(
        images * lax.axis_size("img") * strip_count * row_count * col_count * slab_count
    )
    position = slab_index * col_count - 1 + jnp.arange(col_count + 2, dtype=jnp.int32)
    inside = ((position >= 0) & (position < slab_count * col_count))[None, None, :, None]
    tick_count = strip_count + section_count - 1
    hidden_cols = col_count + 2
    empty_field = jnp.zeros((images, row_count, col_count, channels), jnp.bfloat16)
    saved_field = jnp.zeros((strip_count, images, row_count, col_count + 2, channels), jnp.bfloat16)
    saved_hidden = jnp.zeros((strip_count, images, row_count, hidden_cols, channels), jnp.float32)
    saved_active = jnp.zeros(
        (strip_count, images, row_count, col_count + 2, channels), jnp.bfloat16
    )
    outgoing = empty_field
    for step_no in range(tick_count):
        micro_index = step_no - section_index
        is_valid = (micro_index >= 0) & (micro_index < strip_count)
        slot_index = jnp.clip(micro_index, 0, strip_count - 1)
        if step_no == 0:
            incoming = empty_field
        else:
            incoming = passed_along(outgoing, "section", 1)
        first_strip = lax.dynamic_index_in_dim(strips, slot_index, 1, keepdims=False)
        field_in = jnp.where(section_index == 0, first_strip, incoming)
        wide_deep = padded_2(field_in, (("slab", 2),), 2)
        hidden = convolve(first_forward, wide_deep)
        wide_active = jnp.where(inside, jax.nn.silu(hidden), 0.0).astype(jnp.bfloat16)
        wide_field = wide_deep[:, :, 1:-1, :]
        outgoing = (field_in.astype(jnp.float32) + convolve(second_forward, wide_active)).astype(
            jnp.bfloat16
        )
        saved_field = store(saved_field, wide_field, slot_index, is_valid, 0)
        saved_hidden = store(saved_hidden, hidden, slot_index, is_valid, 0)
        saved_active = store(saved_active, wide_active, slot_index, is_valid, 0)
    grad_slots = jnp.zeros((images, strip_count, row_count, col_count, channels), jnp.bfloat16)
    saved_grad_out = jnp.zeros((strip_count, images, row_count, col_count, channels), jnp.bfloat16)
    saved_grad_hidden = jnp.zeros(
        (strip_count, images, row_count, col_count, channels), jnp.bfloat16
    )
    sending = empty_field
    for step_no in range(tick_count):
        micro_index = step_no - (section_count - 1 - section_index)
        is_valid = (micro_index >= 0) & (micro_index < strip_count)
        slot_index = jnp.clip(micro_index, 0, strip_count - 1)
        if step_no == 0:
            arriving = empty_field
        else:
            arriving = passed_along(sending, "section", -1)
        top_grad = lax.dynamic_index_in_dim(cotangent, slot_index, 1, keepdims=False)
        grad_out = jnp.where(section_index == section_count - 1, top_grad, arriving)
        grad_out = jnp.where(is_valid, grad_out, jnp.zeros_like(grad_out))
        hidden = lax.dynamic_index_in_dim(saved_hidden, slot_index, 0, keepdims=False)
        wide_grad = padded_2(grad_out, (("slab", 2),), 2)
        grad_active = convolve(second_backward, wide_grad)
        wide_hidden_grad = jnp.where(inside, grad_active * silu_slope(hidden), 0.0).astype(
            jnp.bfloat16
        )
        grad_hidden = wide_hidden_grad[:, :, 1:-1, :]
        sending = (
            grad_out.astype(jnp.float32) + convolve(first_backward, wide_hidden_grad)
        ).astype(jnp.bfloat16)
        saved_grad_out = store(saved_grad_out, grad_out, slot_index, is_valid, 0)
        saved_grad_hidden = store(saved_grad_hidden, grad_hidden, slot_index, is_valid, 0)
        grad_slots = store(grad_slots, sending, slot_index, is_valid, 1)
    flat_count = strip_count * images
    lower_part = contract(
        saved_field.reshape(flat_count, row_count, col_count + 2, channels),
        saved_grad_hidden.reshape(flat_count, row_count, col_count, channels),
    )
    upper_part = contract(
        saved_active.reshape(flat_count, row_count, col_count + 2, channels),
        saved_grad_out.reshape(flat_count, row_count, col_count, channels),
    )
    grad_terms = jnp.stack([lower_part, upper_part]).reshape(2, 9, channels, channels)
    row_share = lax.psum_scatter(
        grad_terms.astype(jnp.bfloat16), "slab", scatter_dimension=2, tiled=True
    )
    own_share = lax.psum_scatter(row_share, "img", scatter_dimension=3, tiled=True).astype(
        jnp.float32
    )
    grad_kernels = (own_share * scaling)[None]
    return (grad_kernels, grad_slots[None])


def call(kernel, outs, operands, unread, scratch, aliases, apart=()):
    spaces = {**dict.fromkeys(unread, pl.ANY), **dict.fromkeys(apart, pltpu.HBM)}
    return pl.pallas_call(
        kernel,
        out_shape=outs,
        in_specs=[
            pl.BlockSpec(memory_space=spaces.get(place, pltpu.VMEM))
            for place in range(len(operands))
        ],
        out_specs=[pl.BlockSpec(memory_space=pltpu.VMEM)] * len(outs),
        scratch_shapes=scratch,
        input_output_aliases=aliases,
        compiler_params=pltpu.CompilerParams(vmem_limit_bytes=8 << 20),
    )(*operands)


def half_lanes(count, channels):
    return channels % 128 == 64 and count % 32 == 0


def packed_shape(count, channels):
    return (count * channels // 128, 128) if half_lanes(count, channels) else (count, channels)


def pack(value):
    count, channels = value.shape
    if not half_lanes(count, channels):
        return value
    parts = [value[:, at : at + 128] for at in range(0, channels - 64, 128)]
    rest = value[:, channels - 64 :]
    parts.append(jnp.concatenate([rest[: count // 2], rest[count // 2 :]], axis=1))
    return jnp.concatenate(parts, axis=0)


def unpack(value, count, channels):
    if not half_lanes(count, channels):
        return value
    whole = channels // 128
    parts = [value[k * count : (k + 1) * count] for k in range(whole)]
    rest = value[whole * count :]
    parts.append(jnp.concatenate([rest[:, :64], rest[:, 64:]], axis=0))
    return jnp.concatenate(parts, axis=1)


def neighbours(value, shifted, width):
    count, channels = value.shape
    shifted[8 : 8 + count, :] = value
    column = lax.rem(lax.broadcasted_iota(jnp.int32, (count, channels), 0), width)
    before = jnp.where(column == 0, 0.0, shifted[7 : 7 + count, :])
    after = jnp.where(column == width - 1, 0.0, shifted[9 : 9 + count, :])
    return before, after


def convolved(value, matrix, taps, shifted, width):
    count, channels = value.shape
    before, after = neighbours(value, shifted, width)
    for place, part in enumerate((before, value, after)):
        taps[width : width + count, place * channels : (place + 1) * channels] = part.astype(
            jnp.bfloat16
        )
    edge = jnp.zeros((width, 3 * channels), jnp.bfloat16)
    taps[0:width, :] = edge
    taps[width + count : 2 * width + count, :] = edge
    total = jnp.dot(taps[0:count, :], matrix[0], preferred_element_type=jnp.float32)
    for down in (1, 2):
        total = total + jnp.dot(
            taps[down * width : down * width + count, :],
            matrix[down],
            preferred_element_type=jnp.float32,
        )
    return total


def forward_call(field, weights, state, section, crop, crops, shape, width, last, after):
    count, channels = shape

    def kernel(field_ref, weights_ref, after_ref, *refs):
        *_, saved_ref, hidden_ref, taps, shifted = refs

        @pl.when(lax.axis_index("section") == section)
        def _():
            field_in = field_ref[...]
            if section:
                field_in = unpack(field_in, count, channels)
            wide = field_in.astype(jnp.float32)
            saved_ref[0, crop] = field_in
            hidden = convolved(wide, weights_ref.at[0], taps, shifted, width)
            hidden_ref[crop] = hidden
            active = (hidden * jax.nn.sigmoid(hidden)).astype(jnp.bfloat16)
            saved_ref[1, crop] = active
            if not last:
                added = convolved(
                    active.astype(jnp.float32), weights_ref.at[1], taps, shifted, width
                )
                refs[-5][...] = pack((wide + added).astype(jnp.bfloat16))

    outs = [
        jax.ShapeDtypeStruct(packed_shape(count, channels), jnp.bfloat16),
        jax.ShapeDtypeStruct((2, crops, count, channels), jnp.bfloat16),
        jax.ShapeDtypeStruct((crops, count, channels), jnp.float32),
    ][1 if last else 0 :]
    scratch = [
        pltpu.VMEM((count + 2 * width, 3 * channels), jnp.bfloat16),
        pltpu.VMEM((count + 16, channels), jnp.float32),
    ]
    aliases = {3 + k: k + (0 if last else 1) for k in range(len(state))}
    outputs = call(kernel, outs, [field, weights, after, *state], (2,), scratch, aliases)
    return (None if last else outputs[0]), outputs[-2:]


def backward_call(
    grad, turned, hidden, state, section, crop, crops, shape, width, last, parts, after
):
    count, channels = shape
    share = channels // parts
    first = section == 0

    def kernel(grad_ref, turned_ref, hidden_ref, after_ref, *refs):
        *_, kept_ref, sent_ref, taps, shifted = refs

        @pl.when(lax.axis_index("section") == section)
        def _():
            grad = grad_ref[...]
            if not last:
                grad = unpack(grad, count, channels)
            wide = grad.astype(jnp.float32)
            own = lax.axis_index("img")
            place_parts(sent_ref, (0,), grad, crop, parts, own)
            grad_active = convolved(wide, turned_ref.at[1], taps, shifted, width)
            hidden = hidden_ref[crop]
            gate = jax.nn.sigmoid(hidden)
            grad_hidden = (grad_active * (gate * (1.0 + hidden * (1.0 - gate)))).astype(
                jnp.bfloat16
            )
            place_parts(sent_ref, (1,), grad_hidden, crop, parts, own)
            if first:
                kept_ref[crop] = grad_hidden
            else:
                added = convolved(
                    grad_hidden.astype(jnp.float32), turned_ref.at[0], taps, shifted, width
                )
                result = (wide + added).astype(jnp.bfloat16)
                kept_ref[crop] = result
                refs[-5][...] = pack(result)

    outs = [
        jax.ShapeDtypeStruct(packed_shape(count, channels), jnp.bfloat16),
        jax.ShapeDtypeStruct((crops, count, channels), jnp.bfloat16),
        jax.ShapeDtypeStruct((parts, 2, share, crops * count), jnp.bfloat16),
    ][1 if first else 0 :]
    scratch = [
        pltpu.VMEM((count + 2 * width, 3 * channels), jnp.bfloat16),
        pltpu.VMEM((count + 16, channels), jnp.float32),
    ]
    aliases = {4 + k: k + (0 if first else 1) for k in range(len(state))}
    operands = [grad, turned, hidden, after, *state]
    outputs = call(kernel, outs, operands, (3,), scratch, aliases)
    return (None if first else outputs[0]), outputs[-2:]


def finish_call(grads, turned, kept, width):
    crops, count, channels = kept.shape

    def kernel(turned_ref, *refs):
        kept_ref, taps, shifted = refs[-3:]

        @pl.when(lax.axis_index("section") == 0)
        def _():
            for crop in range(crops):
                wide = unpack(refs[crop][...], count, channels).astype(jnp.float32)
                grad_hidden = kept_ref[crop].astype(jnp.float32)
                added = convolved(grad_hidden, turned_ref.at[0], taps, shifted, width)
                kept_ref[crop] = (wide + added).astype(jnp.bfloat16)

    out = jax.ShapeDtypeStruct(kept.shape, kept.dtype)
    scratch = [
        pltpu.VMEM((count + 2 * width, 3 * channels), jnp.bfloat16),
        pltpu.VMEM((count + 16, channels), jnp.float32),
    ]
    operands = [turned, *grads, kept]
    (kept,) = call(kernel, [out], operands, (), scratch, {len(operands) - 1: 0})
    return kept


def place_parts(target, lead, value, crop, parts, own):
    count, channels = value.shape
    share = channels // parts
    flipped = value.T
    for part in range(parts):
        slot = lax.rem(part + parts - own, parts)
        target[(slot, *lead, slice(None), slice(crop * count, (crop + 1) * count))] = flipped[
            part * share : (part + 1) * share, :
        ]


def flip_call(kept, parts, axis, after):
    def kernel(*refs):
        flipped_ref = refs[-1]
        for crop, (place, index) in enumerate(kept):
            value = refs[place][index]
            place_parts(flipped_ref, (), value, crop, parts, lax.axis_index(axis))

    operands = []
    for array, index in kept:
        if all(array is not other for other in operands):
            operands.append(array)
    kept = [
        ([array is other for other in operands].index(True), index) for array, index in kept
    ]
    count, channels = operands[0].shape[-2:]
    out = jax.ShapeDtypeStruct((parts, channels // parts, len(kept) * count), operands[0].dtype)
    (flipped,) = call(kernel, [out], [*operands, after], (len(operands),), [], {})
    return flipped


def turn_call(loaded, weights, after):
    two, _, _, channels = weights.shape

    def kernel(loaded_ref, weights_ref, after_ref, turned_ref):
        is_first = lax.axis_index("section") == 0
        for which in range(two):
            for tap in range(9):
                down, right = divmod(tap, 3)
                rows = slice(right * channels, (right + 1) * channels)
                value = jnp.where(
                    is_first, loaded_ref[which, down, rows, :], weights_ref[which, down, rows, :]
                )
                down, right = divmod(8 - tap, 3)
                turned_ref[which, down, right * channels : (right + 1) * channels, :] = value.T

    out = jax.ShapeDtypeStruct(weights.shape, weights.dtype)
    (turned,) = call(kernel, [out], [loaded, weights, after], (2,), [], {})
    return turned


def split_call(strips, cotangent, last):
    images, strip_count, rows, cols, channels = strips.shape
    share = strip_count // 2

    def kernel(strips_ref, cotangent_ref, own_ref, other_ref, sems):
        own = lax.axis_index("slab")
        is_last = lax.axis_index("section") == last

        def fetch(source_ref):
            copies = []
            for image in range(images):
                at = pl.ds(image * share, share)
                for side, (ref, half) in enumerate(((own_ref, own), (other_ref, 1 - own))):
                    source = source_ref.at[image, pl.ds(half * share, share)]
                    copies.append(pltpu.make_async_copy(source, ref.at[at], sems.at[2 * image + side]))
            for copy in copies:
                copy.start()
            for copy in copies:
                copy.wait()

        @pl.when(is_last)
        def _():
            fetch(cotangent_ref)

        @pl.when(jnp.logical_not(is_last))
        def _():
            fetch(strips_ref)

    out = jax.ShapeDtypeStruct((images * share, rows, cols, channels), strips.dtype)
    sems = [pltpu.SemaphoreType.DMA((2 * images,))]
    return call(kernel, [out, out], [strips, cotangent], (), sems, {}, (0, 1))


def load_call(weights, first, after):
    def kernel(weights_ref, after_ref, *refs):
        out_ref, sems = refs[-2:]

        @pl.when((lax.axis_index("section") == 0) == first)
        def _():
            copies = [
                pltpu.make_async_copy(weights_ref.at[which], out_ref.at[which], sems.at[which])
                for which in range(2)
            ]
            for copy in copies:
                copy.start()
            for copy in copies:
                copy.wait()

    out = jax.ShapeDtypeStruct(weights.shape, weights.dtype)
    sems = [pltpu.SemaphoreType.DMA((2,))]
    (loaded,) = call(kernel, [out], [weights, after], (1,), sems, {}, (0,))
    return loaded


def join_call(own, other):
    crops, rows, cols, channels = own.shape

    def kernel(own_ref, other_ref, *out_refs):
        is_left = lax.axis_index("slab") == 0
        for crop, out_ref in enumerate(out_refs):
            mine = own_ref[crop].astype(jnp.float32)
            theirs = other_ref[crop].astype(jnp.float32)
            left = jnp.where(is_left, mine, theirs)
            right = jnp.where(is_left, theirs, mine)
            whole = jnp.concatenate([left, right], axis=1)
            out_ref[...] = whole.reshape(rows * 2 * cols, channels).astype(jnp.bfloat16)

    out = jax.ShapeDtypeStruct((rows * 2 * cols, channels), own.dtype)
    return call(kernel, [out] * crops, [own, other], (), [], {})


def part_call(kept, rows, after):
    crops, count, channels = kept.shape
    cols = count // rows // 2

    def kernel(kept_ref, after_ref, own_ref, other_ref):
        is_left = lax.axis_index("slab") == 0
        for crop in range(crops):
            whole = kept_ref[crop].astype(jnp.float32).reshape(rows, 2 * cols, channels)
            left, right = whole[:, :cols], whole[:, cols:]
            own_ref[crop] = jnp.where(is_left, left, right).astype(jnp.bfloat16)
            other_ref[crop] = jnp.where(is_left, right, left).astype(jnp.bfloat16)

    out = jax.ShapeDtypeStruct((crops, rows, cols, channels), kept.dtype)
    return call(kernel, [out, out], [kept, after], (1,), [], {})


def merge_call(own, other, images):
    crops, rows, cols, channels = own.shape
    share = crops // images

    def kernel(own_ref, other_ref, out_ref):
        place = lax.axis_index("slab")
        for image in range(images):
            for crop in range(share):
                out_ref[image, place * share + crop] = own_ref[image * share + crop]
                out_ref[image, (1 - place) * share + crop] = other_ref[image * share + crop]

    out = jax.ShapeDtypeStruct((images, 2 * share, rows, cols, channels), own.dtype)
    (merged,) = call(kernel, [out], [own, other], (), [], {})
    return merged


def stack_call(blocks):
    def kernel(*refs):
        for place in range(len(blocks)):
            refs[-1][place] = refs[place][...]

    out = jax.ShapeDtypeStruct((len(blocks), *blocks[0].shape), blocks[0].dtype)
    (stacked,) = call(kernel, [out], [*blocks], (), [], {})
    return stacked


def remake_call(saved, weights, blocks, width, sections, earlier=None):
    _, crops, count, channels = saved.shape
    share = channels // 2
    each = len(blocks)

    def kernel(saved_ref, weights_ref, *refs):
        home_ref, outer_ref, taps, shifted = refs[-4:]
        is_left = lax.axis_index("slab") == 0
        section = lax.axis_index("section")

        def put(kind, block, crop, value):
            cells = slice(crop * count, (crop + 1) * count)
            flipped = value.T
            low, high = flipped[:share], flipped[share:]
            home_ref[kind, block, :, cells] = jnp.where(is_left, low, high)
            outer_ref[kind, block, :, cells] = jnp.where(is_left, high, low)

        is_active = (section >= sections[0]) & (section <= sections[1])
        if earlier is not None:

            @pl.when(jnp.logical_not(is_active))
            def _():
                outer_ref[...] = refs[each][...]

        @pl.when(is_active)
        def _():
            for crop in range(crops):
                for kind in range(2):
                    put(kind, 0, crop, saved_ref[kind, crop])
            for block in range(each):
                home_ref[0, 1 + block] = refs[block][0]
                outer_ref[0, 1 + block] = refs[block][1]
                for crop in range(crops):
                    cells = slice(crop * count, (crop + 1) * count)
                    mine, theirs = refs[block][0, :, cells], refs[block][1, :, cells]
                    low, high = jnp.where(is_left, mine, theirs), jnp.where(is_left, theirs, mine)
                    field = jnp.concatenate([low, high], axis=0).T.astype(jnp.float32)
                    hidden = convolved(field, weights_ref.at[0], taps, shifted, width)
                    active = (hidden * jax.nn.sigmoid(hidden)).astype(jnp.bfloat16)
                    put(1, 1 + block, crop, active)

    out = jax.ShapeDtypeStruct((2, 1 + each, share, crops * count), saved.dtype)
    scratch = [
        pltpu.VMEM((count + 2 * width, 3 * channels), jnp.bfloat16),
        pltpu.VMEM((count + 16, channels), jnp.float32),
    ]
    operands = [saved, weights, *blocks] + ([] if earlier is None else [earlier])
    return call(kernel, [out, out], operands, (), scratch, {})


def spread_call(first, cells_of, around, place, count, width):
    two, blocks, share, cells = cells_of.shape
    crops = cells // count
    total = 2 * blocks * cells

    def kernel(first_ref, cells_ref, *refs):
        out_ref, shifted = refs[-2:]
        is_first = lax.axis_index("section") == 0
        for kind in range(two):
            for block in range(blocks):
                for crop in range(crops):
                    cell = slice(crop * count, (crop + 1) * count)
                    value = jnp.where(
                        is_first, first_ref[kind, block, :, cell], cells_ref[kind, block, :, cell]
                    )
                    value = value.T.astype(jnp.float32)
                    before, after = neighbours(value, shifted, width)
                    at = (place * blocks + block) * cells + crop * count
                    for side, part in enumerate((before, value, after)):
                        lanes = slice(side * share, (side + 1) * share)
                        out_ref[kind, at : at + count, lanes] = part.astype(jnp.bfloat16)

    out = jax.ShapeDtypeStruct((two, total, 3 * share), jnp.bfloat16)
    scratch = [pltpu.VMEM((count + 16, share), jnp.float32)]
    operands = [first, cells_of] if around is None else [first, cells_of, around]
    aliases = {} if around is None else {2: 0}
    (spread,) = call(kernel, [out], operands, (), scratch, aliases)
    return spread


def terms_call(around, own, other, count, width, scaling):
    blocks, _, columns, cells = own.shape
    rows = around.shape[2] // 3
    crops = cells // count

    def moved(value, down):
        parts = []
        edge = jnp.zeros((columns, width), value.dtype)
        for crop in range(crops):
            part = value[:, crop * count : (crop + 1) * count]
            if down == 0:
                part = jnp.concatenate([part[:, width:], edge], axis=1)
            elif down == 2:
                part = jnp.concatenate([edge, part[:, : count - width]], axis=1)
            parts.append(part)
        return jnp.concatenate(parts, axis=1)

    def kernel(around_ref, own_ref, other_ref, out_ref, held, sems):
        copies = []
        for kind in (1, 0):
            total = None
            for block in range(2 * blocks):
                left = own_ref if block < blocks else other_ref
                left = left[block % blocks, 1 - kind]
                left = jnp.concatenate([moved(left, down) for down in range(3)], axis=0)
                right = around_ref[kind, block * cells : (block + 1) * cells, :]
                term = jnp.dot(left, right, preferred_element_type=jnp.float32)
                total = term if total is None else total + term
            for down in range(3):
                part = total[down * columns : (down + 1) * columns] * scaling
                part = part.T.reshape(3, rows, columns)
                for place in range(3):
                    held[kind, 3 * down + place] = part[place]
            copy = pltpu.make_async_copy(held.at[kind], out_ref.at[kind], sems.at[kind])
            copy.start()
            copies.append(copy)
        for copy in copies:
            copy.wait()

    shape = (2, 9, rows, columns)
    return pl.pallas_call(
        kernel,
        out_shape=jax.ShapeDtypeStruct(shape, jnp.float32),
        in_specs=[pl.BlockSpec(memory_space=pltpu.VMEM)] * 3,
        out_specs=pl.BlockSpec(memory_space=pltpu.HBM),
        scratch_shapes=[pltpu.VMEM(shape, jnp.float32), pltpu.SemaphoreType.DMA((2,))],
        compiler_params=pltpu.CompilerParams(vmem_limit_bytes=8 << 20),
        name="terms",
    )(around, own, other)


def rotated(value, axis, steps):
    count = lax.axis_size(axis)
    return lax.ppermute(value, axis, [(source, (source + steps) % count) for source in range(count)])


def crop_shards(strips, kernels, cotangent):
    sections = lax.axis_size("section")
    slabs, groups = lax.axis_size("slab"), lax.axis_size("img")
    images, strip_count, row_count, col_count, channels = strips.shape
    width = col_count * slabs
    count = row_count * width
    crops = images * strip_count // slabs
    shape = (count, channels)
    last = sections - 1
    early = min(1, last - 1)
    steps = range(1, groups)
    scaling = 1.0 / math.sqrt(images * groups * strip_count * count)

    def hop(values, source, target):
        arrived = []
        for value in values:
            arrived.append(lax.ppermute(value, "section", [(source, target)]))
        return arrived

    def shared(values, step, routes):
        pairs = [
            (place * groups + i, place * groups + (i + step) % groups)
            for place in routes
            for i in range(groups)
        ]
        return lax.ppermute(values, ("section", "img"), pairs)

    def swapped(value):
        return rotated(value, "slab", 1)

    def flipped(saved, after):
        return flip_call([(saved, (0, crop)) for crop in range(crops)], slabs, "slab", after)

    own, other = split_call(
        pltpu.with_memory_space_constraint(strips, pltpu.HBM),
        pltpu.with_memory_space_constraint(cotangent, pltpu.HBM),
        last,
    )
    other = swapped(other)
    weights = kernels[0].reshape(2, 3, 3 * channels, channels)
    stored = pltpu.with_memory_space_constraint(weights, pltpu.HBM)
    loaded = weights = load_call(stored, True, own)
    fields = join_call(own, other)
    incoming = fields
    state = []
    turned, after = None, weights
    grads = []

    def forward(place, crop):
        return forward_call(
            incoming[crop],
            weights,
            state,
            place,
            crop,
            crops,
            shape,
            width,
            place == last,
            after,
        )

    def backward(place, crop, incoming):
        return backward_call(
            incoming[crop],
            turned,
            state[1],
            grads,
            place,
            crop,
            crops,
            shape,
            width,
            place == last,
            groups,
            after,
        )

    for place in range(last):
        outgoing = []
        for crop in range(crops):
            out, state = forward(place, crop)
            outgoing.append(out)
        if place == 0:
            weights = load_call(stored, False, state[0])
        incoming = hop(outgoing, place, place + 1)
        if place == early:
            inputs = flipped(state[0], state[1])
            soon = [shared(inputs, step, [0]) for step in steps]
            turned = turn_call(loaded, weights, state[0])
            after = turned
    outgoing = []
    for crop in range(crops):
        _, state = forward(last, crop)
        out, grads = backward(last, crop, fields)
        after = out
        outgoing.append(out)
    saved, hidden = state
    incoming = hop(outgoing, last, last - 1)
    inputs = flipped(saved, outgoing[-1])
    late = [shared(inputs, step, range(sections)) for step in steps]
    after = hidden
    for place in reversed(range(last)):
        if place == 0:
            first, early_outer = remake_call(saved, loaded, soon, width, (0, 0))
            after = first
        outgoing = []
        for crop in range(crops):
            out, grads = backward(place, crop, incoming)
            outgoing.append(out)
        if place:
            incoming = hop(outgoing, place, place - 1)
    kept, sent = grads
    kept = finish_call(incoming, turned, kept, width)
    own = [sent[0]]
    for step in steps:
        own.append(shared(sent[step], step, range(sections)))
    home, outer = remake_call(saved, weights, late, width, (1, last), early_outer)
    outer = swapped(outer)
    around = spread_call(first, home, None, 0, count, width)
    around = spread_call(outer, outer, around, 1, count, width)
    own = stack_call(own)
    other = swapped(own)
    terms = terms_call(around, own, other, count, width, scaling)
    own, other = part_call(kept, row_count, sent)
    other = swapped(other)
    grad_inputs = merge_call(own, other, images)
    return (terms[None], grad_inputs[None])


def shards(strips, kernels, cotangent):
    slabs, groups = lax.axis_size("slab"), lax.axis_size("img")
    strip_count, row_count, col_count, channels = strips.shape[1:]
    width = col_count * slabs
    whole_crops = strip_count % slabs == 0 and width % 16 == 0 and (row_count * width) % 128 == 0
    whole_crops = whole_crops and slabs == 2 and lax.axis_size("section") > 1
    if whole_crops and channels % (16 * slabs) == 0 and channels % (16 * groups) == 0:
        return crop_shards(strips, kernels, cotangent)
    return column_shards(strips, kernels, cotangent)


def solution(mesh):
    in_specs = (
        P("img", None, None, "slab", None),
        P("section", None, None, None, None),
        P("img", None, None, "slab", None),
    )
    out_specs = (
        P("section", None, None, "slab", "img"),
        P("section", "img", None, None, "slab", None),
    )
    return jax.shard_map(shards, mesh=mesh, in_specs=in_specs, out_specs=out_specs, check_vma=False)
```

```python
import math

import jax
import jax.numpy as jnp
from jax import lax
from jax.experimental import pallas as pl
from jax.experimental.pallas import tpu as pltpu
from jax.sharding import PartitionSpec as P


def passed_along(value, axis, steps):
    count = lax.axis_size(axis)
    initial, last = (max(0, -steps), min(count, count - steps))
    return lax.ppermute(value, axis, [(source, source + steps) for source in range(initial, last)])


def padded_2(cells, sides, width):
    for axis, dim in sides:
        count = lax.axis_size(axis)
        ends = count - 1
        head = lax.slice_in_dim(cells, 0, width, axis=dim)
        tail = lax.slice_in_dim(cells, cells.shape[dim] - width, cells.shape[dim], axis=dim)
        cells = jnp.concatenate(
            [
                lax.ppermute(tail, axis, [(i, (i + 1) % count) for i in range(ends)]),
                cells,
                lax.ppermute(head, axis, [((i + 1) % count, i) for i in range(ends)]),
            ],
            axis=dim,
        )
    return cells


def unfold(padded, row_count, col_count):
    tap_list = [
        padded[:, down_at : down_at + row_count, right_at : right_at + col_count, :]
        for down_at in range(3)
        for right_at in range(3)
    ]
    stacked = jnp.concatenate(tap_list, axis=3)
    return stacked.reshape(-1, stacked.shape[3])


def columns_of(wide_field):
    row_count = wide_field.shape[1]
    col_count = wide_field.shape[2] - 2
    padded = jnp.pad(wide_field, ((0, 0), (1, 1), (0, 0), (0, 0)))
    return unfold(padded, row_count, col_count)


def convolve(matrix, wide_field):
    count, row_count = (wide_field.shape[0], wide_field.shape[1])
    col_count = wide_field.shape[2] - 2
    flat_out = jnp.dot(columns_of(wide_field), matrix, preferred_element_type=jnp.float32)
    return flat_out.reshape(count, row_count, col_count, matrix.shape[1])


def contract(wide_field, grad_out):
    flat_grad = grad_out.reshape(-1, grad_out.shape[3])
    return lax.dot_general(
        columns_of(wide_field),
        flat_grad,
        (((0,), (0,)), ((), ())),
        preferred_element_type=jnp.float32,
    )


def silu_slope(hidden):
    sigmoid_at = jax.nn.sigmoid(hidden)
    return sigmoid_at * (1.0 + hidden * (1.0 - sigmoid_at))


def store(buffer, value, slot_index, is_valid, axis_at):
    current = lax.dynamic_index_in_dim(buffer, slot_index, axis_at, keepdims=False)
    return lax.dynamic_update_index_in_dim(
        buffer, jnp.where(is_valid, value, current), slot_index, axis_at
    )


def column_shards(strips, kernels, cotangent):
    section_count = lax.axis_size("section")
    section_index = lax.axis_index("section")
    slab_count = lax.axis_size("slab")
    slab_index = lax.axis_index("slab")
    images, strip_count, row_count, col_count, channels = strips.shape
    weights = kernels[0]
    first_forward = weights[0].reshape(9 * channels, channels)
    second_forward = weights[1].reshape(9 * channels, channels)
    first_backward = jnp.transpose(weights[0][::-1], (0, 2, 1)).reshape(9 * channels, channels)
    second_backward = jnp.transpose(weights[1][::-1], (0, 2, 1)).reshape(9 * channels, channels)
    scaling = 1.0 / math.sqrt(
        images * lax.axis_size("img") * strip_count * row_count * col_count * slab_count
    )
    position = slab_index * col_count - 1 + jnp.arange(col_count + 2, dtype=jnp.int32)
    inside = ((position >= 0) & (position < slab_count * col_count))[None, None, :, None]
    tick_count = strip_count + section_count - 1
    hidden_cols = col_count + 2
    empty_field = jnp.zeros((images, row_count, col_count, channels), jnp.bfloat16)
    saved_field = jnp.zeros((strip_count, images, row_count, col_count + 2, channels), jnp.bfloat16)
    saved_hidden = jnp.zeros((strip_count, images, row_count, hidden_cols, channels), jnp.float32)
    saved_active = jnp.zeros(
        (strip_count, images, row_count, col_count + 2, channels), jnp.bfloat16
    )
    outgoing = empty_field
    for step_no in range(tick_count):
        micro_index = step_no - section_index
        is_valid = (micro_index >= 0) & (micro_index < strip_count)
        slot_index = jnp.clip(micro_index, 0, strip_count - 1)
        if step_no == 0:
            incoming = empty_field
        else:
            incoming = passed_along(outgoing, "section", 1)
        first_strip = lax.dynamic_index_in_dim(strips, slot_index, 1, keepdims=False)
        field_in = jnp.where(section_index == 0, first_strip, incoming)
        wide_deep = padded_2(field_in, (("slab", 2),), 2)
        hidden = convolve(first_forward, wide_deep)
        wide_active = jnp.where(inside, jax.nn.silu(hidden), 0.0).astype(jnp.bfloat16)
        wide_field = wide_deep[:, :, 1:-1, :]
        outgoing = (field_in.astype(jnp.float32) + convolve(second_forward, wide_active)).astype(
            jnp.bfloat16
        )
        saved_field = store(saved_field, wide_field, slot_index, is_valid, 0)
        saved_hidden = store(saved_hidden, hidden, slot_index, is_valid, 0)
        saved_active = store(saved_active, wide_active, slot_index, is_valid, 0)
    grad_slots = jnp.zeros((images, strip_count, row_count, col_count, channels), jnp.bfloat16)
    saved_grad_out = jnp.zeros((strip_count, images, row_count, col_count, channels), jnp.bfloat16)
    saved_grad_hidden = jnp.zeros(
        (strip_count, images, row_count, col_count, channels), jnp.bfloat16
    )
    sending = empty_field
    for step_no in range(tick_count):
        micro_index = step_no - (section_count - 1 - section_index)
        is_valid = (micro_index >= 0) & (micro_index < strip_count)
        slot_index = jnp.clip(micro_index, 0, strip_count - 1)
        if step_no == 0:
            arriving = empty_field
        else:
            arriving = passed_along(sending, "section", -1)
        top_grad = lax.dynamic_index_in_dim(cotangent, slot_index, 1, keepdims=False)
        grad_out = jnp.where(section_index == section_count - 1, top_grad, arriving)
        grad_out = jnp.where(is_valid, grad_out, jnp.zeros_like(grad_out))
        hidden = lax.dynamic_index_in_dim(saved_hidden, slot_index, 0, keepdims=False)
        wide_grad = padded_2(grad_out, (("slab", 2),), 2)
        grad_active = convolve(second_backward, wide_grad)
        wide_hidden_grad = jnp.where(inside, grad_active * silu_slope(hidden), 0.0).astype(
            jnp.bfloat16
        )
        grad_hidden = wide_hidden_grad[:, :, 1:-1, :]
        sending = (
            grad_out.astype(jnp.float32) + convolve(first_backward, wide_hidden_grad)
        ).astype(jnp.bfloat16)
        saved_grad_out = store(saved_grad_out, grad_out, slot_index, is_valid, 0)
        saved_grad_hidden = store(saved_grad_hidden, grad_hidden, slot_index, is_valid, 0)
        grad_slots = store(grad_slots, sending, slot_index, is_valid, 1)
    flat_count = strip_count * images
    lower_part = contract(
        saved_field.reshape(flat_count, row_count, col_count + 2, channels),
        saved_grad_hidden.reshape(flat_count, row_count, col_count, channels),
    )
    upper_part = contract(
        saved_active.reshape(flat_count, row_count, col_count + 2, channels),
        saved_grad_out.reshape(flat_count, row_count, col_count, channels),
    )
    grad_terms = jnp.stack([lower_part, upper_part]).reshape(2, 9, channels, channels)
    row_share = lax.psum_scatter(
        grad_terms.astype(jnp.bfloat16), "slab", scatter_dimension=2, tiled=True
    )
    own_share = lax.psum_scatter(row_share, "img", scatter_dimension=3, tiled=True).astype(
        jnp.float32
    )
    grad_kernels = (own_share * scaling)[None]
    return (grad_kernels, grad_slots[None])


def call(kernel, outs, operands, unread, scratch, aliases, apart=(), cost=None):
    spaces = {**dict.fromkeys(unread, pl.ANY), **dict.fromkeys(apart, pltpu.HBM)}
    return pl.pallas_call(
        kernel,
        out_shape=outs,
        in_specs=[
            pl.BlockSpec(memory_space=spaces.get(place, pltpu.VMEM))
            for place in range(len(operands))
        ],
        out_specs=[pl.BlockSpec(memory_space=pltpu.VMEM)] * len(outs),
        scratch_shapes=scratch,
        input_output_aliases=aliases,
        compiler_params=pltpu.CompilerParams(vmem_limit_bytes=8 << 20),
        cost_estimate=cost,
    )(*operands)


def half_lanes(count, channels):
    return channels % 128 == 64 and count % 32 == 0


def packed_shape(count, channels):
    return (count * channels // 128, 128) if half_lanes(count, channels) else (count, channels)


def pack(value):
    count, channels = value.shape
    if not half_lanes(count, channels):
        return value
    parts = [value[:, at : at + 128] for at in range(0, channels - 64, 128)]
    rest = value[:, channels - 64 :]
    parts.append(jnp.concatenate([rest[: count // 2], rest[count // 2 :]], axis=1))
    return jnp.concatenate(parts, axis=0)


def unpack(value, count, channels):
    if not half_lanes(count, channels):
        return value
    whole = channels // 128
    parts = [value[k * count : (k + 1) * count] for k in range(whole)]
    rest = value[whole * count :]
    parts.append(jnp.concatenate([rest[:, :64], rest[:, 64:]], axis=0))
    return jnp.concatenate(parts, axis=1)


def neighbours(value, shifted, width):
    count, channels = value.shape
    shifted[8 : 8 + count, :] = value
    column = lax.rem(lax.broadcasted_iota(jnp.int32, (count, channels), 0), width)
    before = jnp.where(column == 0, 0.0, shifted[7 : 7 + count, :])
    after = jnp.where(column == width - 1, 0.0, shifted[9 : 9 + count, :])
    return before, after


def convolved(value, matrix, taps, shifted, width):
    count, channels = value.shape
    before, after = neighbours(value, shifted, width)
    for place, part in enumerate((before, value, after)):
        taps[width : width + count, place * channels : (place + 1) * channels] = part.astype(
            jnp.bfloat16
        )
    edge = jnp.zeros((width, 3 * channels), jnp.bfloat16)
    taps[0:width, :] = edge
    taps[width + count : 2 * width + count, :] = edge
    total = jnp.dot(taps[0:count, :], matrix[0], preferred_element_type=jnp.float32)
    for down in (1, 2):
        total = total + jnp.dot(
            taps[down * width : down * width + count, :],
            matrix[down],
            preferred_element_type=jnp.float32,
        )
    return total


def forward_call(field, weights, state, section, crop, crops, shape, width, last, after):
    count, channels = shape

    def kernel(field_ref, weights_ref, after_ref, *refs):
        *_, saved_ref, hidden_ref, taps, shifted = refs

        @pl.when(lax.axis_index("section") == section)
        def _():
            field_in = field_ref[...]
            if section:
                field_in = unpack(field_in, count, channels)
            wide = field_in.astype(jnp.float32)
            saved_ref[0, crop] = field_in
            hidden = convolved(wide, weights_ref.at[0], taps, shifted, width)
            hidden_ref[crop] = hidden
            active = (hidden * jax.nn.sigmoid(hidden)).astype(jnp.bfloat16)
            saved_ref[1, crop] = active
            if not last:
                added = convolved(
                    active.astype(jnp.float32), weights_ref.at[1], taps, shifted, width
                )
                refs[-5][...] = pack((wide + added).astype(jnp.bfloat16))

    outs = [
        jax.ShapeDtypeStruct(packed_shape(count, channels), jnp.bfloat16),
        jax.ShapeDtypeStruct((2, crops, count, channels), jnp.bfloat16),
        jax.ShapeDtypeStruct((crops, count, channels), jnp.float32),
    ][1 if last else 0 :]
    scratch = [
        pltpu.VMEM((count + 2 * width, 3 * channels), jnp.bfloat16),
        pltpu.VMEM((count + 16, channels), jnp.float32),
    ]
    aliases = {3 + k: k + (0 if last else 1) for k in range(len(state))}
    outputs = call(kernel, outs, [field, weights, after, *state], (2,), scratch, aliases)
    return (None if last else outputs[0]), outputs[-2:]


def backward_call(
    grad, turned, hidden, state, section, crop, crops, shape, width, last, parts, after
):
    count, channels = shape
    share = channels // parts
    first = section == 0

    def kernel(grad_ref, turned_ref, hidden_ref, after_ref, *refs):
        *_, kept_ref, sent_ref, taps, shifted = refs

        @pl.when(lax.axis_index("section") == section)
        def _():
            grad = grad_ref[...]
            if not last:
                grad = unpack(grad, count, channels)
            wide = grad.astype(jnp.float32)
            own = lax.axis_index("img")
            place_parts(sent_ref, (0,), grad, crop, parts, own)
            grad_active = convolved(wide, turned_ref.at[1], taps, shifted, width)
            hidden = hidden_ref[crop]
            gate = jax.nn.sigmoid(hidden)
            grad_hidden = (grad_active * (gate * (1.0 + hidden * (1.0 - gate)))).astype(
                jnp.bfloat16
            )
            place_parts(sent_ref, (1,), grad_hidden, crop, parts, own)
            if first:
                kept_ref[crop] = grad_hidden
            else:
                added = convolved(
                    grad_hidden.astype(jnp.float32), turned_ref.at[0], taps, shifted, width
                )
                result = (wide + added).astype(jnp.bfloat16)
                kept_ref[crop] = result
                refs[-5][...] = pack(result)

    outs = [
        jax.ShapeDtypeStruct(packed_shape(count, channels), jnp.bfloat16),
        jax.ShapeDtypeStruct((crops, count, channels), jnp.bfloat16),
        jax.ShapeDtypeStruct((parts, 2, share, crops * count), jnp.bfloat16),
    ][1 if first else 0 :]
    scratch = [
        pltpu.VMEM((count + 2 * width, 3 * channels), jnp.bfloat16),
        pltpu.VMEM((count + 16, channels), jnp.float32),
    ]
    aliases = {4 + k: k + (0 if first else 1) for k in range(len(state))}
    operands = [grad, turned, hidden, after, *state]
    outputs = call(kernel, outs, operands, (3,), scratch, aliases)
    return (None if first else outputs[0]), outputs[-2:]


def finish_call(grads, turned, kept, width):
    crops, count, channels = kept.shape

    def kernel(turned_ref, *refs):
        kept_ref, taps, shifted = refs[-3:]

        @pl.when(lax.axis_index("section") == 0)
        def _():
            for crop in range(crops):
                wide = unpack(refs[crop][...], count, channels).astype(jnp.float32)
                grad_hidden = kept_ref[crop].astype(jnp.float32)
                added = convolved(grad_hidden, turned_ref.at[0], taps, shifted, width)
                kept_ref[crop] = (wide + added).astype(jnp.bfloat16)

    out = jax.ShapeDtypeStruct(kept.shape, kept.dtype)
    scratch = [
        pltpu.VMEM((count + 2 * width, 3 * channels), jnp.bfloat16),
        pltpu.VMEM((count + 16, channels), jnp.float32),
    ]
    operands = [turned, *grads, kept]
    (kept,) = call(kernel, [out], operands, (), scratch, {len(operands) - 1: 0})
    return kept


def place_parts(target, lead, value, crop, parts, own):
    count, channels = value.shape
    share = channels // parts
    flipped = value.T
    for part in range(parts):
        slot = lax.rem(part + parts - own, parts)
        target[(slot, *lead, slice(None), slice(crop * count, (crop + 1) * count))] = flipped[
            part * share : (part + 1) * share, :
        ]


def flip_call(kept, parts, axis, after):
    def kernel(*refs):
        flipped_ref = refs[-1]
        for crop, (place, index) in enumerate(kept):
            value = refs[place][index]
            place_parts(flipped_ref, (), value, crop, parts, lax.axis_index(axis))

    operands = []
    for array, index in kept:
        if all(array is not other for other in operands):
            operands.append(array)
    kept = [
        ([array is other for other in operands].index(True), index) for array, index in kept
    ]
    count, channels = operands[0].shape[-2:]
    out = jax.ShapeDtypeStruct((parts, channels // parts, len(kept) * count), operands[0].dtype)
    (flipped,) = call(kernel, [out], [*operands, after], (len(operands),), [], {})
    return flipped


def turn_call(loaded, weights, after):
    two, _, _, channels = weights.shape

    def kernel(loaded_ref, weights_ref, after_ref, turned_ref):
        is_first = lax.axis_index("section") == 0
        for which in range(two):
            for tap in range(9):
                down, right = divmod(tap, 3)
                rows = slice(right * channels, (right + 1) * channels)
                value = jnp.where(
                    is_first, loaded_ref[which, down, rows, :], weights_ref[which, down, rows, :]
                )
                down, right = divmod(8 - tap, 3)
                turned_ref[which, down, right * channels : (right + 1) * channels, :] = value.T

    out = jax.ShapeDtypeStruct(weights.shape, weights.dtype)
    (turned,) = call(kernel, [out], [loaded, weights, after], (2,), [], {})
    return turned


def split_call(strips, cotangent, last):
    images, strip_count, rows, cols, channels = strips.shape
    share = strip_count // 2

    def kernel(strips_ref, cotangent_ref, own_ref, other_ref, sems):
        own = lax.axis_index("slab")
        is_last = lax.axis_index("section") == last

        def fetch(source_ref):
            copies = []
            for image in range(images):
                at = pl.ds(image * share, share)
                for side, (ref, half) in enumerate(((own_ref, own), (other_ref, 1 - own))):
                    source = source_ref.at[image, pl.ds(half * share, share)]
                    copies.append(pltpu.make_async_copy(source, ref.at[at], sems.at[2 * image + side]))
            for copy in copies:
                copy.start()
            for copy in copies:
                copy.wait()

        @pl.when(is_last)
        def _():
            fetch(cotangent_ref)

        @pl.when(jnp.logical_not(is_last))
        def _():
            fetch(strips_ref)

    out = jax.ShapeDtypeStruct((images * share, rows, cols, channels), strips.dtype)
    sems = [pltpu.SemaphoreType.DMA((2 * images,))]
    return call(kernel, [out, out], [strips, cotangent], (), sems, {}, (0, 1), pl.CostEstimate(flops=10**10, transcendentals=0, bytes_accessed=10**6))


def load_call(weights, first, after):
    def kernel(weights_ref, after_ref, *refs):
        out_ref, sems = refs[-2:]

        @pl.when((lax.axis_index("section") == 0) == first)
        def _():
            copies = [
                pltpu.make_async_copy(weights_ref.at[which], out_ref.at[which], sems.at[which])
                for which in range(2)
            ]
            for copy in copies:
                copy.start()
            for copy in copies:
                copy.wait()

    out = jax.ShapeDtypeStruct(weights.shape, weights.dtype)
    sems = [pltpu.SemaphoreType.DMA((2,))]
    (loaded,) = call(kernel, [out], [weights, after], (1,), sems, {}, (0,))
    return loaded


def join_call(own, other):
    crops, rows, cols, channels = own.shape

    def kernel(own_ref, other_ref, *out_refs):
        is_left = lax.axis_index("slab") == 0
        for crop, out_ref in enumerate(out_refs):
            mine = own_ref[crop].astype(jnp.float32)
            theirs = other_ref[crop].astype(jnp.float32)
            left = jnp.where(is_left, mine, theirs)
            right = jnp.where(is_left, theirs, mine)
            whole = jnp.concatenate([left, right], axis=1)
            out_ref[...] = whole.reshape(rows * 2 * cols, channels).astype(jnp.bfloat16)

    out = jax.ShapeDtypeStruct((rows * 2 * cols, channels), own.dtype)
    return call(kernel, [out] * crops, [own, other], (), [], {})


def part_call(kept, rows, after):
    crops, count, channels = kept.shape
    cols = count // rows // 2

    def kernel(kept_ref, after_ref, own_ref, other_ref):
        is_left = lax.axis_index("slab") == 0
        for crop in range(crops):
            whole = kept_ref[crop].astype(jnp.float32).reshape(rows, 2 * cols, channels)
            left, right = whole[:, :cols], whole[:, cols:]
            own_ref[crop] = jnp.where(is_left, left, right).astype(jnp.bfloat16)
            other_ref[crop] = jnp.where(is_left, right, left).astype(jnp.bfloat16)

    out = jax.ShapeDtypeStruct((crops, rows, cols, channels), kept.dtype)
    return call(kernel, [out, out], [kept, after], (1,), [], {})


def merge_call(own, other, images):
    crops, rows, cols, channels = own.shape
    share = crops // images

    def kernel(own_ref, other_ref, out_ref):
        place = lax.axis_index("slab")
        for image in range(images):
            for crop in range(share):
                out_ref[image, place * share + crop] = own_ref[image * share + crop]
                out_ref[image, (1 - place) * share + crop] = other_ref[image * share + crop]

    out = jax.ShapeDtypeStruct((images, 2 * share, rows, cols, channels), own.dtype)
    (merged,) = call(kernel, [out], [own, other], (), [], {})
    return merged


def stack_call(blocks):
    def kernel(*refs):
        for place in range(len(blocks)):
            refs[-1][place] = refs[place][...]

    out = jax.ShapeDtypeStruct((len(blocks), *blocks[0].shape), blocks[0].dtype)
    (stacked,) = call(kernel, [out], [*blocks], (), [], {})
    return stacked


def remake_call(saved, weights, blocks, width, sections, earlier=None):
    _, crops, count, channels = saved.shape
    share = channels // 2
    each = len(blocks)

    def kernel(saved_ref, weights_ref, *refs):
        home_ref, outer_ref, taps, shifted = refs[-4:]
        is_left = lax.axis_index("slab") == 0
        section = lax.axis_index("section")

        def put(kind, block, crop, value):
            cells = slice(crop * count, (crop + 1) * count)
            flipped = value.T
            low, high = flipped[:share], flipped[share:]
            home_ref[kind, block, :, cells] = jnp.where(is_left, low, high)
            outer_ref[kind, block, :, cells] = jnp.where(is_left, high, low)

        is_active = (section >= sections[0]) & (section <= sections[1])
        if earlier is not None:

            @pl.when(jnp.logical_not(is_active))
            def _():
                outer_ref[...] = refs[each][...]

        @pl.when(is_active)
        def _():
            for crop in range(crops):
                for kind in range(2):
                    put(kind, 0, crop, saved_ref[kind, crop])
            for block in range(each):
                home_ref[0, 1 + block] = refs[block][0]
                outer_ref[0, 1 + block] = refs[block][1]
                for crop in range(crops):
                    cells = slice(crop * count, (crop + 1) * count)
                    mine, theirs = refs[block][0, :, cells], refs[block][1, :, cells]
                    low, high = jnp.where(is_left, mine, theirs), jnp.where(is_left, theirs, mine)
                    field = jnp.concatenate([low, high], axis=0).T.astype(jnp.float32)
                    hidden = convolved(field, weights_ref.at[0], taps, shifted, width)
                    active = (hidden * jax.nn.sigmoid(hidden)).astype(jnp.bfloat16)
                    put(1, 1 + block, crop, active)

    out = jax.ShapeDtypeStruct((2, 1 + each, share, crops * count), saved.dtype)
    scratch = [
        pltpu.VMEM((count + 2 * width, 3 * channels), jnp.bfloat16),
        pltpu.VMEM((count + 16, channels), jnp.float32),
    ]
    operands = [saved, weights, *blocks] + ([] if earlier is None else [earlier])
    return call(kernel, [out, out], operands, (), scratch, {})


def spread_call(first, cells_of, around, place, count, width):
    two, blocks, share, cells = cells_of.shape
    crops = cells // count
    total = 2 * blocks * cells

    def kernel(first_ref, cells_ref, *refs):
        out_ref, shifted = refs[-2:]
        is_first = lax.axis_index("section") == 0
        for kind in range(two):
            for block in range(blocks):
                for crop in range(crops):
                    cell = slice(crop * count, (crop + 1) * count)
                    value = jnp.where(
                        is_first, first_ref[kind, block, :, cell], cells_ref[kind, block, :, cell]
                    )
                    value = value.T.astype(jnp.float32)
                    before, after = neighbours(value, shifted, width)
                    at = (place * blocks + block) * cells + crop * count
                    for side, part in enumerate((before, value, after)):
                        lanes = slice(side * share, (side + 1) * share)
                        out_ref[kind, at : at + count, lanes] = part.astype(jnp.bfloat16)

    out = jax.ShapeDtypeStruct((two, total, 3 * share), jnp.bfloat16)
    scratch = [pltpu.VMEM((count + 16, share), jnp.float32)]
    operands = [first, cells_of] if around is None else [first, cells_of, around]
    aliases = {} if around is None else {2: 0}
    (spread,) = call(kernel, [out], operands, (), scratch, aliases)
    return spread


def terms_call(around, own, other, count, width, scaling):
    blocks, _, columns, cells = own.shape
    rows = around.shape[2] // 3
    crops = cells // count

    def moved(value, down):
        parts = []
        edge = jnp.zeros((columns, width), value.dtype)
        for crop in range(crops):
            part = value[:, crop * count : (crop + 1) * count]
            if down == 0:
                part = jnp.concatenate([part[:, width:], edge], axis=1)
            elif down == 2:
                part = jnp.concatenate([edge, part[:, : count - width]], axis=1)
            parts.append(part)
        return jnp.concatenate(parts, axis=1)

    def kernel(around_ref, own_ref, other_ref, out_ref, held, sems):
        copies = []
        for kind in (1, 0):
            total = None
            for block in range(2 * blocks):
                left = own_ref if block < blocks else other_ref
                left = left[block % blocks, 1 - kind]
                left = jnp.concatenate([moved(left, down) for down in range(3)], axis=0)
                right = around_ref[kind, block * cells : (block + 1) * cells, :]
                term = jnp.dot(left, right, preferred_element_type=jnp.float32)
                total = term if total is None else total + term
            for down in range(3):
                part = total[down * columns : (down + 1) * columns] * scaling
                part = part.T.reshape(3, rows, columns)
                for place in range(3):
                    held[kind, 3 * down + place] = part[place]
            copy = pltpu.make_async_copy(held.at[kind], out_ref.at[kind], sems.at[kind])
            copy.start()
            copies.append(copy)
        for copy in copies:
            copy.wait()

    shape = (2, 9, rows, columns)
    return pl.pallas_call(
        kernel,
        out_shape=jax.ShapeDtypeStruct(shape, jnp.float32),
        in_specs=[pl.BlockSpec(memory_space=pltpu.VMEM)] * 3,
        out_specs=pl.BlockSpec(memory_space=pltpu.HBM),
        scratch_shapes=[pltpu.VMEM(shape, jnp.float32), pltpu.SemaphoreType.DMA((2,))],
        compiler_params=pltpu.CompilerParams(vmem_limit_bytes=8 << 20),
        name="terms",
    )(around, own, other)


def rotated(value, axis, steps):
    count = lax.axis_size(axis)
    return lax.ppermute(value, axis, [(source, (source + steps) % count) for source in range(count)])


def crop_shards(strips, kernels, cotangent):
    sections = lax.axis_size("section")
    slabs, groups = lax.axis_size("slab"), lax.axis_size("img")
    images, strip_count, row_count, col_count, channels = strips.shape
    width = col_count * slabs
    count = row_count * width
    crops = images * strip_count // slabs
    shape = (count, channels)
    last = sections - 1
    early = min(1, last - 1)
    steps = range(1, groups)
    scaling = 1.0 / math.sqrt(images * groups * strip_count * count)

    def hop(values, source, target):
        arrived = []
        for value in values:
            arrived.append(lax.ppermute(value, "section", [(source, target)]))
        return arrived

    def shared(values, step, routes):
        pairs = [
            (place * groups + i, place * groups + (i + step) % groups)
            for place in routes
            for i in range(groups)
        ]
        return lax.ppermute(values, ("section", "img"), pairs)

    def swapped(value):
        return rotated(value, "slab", 1)

    def flipped(saved, after):
        return flip_call([(saved, (0, crop)) for crop in range(crops)], slabs, "slab", after)

    own, other = split_call(
        pltpu.with_memory_space_constraint(strips, pltpu.HBM),
        pltpu.with_memory_space_constraint(cotangent, pltpu.HBM),
        last,
    )
    other = swapped(other)
    weights = kernels[0].reshape(2, 3, 3 * channels, channels)
    stored = pltpu.with_memory_space_constraint(weights, pltpu.HBM)
    loaded = weights
    fields = join_call(own, other)
    incoming = fields
    state = []
    turned, after = None, weights
    grads = []

    def forward(place, crop):
        return forward_call(
            incoming[crop],
            weights,
            state,
            place,
            crop,
            crops,
            shape,
            width,
            place == last,
            after,
        )

    def backward(place, crop, incoming):
        return backward_call(
            incoming[crop],
            turned,
            state[1],
            grads,
            place,
            crop,
            crops,
            shape,
            width,
            place == last,
            groups,
            after,
        )

    for place in range(last):
        outgoing = []
        for crop in range(crops):
            out, state = forward(place, crop)
            outgoing.append(out)
        if place == 0:
            weights = load_call(stored, False, state[0])
        incoming = hop(outgoing, place, place + 1)
        if place == early:
            inputs = flipped(state[0], state[1])
            soon = [shared(inputs, step, [0]) for step in steps]
            turned = turn_call(loaded, weights, state[0])
            after = turned
    outgoing = []
    for crop in range(crops):
        _, state = forward(last, crop)
        out, grads = backward(last, crop, fields)
        after = out
        outgoing.append(out)
    saved, hidden = state
    incoming = hop(outgoing, last, last - 1)
    inputs = flipped(saved, outgoing[-1])
    late = [shared(inputs, step, range(sections)) for step in steps]
    after = hidden
    for place in reversed(range(last)):
        if place == 0:
            first, early_outer = remake_call(saved, loaded, soon, width, (0, 0))
            after = first
        outgoing = []
        for crop in range(crops):
            out, grads = backward(place, crop, incoming)
            outgoing.append(out)
        if place:
            incoming = hop(outgoing, place, place - 1)
    kept, sent = grads
    kept = finish_call(incoming, turned, kept, width)
    own = [sent[0]]
    for step in steps:
        own.append(shared(sent[step], step, range(sections)))
    home, outer = remake_call(saved, weights, late, width, (1, last), early_outer)
    outer = swapped(outer)
    around = spread_call(first, home, None, 0, count, width)
    around = spread_call(outer, outer, around, 1, count, width)
    own = stack_call(own)
    other = swapped(own)
    terms = terms_call(around, own, other, count, width, scaling)
    own, other = part_call(kept, row_count, sent)
    other = swapped(other)
    grad_inputs = merge_call(own, other, images)
    return (terms[None], grad_inputs[None])


def shards(strips, kernels, cotangent):
    slabs, groups = lax.axis_size("slab"), lax.axis_size("img")
    strip_count, row_count, col_count, channels = strips.shape[1:]
    width = col_count * slabs
    whole_crops = strip_count % slabs == 0 and width % 16 == 0 and (row_count * width) % 128 == 0
    whole_crops = whole_crops and slabs == 2 and lax.axis_size("section") > 1
    if whole_crops and channels % (16 * slabs) == 0 and channels % (16 * groups) == 0:
        return crop_shards(strips, kernels, cotangent)
    return column_shards(strips, kernels, cotangent)


def solution(mesh):
    in_specs = (
        P("img", None, None, "slab", None),
        P("section", None, None, None, None),
        P("img", None, None, "slab", None),
    )
    out_specs = (
        P("section", None, None, "slab", "img"),
        P("section", "img", None, None, "slab", None),
    )
    return jax.shard_map(shards, mesh=mesh, in_specs=in_specs, out_specs=out_specs, check_vma=False)
```

```python
import math

import jax
import jax.numpy as jnp
from jax import lax
from jax.experimental import pallas as pl
from jax.experimental.pallas import tpu as pltpu
from jax.sharding import PartitionSpec as P


def passed_along(value, axis, steps):
    count = lax.axis_size(axis)
    initial, last = (max(0, -steps), min(count, count - steps))
    return lax.ppermute(value, axis, [(source, source + steps) for source in range(initial, last)])


def padded_2(cells, sides, width):
    for axis, dim in sides:
        count = lax.axis_size(axis)
        ends = count - 1
        head = lax.slice_in_dim(cells, 0, width, axis=dim)
        tail = lax.slice_in_dim(cells, cells.shape[dim] - width, cells.shape[dim], axis=dim)
        cells = jnp.concatenate(
            [
                lax.ppermute(tail, axis, [(i, (i + 1) % count) for i in range(ends)]),
                cells,
                lax.ppermute(head, axis, [((i + 1) % count, i) for i in range(ends)]),
            ],
            axis=dim,
        )
    return cells


def unfold(padded, row_count, col_count):
    tap_list = [
        padded[:, down_at : down_at + row_count, right_at : right_at + col_count, :]
        for down_at in range(3)
        for right_at in range(3)
    ]
    stacked = jnp.concatenate(tap_list, axis=3)
    return stacked.reshape(-1, stacked.shape[3])


def columns_of(wide_field):
    row_count = wide_field.shape[1]
    col_count = wide_field.shape[2] - 2
    padded = jnp.pad(wide_field, ((0, 0), (1, 1), (0, 0), (0, 0)))
    return unfold(padded, row_count, col_count)


def convolve(matrix, wide_field):
    count, row_count = (wide_field.shape[0], wide_field.shape[1])
    col_count = wide_field.shape[2] - 2
    flat_out = jnp.dot(columns_of(wide_field), matrix, preferred_element_type=jnp.float32)
    return flat_out.reshape(count, row_count, col_count, matrix.shape[1])


def contract(wide_field, grad_out):
    flat_grad = grad_out.reshape(-1, grad_out.shape[3])
    return lax.dot_general(
        columns_of(wide_field),
        flat_grad,
        (((0,), (0,)), ((), ())),
        preferred_element_type=jnp.float32,
    )


def silu_slope(hidden):
    sigmoid_at = jax.nn.sigmoid(hidden)
    return sigmoid_at * (1.0 + hidden * (1.0 - sigmoid_at))


def store(buffer, value, slot_index, is_valid, axis_at):
    current = lax.dynamic_index_in_dim(buffer, slot_index, axis_at, keepdims=False)
    return lax.dynamic_update_index_in_dim(
        buffer, jnp.where(is_valid, value, current), slot_index, axis_at
    )


def column_shards(strips, kernels, cotangent):
    section_count = lax.axis_size("section")
    section_index = lax.axis_index("section")
    slab_count = lax.axis_size("slab")
    slab_index = lax.axis_index("slab")
    images, strip_count, row_count, col_count, channels = strips.shape
    weights = kernels[0]
    first_forward = weights[0].reshape(9 * channels, channels)
    second_forward = weights[1].reshape(9 * channels, channels)
    first_backward = jnp.transpose(weights[0][::-1], (0, 2, 1)).reshape(9 * channels, channels)
    second_backward = jnp.transpose(weights[1][::-1], (0, 2, 1)).reshape(9 * channels, channels)
    scaling = 1.0 / math.sqrt(
        images * lax.axis_size("img") * strip_count * row_count * col_count * slab_count
    )
    position = slab_index * col_count - 1 + jnp.arange(col_count + 2, dtype=jnp.int32)
    inside = ((position >= 0) & (position < slab_count * col_count))[None, None, :, None]
    tick_count = strip_count + section_count - 1
    hidden_cols = col_count + 2
    empty_field = jnp.zeros((images, row_count, col_count, channels), jnp.bfloat16)
    saved_field = jnp.zeros((strip_count, images, row_count, col_count + 2, channels), jnp.bfloat16)
    saved_hidden = jnp.zeros((strip_count, images, row_count, hidden_cols, channels), jnp.float32)
    saved_active = jnp.zeros(
        (strip_count, images, row_count, col_count + 2, channels), jnp.bfloat16
    )
    outgoing = empty_field
    for step_no in range(tick_count):
        micro_index = step_no - section_index
        is_valid = (micro_index >= 0) & (micro_index < strip_count)
        slot_index = jnp.clip(micro_index, 0, strip_count - 1)
        if step_no == 0:
            incoming = empty_field
        else:
            incoming = passed_along(outgoing, "section", 1)
        first_strip = lax.dynamic_index_in_dim(strips, slot_index, 1, keepdims=False)
        field_in = jnp.where(section_index == 0, first_strip, incoming)
        wide_deep = padded_2(field_in, (("slab", 2),), 2)
        hidden = convolve(first_forward, wide_deep)
        wide_active = jnp.where(inside, jax.nn.silu(hidden), 0.0).astype(jnp.bfloat16)
        wide_field = wide_deep[:, :, 1:-1, :]
        outgoing = (field_in.astype(jnp.float32) + convolve(second_forward, wide_active)).astype(
            jnp.bfloat16
        )
        saved_field = store(saved_field, wide_field, slot_index, is_valid, 0)
        saved_hidden = store(saved_hidden, hidden, slot_index, is_valid, 0)
        saved_active = store(saved_active, wide_active, slot_index, is_valid, 0)
    grad_slots = jnp.zeros((images, strip_count, row_count, col_count, channels), jnp.bfloat16)
    saved_grad_out = jnp.zeros((strip_count, images, row_count, col_count, channels), jnp.bfloat16)
    saved_grad_hidden = jnp.zeros(
        (strip_count, images, row_count, col_count, channels), jnp.bfloat16
    )
    sending = empty_field
    for step_no in range(tick_count):
        micro_index = step_no - (section_count - 1 - section_index)
        is_valid = (micro_index >= 0) & (micro_index < strip_count)
        slot_index = jnp.clip(micro_index, 0, strip_count - 1)
        if step_no == 0:
            arriving = empty_field
        else:
            arriving = passed_along(sending, "section", -1)
        top_grad = lax.dynamic_index_in_dim(cotangent, slot_index, 1, keepdims=False)
        grad_out = jnp.where(section_index == section_count - 1, top_grad, arriving)
        grad_out = jnp.where(is_valid, grad_out, jnp.zeros_like(grad_out))
        hidden = lax.dynamic_index_in_dim(saved_hidden, slot_index, 0, keepdims=False)
        wide_grad = padded_2(grad_out, (("slab", 2),), 2)
        grad_active = convolve(second_backward, wide_grad)
        wide_hidden_grad = jnp.where(inside, grad_active * silu_slope(hidden), 0.0).astype(
            jnp.bfloat16
        )
        grad_hidden = wide_hidden_grad[:, :, 1:-1, :]
        sending = (
            grad_out.astype(jnp.float32) + convolve(first_backward, wide_hidden_grad)
        ).astype(jnp.bfloat16)
        saved_grad_out = store(saved_grad_out, grad_out, slot_index, is_valid, 0)
        saved_grad_hidden = store(saved_grad_hidden, grad_hidden, slot_index, is_valid, 0)
        grad_slots = store(grad_slots, sending, slot_index, is_valid, 1)
    flat_count = strip_count * images
    lower_part = contract(
        saved_field.reshape(flat_count, row_count, col_count + 2, channels),
        saved_grad_hidden.reshape(flat_count, row_count, col_count, channels),
    )
    upper_part = contract(
        saved_active.reshape(flat_count, row_count, col_count + 2, channels),
        saved_grad_out.reshape(flat_count, row_count, col_count, channels),
    )
    grad_terms = jnp.stack([lower_part, upper_part]).reshape(2, 9, channels, channels)
    row_share = lax.psum_scatter(
        grad_terms.astype(jnp.bfloat16), "slab", scatter_dimension=2, tiled=True
    )
    own_share = lax.psum_scatter(row_share, "img", scatter_dimension=3, tiled=True).astype(
        jnp.float32
    )
    grad_kernels = (own_share * scaling)[None]
    return (grad_kernels, grad_slots[None])


def call(kernel, outs, operands, unread, scratch, aliases, apart=(), cost=None):
    spaces = {**dict.fromkeys(unread, pl.ANY), **dict.fromkeys(apart, pltpu.HBM)}
    return pl.pallas_call(
        kernel,
        out_shape=outs,
        in_specs=[
            pl.BlockSpec(memory_space=spaces.get(place, pltpu.VMEM))
            for place in range(len(operands))
        ],
        out_specs=[pl.BlockSpec(memory_space=pltpu.VMEM)] * len(outs),
        scratch_shapes=scratch,
        input_output_aliases=aliases,
        compiler_params=pltpu.CompilerParams(vmem_limit_bytes=8 << 20),
        cost_estimate=cost,
    )(*operands)


def half_lanes(count, channels):
    return channels % 128 == 64 and count % 32 == 0


def packed_shape(count, channels):
    return (count * channels // 128, 128) if half_lanes(count, channels) else (count, channels)


def pack(value):
    count, channels = value.shape
    if not half_lanes(count, channels):
        return value
    parts = [value[:, at : at + 128] for at in range(0, channels - 64, 128)]
    rest = value[:, channels - 64 :]
    parts.append(jnp.concatenate([rest[: count // 2], rest[count // 2 :]], axis=1))
    return jnp.concatenate(parts, axis=0)


def unpack(value, count, channels):
    if not half_lanes(count, channels):
        return value
    whole = channels // 128
    parts = [value[k * count : (k + 1) * count] for k in range(whole)]
    rest = value[whole * count :]
    parts.append(jnp.concatenate([rest[:, :64], rest[:, 64:]], axis=0))
    return jnp.concatenate(parts, axis=1)


def neighbours(value, shifted, width):
    count, channels = value.shape
    shifted[8 : 8 + count, :] = value
    column = lax.rem(lax.broadcasted_iota(jnp.int32, (count, channels), 0), width)
    before = jnp.where(column == 0, 0.0, shifted[7 : 7 + count, :])
    after = jnp.where(column == width - 1, 0.0, shifted[9 : 9 + count, :])
    return before, after


def convolved(value, matrix, taps, shifted, width):
    count, channels = value.shape
    before, after = neighbours(value, shifted, width)
    for place, part in enumerate((before, value, after)):
        taps[width : width + count, place * channels : (place + 1) * channels] = part.astype(
            jnp.bfloat16
        )
    edge = jnp.zeros((width, 3 * channels), jnp.bfloat16)
    taps[0:width, :] = edge
    taps[width + count : 2 * width + count, :] = edge
    total = jnp.dot(taps[0:count, :], matrix[0], preferred_element_type=jnp.float32)
    for down in (1, 2):
        total = total + jnp.dot(
            taps[down * width : down * width + count, :],
            matrix[down],
            preferred_element_type=jnp.float32,
        )
    return total


def forward_call(field, weights, state, section, crop, crops, shape, width, last, after):
    count, channels = shape

    def kernel(field_ref, weights_ref, after_ref, *refs):
        *_, saved_ref, hidden_ref, taps, shifted = refs

        @pl.when(lax.axis_index("section") == section)
        def _():
            field_in = field_ref[...]
            if section:
                field_in = unpack(field_in, count, channels)
            wide = field_in.astype(jnp.float32)
            saved_ref[0, crop] = field_in
            hidden = convolved(wide, weights_ref.at[0], taps, shifted, width)
            hidden_ref[crop] = hidden
            active = (hidden * jax.nn.sigmoid(hidden)).astype(jnp.bfloat16)
            saved_ref[1, crop] = active
            if not last:
                added = convolved(
                    active.astype(jnp.float32), weights_ref.at[1], taps, shifted, width
                )
                refs[-5][...] = pack((wide + added).astype(jnp.bfloat16))

    outs = [
        jax.ShapeDtypeStruct(packed_shape(count, channels), jnp.bfloat16),
        jax.ShapeDtypeStruct((2, crops, count, channels), jnp.bfloat16),
        jax.ShapeDtypeStruct((crops, count, channels), jnp.float32),
    ][1 if last else 0 :]
    scratch = [
        pltpu.VMEM((count + 2 * width, 3 * channels), jnp.bfloat16),
        pltpu.VMEM((count + 16, channels), jnp.float32),
    ]
    aliases = {3 + k: k + (0 if last else 1) for k in range(len(state))}
    outputs = call(kernel, outs, [field, weights, after, *state], (2,), scratch, aliases)
    return (None if last else outputs[0]), outputs[-2:]


def backward_call(
    grad, turned, hidden, state, section, crop, crops, shape, width, last, parts, after
):
    count, channels = shape
    share = channels // parts
    first = section == 0

    def kernel(grad_ref, turned_ref, hidden_ref, after_ref, *refs):
        *_, kept_ref, sent_ref, taps, shifted = refs

        @pl.when(lax.axis_index("section") == section)
        def _():
            grad = grad_ref[...]
            if not last:
                grad = unpack(grad, count, channels)
            wide = grad.astype(jnp.float32)
            own = lax.axis_index("img")
            place_parts(sent_ref, (0,), grad, crop, parts, own)
            grad_active = convolved(wide, turned_ref.at[1], taps, shifted, width)
            hidden = hidden_ref[crop]
            gate = jax.nn.sigmoid(hidden)
            grad_hidden = (grad_active * (gate * (1.0 + hidden * (1.0 - gate)))).astype(
                jnp.bfloat16
            )
            place_parts(sent_ref, (1,), grad_hidden, crop, parts, own)
            if first:
                kept_ref[crop] = grad_hidden
            else:
                added = convolved(
                    grad_hidden.astype(jnp.float32), turned_ref.at[0], taps, shifted, width
                )
                result = (wide + added).astype(jnp.bfloat16)
                kept_ref[crop] = result
                refs[-5][...] = pack(result)

    outs = [
        jax.ShapeDtypeStruct(packed_shape(count, channels), jnp.bfloat16),
        jax.ShapeDtypeStruct((crops, count, channels), jnp.bfloat16),
        jax.ShapeDtypeStruct((parts, 2, share, crops * count), jnp.bfloat16),
    ][1 if first else 0 :]
    scratch = [
        pltpu.VMEM((count + 2 * width, 3 * channels), jnp.bfloat16),
        pltpu.VMEM((count + 16, channels), jnp.float32),
    ]
    aliases = {4 + k: k + (0 if first else 1) for k in range(len(state))}
    operands = [grad, turned, hidden, after, *state]
    outputs = call(kernel, outs, operands, (3,), scratch, aliases)
    return (None if first else outputs[0]), outputs[-2:]


def finish_call(grads, turned, kept, width):
    crops, count, channels = kept.shape

    def kernel(turned_ref, *refs):
        kept_ref, taps, shifted = refs[-3:]

        @pl.when(lax.axis_index("section") == 0)
        def _():
            for crop in range(crops):
                wide = unpack(refs[crop][...], count, channels).astype(jnp.float32)
                grad_hidden = kept_ref[crop].astype(jnp.float32)
                added = convolved(grad_hidden, turned_ref.at[0], taps, shifted, width)
                kept_ref[crop] = (wide + added).astype(jnp.bfloat16)

    out = jax.ShapeDtypeStruct(kept.shape, kept.dtype)
    scratch = [
        pltpu.VMEM((count + 2 * width, 3 * channels), jnp.bfloat16),
        pltpu.VMEM((count + 16, channels), jnp.float32),
    ]
    operands = [turned, *grads, kept]
    (kept,) = call(kernel, [out], operands, (), scratch, {len(operands) - 1: 0})
    return kept


def place_parts(target, lead, value, crop, parts, own):
    count, channels = value.shape
    share = channels // parts
    flipped = value.T
    for part in range(parts):
        slot = lax.rem(part + parts - own, parts)
        target[(slot, *lead, slice(None), slice(crop * count, (crop + 1) * count))] = flipped[
            part * share : (part + 1) * share, :
        ]


def flip_call(kept, parts, axis, after):
    def kernel(*refs):
        flipped_ref = refs[-1]
        for crop, (place, index) in enumerate(kept):
            value = refs[place][index]
            place_parts(flipped_ref, (), value, crop, parts, lax.axis_index(axis))

    operands = []
    for array, index in kept:
        if all(array is not other for other in operands):
            operands.append(array)
    kept = [
        ([array is other for other in operands].index(True), index) for array, index in kept
    ]
    count, channels = operands[0].shape[-2:]
    out = jax.ShapeDtypeStruct((parts, channels // parts, len(kept) * count), operands[0].dtype)
    (flipped,) = call(kernel, [out], [*operands, after], (len(operands),), [], {})
    return flipped


def turn_call(loaded, weights, after):
    two, _, _, channels = weights.shape

    def kernel(loaded_ref, weights_ref, after_ref, turned_ref):
        is_first = lax.axis_index("section") == 0
        for which in range(two):
            for tap in range(9):
                down, right = divmod(tap, 3)
                rows = slice(right * channels, (right + 1) * channels)
                value = jnp.where(
                    is_first, loaded_ref[which, down, rows, :], weights_ref[which, down, rows, :]
                )
                down, right = divmod(8 - tap, 3)
                turned_ref[which, down, right * channels : (right + 1) * channels, :] = value.T

    out = jax.ShapeDtypeStruct(weights.shape, weights.dtype)
    (turned,) = call(kernel, [out], [loaded, weights, after], (2,), [], {})
    return turned


def split_call(strips, cotangent, last):
    images, strip_count, rows, cols, channels = strips.shape
    share = strip_count // 2

    def kernel(strips_ref, cotangent_ref, own_ref, other_ref, sems):
        own = lax.axis_index("slab")
        is_last = lax.axis_index("section") == last

        def fetch(source_ref):
            copies = []
            for image in range(images):
                at = pl.ds(image * share, share)
                for side, (ref, half) in enumerate(((own_ref, own), (other_ref, 1 - own))):
                    source = source_ref.at[image, pl.ds(half * share, share)]
                    copies.append(pltpu.make_async_copy(source, ref.at[at], sems.at[2 * image + side]))
            for copy in copies:
                copy.start()
            for copy in copies:
                copy.wait()

        @pl.when(is_last)
        def _():
            fetch(cotangent_ref)

        @pl.when(jnp.logical_not(is_last))
        def _():
            fetch(strips_ref)

    out = jax.ShapeDtypeStruct((images * share, rows, cols, channels), strips.dtype)
    sems = [pltpu.SemaphoreType.DMA((2 * images,))]
    return call(kernel, [out, out], [strips, cotangent], (), sems, {}, (0, 1), pl.CostEstimate(flops=10**10, transcendentals=0, bytes_accessed=10**6))


def load_call(weights, first, after):
    def kernel(weights_ref, after_ref, *refs):
        out_ref, sems = refs[-2:]

        @pl.when((lax.axis_index("section") == 0) == first)
        def _():
            copies = [
                pltpu.make_async_copy(weights_ref.at[which], out_ref.at[which], sems.at[which])
                for which in range(2)
            ]
            for copy in copies:
                copy.start()
            for copy in copies:
                copy.wait()

    out = jax.ShapeDtypeStruct(weights.shape, weights.dtype)
    sems = [pltpu.SemaphoreType.DMA((2,))]
    (loaded,) = call(kernel, [out], [weights, after], (1,), sems, {}, (0,))
    return loaded


def join_call(own, other):
    crops, rows, cols, channels = own.shape

    def kernel(own_ref, other_ref, *out_refs):
        is_left = lax.axis_index("slab") == 0
        for crop, out_ref in enumerate(out_refs):
            mine = own_ref[crop].astype(jnp.float32)
            theirs = other_ref[crop].astype(jnp.float32)
            left = jnp.where(is_left, mine, theirs)
            right = jnp.where(is_left, theirs, mine)
            whole = jnp.concatenate([left, right], axis=1)
            out_ref[...] = whole.reshape(rows * 2 * cols, channels).astype(jnp.bfloat16)

    out = jax.ShapeDtypeStruct((rows * 2 * cols, channels), own.dtype)
    return call(kernel, [out] * crops, [own, other], (), [], {})


def part_call(kept, rows, after):
    crops, count, channels = kept.shape
    cols = count // rows // 2

    def kernel(kept_ref, after_ref, own_ref, other_ref):
        is_left = lax.axis_index("slab") == 0
        for crop in range(crops):
            whole = kept_ref[crop].astype(jnp.float32).reshape(rows, 2 * cols, channels)
            left, right = whole[:, :cols], whole[:, cols:]
            own_ref[crop] = jnp.where(is_left, left, right).astype(jnp.bfloat16)
            other_ref[crop] = jnp.where(is_left, right, left).astype(jnp.bfloat16)

    out = jax.ShapeDtypeStruct((crops, rows, cols, channels), kept.dtype)
    return call(kernel, [out, out], [kept, after], (1,), [], {})


def merge_call(own, other, images):
    crops, rows, cols, channels = own.shape
    share = crops // images

    def kernel(own_ref, other_ref, out_ref):
        place = lax.axis_index("slab")
        for image in range(images):
            for crop in range(share):
                out_ref[image, place * share + crop] = own_ref[image * share + crop]
                out_ref[image, (1 - place) * share + crop] = other_ref[image * share + crop]

    out = jax.ShapeDtypeStruct((images, 2 * share, rows, cols, channels), own.dtype)
    (merged,) = call(kernel, [out], [own, other], (), [], {})
    return merged


def stack_call(blocks):
    def kernel(*refs):
        for place in range(len(blocks)):
            refs[-1][place] = refs[place][...]

    out = jax.ShapeDtypeStruct((len(blocks), *blocks[0].shape), blocks[0].dtype)
    (stacked,) = call(kernel, [out], [*blocks], (), [], {})
    return stacked


def remake_call(saved, weights, blocks, width, sections, earlier=None):
    _, crops, count, channels = saved.shape
    share = channels // 2
    each = len(blocks)

    def kernel(saved_ref, weights_ref, *refs):
        home_ref, outer_ref, taps, shifted = refs[-4:]
        is_left = lax.axis_index("slab") == 0
        section = lax.axis_index("section")

        def put(kind, block, crop, value):
            cells = slice(crop * count, (crop + 1) * count)
            flipped = value.T
            low, high = flipped[:share], flipped[share:]
            home_ref[kind, block, :, cells] = jnp.where(is_left, low, high)
            outer_ref[kind, block, :, cells] = jnp.where(is_left, high, low)

        is_active = (section >= sections[0]) & (section <= sections[1])
        if earlier is not None:

            @pl.when(jnp.logical_not(is_active))
            def _():
                outer_ref[...] = refs[each][...]

        @pl.when(is_active)
        def _():
            for crop in range(crops):
                for kind in range(2):
                    put(kind, 0, crop, saved_ref[kind, crop])
            for block in range(each):
                home_ref[0, 1 + block] = refs[block][0]
                outer_ref[0, 1 + block] = refs[block][1]
                for crop in range(crops):
                    cells = slice(crop * count, (crop + 1) * count)
                    mine, theirs = refs[block][0, :, cells], refs[block][1, :, cells]
                    low, high = jnp.where(is_left, mine, theirs), jnp.where(is_left, theirs, mine)
                    field = jnp.concatenate([low, high], axis=0).T.astype(jnp.float32)
                    hidden = convolved(field, weights_ref.at[0], taps, shifted, width)
                    active = (hidden * jax.nn.sigmoid(hidden)).astype(jnp.bfloat16)
                    put(1, 1 + block, crop, active)

    out = jax.ShapeDtypeStruct((2, 1 + each, share, crops * count), saved.dtype)
    scratch = [
        pltpu.VMEM((count + 2 * width, 3 * channels), jnp.bfloat16),
        pltpu.VMEM((count + 16, channels), jnp.float32),
    ]
    operands = [saved, weights, *blocks] + ([] if earlier is None else [earlier])
    return call(kernel, [out, out], operands, (), scratch, {})


def spread_call(first, cells_of, around, place, count, width):
    two, blocks, share, cells = cells_of.shape
    crops = cells // count
    total = 2 * blocks * cells

    def kernel(first_ref, cells_ref, *refs):
        out_ref, shifted = refs[-2:]
        is_first = lax.axis_index("section") == 0
        for kind in range(two):
            for block in range(blocks):
                for crop in range(crops):
                    cell = slice(crop * count, (crop + 1) * count)
                    value = jnp.where(
                        is_first, first_ref[kind, block, :, cell], cells_ref[kind, block, :, cell]
                    )
                    value = value.T.astype(jnp.float32)
                    before, after = neighbours(value, shifted, width)
                    at = (place * blocks + block) * cells + crop * count
                    for side, part in enumerate((before, value, after)):
                        lanes = slice(side * share, (side + 1) * share)
                        out_ref[kind, at : at + count, lanes] = part.astype(jnp.bfloat16)

    out = jax.ShapeDtypeStruct((two, total, 3 * share), jnp.bfloat16)
    scratch = [pltpu.VMEM((count + 16, share), jnp.float32)]
    operands = [first, cells_of] if around is None else [first, cells_of, around]
    aliases = {} if around is None else {2: 0}
    (spread,) = call(kernel, [out], operands, (), scratch, aliases)
    return spread


def terms_call(around, own, other, count, width, scaling):
    blocks, _, columns, cells = own.shape
    rows = around.shape[2] // 3
    crops = cells // count

    def moved(value, down):
        parts = []
        edge = jnp.zeros((columns, width), value.dtype)
        for crop in range(crops):
            part = value[:, crop * count : (crop + 1) * count]
            if down == 0:
                part = jnp.concatenate([part[:, width:], edge], axis=1)
            elif down == 2:
                part = jnp.concatenate([edge, part[:, : count - width]], axis=1)
            parts.append(part)
        return jnp.concatenate(parts, axis=1)

    def kernel(around_ref, own_ref, other_ref, out_ref, held, sems):
        copies = []
        for kind in (1, 0):
            total = None
            for block in range(2 * blocks):
                left = own_ref if block < blocks else other_ref
                left = left[block % blocks, 1 - kind]
                left = jnp.concatenate([moved(left, down) for down in range(3)], axis=0)
                right = around_ref[kind, block * cells : (block + 1) * cells, :]
                term = jnp.dot(left, right, preferred_element_type=jnp.float32)
                total = term if total is None else total + term
            for down in range(3):
                part = total[down * columns : (down + 1) * columns] * scaling
                part = part.T.reshape(3, rows, columns)
                for place in range(3):
                    held[kind, 3 * down + place] = part[place]
                third = pl.ds(3 * down, 3)
                copy = pltpu.make_async_copy(
                    held.at[kind, third], out_ref.at[kind, third], sems.at[3 * kind + down]
                )
                copy.start()
                copies.append(copy)
        for copy in copies:
            copy.wait()

    shape = (2, 9, rows, columns)
    return pl.pallas_call(
        kernel,
        out_shape=jax.ShapeDtypeStruct(shape, jnp.float32),
        in_specs=[pl.BlockSpec(memory_space=pltpu.VMEM)] * 3,
        out_specs=pl.BlockSpec(memory_space=pltpu.HBM),
        scratch_shapes=[pltpu.VMEM(shape, jnp.float32), pltpu.SemaphoreType.DMA((6,))],
        compiler_params=pltpu.CompilerParams(vmem_limit_bytes=8 << 20),
        name="terms",
    )(around, own, other)


def rotated(value, axis, steps):
    count = lax.axis_size(axis)
    return lax.ppermute(value, axis, [(source, (source + steps) % count) for source in range(count)])


def crop_shards(strips, kernels, cotangent):
    sections = lax.axis_size("section")
    slabs, groups = lax.axis_size("slab"), lax.axis_size("img")
    images, strip_count, row_count, col_count, channels = strips.shape
    width = col_count * slabs
    count = row_count * width
    crops = images * strip_count // slabs
    shape = (count, channels)
    last = sections - 1
    early = min(1, last - 1)
    steps = range(1, groups)
    scaling = 1.0 / math.sqrt(images * groups * strip_count * count)

    def hop(values, source, target):
        arrived = []
        for value in values:
            arrived.append(lax.ppermute(value, "section", [(source, target)]))
        return arrived

    def shared(values, step, routes):
        pairs = [
            (place * groups + i, place * groups + (i + step) % groups)
            for place in routes
            for i in range(groups)
        ]
        return lax.ppermute(values, ("section", "img"), pairs)

    def swapped(value):
        return rotated(value, "slab", 1)

    def flipped(saved, after):
        return flip_call([(saved, (0, crop)) for crop in range(crops)], slabs, "slab", after)

    own, other = split_call(
        pltpu.with_memory_space_constraint(strips, pltpu.HBM),
        pltpu.with_memory_space_constraint(cotangent, pltpu.HBM),
        last,
    )
    other = swapped(other)
    weights = kernels[0].reshape(2, 3, 3 * channels, channels)
    stored = pltpu.with_memory_space_constraint(weights, pltpu.HBM)
    loaded = weights
    fields = join_call(own, other)
    incoming = fields
    state = []
    turned, after = None, weights
    grads = []

    def forward(place, crop):
        return forward_call(
            incoming[crop],
            weights,
            state,
            place,
            crop,
            crops,
            shape,
            width,
            place == last,
            after,
        )

    def backward(place, crop, incoming):
        return backward_call(
            incoming[crop],
            turned,
            state[1],
            grads,
            place,
            crop,
            crops,
            shape,
            width,
            place == last,
            groups,
            after,
        )

    for place in range(last):
        outgoing = []
        for crop in range(crops):
            out, state = forward(place, crop)
            outgoing.append(out)
        if place == 0:
            weights = load_call(stored, False, state[0])
        incoming = hop(outgoing, place, place + 1)
        if place == early:
            inputs = flipped(state[0], state[1])
            soon = [shared(inputs, step, [0]) for step in steps]
            turned = turn_call(loaded, weights, state[0])
            after = turned
    outgoing = []
    for crop in range(crops):
        _, state = forward(last, crop)
        out, grads = backward(last, crop, fields)
        after = out
        outgoing.append(out)
    saved, hidden = state
    incoming = hop(outgoing, last, last - 1)
    inputs = flipped(saved, outgoing[-1])
    late = [shared(inputs, step, range(sections)) for step in steps]
    after = hidden
    for place in reversed(range(last)):
        if place == 0:
            first, early_outer = remake_call(saved, loaded, soon, width, (0, 0))
            after = first
        outgoing = []
        for crop in range(crops):
            out, grads = backward(place, crop, incoming)
            outgoing.append(out)
        if place:
            incoming = hop(outgoing, place, place - 1)
    kept, sent = grads
    kept = finish_call(incoming, turned, kept, width)
    own = [sent[0]]
    for step in steps:
        own.append(shared(sent[step], step, range(sections)))
    home, outer = remake_call(saved, weights, late, width, (1, last), early_outer)
    outer = swapped(outer)
    around = spread_call(first, home, None, 0, count, width)
    around = spread_call(outer, outer, around, 1, count, width)
    own = stack_call(own)
    other = swapped(own)
    terms = terms_call(around, own, other, count, width, scaling)
    own, other = part_call(kept, row_count, sent)
    other = swapped(other)
    grad_inputs = merge_call(own, other, images)
    return (terms[None], grad_inputs[None])


def shards(strips, kernels, cotangent):
    slabs, groups = lax.axis_size("slab"), lax.axis_size("img")
    strip_count, row_count, col_count, channels = strips.shape[1:]
    width = col_count * slabs
    whole_crops = strip_count % slabs == 0 and width % 16 == 0 and (row_count * width) % 128 == 0
    whole_crops = whole_crops and slabs == 2 and lax.axis_size("section") > 1
    if whole_crops and channels % (16 * slabs) == 0 and channels % (16 * groups) == 0:
        return crop_shards(strips, kernels, cotangent)
    return column_shards(strips, kernels, cotangent)


def solution(mesh):
    in_specs = (
        P("img", None, None, "slab", None),
        P("section", None, None, None, None),
        P("img", None, None, "slab", None),
    )
    out_specs = (
        P("section", None, None, "slab", "img"),
        P("section", "img", None, None, "slab", None),
    )
    return jax.shard_map(shards, mesh=mesh, in_specs=in_specs, out_specs=out_specs, check_vma=False)
```
